32 devices in a mesh: dp: 8 (over y, x, core), tensor: 4 (over z).
Axes of the slice: x: 2, y: 2, z: 4, core: 2. Of those that a mesh axis runs over, the one named last changes fastest.
Arguments:
- tokens: bfloat16 [16, 320, 1536], P('dp', 'tensor'), may hold values from -6 to 6
- cotangent: bfloat16 [16, 320, 1536], P('dp', 'tensor'), may hold values from -6 to 6
- order: int32 [16, 320], P('dp'), may hold values from 0 to 319, each once within a row
- lengths: int32 [16, 3], P('dp'), may hold values from 1 to 256, 320 in all within a row
- gain_attn: bfloat16 [1536], P('dp'), may hold values from 0.5 to 1.5
- w_query: bfloat16 [1536, 1536], P('dp', 'tensor'), may hold values from -0.15625 to 0.15625
- w_key: bfloat16 [1536, 768], P('dp', 'tensor'), may hold values from -0.15625 to 0.15625
- w_value: bfloat16 [1536, 768], P('dp', 'tensor'), may hold values from -0.15625 to 0.15625
- w_out: bfloat16 [1536, 1536], P('tensor', 'dp'), may hold values from -1.5 to 1.5
- gain_ffn: bfloat16 [1536], P('dp'), may hold values from 0.5 to 1.5
- w_gate: bfloat16 [1536, 4096], P('dp', 'tensor'), may hold values from -0.15625 to 0.15625
- w_up: bfloat16 [1536, 4096], P('dp', 'tensor'), may hold values from -0.15625 to 0.15625
- w_down: bfloat16 [4096, 1536], P('tensor', 'dp'), may hold values from -0.09375 to 0.09375
Outputs:
- output: bfloat16 [16, 320, 1536], P('dp', 'tensor')
- grad_tokens: float32 [16, 320, 1536], P('dp', 'tensor')
- grad_gain_attn: float32 [1536], P('dp')
- grad_query: float32 [1536, 1536], P('dp', 'tensor')
- grad_key: float32 [1536, 768], P('dp', 'tensor')
- grad_value: float32 [1536, 768], P('dp', 'tensor')
- grad_out: float32 [1536, 1536], P('tensor', 'dp')
- grad_gain_ffn: float32 [1536], P('dp')
- grad_gate: float32 [1536, 4096], P('dp', 'tensor')
- grad_up: float32 [1536, 4096], P('dp', 'tensor')
- grad_down: float32 [4096, 1536], P('tensor', 'dp')
The draws below stay inside these ranges and needn't reach their ends.
Inputs may be any that keep to these rules, and one draw needn't show every extreme that they name: `order`: each row is a permutation of 0 to 319. `lengths`: each row sums to 320; its largest entry is 256; the last document of each stream is padding.
All inputs are finite; a program needn't handle non-finite values.
Results may differ from the reference program's by a relative error of at most 0.012.
Values may be sent and summed in bfloat16 or wider, within the bound.
A program may use at most 128 MiB of HBM per device.

```python
import math
import jax
import jax.numpy as jnp
import numpy as np
from jax import lax

D = 1536
HEADS = 16
KV_HEADS = 8
HEAD = 96
FF = 4096
TOK_GRP = 320
NDOC = 3
STREAMS = 16
MAXDOC = 256


def spiked(entries, stream_key, source, target, shards_of, factor):
    def block_of(axis_at):
        return (jnp.arange(entries.shape[axis_at]) // (entries.shape[axis_at] // shards_of)).reshape((-1,) + (1,) * (entries.ndim - 1 - axis_at))

    near = jax.random.permutation(stream_key, shards_of)[block_of(target)]
    other_side = (block_of(target) + shards_of // 2) % shards_of
    return jnp.where((block_of(source) == near) | (block_of(source) == other_side), factor * entries, entries)


def levels(stream_key, dims, split, smallest, high):
    loudness, own = 1.0, jax.random.fold_in(stream_key, 6)
    for axis_at, shards_of in split:
        heights = jnp.exp(jax.random.uniform(jax.random.fold_in(own, axis_at), (shards_of,), jnp.float32, smallest / len(split), high / len(split)))
        loudness = loudness * jnp.repeat(heights, dims[axis_at] // shards_of).reshape([-1 if axis == axis_at else 1 for axis in range(len(dims))])
    return loudness


def split_up(count, total, reach, lean):
    loads = [(1 << 20) // math.isqrt(rank ** lean) + 1 for rank in range(2, count + 1)]
    spare, counts = total - reach - (count - 1), [1] * (count - 1)
    while spare > 0:
        free = [i for i in range(count - 1) if counts[i] < reach]
        mass, left = sum([loads[i] for i in free]), spare
        for i in free:
            extra = min(reach - counts[i], max(1, left * loads[i] // mass), spare)
            counts[i] = counts[i] + extra
            spare = spare - extra
    return np.array([reach] + counts)


def uneven_parts(stream_key, number_of, total, most, lean):
    if number_of == 2:
        one = jax.random.randint(stream_key, (), max(1, total - most), min(most, total - 1) + 1)
        return jnp.stack([one, total - one])
    sizes = jnp.asarray(split_up(number_of, total, most, lean), jnp.int32)
    twos = (number_of - 1) // 2
    giver, taker = sizes[1:1 + 2 * twos:2], sizes[2:2 + 2 * twos:2]
    room = jnp.minimum(giver - 1, most - taker)
    passed = jax.random.randint(jax.random.fold_in(stream_key, 1), (twos,), 0, 1 << 20) % (room + 1)
    sizes = sizes.at[1:1 + 2 * twos:2].set(giver - passed).at[2:2 + 2 * twos:2].set(taker + passed)
    return sizes[jax.random.permutation(jax.random.fold_in(stream_key, 2), number_of)]


def bell_draw(own_key, dims, deviation, reach, split=(), held_as=jnp.bfloat16):
    values = jax.random.normal(own_key, dims, jnp.float32) * deviation
    if len(split) > 0:
        values = levels(own_key, dims, split, -0.22, 0.18) * values
    return jnp.clip(values, min=-reach, max=reach).astype(held_as)


def noise_with(stream_key, shape, deviation, most, pieces, heavy, held_as=jnp.bfloat16):
    values = deviation * jax.random.normal(stream_key, shape, jnp.float32)
    if pieces:
        values = values * levels(stream_key, shape, pieces, -0.22, 0.18)
    return jnp.clip(spiked(values, jax.random.fold_in(stream_key, 3), *heavy), -most, most).astype(held_as)


def setup_inputs(seed: int = 0) -> dict:
    key_of = jax.random.split(jax.random.key(seed), 14)
    return {
        "tokens": noise_with(key_of[0], (STREAMS, TOK_GRP, D), 1.0, 6.0, ((0, 8), (1, 4)), (0, 2, 8, 2.0)),
        "cotangent": noise_with(key_of[1], (STREAMS, TOK_GRP, D), 1.0, 6.0, ((0, 8), (1, 4)), (0, 2, 8, 2.0)),
        "order": jax.vmap(lambda own: jax.random.permutation(own, TOK_GRP))(jax.random.split(key_of[2], STREAMS)).reshape((STREAMS, TOK_GRP)).astype(jnp.int32),
        "lengths": jax.vmap(lambda own: uneven_parts(own, NDOC, TOK_GRP, MAXDOC, 2))(jax.random.split(key_of[3], STREAMS)).reshape((STREAMS, NDOC)).astype(jnp.int32),
        "gain_attn": jnp.clip(1.0 + 0.1 * jax.random.normal(key_of[4], (D,), jnp.float32), 0.5, 1.5).astype(jnp.bfloat16),
        "w_query": bell_draw(key_of[5], (D, D), D ** -0.5, 0.15625, ((0, 8), (1, 4))),
        "w_key": bell_draw(key_of[6], (D, KV_HEADS * HEAD), D ** -0.5, 0.15625, ((0, 8), (1, 4))),
        "w_value": bell_draw(key_of[7], (D, KV_HEADS * HEAD), D ** -0.5, 0.15625, ((0, 8), (1, 4))),
        "w_out": bell_draw(key_of[8], (D, D), (max(D // 96, 4)) ** -0.5, 1.5, ((0, 4), (1, 8))),
        "gain_ffn": jnp.clip(1.0 + 0.1 * jax.random.normal(key_of[9], (D,), jnp.float32), 0.5, 1.5).astype(jnp.bfloat16),
        "w_gate": bell_draw(key_of[10], (D, FF), D ** -0.5, 0.15625, ((0, 8), (1, 4))),
        "w_up": bell_draw(key_of[11], (D, FF), D ** -0.5, 0.15625, ((0, 8), (1, 4))),
        "w_down": bell_draw(key_of[12], (FF, D), FF ** -0.5, 0.09375, ((0, 4), (1, 8))),
    }


@jax.custom_vjp
def low(v):
    return lax.optimization_barrier(v.astype(jnp.bfloat16)).astype(jnp.float32)

@jax.custom_vjp
def low_back(v):
    return v

def low_keep(v):
    return (low(v), None)

def low_pass(kept, grad):
    return (grad,)

def back_keep(v):
    return (v, None)

def back_low(kept, grad):
    return (low(grad),)
low.defvjp(low_keep, low_pass)
low_back.defvjp(back_keep, back_low)
eps = 1e-05
rope_base = 100000.0

def rotate(field, angles):
    half = field.shape[-1] // 2
    cosine = jnp.cos(angles)[:, None, :]
    sine = jnp.sin(angles)[:, None, :]
    first = field[..., :half]
    second = field[..., half:]
    return jnp.concatenate([first * cosine - second * sine, second * cosine + first * sine], axis=-1)

def layout(order, lengths):
    starts = jnp.cumsum(lengths, dtype=jnp.int32) - lengths
    docs = lax.optimization_barrier(jnp.sum((order[:, None] >= starts[None, 1:]).astype(jnp.int32), axis=1, dtype=jnp.int32))
    onehot = docs[:, None] == jnp.arange(lengths.shape[0], dtype=jnp.int32)[None, :]
    first = lax.optimization_barrier(jnp.sum(jnp.where(onehot, starts[None, :], 0), axis=1, dtype=jnp.int32))
    positions = (order - first).astype(jnp.float32)
    mask = (docs[:, None] == docs[None, :]) & (order[None, :] <= order[:, None])
    real = (docs < lengths.shape[0] - 1).astype(jnp.float32)
    return (positions, mask, real)

def norm_rows(rows, gain):
    scale = lax.rsqrt(lax.optimization_barrier(jnp.mean(rows * rows, axis=-1, keepdims=True)) + eps)
    return rows * scale * gain

def stream_forward(rows, order, lengths, weights):
    gain_attn, w_query, w_key, w_value, w_out, gain_ffn, w_gate, w_up, w_down = weights
    highest = lax.Precision.HIGHEST
    count = rows.shape[0]
    group = HEADS // KV_HEADS
    positions, mask, real = layout(order, lengths)
    freqs = rope_base ** (-2.0 * jnp.arange(HEAD // 2, dtype=jnp.float32) / HEAD)
    angles = positions[:, None] * freqs[None, :]
    normed = low(norm_rows(rows, gain_attn))
    query = low_back(jnp.dot(normed, w_query, precision=highest)).reshape(count, HEADS, HEAD)
    query = low(rotate(query, angles) * HEAD ** (-0.5)).reshape(count, KV_HEADS, group, HEAD)
    keys = low_back(jnp.dot(normed, w_key, precision=highest)).reshape(count, KV_HEADS, HEAD)
    keys = low(rotate(keys, angles))
    values = low(low_back(jnp.dot(normed, w_value, precision=highest))).reshape(count, KV_HEADS, HEAD)
    scores = low_back(jnp.einsum('qkgd,skd->kgqs', query, keys, precision=highest))
    scores = jnp.where(mask, scores, -1e+30)
    peak = lax.optimization_barrier(jnp.max(scores, axis=-1, keepdims=True))
    expon = jnp.exp(scores - peak)
    probs = low(expon / lax.optimization_barrier(jnp.sum(expon, axis=-1, keepdims=True)))
    mixed = jnp.einsum('kgqs,skd->qkgd', probs, values, precision=highest).reshape(count, HEADS * HEAD)
    mixed = low(low_back(mixed))
    branch = low_back(jnp.dot(mixed, w_out, precision=highest))
    resid = rows + branch
    normed_ffn = low(norm_rows(resid, gain_ffn))
    gate = low_back(jnp.dot(normed_ffn, w_gate, precision=highest))
    upper = low_back(jnp.dot(normed_ffn, w_up, precision=highest))
    hidden = low(gate * jax.nn.sigmoid(gate) * upper)
    ffn = low_back(jnp.dot(hidden, w_down, precision=highest))
    return (resid + ffn) * real[:, None]

def block_forward(weights, item):
    block_rows, block_order, block_lengths = item
    return jax.vmap(stream_forward, in_axes=(0, 0, 0, None))(block_rows, block_order, block_lengths, weights)

def reference(tokens, cotangent, order, lengths, gain_attn, w_query, w_key, w_value, w_out, gain_ffn, w_gate, w_up, w_down):
    block = math.gcd(STREAMS, 4)
    steps_count = STREAMS // block
    checked = jax.checkpoint(block_forward)

    def forward(rows, g_attn, wq, wk, wv, wo, g_ffn, wg, wu, wd):
        weights = (g_attn, wq, wk, wv, wo, g_ffn, wg, wu, wd)

        def scan_body(carry, item):
            return (carry, checked(weights, item))
        items = (rows.reshape(steps_count, block, TOK_GRP, D), order.reshape(steps_count, block, TOK_GRP), lengths.reshape(steps_count, block, NDOC))
        carry_out, result = lax.scan(scan_body, jnp.zeros((), jnp.float32), items)
        return result.reshape(STREAMS, TOK_GRP, D)
    inputs = tokens.astype(jnp.float32)
    result, pullback = jax.vjp(forward, inputs, gain_attn.astype(jnp.float32), w_query.astype(jnp.float32), w_key.astype(jnp.float32), w_value.astype(jnp.float32), w_out.astype(jnp.float32), gain_ffn.astype(jnp.float32), w_gate.astype(jnp.float32), w_up.astype(jnp.float32), w_down.astype(jnp.float32))
    grads = pullback(cotangent.astype(jnp.float32))
    return (result.astype(jnp.bfloat16), grads[0], grads[1], grads[2], grads[3], grads[4], grads[5], grads[6], grads[7], grads[8], grads[9])
```

```python
import jax
import jax.numpy as jnp
from jax import lax
from jax.sharding import PartitionSpec as P

HEAD = 96


eps = 1e-05
rope_base = 100000.0


def rotate(field, cosine, sine):
    half = field.shape[-1] // 2
    first = field[..., :half]
    second = field[..., half:]
    return jnp.concatenate(
        [first * cosine - second * sine, second * cosine + first * sine], axis=-1
    )


def rotate_back(field, cosine, sine):
    half = field.shape[-1] // 2
    first = field[..., :half]
    second = field[..., half:]
    return jnp.concatenate(
        [first * cosine + second * sine, second * cosine - first * sine], axis=-1
    )


def layout(order, lengths):
    starts = jnp.cumsum(lengths, dtype=jnp.int32) - lengths
    docs = jnp.sum((order[:, None] >= starts[None, 1:]).astype(jnp.int32), axis=1, dtype=jnp.int32)
    onehot = docs[:, None] == jnp.arange(lengths.shape[0], dtype=jnp.int32)[None, :]
    first = jnp.sum(jnp.where(onehot, starts[None, :], 0), axis=1, dtype=jnp.int32)
    positions = (order - first).astype(jnp.float32)
    mask = (docs[:, None] == docs[None, :]) & (order[None, :] <= order[:, None])
    real = (docs < lengths.shape[0] - 1).astype(jnp.float32)
    return (positions, mask, real)


def norm_forward(rows, gain):
    scale = lax.rsqrt(jnp.mean(rows * rows, axis=-1, keepdims=True) + eps)
    unit = rows * scale
    return (unit, scale, (unit * gain).astype(jnp.bfloat16))


def norm_backward(grad, unit, scale, gain):
    inner = grad * gain
    return scale * (inner - unit * jnp.mean(inner * unit, axis=-1, keepdims=True))


def contract_rows(left, right):
    return lax.dot_general(
        left, right, (((0,), (0,)), ((), ())), preferred_element_type=jnp.float32
    )


def times_transpose(left, right):
    return lax.dot_general(
        left, right, (((1,), (1,)), ((), ())), preferred_element_type=jnp.float32
    )


def gather_weights(gain_attn, w_query, w_key, w_value, w_out, gain_ffn, w_gate, w_up, w_down):
    gains = lax.all_gather(jnp.stack([gain_attn, gain_ffn], axis=0), "dp", axis=1, tiled=True)
    attn = lax.all_gather(
        jnp.concatenate([w_query, w_key, w_value, w_out.T], axis=1), "dp", axis=0, tiled=True
    )
    gate_up = lax.all_gather(jnp.concatenate([w_gate, w_up], axis=1), "dp", axis=0, tiled=True)
    down = lax.all_gather(w_down.T, "dp", axis=0, tiled=True)
    return gains, attn, gate_up, down


def gather_rows(rows):
    return lax.all_gather(rows, "tensor", axis=1, tiled=True)


def scatter_rows(partial):
    low = partial.astype(jnp.bfloat16)
    return lax.psum_scatter(low, "tensor", scatter_dimension=1, tiled=True).astype(jnp.float32)


def reduce_weights(term):
    low = term.astype(jnp.bfloat16)
    return lax.psum_scatter(low, "dp", scatter_dimension=0, tiled=True).astype(jnp.float32)


def local(
    tokens,
    cotangent,
    order,
    lengths,
    gain_attn,
    w_query,
    w_key,
    w_value,
    w_out,
    gain_ffn,
    w_gate,
    w_up,
    w_down,
):
    micro, rows, width = tokens.shape
    seq = rows * lax.axis_size("tensor")
    q_cols, k_cols, ff_cols = w_query.shape[1], w_key.shape[1], w_gate.shape[1]
    local_heads, local_kv = q_cols // HEAD, k_cols // HEAD
    group = local_heads // local_kv
    first_row = lax.axis_index("tensor") * rows
    freqs = rope_base ** (-2.0 * jnp.arange(HEAD // 2, dtype=jnp.float32) / HEAD)
    head_scale = HEAD ** (-0.5)

    gains, attn, gate_up, down = gather_weights(
        gain_attn, w_query, w_key, w_value, w_out, gain_ffn, w_gate, w_up, w_down
    )
    gain1, gain2 = gains[0].astype(jnp.float32), gains[1].astype(jnp.float32)
    in_cols = q_cols + 2 * k_cols
    w_in, w_out_t = attn[:, :in_cols], attn[:, in_cols:]

    positions, mask, real = jax.vmap(layout)(order, lengths)
    angles = positions[:, :, None] * freqs
    cosine, sine = jnp.cos(angles)[:, :, None, :], jnp.sin(angles)[:, :, None, :]
    mask = mask[:, None, None]
    real_rows = lax.dynamic_slice_in_dim(real, first_row, rows, 1)[:, :, None]

    stream = tokens.astype(jnp.float32)
    unit1, scale1, normed1 = norm_forward(stream, gain1)
    full1 = gather_rows(normed1)
    grad_out_rows = cotangent.astype(jnp.float32) * real_rows
    full_grad = gather_rows(grad_out_rows.astype(jnp.bfloat16))
    flat1 = full1.reshape(micro * seq, width)
    flat_grad = full_grad.reshape(micro * seq, width)

    mixed_in = jnp.dot(flat1, w_in, preferred_element_type=jnp.float32).reshape(micro, seq, in_cols)
    query = mixed_in[..., :q_cols].reshape(micro, seq, local_heads, HEAD)
    keys = mixed_in[..., q_cols : q_cols + k_cols].reshape(micro, seq, local_kv, HEAD)
    values = mixed_in[..., q_cols + k_cols :].reshape(micro, seq, local_kv, HEAD).astype(jnp.bfloat16)
    query = (rotate(query, cosine, sine) * head_scale).astype(jnp.bfloat16)
    query = query.reshape(micro, seq, local_kv, group, HEAD)
    keys = rotate(keys, cosine, sine).astype(jnp.bfloat16)
    scores = jnp.einsum("bqkgd,bskd->bkgqs", query, keys, preferred_element_type=jnp.float32)
    scores = jnp.where(mask, scores, -1e30)
    peak = jnp.max(scores, axis=-1, keepdims=True)
    expon = jnp.exp(scores - peak)
    total = jnp.sum(expon, axis=-1, keepdims=True)
    probs = expon / total
    probs_low = probs.astype(jnp.bfloat16)
    mixed = jnp.einsum("bkgqs,bskd->bqkgd", probs_low, values, preferred_element_type=jnp.float32)
    mixed = mixed.reshape(micro * seq, q_cols).astype(jnp.bfloat16)
    branch = scatter_rows(times_transpose(mixed, w_out_t).reshape(micro, seq, width))
    resid = stream + branch
    unit2, scale2, normed2 = norm_forward(resid, gain2)
    full2 = gather_rows(normed2).reshape(micro * seq, width)

    both = jnp.dot(full2, gate_up, preferred_element_type=jnp.float32)
    gate, upper = both[:, :ff_cols], both[:, ff_cols:]
    sigma = jax.nn.sigmoid(gate)
    hidden = (gate * sigma * upper).astype(jnp.bfloat16)
    ffn = scatter_rows(times_transpose(hidden, down).reshape(micro, seq, width))
    output = ((resid + ffn) * real_rows).astype(jnp.bfloat16)

    grad_hidden = jnp.dot(flat_grad, down, preferred_element_type=jnp.float32)
    grad_gate = (grad_hidden * upper * sigma * (1.0 + gate * (1.0 - sigma))).astype(jnp.bfloat16)
    grad_up = (grad_hidden * gate * sigma).astype(jnp.bfloat16)
    grad_both = jnp.concatenate([grad_gate, grad_up], axis=1)
    grad_norm2 = scatter_rows(times_transpose(grad_both, gate_up).reshape(micro, seq, width))
    final_down = reduce_weights(contract_rows(flat_grad, hidden))
    final_gate = reduce_weights(contract_rows(full2, grad_gate))
    final_up = reduce_weights(contract_rows(full2, grad_up))
    term_gain2 = jnp.sum(grad_norm2 * unit2, axis=(0, 1))
    grad_resid = grad_out_rows + norm_backward(grad_norm2, unit2, scale2, gain2)

    full_resid = gather_rows(grad_resid.astype(jnp.bfloat16)).reshape(micro * seq, width)
    grad_mixed = jnp.dot(full_resid, w_out_t, preferred_element_type=jnp.float32).astype(jnp.bfloat16)
    final_out = reduce_weights(contract_rows(full_resid, mixed))
    grad_heads = grad_mixed.reshape(micro, seq, local_kv, group, HEAD)
    grad_probs = jnp.einsum(
        "bqkgd,bskd->bkgqs", grad_heads, values, preferred_element_type=jnp.float32
    )
    grad_values = jnp.einsum(
        "bkgqs,bqkgd->bskd", probs_low, grad_heads, preferred_element_type=jnp.float32
    )
    grad_scores = (
        probs * (grad_probs - jnp.sum(probs * grad_probs, axis=-1, keepdims=True))
    ).astype(jnp.bfloat16)
    grad_query = jnp.einsum(
        "bkgqs,bskd->bqkgd", grad_scores, keys, preferred_element_type=jnp.float32
    ).reshape(micro, seq, local_heads, HEAD)
    grad_keys = jnp.einsum(
        "bkgqs,bqkgd->bskd", grad_scores, query, preferred_element_type=jnp.float32
    )
    grad_query = rotate_back(grad_query * head_scale, cosine, sine).reshape(micro * seq, q_cols)
    grad_keys = rotate_back(grad_keys, cosine, sine).reshape(micro * seq, k_cols)
    grad_values = grad_values.reshape(micro * seq, k_cols)
    grad_in = jnp.concatenate(
        [grad_query.astype(jnp.bfloat16), grad_keys.astype(jnp.bfloat16), grad_values.astype(jnp.bfloat16)],
        axis=1,
    )
    grad_norm1 = scatter_rows(times_transpose(grad_in, w_in).reshape(micro, seq, width))
    final_in = reduce_weights(contract_rows(flat1, grad_in))
    term_gain1 = jnp.sum(grad_norm1 * unit1, axis=(0, 1))
    grad_tokens = grad_resid + norm_backward(grad_norm1, unit1, scale1, gain1)

    gain_terms = lax.psum(jnp.stack([term_gain1, term_gain2], axis=0), ("dp", "tensor"))
    own = gain_attn.shape[0]
    gain_own = lax.dynamic_slice_in_dim(gain_terms, lax.axis_index("dp") * own, own, 1)
    return (
        output,
        grad_tokens,
        gain_own[0],
        final_in[:, :q_cols],
        final_in[:, q_cols : q_cols + k_cols],
        final_in[:, q_cols + k_cols :],
        final_out.T,
        gain_own[1],
        final_gate,
        final_up,
        final_down.T,
    )


def solution(mesh):
    return jax.shard_map(
        local,
        mesh=mesh,
        in_specs=(
            P("dp", "tensor", None),
            P("dp", "tensor", None),
            P("dp", None),
            P("dp", None),
            P("dp"),
            P("dp", "tensor"),
            P("dp", "tensor"),
            P("dp", "tensor"),
            P("tensor", "dp"),
            P("dp"),
            P("dp", "tensor"),
            P("dp", "tensor"),
            P("tensor", "dp"),
        ),
        out_specs=(
            P("dp", "tensor", None),
            P("dp", "tensor", None),
            P("dp"),
            P("dp", "tensor"),
            P("dp", "tensor"),
            P("dp", "tensor"),
            P("tensor", "dp"),
            P("dp"),
            P("dp", "tensor"),
            P("dp", "tensor"),
            P("tensor", "dp"),
        ),
        check_vma=False,
    )
```

```python
import functools

import jax
import jax.numpy as jnp
from jax import lax
from jax.experimental import pallas as pl
from jax.experimental.pallas import tpu as pltpu
from jax.sharding import PartitionSpec as P

HEAD = 96


eps = 1e-05
rope_base = 100000.0


def rotate(field, cosine, sine):
    half = field.shape[-1] // 2
    first = field[..., :half]
    second = field[..., half:]
    return jnp.concatenate(
        [first * cosine - second * sine, second * cosine + first * sine], axis=-1
    )


def rotate_back(field, cosine, sine):
    half = field.shape[-1] // 2
    first = field[..., :half]
    second = field[..., half:]
    return jnp.concatenate(
        [first * cosine + second * sine, second * cosine - first * sine], axis=-1
    )


def layout(order, lengths):
    starts = jnp.cumsum(lengths, dtype=jnp.int32) - lengths
    docs = jnp.sum((order[:, None] >= starts[None, 1:]).astype(jnp.int32), axis=1, dtype=jnp.int32)
    onehot = docs[:, None] == jnp.arange(lengths.shape[0], dtype=jnp.int32)[None, :]
    first = jnp.sum(jnp.where(onehot, starts[None, :], 0), axis=1, dtype=jnp.int32)
    positions = (order - first).astype(jnp.float32)
    mask = (docs[:, None] == docs[None, :]) & (order[None, :] <= order[:, None])
    real = (docs < lengths.shape[0] - 1).astype(jnp.float32)
    return (positions, mask, real)


def norm_forward(rows, gain):
    scale = lax.rsqrt(jnp.mean(rows * rows, axis=-1, keepdims=True) + eps)
    unit = rows * scale
    return (unit, scale, (unit * gain).astype(jnp.bfloat16))


def norm_backward(grad, unit, scale, gain):
    inner = grad * gain
    return scale * (inner - unit * jnp.mean(inner * unit, axis=-1, keepdims=True))


def contract_rows(left, right):
    return lax.dot_general(
        left, right, (((0,), (0,)), ((), ())), preferred_element_type=jnp.float32
    )


def times_transpose(left, right):
    return lax.dot_general(
        left, right, (((1,), (1,)), ((), ())), preferred_element_type=jnp.float32
    )


def gather_weights(gain_attn, w_query, w_key, w_value, w_out, gain_ffn, w_gate, w_up, w_down):
    gains = lax.all_gather(jnp.stack([gain_attn, gain_ffn], axis=0), "dp", axis=1, tiled=True)
    attn = lax.all_gather(
        jnp.concatenate([w_query, w_key, w_value, w_out.T], axis=1), "dp", axis=0, tiled=True
    )
    gate_up = lax.all_gather(jnp.concatenate([w_gate, w_up], axis=1), "dp", axis=0, tiled=True)
    down = lax.all_gather(w_down.T, "dp", axis=0, tiled=True)
    return gains, attn, gate_up, down


def gather_rows(rows):
    return lax.all_gather(rows, "tensor", axis=1, tiled=True)


def scatter_rows(partial):
    low = partial.astype(jnp.bfloat16)
    return lax.psum_scatter(low, "tensor", scatter_dimension=1, tiled=True).astype(jnp.float32)


def reduce_weights(term):
    low = term.astype(jnp.bfloat16)
    return lax.psum_scatter(low, "dp", scatter_dimension=0, tiled=True).astype(jnp.float32)


def spread_out(
    tokens,
    cotangent,
    order,
    lengths,
    gain_attn,
    w_query,
    w_key,
    w_value,
    w_out,
    gain_ffn,
    w_gate,
    w_up,
    w_down,
):
    micro, rows, width = tokens.shape
    seq = rows * lax.axis_size("tensor")
    q_cols, k_cols, ff_cols = w_query.shape[1], w_key.shape[1], w_gate.shape[1]
    local_heads, local_kv = q_cols // HEAD, k_cols // HEAD
    group = local_heads // local_kv
    first_row = lax.axis_index("tensor") * rows
    freqs = rope_base ** (-2.0 * jnp.arange(HEAD // 2, dtype=jnp.float32) / HEAD)
    head_scale = HEAD ** (-0.5)

    gains, attn, gate_up, down = gather_weights(
        gain_attn, w_query, w_key, w_value, w_out, gain_ffn, w_gate, w_up, w_down
    )
    gain1, gain2 = gains[0].astype(jnp.float32), gains[1].astype(jnp.float32)
    in_cols = q_cols + 2 * k_cols
    w_in, w_out_t = attn[:, :in_cols], attn[:, in_cols:]

    positions, mask, real = jax.vmap(layout)(order, lengths)
    angles = positions[:, :, None] * freqs
    cosine, sine = jnp.cos(angles)[:, :, None, :], jnp.sin(angles)[:, :, None, :]
    mask = mask[:, None, None]
    real_rows = lax.dynamic_slice_in_dim(real, first_row, rows, 1)[:, :, None]

    stream = tokens.astype(jnp.float32)
    unit1, scale1, normed1 = norm_forward(stream, gain1)
    full1 = gather_rows(normed1)
    grad_out_rows = cotangent.astype(jnp.float32) * real_rows
    full_grad = gather_rows(grad_out_rows.astype(jnp.bfloat16))
    flat1 = full1.reshape(micro * seq, width)
    flat_grad = full_grad.reshape(micro * seq, width)

    mixed_in = jnp.dot(flat1, w_in, preferred_element_type=jnp.float32).reshape(micro, seq, in_cols)
    query = mixed_in[..., :q_cols].reshape(micro, seq, local_heads, HEAD)
    keys = mixed_in[..., q_cols : q_cols + k_cols].reshape(micro, seq, local_kv, HEAD)
    values = mixed_in[..., q_cols + k_cols :].reshape(micro, seq, local_kv, HEAD).astype(jnp.bfloat16)
    query = (rotate(query, cosine, sine) * head_scale).astype(jnp.bfloat16)
    query = query.reshape(micro, seq, local_kv, group, HEAD)
    keys = rotate(keys, cosine, sine).astype(jnp.bfloat16)
    scores = jnp.einsum("bqkgd,bskd->bkgqs", query, keys, preferred_element_type=jnp.float32)
    scores = jnp.where(mask, scores, -1e30)
    peak = jnp.max(scores, axis=-1, keepdims=True)
    expon = jnp.exp(scores - peak)
    total = jnp.sum(expon, axis=-1, keepdims=True)
    probs = expon / total
    probs_low = probs.astype(jnp.bfloat16)
    mixed = jnp.einsum("bkgqs,bskd->bqkgd", probs_low, values, preferred_element_type=jnp.float32)
    mixed = mixed.reshape(micro * seq, q_cols).astype(jnp.bfloat16)
    branch = scatter_rows(times_transpose(mixed, w_out_t).reshape(micro, seq, width))
    resid = stream + branch
    unit2, scale2, normed2 = norm_forward(resid, gain2)
    full2 = gather_rows(normed2).reshape(micro * seq, width)

    both = jnp.dot(full2, gate_up, preferred_element_type=jnp.float32)
    gate, upper = both[:, :ff_cols], both[:, ff_cols:]
    sigma = jax.nn.sigmoid(gate)
    hidden = (gate * sigma * upper).astype(jnp.bfloat16)
    ffn = scatter_rows(times_transpose(hidden, down).reshape(micro, seq, width))
    output = ((resid + ffn) * real_rows).astype(jnp.bfloat16)

    grad_hidden = jnp.dot(flat_grad, down, preferred_element_type=jnp.float32)
    grad_gate = (grad_hidden * upper * sigma * (1.0 + gate * (1.0 - sigma))).astype(jnp.bfloat16)
    grad_up = (grad_hidden * gate * sigma).astype(jnp.bfloat16)
    grad_both = jnp.concatenate([grad_gate, grad_up], axis=1)
    grad_norm2 = scatter_rows(times_transpose(grad_both, gate_up).reshape(micro, seq, width))
    final_down = reduce_weights(contract_rows(flat_grad, hidden))
    final_gate = reduce_weights(contract_rows(full2, grad_gate))
    final_up = reduce_weights(contract_rows(full2, grad_up))
    term_gain2 = jnp.sum(grad_norm2 * unit2, axis=(0, 1))
    grad_resid = grad_out_rows + norm_backward(grad_norm2, unit2, scale2, gain2)

    full_resid = gather_rows(grad_resid.astype(jnp.bfloat16)).reshape(micro * seq, width)
    grad_mixed = jnp.dot(full_resid, w_out_t, preferred_element_type=jnp.float32).astype(jnp.bfloat16)
    final_out = reduce_weights(contract_rows(full_resid, mixed))
    grad_heads = grad_mixed.reshape(micro, seq, local_kv, group, HEAD)
    grad_probs = jnp.einsum(
        "bqkgd,bskd->bkgqs", grad_heads, values, preferred_element_type=jnp.float32
    )
    grad_values = jnp.einsum(
        "bkgqs,bqkgd->bskd", probs_low, grad_heads, preferred_element_type=jnp.float32
    )
    grad_scores = (
        probs * (grad_probs - jnp.sum(probs * grad_probs, axis=-1, keepdims=True))
    ).astype(jnp.bfloat16)
    grad_query = jnp.einsum(
        "bkgqs,bskd->bqkgd", grad_scores, keys, preferred_element_type=jnp.float32
    ).reshape(micro, seq, local_heads, HEAD)
    grad_keys = jnp.einsum(
        "bkgqs,bqkgd->bskd", grad_scores, query, preferred_element_type=jnp.float32
    )
    grad_query = rotate_back(grad_query * head_scale, cosine, sine).reshape(micro * seq, q_cols)
    grad_keys = rotate_back(grad_keys, cosine, sine).reshape(micro * seq, k_cols)
    grad_values = grad_values.reshape(micro * seq, k_cols)
    grad_in = jnp.concatenate(
        [grad_query.astype(jnp.bfloat16), grad_keys.astype(jnp.bfloat16), grad_values.astype(jnp.bfloat16)],
        axis=1,
    )
    grad_norm1 = scatter_rows(times_transpose(grad_in, w_in).reshape(micro, seq, width))
    final_in = reduce_weights(contract_rows(flat1, grad_in))
    term_gain1 = jnp.sum(grad_norm1 * unit1, axis=(0, 1))
    grad_tokens = grad_resid + norm_backward(grad_norm1, unit1, scale1, gain1)

    gain_terms = lax.psum(jnp.stack([term_gain1, term_gain2], axis=0), ("dp", "tensor"))
    own = gain_attn.shape[0]
    gain_own = lax.dynamic_slice_in_dim(gain_terms, lax.axis_index("dp") * own, own, 1)
    return (
        output,
        grad_tokens,
        gain_own[0],
        final_in[:, :q_cols],
        final_in[:, q_cols : q_cols + k_cols],
        final_in[:, q_cols + k_cols :],
        final_out.T,
        gain_own[1],
        final_gate,
        final_up,
        final_down.T,
    )


BF = jnp.bfloat16
F32 = jnp.float32
MESH = pl.DeviceIdType.MESH
LANES = 128


def nn(left, right):
    return lax.dot_general(left, right, (((1,), (0,)), ((), ())), preferred_element_type=F32)


def nt(left, right):
    return lax.dot_general(left, right, (((1,), (1,)), ((), ())), preferred_element_type=F32)


def tn(left, right):
    return lax.dot_general(left, right, (((0,), (0,)), ((), ())), preferred_element_type=F32)


def al(value, unit):
    return pl.multiple_of(value, unit)


def block_kernel(dims, *refs):
    (rows, seq, width, shard, qp, kp, ff, groups) = dims
    (tok, cot, wg_h, wi_h, wo_h, wu_h, wd_h, ordr, cols, cosr, sinr) = refs[:11]
    (out_h, gtok_h, gdown_h, ggate_h, gup_h, gout_h, gin_h, ggain_h) = refs[11:19]
    (wgn, wi, wo, wu, wd, xf, n1, n2, gf, qkv, ob, dob, act, dgu, pr, hb, dh, pa, pb, ra, rb,
     gb, xb, hop, fin, stage, acc, gains, gsum, gex, ybuf, tbuf,
     wsend, wrecv, zsend, zrecv, rsend, rrecv, gsend, grecv, esend, erecv, lsem, osem, credit, zfree) = refs[19:]
    ghf = xf
    heads = qp // LANES
    per_group = heads // groups
    inw = qp + 2 * kp
    d = lax.axis_index("dp")
    z = lax.axis_index("tensor")
    c = d % 2
    flip = 1 - 2 * c
    near_x = d + 2 - 4 * ((d // 2) % 2)
    near_y = d + 4 - 8 * (d // 4)
    aa = near_x * (1 - c) + near_y * c
    bb = near_y * (1 - c) + near_x * c
    dd = aa + bb - d
    pp = d + flip
    chip_own, chip_a, chip_b, chip_d = d // 2, aa // 2, bb // 2, dd // 2
    chip_x, chip_y = near_x // 2, near_y // 2
    own = 1 * z * rows
    zdev = {"tensor": z + 1}, {"tensor": z - 1}

    def rcopy(src, dst, ssem, rsem, dev):
        return pltpu.make_async_remote_copy(
            src_ref=src, dst_ref=dst, send_sem=ssem, recv_sem=rsem, device_id=dev, device_id_type=MESH
        )

    barrier = pltpu.get_barrier_semaphore()
    for dev in (pp, aa, bb):
        pl.semaphore_signal(barrier, inc=1, device_id={"dp": dev}, device_id_type=MESH)
    for step in (1, 2, 3):
        pl.semaphore_signal(
            barrier, inc=1, device_id={"tensor": (z + step) % 4}, device_id_type=MESH
        )
    pl.semaphore_wait(barrier, 6)

    wunits = ((wg_h, wgn, 16), (wi_h, wi, shard), (wo_h, wo, shard), (wu_h, wu, shard), (wd_h, wd, shard))

    def wblk(u, i):
        n = wunits[u][2]
        return wunits[u][1].at[pl.ds(al(n * i, 16), n)]

    def w_start(u):
        src = wunits[u][0]
        pltpu.make_async_copy(src, wblk(u, d), lsem.at[u]).start()
        rcopy(src, wblk(u, d), wsend.at[u, 0], wrecv.at[u, 0], {"dp": aa}).start()
        rcopy(src, wblk(u, d), wsend.at[u, 1], wrecv.at[u, 1], {"dp": bb}).start()
        rcopy(src, wblk(u, d), wsend.at[u, 2], wrecv.at[u, 3], {"dp": pp}).start()

    def w_wait(u, slot, i):
        rcopy(wblk(u, i), wblk(u, i), wsend.at[u, 0], wrecv.at[u, slot], {"dp": aa}).wait_recv()

    def w_relay(u):
        w_wait(u, 1, bb)
        rcopy(wblk(u, bb), wblk(u, bb), wsend.at[u, 3], wrecv.at[u, 2], {"dp": aa}).start()
        rcopy(wblk(u, bb), wblk(u, bb), wsend.at[u, 4], wrecv.at[u, 5], {"dp": pp}).start()
        w_wait(u, 0, aa)
        rcopy(wblk(u, aa), wblk(u, aa), wsend.at[u, 5], wrecv.at[u, 4], {"dp": pp}).start()

    def w_diag(u):
        w_wait(u, 2, dd)
        rcopy(wblk(u, dd), wblk(u, dd), wsend.at[u, 6], wrecv.at[u, 6], {"dp": pp}).start()

    def w_done(u):
        w_wait(u, 3, pp)
        w_wait(u, 4, bb + flip)
        w_wait(u, 5, aa + flip)
        w_wait(u, 6, dd + flip)
        pltpu.make_async_copy(wunits[u][0], wblk(u, d), lsem.at[u]).wait()

    def w_sent(u):
        for slot in range(7):
            rcopy(wblk(u, d), wblk(u, d), wsend.at[u, slot], wrecv.at[u, 0], {"dp": aa}).wait_send()

    zfull = (xf, gf, n2, ghf)
    zhbm = (tok, cot, None, None)

    def zblk(u, s, i):
        return zfull[u].at[pl.ds(al(s * seq + i * rows, 16), rows)]

    def zag_send(u, s, k, way):
        i = z - k if way == 0 else z + k
        go = (z < 3) & (i >= 0) if way == 0 else (z > 0) & (i <= 3)

        @pl.when(go)
        def _():
            src = zhbm[u].at[s] if k == 0 and zhbm[u] is not None else zblk(u, s, i)
            rcopy(src, zblk(u, s, i), zsend.at[u, s, way, k], zrecv.at[u, s, way, k], zdev[way]).start()

    def zag_recv(u, s, k, way):
        i = z - 1 - k if way == 0 else z + 1 + k
        go = (i >= 0) if way == 0 else (i <= 3)

        @pl.when(go)
        def _():
            rcopy(
                zblk(u, s, i), zblk(u, s, i), zsend.at[u, s, way, k], zrecv.at[u, s, way, k], zdev[way]
            ).wait_recv()

    def zag_start(u, s):
        if zhbm[u] is not None:
            pltpu.make_async_copy(zhbm[u].at[s], zblk(u, s, z), lsem.at[8 + 2 * u + s]).start()
        for way in (0, 1):
            zag_send(u, s, 0, way)

    def zag_fwd(u, s, k):
        for way in (0, 1):
            zag_recv(u, s, k - 1, way)
            zag_send(u, s, k, way)

    def zag_done(u, s):
        for way in (0, 1):
            zag_recv(u, s, 2, way)
        if zhbm[u] is not None:
            pltpu.make_async_copy(zhbm[u].at[s], zblk(u, s, z), lsem.at[8 + 2 * u + s]).wait()

    def zag_sent(u, s):
        for k in range(3):
            for way in (0, 1):
                i = z - k if way == 0 else z + k
                go = (z < 3) & (i >= 0) if way == 0 else (z > 0) & (i <= 3)

                @pl.when(go)
                def _():
                    rcopy(
                        zblk(u, s, i), zblk(u, s, i), zsend.at[u, s, way, k], zrecv.at[u, s, way, k], zdev[way]
                    ).wait_send()

    zpart = (pa, pb, pa, pb)
    zgot = (ra, rb, ra, rb)

    def pblk(u, s, i):
        return zpart[u].at[pl.ds(al(s * seq + i * rows, 16), rows)]

    def rblk(u, s, way, i):
        return zgot[u].at[s, way, i]

    def rs_copy(u, s, way, k):
        dest = 3 - k if way == 0 else k
        slot = dest - 1 if way == 0 else dest
        return rcopy(
            pblk(u, s, dest), rblk(u, s, way, slot), rsend.at[u, s, way, k], rrecv.at[u, s, way, k], zdev[way]
        )

    def add_rows(u, s, dest, way, slot):
        base = s * seq + dest * rows

        def body(i, carry):
            at = pl.ds(al(base + i * 16, 16), 16)
            got = zgot[u][s, way, slot, pl.ds(al(i * 16, 16), 16), :]
            zpart[u][at, :] = (zpart[u][at, :].astype(F32) + got.astype(F32)).astype(BF)
            return carry

        lax.fori_loop(0, rows // 16, body, 0)

    def rs_step(u, s, k):
        if u == 3 and k == 0:
            @pl.when(z > 0)
            def _():
                pl.semaphore_wait(zfree.at[s, 0], 1)

            @pl.when(z < 3)
            def _():
                pl.semaphore_wait(zfree.at[s, 1], 1)

        for way in (0, 1):
            dest = 3 - k if way == 0 else k
            slot = dest - 1 if way == 0 else dest
            sends = (z < dest) if way == 0 else (z > dest)
            inner = (z > 0) if way == 0 else (z < 3)

            @pl.when(sends)
            def _():
                @pl.when(inner)
                def _():
                    rs_copy(u, s, way, k).wait_recv()
                    add_rows(u, s, dest, way, slot)

                rs_copy(u, s, way, k).start()

    def rs_final(u, s):
        def first(i, carry):
            at = pl.ds(al(i * 16, 16), 16)
            acc[at, :] = zpart[u][pl.ds(al(s * seq + own + i * 16, 16), 16), :].astype(F32)
            return carry

        lax.fori_loop(0, rows // 16, first, 0)
        for way in (0, 1):
            there = (z > 0) if way == 0 else (z < 3)
            slot = z - 1 if way == 0 else z
            k = 3 - z if way == 0 else z

            @pl.when(there)
            def _():
                rcopy(
                    pblk(u, s, z), rblk(u, s, way, slot), rsend.at[u, s, way, k], rrecv.at[u, s, way, k], zdev[way]
                ).wait_recv()

                def more(i, carry):
                    at = pl.ds(al(i * 16, 16), 16)
                    acc[at, :] += zgot[u][s, way, slot, at, :].astype(F32)
                    return carry

                lax.fori_loop(0, rows // 16, more, 0)

        if u == 1:
            @pl.when(z < 3)
            def _():
                pl.semaphore_signal(zfree.at[s, 0], inc=1, device_id=zdev[0], device_id_type=MESH)

            @pl.when(z > 0)
            def _():
                pl.semaphore_signal(zfree.at[s, 1], inc=1, device_id=zdev[1], device_id_type=MESH)

    def rs_sent(u, s):
        for way in (0, 1):
            for k in range(3):
                dest = 3 - k if way == 0 else k
                sends = (z < dest) if way == 0 else (z > dest)

                @pl.when(sends)
                def _():
                    rs_copy(u, s, way, k).wait_send()

    gunits = (
        (gf, act, 0, ff, gdown_h),
        (n2, dgu, 0, ff, ggate_h),
        (n2, dgu, ff, ff, gup_h),
        (ghf, ob, 0, qp, gout_h),
        (n1, act, 0, inw, gin_h),
    )
    pair = 2 * shard

    def xslot(u, chip):
        b, n = u % 2, gunits[u][3]
        return xb.at[b, pl.ds(al(chip * shard, 16), shard), pl.ds(0, n)]

    def gslot(u, chip, core):
        b, n = u % 2, gunits[u][3]
        return gb.at[b, pl.ds(al(chip * pair + core * shard, 16), shard), pl.ds(0, n)]

    def g_exchange(u, chip, i):
        return rcopy(gslot(u, chip, 1 - c), xslot(u, chip), gsend.at[u, i], grecv.at[u, i], {"dp": pp})

    chips = (chip_d, chip_x, chip_y, chip_own)

    def g_compute(u):
        left, right, at, n, _ = gunits[u]
        if u >= 2:
            pl.semaphore_wait(credit.at[0], 1)
        for i, chip in enumerate(chips):
            tile = 256

            def body(j, carry):
                lhs = left[:, pl.ds(al(chip * pair, LANES), pair)]
                got = tn(lhs, right[:, pl.ds(al(at + j * tile, tile), tile)])
                gb[u % 2, pl.ds(al(chip * pair, 16), pair), pl.ds(al(j * tile, tile), tile)] = got.astype(BF)
                return carry

            lax.fori_loop(0, n // tile, body, 0)
            g_exchange(u, chip, i).start()

    def g_add(u, chip, extra=None):
        b, n = u % 2, gunits[u][3]

        def body(i, carry):
            at = pl.ds(al(chip * shard + i * 16, 16), 16)
            mine = gb[b, pl.ds(al(chip * pair + c * shard + i * 16, 16), 16), pl.ds(0, n)].astype(F32)
            total = mine + xb[b, at, pl.ds(0, n)].astype(F32)
            if extra is not None:
                total = total + extra[b, pl.ds(al(i * 16, 16), 16), pl.ds(0, n)].astype(F32)
            xb[b, at, pl.ds(0, n)] = total.astype(BF)
            return carry

        lax.fori_loop(0, shard // 16, body, 0)

    def g_hop(u):
        b, n = u % 2, gunits[u][3]
        return rcopy(xslot(u, chip_d), hop.at[b, :, pl.ds(0, n)], gsend.at[u, 4], grecv.at[u, 4], {"dp": aa})

    def g_last(u, way):
        b, n = u % 2, gunits[u][3]
        chip, dev = (chip_a, aa) if way == 0 else (chip_b, bb)
        return rcopy(
            xslot(u, chip), fin.at[b, way, :, pl.ds(0, n)], gsend.at[u, 5 + way], grecv.at[u, 5 + way], {"dp": dev}
        )

    def g_first(u):
        g_exchange(u, chip_d, 0).wait_recv()
        g_add(u, chip_d)
        if u >= 2:
            pl.semaphore_wait(credit.at[1], 1)
        g_hop(u).start()
        g_exchange(u, chip_x, 1).wait_recv()
        g_exchange(u, chip_y, 2).wait_recv()
        g_add(u, chip_a)
        g_last(u, 0).start()

    def g_second(u):
        g_hop(u).wait_recv()
        g_add(u, chip_b, hop)
        if u >= 2:
            pl.semaphore_wait(credit.at[2], 1)
        g_last(u, 1).start()

    def g_finish(u):
        b, n, out = u % 2, gunits[u][3], gunits[u][4]
        g_exchange(u, chip_own, 3).wait_recv()
        g_last(u, 0).wait_recv()
        g_last(u, 1).wait_recv()

        def body(i, carry):
            at = pl.ds(al(i * 16, 16), 16)
            total = gb[b, pl.ds(al(chip_own * pair + c * shard + i * 16, 16), 16), pl.ds(0, n)].astype(F32)
            total = total + xb[b, pl.ds(al(chip_own * shard + i * 16, 16), 16), pl.ds(0, n)].astype(F32)
            total = total + fin[b, 0, at, pl.ds(0, n)].astype(F32)
            stage[b, at, pl.ds(0, n)] = total + fin[b, 1, at, pl.ds(0, n)].astype(F32)
            return carry

        if u >= 2:
            g_out(u - 2).wait()
        lax.fori_loop(0, shard // 16, body, 0)
        g_out(u).start()
        for i in range(4):
            g_exchange(u, chips[i], i).wait_send()
        g_hop(u).wait_send()
        g_last(u, 0).wait_send()
        g_last(u, 1).wait_send()
        if u < 3:
            pl.semaphore_signal(credit.at[0], inc=1, device_id={"dp": pp}, device_id_type=MESH)
            pl.semaphore_signal(credit.at[1], inc=1, device_id={"dp": aa}, device_id_type=MESH)
            pl.semaphore_signal(credit.at[2], inc=1, device_id={"dp": bb}, device_id_type=MESH)

    def g_out(u):
        b, n, out = u % 2, gunits[u][3], gunits[u][4]
        return pltpu.make_async_copy(stage.at[b, :, pl.ds(0, n)], out, osem.at[u])

    def norm1(s):
        gain = gains[0:1, :]

        def body(i, carry):
            at = pl.ds(al(s * seq + i * 16, 16), 16)
            x = xf[at, :].astype(F32)
            scale = lax.rsqrt(jnp.mean(x * x, axis=-1, keepdims=True) + eps)
            n1[at, :] = (x * scale * gain).astype(BF)
            return carry

        lax.fori_loop(0, seq // 16, body, 0)

    head_scale = HEAD ** (-0.5)

    def project(s):
        at = pl.ds(s * seq, seq)
        cosine, sine = cosr[s], sinr[s]
        for j in range(inw // 256):
            both = nn(n1[at, :], wi[:, pl.ds(j * 256, 256)])
            for half in range(2):
                col = j * 256 + half * LANES
                part = both[:, half * LANES : (half + 1) * LANES]
                if col < qp + kp:
                    part = part * cosine + pltpu.roll(part, LANES // 2, 1) * sine
                if col < qp:
                    part = part * head_scale
                qkv[at, pl.ds(col, LANES)] = part.astype(BF)

    def attend(s):
        at = pl.ds(s * seq, seq)
        oc = ordr[s]
        mask = (oc <= cols[s, :, 0:1]) & (oc >= cols[s, :, 1:2])

        def body(h, carry):
            g = h // per_group
            q = qkv[at, pl.ds(al(h * LANES, LANES), LANES)]
            k = qkv[at, pl.ds(al(qp + g * LANES, LANES), LANES)]
            v = qkv[at, pl.ds(al(qp + kp + g * LANES, LANES), LANES)]
            sc = jnp.where(mask, nt(q, k), -1e30)
            e = jnp.exp(sc - jnp.max(sc, axis=-1, keepdims=True))
            p = e * (1.0 / jnp.sum(e, axis=-1, keepdims=True))
            pr[s * heads + h] = p
            ob[at, pl.ds(al(h * LANES, LANES), LANES)] = nn(p.astype(BF), v).astype(BF)
            return carry

        lax.fori_loop(0, heads, body, 0)

    def spread(s, dst, left, weight, tile):
        at = pl.ds(s * seq, seq)

        def body(j, carry):
            col = al(j * tile, tile)
            dst[at, pl.ds(col, tile)] = nt(left[at, :], weight[pl.ds(col, tile), :]).astype(BF)
            return carry

        lax.fori_loop(0, width // tile, body, 0)

    def norm2(s):
        gain = gains[1:2, :]
        base = s * rows

        def body(i, carry):
            r = pl.ds(al(i * 16, 16), 16)
            h = tbuf[s, r, :].astype(F32) + acc[r, :]
            hb[pl.ds(al(base + i * 16, 16), 16), :] = h
            scale = lax.rsqrt(jnp.mean(h * h, axis=-1, keepdims=True) + eps)
            n2[pl.ds(al(s * seq + own + i * 16, 16), 16), :] = (h * scale * gain).astype(BF)
            return carry

        lax.fori_loop(0, rows // 16, body, 0)

    def mask_grad(s):
        def body(i, carry):
            at = pl.ds(al(s * seq + i * 16, 16), 16)
            gf[at, :] = (gf[at, :].astype(F32) * cols[s, pl.ds(al(i * 16, 16), 16), 2:3]).astype(BF)
            return carry

        lax.fori_loop(0, seq // 16, body, 0)

    def feed(s):
        at = pl.ds(s * seq, seq)

        def body(t, carry):
            col = al(t * 256, 256)
            gate = nn(n2[at, :], wu[:, pl.ds(col, 256)])
            upper = nn(n2[at, :], wu[:, pl.ds(al(ff + t * 256, 256), 256)])
            back = nn(gf[at, :], wd[:, pl.ds(col, 256)])
            sigma = 1.0 / (1.0 + jnp.exp(-gate))
            swish = gate * sigma
            act[at, pl.ds(col, 256)] = (swish * upper).astype(BF)
            dgu[at, pl.ds(col, 256)] = (back * upper * sigma * (1.0 + gate * (1.0 - sigma))).astype(BF)
            dgu[at, pl.ds(al(ff + t * 256, 256), 256)] = (back * swish).astype(BF)
            return carry

        lax.fori_loop(0, ff // 256, body, 0)

    def finish_out(s):
        def body(i, carry):
            r = pl.ds(al(i * 16, 16), 16)
            real = cols[s, pl.ds(al(own + i * 16, 16), 16), 2:3]
            y = (hb[pl.ds(al(s * rows + i * 16, 16), 16), :] + acc[r, :]) * real
            ybuf[s, r, :] = y.astype(BF)
            return carry

        lax.fori_loop(0, rows // 16, body, 0)
        pltpu.make_async_copy(ybuf.at[s], out_h.at[s], osem.at[5 + s]).start()

    def norm2_back(s):
        gain = gains[1:2, :]

        def body(i, carry):
            r = pl.ds(al(i * 16, 16), 16)
            ro = pl.ds(al(s * rows + i * 16, 16), 16)
            h = hb[ro, :]
            scale = lax.rsqrt(jnp.mean(h * h, axis=-1, keepdims=True) + eps)
            unit = h * scale
            grad = acc[r, :]
            inner = grad * gain
            dy = gf[pl.ds(al(s * seq + own + i * 16, 16), 16), :].astype(F32)
            dhr = dy + scale * (inner - unit * jnp.mean(inner * unit, axis=-1, keepdims=True))
            dh[ro, :] = dhr
            ghf[pl.ds(al(s * seq + own + i * 16, 16), 16), :] = dhr.astype(BF)
            return carry + jnp.sum(grad * unit, axis=0, keepdims=True)

        return lax.fori_loop(0, rows // 16, body, jnp.zeros((1, width), F32))

    def grad_heads(s):
        at = pl.ds(s * seq, seq)
        for j in range(qp // 256):
            dob[at, pl.ds(j * 256, 256)] = nn(ghf[at, :], wo[:, pl.ds(j * 256, 256)]).astype(BF)

    def attend_back(s):
        at = pl.ds(s * seq, seq)
        cosine, sine = cosr[s], sinr[s]

        def body(g, carry):
            k = qkv[at, pl.ds(al(qp + g * LANES, LANES), LANES)]
            v = qkv[at, pl.ds(al(qp + kp + g * LANES, LANES), LANES)]
            dk = jnp.zeros((seq, LANES), F32)
            dv = jnp.zeros((seq, LANES), F32)
            for m in range(per_group):
                h = g * per_group + m
                hat = pl.ds(al(h * LANES, LANES), LANES)
                q = qkv[at, hat]
                do = dob[at, hat]
                p = pr[s * heads + h]
                dp = nt(do, v)
                ds = (p * (dp - jnp.sum(p * dp, axis=-1, keepdims=True))).astype(BF)
                dv = dv + tn(p.astype(BF), do)
                dk = dk + tn(ds, q)
                dq = nn(ds, k) * head_scale
                act[at, hat] = (dq * cosine - pltpu.roll(dq, LANES // 2, 1) * sine).astype(BF)
            act[at, pl.ds(al(qp + g * LANES, LANES), LANES)] = (
                dk * cosine - pltpu.roll(dk, LANES // 2, 1) * sine
            ).astype(BF)
            act[at, pl.ds(al(qp + kp + g * LANES, LANES), LANES)] = dv.astype(BF)
            return carry

        lax.fori_loop(0, groups, body, 0)

    def norm1_back(s):
        gain = gains[0:1, :]

        def body(i, carry):
            r = pl.ds(al(i * 16, 16), 16)
            ro = pl.ds(al(s * rows + i * 16, 16), 16)
            x = tbuf[s, r, :].astype(F32)
            scale = lax.rsqrt(jnp.mean(x * x, axis=-1, keepdims=True) + eps)
            unit = x * scale
            grad = acc[r, :]
            inner = grad * gain
            dh[ro, :] = dh[ro, :] + scale * (inner - unit * jnp.mean(inner * unit, axis=-1, keepdims=True))
            return carry + jnp.sum(grad * unit, axis=0, keepdims=True)

        total = lax.fori_loop(0, rows // 16, body, jnp.zeros((1, width), F32))
        pltpu.make_async_copy(
            dh.at[pl.ds(s * rows, rows)], gtok_h.at[s], osem.at[7 + s]
        ).start()
        return total

    for s in (0, 1):
        pltpu.make_async_copy(tok.at[s], tbuf.at[s], lsem.at[5 + s]).start()
    zag_start(0, 0)
    w_start(0)
    w_start(1)
    w_start(2)
    zag_fwd(0, 0, 1)
    zag_start(0, 1)
    w_relay(0)
    w_relay(1)
    w_start(3)
    zag_fwd(0, 0, 2)
    zag_fwd(0, 1, 1)
    w_relay(2)
    w_start(4)
    w_diag(0)
    w_diag(1)
    w_diag(2)
    w_done(0)
    for j in range(4):
        at = pl.ds(j * pair, pair)
        gains[:, at] = (
            wgn[pl.ds(32 * j, 16), :].astype(F32) + wgn[pl.ds(32 * j + 16, 16), :].astype(F32)
        )
    zag_done(0, 0)
    zag_fwd(0, 1, 2)
    zag_start(1, 0)
    norm1(0)
    w_done(1)
    project(0)
    w_relay(3)
    zag_done(0, 1)
    zag_fwd(1, 0, 1)
    zag_start(1, 1)
    attend(0)
    w_done(2)
    spread(0, pa, ob, wo, 512)
    rs_step(0, 0, 0)
    zag_fwd(1, 0, 2)
    zag_fwd(1, 1, 1)
    w_relay(4)
    w_diag(3)
    norm1(1)
    rs_step(0, 0, 1)
    project(1)
    rs_step(0, 0, 2)
    zag_fwd(1, 1, 2)
    attend(1)
    for s in (0, 1):
        pltpu.make_async_copy(tok.at[s], tbuf.at[s], lsem.at[5 + s]).wait()
        zag_sent(0, s)
    spread(1, pa, ob, wo, 512)
    rs_step(0, 1, 0)
    rs_final(0, 0)
    norm2(0)
    zag_start(2, 0)
    w_diag(4)
    zag_done(1, 0)
    mask_prep = mask_grad
    rs_step(0, 1, 1)
    zag_fwd(2, 0, 1)
    rs_step(0, 1, 2)
    zag_sent(1, 0)
    mask_prep(0)
    rs_final(0, 1)
    norm2(1)
    zag_start(2, 1)
    zag_fwd(2, 0, 2)
    zag_done(1, 1)
    zag_fwd(2, 1, 1)
    zag_sent(1, 1)
    mask_prep(1)
    w_done(3)
    w_done(4)
    rs_sent(0, 0)
    rs_sent(0, 1)
    zag_done(2, 0)
    feed(0)
    zag_fwd(2, 1, 2)
    spread(0, pa, dgu, wu, 256)
    rs_step(2, 0, 0)
    zag_done(2, 1)
    spread(0, pb, act, wd, 512)
    rs_step(2, 0, 1)
    feed(1)
    rs_step(2, 0, 2)
    spread(1, pa, dgu, wu, 256)
    rs_step(2, 1, 0)
    rs_final(2, 0)
    gain2 = norm2_back(0)
    zag_start(3, 0)
    rs_step(1, 0, 0)
    spread(1, pb, act, wd, 512)
    rs_step(2, 1, 1)
    zag_fwd(3, 0, 1)
    g_compute(0)
    rs_step(2, 1, 2)
    zag_fwd(3, 0, 2)
    rs_step(1, 1, 0)
    rs_final(2, 1)
    gain2 = gain2 + norm2_back(1)
    for j in range(4):
        gsum[4 + j : 5 + j, :] = gain2[:, j * pair : (j + 1) * pair]
    zag_start(3, 1)
    g_first(0)
    g_compute(1)
    rs_step(1, 0, 1)
    zag_fwd(3, 1, 1)
    zag_done(3, 0)
    grad_heads(0)
    rs_step(1, 0, 2)
    rs_step(1, 1, 1)
    zag_fwd(3, 1, 2)
    rs_step(1, 1, 2)
    g_second(0)
    g_first(1)
    rs_final(1, 0)
    finish_out(0)
    rs_final(1, 1)
    finish_out(1)
    rs_sent(1, 0)
    rs_sent(1, 1)
    g_finish(0)
    g_compute(2)
    attend_back(0)
    spread(0, pb, act, wi, 512)
    rs_step(3, 0, 0)
    g_second(1)
    g_first(2)
    zag_done(3, 1)
    grad_heads(1)
    rs_step(3, 0, 1)
    attend_back(1)
    rs_step(3, 0, 2)
    spread(1, pb, act, wi, 512)
    rs_step(3, 1, 0)
    g_finish(1)
    g_second(2)
    g_compute(3)
    rs_step(3, 1, 1)
    g_first(3)
    g_finish(2)
    g_compute(4)
    rs_step(3, 1, 2)
    g_first(4)
    g_second(3)
    rs_final(3, 0)
    gain1 = norm1_back(0)
    g_second(4)
    g_finish(3)
    rs_final(3, 1)
    gain1 = gain1 + norm1_back(1)
    for j in range(4):
        gsum[j : j + 1, :] = gain1[:, j * pair : (j + 1) * pair]

    def e_copy(i, dev, src):
        return rcopy(src, gex.at[i], esend.at[i], erecv.at[i], dev)

    for step in (1, 2, 3):
        e_copy(step - 1, {"tensor": (z + step) % 4}, gsum).start()
    for step in (1, 2, 3):
        e_copy(step - 1, {"tensor": (z + step) % 4}, gsum).wait()
    gsum2 = gsum[...] + gex[0] + gex[1] + gex[2]
    gex[6] = gsum2
    e_copy(3, {"dp": pp}, gex.at[6]).start()
    g_finish(4)
    e_copy(3, {"dp": pp}, gex.at[6]).wait()
    gex[7] = gex[6] + gex[3]
    e_copy(4, {"dp": aa}, gex.at[7]).start()
    e_copy(4, {"dp": aa}, gex.at[7]).wait()
    gex[8] = gex[7] + gex[4]
    e_copy(5, {"dp": bb}, gex.at[8]).start()
    e_copy(5, {"dp": bb}, gex.at[8]).wait()
    gsum[...] = gex[8] + gex[5]
    last = pltpu.make_async_copy(gsum, ggain_h, osem.at[9])
    last.start()
    for u in range(5):
        w_sent(u)
    for u in (2, 3):
        for s in (0, 1):
            zag_sent(u, s)
    for u in (2, 3):
        for s in (0, 1):
            rs_sent(u, s)
    g_out(3).wait()
    g_out(4).wait()
    for s in (0, 1):
        pltpu.make_async_copy(ybuf.at[s], out_h.at[s], osem.at[5 + s]).wait()
        pltpu.make_async_copy(dh.at[pl.ds(s * rows, rows)], gtok_h.at[s], osem.at[7 + s]).wait()
    last.wait()


def pad_heads(weight):
    depth = weight.shape[0]
    halves = weight.reshape(depth, -1, 2, HEAD // 2)
    return jnp.pad(halves, ((0, 0), (0, 0), (0, 0), (0, 64 - HEAD // 2))).reshape(depth, -1)


def cut_heads(grad):
    depth = grad.shape[0]
    return grad.reshape(depth, -1, 2, 64)[..., : HEAD // 2].reshape(depth, -1)


def fused(
    tokens,
    cotangent,
    order,
    lengths,
    gain_attn,
    w_query,
    w_key,
    w_value,
    w_out,
    gain_ffn,
    w_gate,
    w_up,
    w_down,
):
    micro, rows, width = tokens.shape
    seq = rows * lax.axis_size("tensor")
    shard = w_query.shape[0]
    ff = w_gate.shape[1]
    groups = w_key.shape[1] // HEAD
    w_in = pad_heads(jnp.concatenate([w_query, w_key, w_value], axis=1))
    qp = w_query.shape[1] // HEAD * LANES
    kp = groups * LANES
    inw = qp + 2 * kp
    w_back = pad_heads(w_out.T)
    gate_up = jnp.concatenate([w_gate, w_up], axis=1)
    gain = jnp.stack([gain_attn, gain_ffn], axis=0)
    low = jnp.pad(gain, ((0, 14), (0, shard)))
    high = jnp.pad(gain, ((0, 14), (shard, 0)))
    gain = jnp.where(lax.axis_index("dp") % 2 == 0, low, high)

    starts = jnp.cumsum(lengths, axis=1, dtype=jnp.int32) - lengths
    docs = jnp.sum((order[:, :, None] >= starts[:, None, 1:]).astype(jnp.int32), axis=2)
    onehot = docs[:, :, None] == jnp.arange(lengths.shape[1], dtype=jnp.int32)
    first = jnp.sum(jnp.where(onehot, starts[:, None, :], 0), axis=2)
    real = (docs < lengths.shape[1] - 1).astype(F32)
    cols = jnp.stack([order.astype(F32), first.astype(F32), real], axis=2)
    freqs = rope_base ** (-2.0 * jnp.arange(HEAD // 2, dtype=F32) / HEAD)
    angles = (order - first).astype(F32)[:, :, None] * freqs
    gap = ((0, 0), (0, 0), (0, 64 - HEAD // 2))
    cosine, sine = jnp.pad(jnp.cos(angles), gap), jnp.pad(jnp.sin(angles), gap)
    cosine = jnp.concatenate([cosine, cosine], axis=2)
    sine = jnp.concatenate([-sine, sine], axis=2)

    total = micro * seq
    vm = pltpu.VMEM
    dma = pltpu.SemaphoreType.DMA
    scratch = [
        vm((8 * 16, 2 * shard), BF),
        vm((width, inw), BF),
        vm((width, qp), BF),
        vm((width, 2 * ff), BF),
        vm((width, ff), BF),
        vm((total, width), BF),
        vm((total, width), BF),
        vm((total, width), BF),
        vm((total, width), BF),
        vm((total, inw), BF),
        vm((total, qp), BF),
        vm((total, qp), BF),
        vm((total, ff), BF),
        vm((total, 2 * ff), BF),
        vm((micro * qp // LANES, seq, seq), F32),
        vm((micro * rows, width), F32),
        vm((micro * rows, width), F32),
        vm((total, width), BF),
        vm((total, width), BF),
        vm((micro, 2, 3, rows, width), BF),
        vm((micro, 2, 3, rows, width), BF),
        vm((2, width, ff), BF),
        vm((2, width // 2, ff), BF),
        vm((2, shard, ff), BF),
        vm((2, 2, shard, ff), BF),
        vm((2, shard, ff), F32),
        vm((rows, width), F32),
        vm((16, width), F32),
        vm((8, width // 4), F32),
        vm((9, 8, width // 4), F32),
        vm((micro, rows, width), BF),
        vm((micro, rows, width), BF),
        dma((5, 7)),
        dma((5, 7)),
        dma((4, 2, 2, 3)),
        dma((4, 2, 2, 3)),
        dma((4, 2, 2, 3)),
        dma((4, 2, 2, 3)),
        dma((5, 7)),
        dma((5, 7)),
        dma((6,)),
        dma((6,)),
        dma((12,)),
        dma((10,)),
        pltpu.SemaphoreType.REGULAR((3,)),
        pltpu.SemaphoreType.REGULAR((2, 2)),
    ]
    hbm = pl.BlockSpec(memory_space=pl.ANY)
    vmem = pl.BlockSpec(memory_space=pltpu.VMEM)
    shapes = [
        jax.ShapeDtypeStruct((micro, rows, width), BF),
        jax.ShapeDtypeStruct((micro, rows, width), F32),
        jax.ShapeDtypeStruct((shard, ff), F32),
        jax.ShapeDtypeStruct((shard, ff), F32),
        jax.ShapeDtypeStruct((shard, ff), F32),
        jax.ShapeDtypeStruct((shard, qp), F32),
        jax.ShapeDtypeStruct((shard, inw), F32),
        jax.ShapeDtypeStruct((8, width // 4), F32),
    ]
    dims = (rows, seq, width, shard, qp, kp, ff, groups)
    out, gtok, gdown, ggate, gup, gout, gin, ggain = pl.pallas_call(
        functools.partial(block_kernel, dims),
        out_shape=shapes,
        in_specs=[hbm] * 7 + [vmem] * 4,
        out_specs=[hbm] * 8,
        scratch_shapes=scratch,
        compiler_params=pltpu.CompilerParams(
            collective_id=0, has_side_effects=True, vmem_limit_bytes=67_043_328
        ),
        name="block",
    )(
        tokens,
        cotangent,
        gain,
        w_in,
        w_back,
        gate_up,
        w_down.T,
        order.astype(F32)[:, None, :],
        cols,
        cosine,
        sine,
    )
    gains = ggain.reshape(2, width)
    gain_own = lax.dynamic_slice_in_dim(gains, lax.axis_index("dp") * shard, shard, 1)
    grads_in = cut_heads(gin)
    q_cols, k_cols = w_query.shape[1], w_key.shape[1]
    return (
        out,
        gtok,
        gain_own[0],
        grads_in[:, :q_cols],
        grads_in[:, q_cols : q_cols + k_cols],
        grads_in[:, q_cols + k_cols :],
        cut_heads(gout).T,
        gain_own[1],
        ggate,
        gup,
        gdown.T,
    )


def local(tokens, *rest):
    fits = lax.axis_size("dp") == 8 and lax.axis_size("tensor") == 4 and tokens.shape[0] == 2
    return (fused if fits else spread_out)(tokens, *rest)


def solution(mesh):
    return jax.shard_map(
        local,
        mesh=mesh,
        in_specs=(
            P("dp", "tensor", None),
            P("dp", "tensor", None),
            P("dp", None),
            P("dp", None),
            P("dp"),
            P("dp", "tensor"),
            P("dp", "tensor"),
            P("dp", "tensor"),
            P("tensor", "dp"),
            P("dp"),
            P("dp", "tensor"),
            P("dp", "tensor"),
            P("tensor", "dp"),
        ),
        out_specs=(
            P("dp", "tensor", None),
            P("dp", "tensor", None),
            P("dp"),
            P("dp", "tensor"),
            P("dp", "tensor"),
            P("dp", "tensor"),
            P("tensor", "dp"),
            P("dp"),
            P("dp", "tensor"),
            P("dp", "tensor"),
            P("tensor", "dp"),
        ),
        check_vma=False,
    )
```

```python
import functools

import jax
import jax.numpy as jnp
from jax import lax
from jax.experimental import pallas as pl
from jax.experimental.pallas import tpu as pltpu
from jax.sharding import PartitionSpec as P

HEAD = 96


eps = 1e-05
rope_base = 100000.0


def rotate(field, cosine, sine):
    half = field.shape[-1] // 2
    first = field[..., :half]
    second = field[..., half:]
    return jnp.concatenate(
        [first * cosine - second * sine, second * cosine + first * sine], axis=-1
    )


def rotate_back(field, cosine, sine):
    half = field.shape[-1] // 2
    first = field[..., :half]
    second = field[..., half:]
    return jnp.concatenate(
        [first * cosine + second * sine, second * cosine - first * sine], axis=-1
    )


def layout(order, lengths):
    starts = jnp.cumsum(lengths, dtype=jnp.int32) - lengths
    docs = jnp.sum((order[:, None] >= starts[None, 1:]).astype(jnp.int32), axis=1, dtype=jnp.int32)
    onehot = docs[:, None] == jnp.arange(lengths.shape[0], dtype=jnp.int32)[None, :]
    first = jnp.sum(jnp.where(onehot, starts[None, :], 0), axis=1, dtype=jnp.int32)
    positions = (order - first).astype(jnp.float32)
    mask = (docs[:, None] == docs[None, :]) & (order[None, :] <= order[:, None])
    real = (docs < lengths.shape[0] - 1).astype(jnp.float32)
    return (positions, mask, real)


def norm_forward(rows, gain):
    scale = lax.rsqrt(jnp.mean(rows * rows, axis=-1, keepdims=True) + eps)
    unit = rows * scale
    return (unit, scale, (unit * gain).astype(jnp.bfloat16))


def norm_backward(grad, unit, scale, gain):
    inner = grad * gain
    return scale * (inner - unit * jnp.mean(inner * unit, axis=-1, keepdims=True))


def contract_rows(left, right):
    return lax.dot_general(
        left, right, (((0,), (0,)), ((), ())), preferred_element_type=jnp.float32
    )


def times_transpose(left, right):
    return lax.dot_general(
        left, right, (((1,), (1,)), ((), ())), preferred_element_type=jnp.float32
    )


def gather_weights(gain_attn, w_query, w_key, w_value, w_out, gain_ffn, w_gate, w_up, w_down):
    gains = lax.all_gather(jnp.stack([gain_attn, gain_ffn], axis=0), "dp", axis=1, tiled=True)
    attn = lax.all_gather(
        jnp.concatenate([w_query, w_key, w_value, w_out.T], axis=1), "dp", axis=0, tiled=True
    )
    gate_up = lax.all_gather(jnp.concatenate([w_gate, w_up], axis=1), "dp", axis=0, tiled=True)
    down = lax.all_gather(w_down.T, "dp", axis=0, tiled=True)
    return gains, attn, gate_up, down


def gather_rows(rows):
    return lax.all_gather(rows, "tensor", axis=1, tiled=True)


def scatter_rows(partial):
    low = partial.astype(jnp.bfloat16)
    return lax.psum_scatter(low, "tensor", scatter_dimension=1, tiled=True).astype(jnp.float32)


def reduce_weights(term):
    low = term.astype(jnp.bfloat16)
    return lax.psum_scatter(low, "dp", scatter_dimension=0, tiled=True).astype(jnp.float32)


def spread_out(
    tokens,
    cotangent,
    order,
    lengths,
    gain_attn,
    w_query,
    w_key,
    w_value,
    w_out,
    gain_ffn,
    w_gate,
    w_up,
    w_down,
):
    micro, rows, width = tokens.shape
    seq = rows * lax.axis_size("tensor")
    q_cols, k_cols, ff_cols = w_query.shape[1], w_key.shape[1], w_gate.shape[1]
    local_heads, local_kv = q_cols // HEAD, k_cols // HEAD
    group = local_heads // local_kv
    first_row = lax.axis_index("tensor") * rows
    freqs = rope_base ** (-2.0 * jnp.arange(HEAD // 2, dtype=jnp.float32) / HEAD)
    head_scale = HEAD ** (-0.5)

    gains, attn, gate_up, down = gather_weights(
        gain_attn, w_query, w_key, w_value, w_out, gain_ffn, w_gate, w_up, w_down
    )
    gain1, gain2 = gains[0].astype(jnp.float32), gains[1].astype(jnp.float32)
    in_cols = q_cols + 2 * k_cols
    w_in, w_out_t = attn[:, :in_cols], attn[:, in_cols:]

    positions, mask, real = jax.vmap(layout)(order, lengths)
    angles = positions[:, :, None] * freqs
    cosine, sine = jnp.cos(angles)[:, :, None, :], jnp.sin(angles)[:, :, None, :]
    mask = mask[:, None, None]
    real_rows = lax.dynamic_slice_in_dim(real, first_row, rows, 1)[:, :, None]

    stream = tokens.astype(jnp.float32)
    unit1, scale1, normed1 = norm_forward(stream, gain1)
    full1 = gather_rows(normed1)
    grad_out_rows = cotangent.astype(jnp.float32) * real_rows
    full_grad = gather_rows(grad_out_rows.astype(jnp.bfloat16))
    flat1 = full1.reshape(micro * seq, width)
    flat_grad = full_grad.reshape(micro * seq, width)

    mixed_in = jnp.dot(flat1, w_in, preferred_element_type=jnp.float32).reshape(micro, seq, in_cols)
    query = mixed_in[..., :q_cols].reshape(micro, seq, local_heads, HEAD)
    keys = mixed_in[..., q_cols : q_cols + k_cols].reshape(micro, seq, local_kv, HEAD)
    values = mixed_in[..., q_cols + k_cols :].reshape(micro, seq, local_kv, HEAD).astype(jnp.bfloat16)
    query = (rotate(query, cosine, sine) * head_scale).astype(jnp.bfloat16)
    query = query.reshape(micro, seq, local_kv, group, HEAD)
    keys = rotate(keys, cosine, sine).astype(jnp.bfloat16)
    scores = jnp.einsum("bqkgd,bskd->bkgqs", query, keys, preferred_element_type=jnp.float32)
    scores = jnp.where(mask, scores, -1e30)
    peak = jnp.max(scores, axis=-1, keepdims=True)
    expon = jnp.exp(scores - peak)
    total = jnp.sum(expon, axis=-1, keepdims=True)
    probs = expon / total
    probs_low = probs.astype(jnp.bfloat16)
    mixed = jnp.einsum("bkgqs,bskd->bqkgd", probs_low, values, preferred_element_type=jnp.float32)
    mixed = mixed.reshape(micro * seq, q_cols).astype(jnp.bfloat16)
    branch = scatter_rows(times_transpose(mixed, w_out_t).reshape(micro, seq, width))
    resid = stream + branch
    unit2, scale2, normed2 = norm_forward(resid, gain2)
    full2 = gather_rows(normed2).reshape(micro * seq, width)

    both = jnp.dot(full2, gate_up, preferred_element_type=jnp.float32)
    gate, upper = both[:, :ff_cols], both[:, ff_cols:]
    sigma = jax.nn.sigmoid(gate)
    hidden = (gate * sigma * upper).astype(jnp.bfloat16)
    ffn = scatter_rows(times_transpose(hidden, down).reshape(micro, seq, width))
    output = ((resid + ffn) * real_rows).astype(jnp.bfloat16)

    grad_hidden = jnp.dot(flat_grad, down, preferred_element_type=jnp.float32)
    grad_gate = (grad_hidden * upper * sigma * (1.0 + gate * (1.0 - sigma))).astype(jnp.bfloat16)
    grad_up = (grad_hidden * gate * sigma).astype(jnp.bfloat16)
    grad_both = jnp.concatenate([grad_gate, grad_up], axis=1)
    grad_norm2 = scatter_rows(times_transpose(grad_both, gate_up).reshape(micro, seq, width))
    final_down = reduce_weights(contract_rows(flat_grad, hidden))
    final_gate = reduce_weights(contract_rows(full2, grad_gate))
    final_up = reduce_weights(contract_rows(full2, grad_up))
    term_gain2 = jnp.sum(grad_norm2 * unit2, axis=(0, 1))
    grad_resid = grad_out_rows + norm_backward(grad_norm2, unit2, scale2, gain2)

    full_resid = gather_rows(grad_resid.astype(jnp.bfloat16)).reshape(micro * seq, width)
    grad_mixed = jnp.dot(full_resid, w_out_t, preferred_element_type=jnp.float32).astype(jnp.bfloat16)
    final_out = reduce_weights(contract_rows(full_resid, mixed))
    grad_heads = grad_mixed.reshape(micro, seq, local_kv, group, HEAD)
    grad_probs = jnp.einsum(
        "bqkgd,bskd->bkgqs", grad_heads, values, preferred_element_type=jnp.float32
    )
    grad_values = jnp.einsum(
        "bkgqs,bqkgd->bskd", probs_low, grad_heads, preferred_element_type=jnp.float32
    )
    grad_scores = (
        probs * (grad_probs - jnp.sum(probs * grad_probs, axis=-1, keepdims=True))
    ).astype(jnp.bfloat16)
    grad_query = jnp.einsum(
        "bkgqs,bskd->bqkgd", grad_scores, keys, preferred_element_type=jnp.float32
    ).reshape(micro, seq, local_heads, HEAD)
    grad_keys = jnp.einsum(
        "bkgqs,bqkgd->bskd", grad_scores, query, preferred_element_type=jnp.float32
    )
    grad_query = rotate_back(grad_query * head_scale, cosine, sine).reshape(micro * seq, q_cols)
    grad_keys = rotate_back(grad_keys, cosine, sine).reshape(micro * seq, k_cols)
    grad_values = grad_values.reshape(micro * seq, k_cols)
    grad_in = jnp.concatenate(
        [grad_query.astype(jnp.bfloat16), grad_keys.astype(jnp.bfloat16), grad_values.astype(jnp.bfloat16)],
        axis=1,
    )
    grad_norm1 = scatter_rows(times_transpose(grad_in, w_in).reshape(micro, seq, width))
    final_in = reduce_weights(contract_rows(flat1, grad_in))
    term_gain1 = jnp.sum(grad_norm1 * unit1, axis=(0, 1))
    grad_tokens = grad_resid + norm_backward(grad_norm1, unit1, scale1, gain1)

    gain_terms = lax.psum(jnp.stack([term_gain1, term_gain2], axis=0), ("dp", "tensor"))
    own = gain_attn.shape[0]
    gain_own = lax.dynamic_slice_in_dim(gain_terms, lax.axis_index("dp") * own, own, 1)
    return (
        output,
        grad_tokens,
        gain_own[0],
        final_in[:, :q_cols],
        final_in[:, q_cols : q_cols + k_cols],
        final_in[:, q_cols + k_cols :],
        final_out.T,
        gain_own[1],
        final_gate,
        final_up,
        final_down.T,
    )


BF = jnp.bfloat16
F32 = jnp.float32
MESH = pl.DeviceIdType.MESH
LANES = 128


def nn(left, right):
    return lax.dot_general(left, right, (((1,), (0,)), ((), ())), preferred_element_type=F32)


def nt(left, right):
    return lax.dot_general(left, right, (((1,), (1,)), ((), ())), preferred_element_type=F32)


def tn(left, right):
    return lax.dot_general(left, right, (((0,), (0,)), ((), ())), preferred_element_type=F32)


def al(value, unit):
    return pl.multiple_of(value, unit)


def block_kernel(dims, *refs):
    (rows, seq, width, shard, qp, kp, ff, groups) = dims
    (tok, cot, wg_h, wi_h, wo_h, wu_h, wd_h, ordr, cols, cosr, sinr) = refs[:11]
    (out_h, gtok_h, gdown_h, ggate_h, gup_h, gout_h, gin_h, ggain_h) = refs[11:19]
    (wgn, wi, wo, wu, wd, xf, n1, n2, gf, qkv, ob, dob, act, dq3, dgu, pr, hb, dh, pa, pb, ra, rb,
     gb, xb, hop, fin, stage, acc, gains, gsum, gex, ybuf, tbuf,
     wsend, wrecv, zsend, zrecv, rsend, rrecv, gsend, grecv, esend, erecv, lsem, osem, credit) = refs[19:]
    ghf = xf
    heads = qp // LANES
    per_group = heads // groups
    inw = qp + 2 * kp
    d = lax.axis_index("dp")
    z = lax.axis_index("tensor")
    c = d % 2
    flip = 1 - 2 * c
    near_x = d + 2 - 4 * ((d // 2) % 2)
    near_y = d + 4 - 8 * (d // 4)
    aa = near_x * (1 - c) + near_y * c
    bb = near_y * (1 - c) + near_x * c
    dd = aa + bb - d
    pp = d + flip
    chip_own, chip_a, chip_b, chip_d = d // 2, aa // 2, bb // 2, dd // 2
    chip_x, chip_y = near_x // 2, near_y // 2
    own = 1 * z * rows
    zdev = {"tensor": z + 1}, {"tensor": z - 1}

    def rcopy(src, dst, ssem, rsem, dev):
        return pltpu.make_async_remote_copy(
            src_ref=src, dst_ref=dst, send_sem=ssem, recv_sem=rsem, device_id=dev, device_id_type=MESH
        )

    barrier = pltpu.get_barrier_semaphore()
    for step in range(1, 8):
        pl.semaphore_signal(barrier, inc=1, device_id={"dp": (d + step) % 8}, device_id_type=MESH)
    for step in (1, 2, 3):
        pl.semaphore_signal(
            barrier, inc=1, device_id={"tensor": (z + step) % 4}, device_id_type=MESH
        )
    pl.semaphore_wait(barrier, 10)

    wunits = ((wg_h, wgn, 16), (wi_h, wi, shard), (wo_h, wo, shard), (wu_h, wu, shard), (wd_h, wd, shard))

    def wblk(u, i):
        n = wunits[u][2]
        return wunits[u][1].at[pl.ds(al(n * i, 16), n)]

    def w_start(u):
        src = wunits[u][0]
        pltpu.make_async_copy(src, wblk(u, d), lsem.at[u]).start()
        rcopy(src, wblk(u, d), wsend.at[u, 0], wrecv.at[u, 0], {"dp": aa}).start()
        rcopy(src, wblk(u, d), wsend.at[u, 1], wrecv.at[u, 1], {"dp": bb}).start()
        rcopy(src, wblk(u, d), wsend.at[u, 2], wrecv.at[u, 3], {"dp": pp}).start()

    def w_wait(u, slot, i):
        rcopy(wblk(u, i), wblk(u, i), wsend.at[u, 0], wrecv.at[u, slot], {"dp": aa}).wait_recv()

    def w_relay(u):
        w_wait(u, 1, bb)
        rcopy(wblk(u, bb), wblk(u, bb), wsend.at[u, 3], wrecv.at[u, 2], {"dp": aa}).start()
        rcopy(wblk(u, bb), wblk(u, bb), wsend.at[u, 4], wrecv.at[u, 5], {"dp": pp}).start()
        w_wait(u, 0, aa)
        rcopy(wblk(u, aa), wblk(u, aa), wsend.at[u, 5], wrecv.at[u, 4], {"dp": pp}).start()

    def w_diag(u):
        w_wait(u, 2, dd)
        rcopy(wblk(u, dd), wblk(u, dd), wsend.at[u, 6], wrecv.at[u, 6], {"dp": pp}).start()

    def w_done(u):
        w_wait(u, 3, pp)
        w_wait(u, 4, bb + flip)
        w_wait(u, 5, aa + flip)
        w_wait(u, 6, dd + flip)
        pltpu.make_async_copy(wunits[u][0], wblk(u, d), lsem.at[u]).wait()

    def w_sent(u):
        for slot in range(7):
            rcopy(wblk(u, d), wblk(u, d), wsend.at[u, slot], wrecv.at[u, 0], {"dp": aa}).wait_send()

    zfull = (xf, gf, n2, ghf)
    zhbm = (tok, cot, None, None)

    def zblk(u, s, i):
        return zfull[u].at[pl.ds(al(s * seq + i * rows, 16), rows)]

    def zag_send(u, s, k, way):
        i = z - k if way == 0 else z + k
        go = (z < 3) & (i >= 0) if way == 0 else (z > 0) & (i <= 3)

        @pl.when(go)
        def _():
            src = zhbm[u].at[s] if k == 0 and zhbm[u] is not None else zblk(u, s, i)
            rcopy(src, zblk(u, s, i), zsend.at[u, s, way, k], zrecv.at[u, s, way, k], zdev[way]).start()

    def zag_recv(u, s, k, way):
        i = z - 1 - k if way == 0 else z + 1 + k
        go = (i >= 0) if way == 0 else (i <= 3)

        @pl.when(go)
        def _():
            rcopy(
                zblk(u, s, i), zblk(u, s, i), zsend.at[u, s, way, k], zrecv.at[u, s, way, k], zdev[way]
            ).wait_recv()

    def zag_start(u, s):
        if zhbm[u] is not None:
            pltpu.make_async_copy(zhbm[u].at[s], zblk(u, s, z), lsem.at[8 + 2 * u + s]).start()
        for way in (0, 1):
            zag_send(u, s, 0, way)

    def zag_fwd(u, s, k):
        for way in (0, 1):
            zag_recv(u, s, k - 1, way)
            zag_send(u, s, k, way)

    def zag_done(u, s):
        for way in (0, 1):
            zag_recv(u, s, 2, way)
        if zhbm[u] is not None:
            pltpu.make_async_copy(zhbm[u].at[s], zblk(u, s, z), lsem.at[8 + 2 * u + s]).wait()

    def ag(u, s, t):
        if t == 0:
            zag_start(u, s)
        elif t < 3:
            zag_fwd(u, s, t)
        else:
            zag_done(u, s)

    def zag_sent(u, s):
        for k in range(3):
            for way in (0, 1):
                i = z - k if way == 0 else z + k
                go = (z < 3) & (i >= 0) if way == 0 else (z > 0) & (i <= 3)

                @pl.when(go)
                def _():
                    rcopy(
                        zblk(u, s, i), zblk(u, s, i), zsend.at[u, s, way, k], zrecv.at[u, s, way, k], zdev[way]
                    ).wait_send()

    zpart = (pa, pb, pa, pa)
    zgot = (ra, rb, ra, ra)

    def rs_copy(u, s, way, t, dest):
        return rcopy(
            zpart[u].at[pl.ds(al(s * seq + dest * rows, 16), rows)],
            zgot[u].at[s, way, t],
            rsend.at[u, s, way, t],
            rrecv.at[u, s, way, t],
            zdev[way],
        )

    def rs(u, s, t):
        for way in (0, 1):
            from_end = z if way == 0 else 3 - z

            def wait_and(target, base):
                rs_copy(u, s, way, t - 1, z).wait_recv()

                def body(i, carry):
                    at = pl.ds(al(base + i * 16, 16), 16)
                    got = zgot[u][s, way, t - 1, pl.ds(al(i * 16, 16), 16), :].astype(F32)
                    target[at, :] = (target[at, :].astype(F32) + got).astype(target.dtype)
                    return carry

                lax.fori_loop(0, rows // 16, body, 0)

            if t == 3:
                if way == 0:
                    def first(i, carry):
                        at = pl.ds(al(i * 16, 16), 16)
                        acc[at, :] = zpart[u][pl.ds(al(s * seq + own + i * 16, 16), 16), :].astype(F32)
                        return carry

                    lax.fori_loop(0, rows // 16, first, 0)

                @pl.when(from_end > 0)
                def _():
                    wait_and(acc, 0)
            else:
                dest = 3 + z - t if way == 0 else t - from_end

                @pl.when(from_end <= t)
                def _():
                    if t > 0:
                        @pl.when(from_end > 0)
                        def _():
                            wait_and(zpart[u], s * seq + dest * rows)

                    rs_copy(u, s, way, t, dest).start()

    def rs_sent(u, s):
        for way in (0, 1):
            from_end = z if way == 0 else 3 - z
            for t in range(3):
                @pl.when(from_end <= t)
                def _():
                    rs_copy(u, s, way, t, z).wait_send()

    gunits = (
        (gf, act, 0, ff, gdown_h),
        (n2, dgu, 0, ff, ggate_h),
        (n2, dgu, ff, ff, gup_h),
        (ghf, ob, 0, qp, gout_h),
        (n1, dq3, 0, inw, gin_h),
    )
    pair = 2 * shard

    def xslot(u, chip):
        b, n = u % 2, gunits[u][3]
        return xb.at[b, pl.ds(al(chip * shard, 16), shard), pl.ds(0, n)]

    def gslot(u, chip, core):
        b, n = u % 2, gunits[u][3]
        return gb.at[b, pl.ds(al(chip * pair + core * shard, 16), shard), pl.ds(0, n)]

    def g_exchange(u, chip, i):
        return rcopy(gslot(u, chip, 1 - c), xslot(u, chip), gsend.at[u, i], grecv.at[u, i], {"dp": pp})

    chips = (chip_d, chip_x, chip_y, chip_own)

    def g_compute(u):
        left, right, at, n, _ = gunits[u]
        if u >= 2:
            pl.semaphore_wait(credit.at[0], 1)
        for i, chip in enumerate(chips):
            tile = 256

            def body(j, carry):
                lhs = left[:, pl.ds(al(chip * pair, LANES), pair)]
                got = tn(lhs, right[:, pl.ds(al(at + j * tile, tile), tile)])
                gb[u % 2, pl.ds(al(chip * pair, 16), pair), pl.ds(al(j * tile, tile), tile)] = got.astype(BF)
                return carry

            lax.fori_loop(0, n // tile, body, 0)
            g_exchange(u, chip, i).start()

    def g_add(u, chip, extra=None):
        b, n = u % 2, gunits[u][3]

        def body(i, carry):
            at = pl.ds(al(chip * shard + i * 16, 16), 16)
            mine = gb[b, pl.ds(al(chip * pair + c * shard + i * 16, 16), 16), pl.ds(0, n)].astype(F32)
            total = mine + xb[b, at, pl.ds(0, n)].astype(F32)
            if extra is not None:
                total = total + extra[b, pl.ds(al(i * 16, 16), 16), pl.ds(0, n)].astype(F32)
            xb[b, at, pl.ds(0, n)] = total.astype(BF)
            return carry

        lax.fori_loop(0, shard // 16, body, 0)

    def g_hop(u):
        b, n = u % 2, gunits[u][3]
        return rcopy(xslot(u, chip_d), hop.at[b, :, pl.ds(0, n)], gsend.at[u, 4], grecv.at[u, 4], {"dp": aa})

    def g_last(u, way):
        b, n = u % 2, gunits[u][3]
        chip, dev = (chip_a, aa) if way == 0 else (chip_b, bb)
        return rcopy(
            xslot(u, chip), fin.at[b, way, :, pl.ds(0, n)], gsend.at[u, 5 + way], grecv.at[u, 5 + way], {"dp": dev}
        )

    def g_first(u):
        g_exchange(u, chip_d, 0).wait_recv()
        g_add(u, chip_d)
        if u >= 2:
            pl.semaphore_wait(credit.at[1], 1)
        g_hop(u).start()
        g_exchange(u, chip_x, 1).wait_recv()
        g_exchange(u, chip_y, 2).wait_recv()
        g_add(u, chip_a)
        g_last(u, 0).start()

    def g_second(u):
        g_hop(u).wait_recv()
        g_add(u, chip_b, hop)
        if u >= 2:
            pl.semaphore_wait(credit.at[2], 1)
        g_last(u, 1).start()

    def g_finish(u):
        b, n, out = u % 2, gunits[u][3], gunits[u][4]
        g_exchange(u, chip_own, 3).wait_recv()
        g_last(u, 0).wait_recv()
        g_last(u, 1).wait_recv()

        def body(i, carry):
            at = pl.ds(al(i * 16, 16), 16)
            total = gb[b, pl.ds(al(chip_own * pair + c * shard + i * 16, 16), 16), pl.ds(0, n)].astype(F32)
            total = total + xb[b, pl.ds(al(chip_own * shard + i * 16, 16), 16), pl.ds(0, n)].astype(F32)
            total = total + fin[b, 0, at, pl.ds(0, n)].astype(F32)
            stage[b, at, pl.ds(0, n)] = total + fin[b, 1, at, pl.ds(0, n)].astype(F32)
            return carry

        if u >= 2:
            g_out(u - 2).wait()
        lax.fori_loop(0, shard // 16, body, 0)
        g_out(u).start()
        for i in range(4):
            g_exchange(u, chips[i], i).wait_send()
        g_hop(u).wait_send()
        g_last(u, 0).wait_send()
        g_last(u, 1).wait_send()
        if u < 3:
            pl.semaphore_signal(credit.at[0], inc=1, device_id={"dp": pp}, device_id_type=MESH)
            pl.semaphore_signal(credit.at[1], inc=1, device_id={"dp": aa}, device_id_type=MESH)
            pl.semaphore_signal(credit.at[2], inc=1, device_id={"dp": bb}, device_id_type=MESH)

    def g_out(u):
        b, n, out = u % 2, gunits[u][3], gunits[u][4]
        return pltpu.make_async_copy(stage.at[b, :, pl.ds(0, n)], out, osem.at[u])

    def norm1(s):
        gain = gains[0:1, :]

        def body(i, carry):
            at = pl.ds(al(s * seq + i * 16, 16), 16)
            x = xf[at, :].astype(F32)
            scale = lax.rsqrt(jnp.mean(x * x, axis=-1, keepdims=True) + eps)
            n1[at, :] = (x * scale * gain).astype(BF)
            return carry

        lax.fori_loop(0, seq // 16, body, 0)

    head_scale = HEAD ** (-0.5)

    def project(s):
        at = pl.ds(s * seq, seq)
        cosine, sine = cosr[s], sinr[s]
        for j in range(inw // 256):
            both = nn(n1[at, :], wi[:, pl.ds(j * 256, 256)])
            for half in range(2):
                col = j * 256 + half * LANES
                part = both[:, half * LANES : (half + 1) * LANES]
                if col < qp + kp:
                    part = part * cosine + pltpu.roll(part, LANES // 2, 1) * sine
                if col < qp:
                    part = part * head_scale
                qkv[at, pl.ds(col, LANES)] = part.astype(BF)

    def attend(s):
        at = pl.ds(s * seq, seq)
        oc = ordr[s]
        mask = (oc <= cols[s, :, 0:1]) & (oc >= cols[s, :, 1:2])

        def body(h, carry):
            g = h // per_group
            q = qkv[at, pl.ds(al(h * LANES, LANES), LANES)]
            k = qkv[at, pl.ds(al(qp + g * LANES, LANES), LANES)]
            v = qkv[at, pl.ds(al(qp + kp + g * LANES, LANES), LANES)]
            sc = jnp.where(mask, nt(q, k), -1e30)
            e = jnp.exp(sc - jnp.max(sc, axis=-1, keepdims=True))
            p = e * (1.0 / jnp.sum(e, axis=-1, keepdims=True))
            pr[s * heads + h] = p
            ob[at, pl.ds(al(h * LANES, LANES), LANES)] = nn(p.astype(BF), v).astype(BF)
            return carry

        lax.fori_loop(0, heads, body, 0)

    def spread(s, dst, left, weight, tile):
        at = pl.ds(s * seq, seq)

        def body(j, carry):
            col = al(j * tile, tile)
            dst[at, pl.ds(col, tile)] = nt(left[at, :], weight[pl.ds(col, tile), :]).astype(BF)
            return carry

        lax.fori_loop(0, width // tile, body, 0)

    def norm2(s):
        gain = gains[1:2, :]
        base = s * rows

        def body(i, carry):
            r = pl.ds(al(i * 16, 16), 16)
            h = tbuf[s, r, :].astype(F32) + acc[r, :]
            hb[pl.ds(al(base + i * 16, 16), 16), :] = h
            scale = lax.rsqrt(jnp.mean(h * h, axis=-1, keepdims=True) + eps)
            n2[pl.ds(al(s * seq + own + i * 16, 16), 16), :] = (h * scale * gain).astype(BF)
            return carry

        lax.fori_loop(0, rows // 16, body, 0)

    def mask_grad(s):
        def body(i, carry):
            at = pl.ds(al(s * seq + i * 16, 16), 16)
            gf[at, :] = (gf[at, :].astype(F32) * cols[s, pl.ds(al(i * 16, 16), 16), 2:3]).astype(BF)
            return carry

        lax.fori_loop(0, seq // 16, body, 0)

    def feed(s):
        at = pl.ds(s * seq, seq)

        def body(t, carry):
            col = al(t * 256, 256)
            gate = nn(n2[at, :], wu[:, pl.ds(col, 256)])
            upper = nn(n2[at, :], wu[:, pl.ds(al(ff + t * 256, 256), 256)])
            back = nn(gf[at, :], wd[:, pl.ds(col, 256)])
            sigma = 1.0 / (1.0 + jnp.exp(-gate))
            swish = gate * sigma
            act[at, pl.ds(col, 256)] = (swish * upper).astype(BF)
            dgu[at, pl.ds(col, 256)] = (back * upper * sigma * (1.0 + gate * (1.0 - sigma))).astype(BF)
            dgu[at, pl.ds(al(ff + t * 256, 256), 256)] = (back * swish).astype(BF)
            return carry

        lax.fori_loop(0, ff // 256, body, 0)

    def finish_out(s):
        def body(i, carry):
            r = pl.ds(al(i * 16, 16), 16)
            real = cols[s, pl.ds(al(own + i * 16, 16), 16), 2:3]
            y = (hb[pl.ds(al(s * rows + i * 16, 16), 16), :] + acc[r, :]) * real
            ybuf[s, r, :] = y.astype(BF)
            return carry

        lax.fori_loop(0, rows // 16, body, 0)
        pltpu.make_async_copy(ybuf.at[s], out_h.at[s], osem.at[5 + s]).start()

    def norm2_back(s):
        gain = gains[1:2, :]

        def body(i, carry):
            r = pl.ds(al(i * 16, 16), 16)
            ro = pl.ds(al(s * rows + i * 16, 16), 16)
            h = hb[ro, :]
            scale = lax.rsqrt(jnp.mean(h * h, axis=-1, keepdims=True) + eps)
            unit = h * scale
            grad = acc[r, :]
            inner = grad * gain
            dy = gf[pl.ds(al(s * seq + own + i * 16, 16), 16), :].astype(F32)
            dhr = dy + scale * (inner - unit * jnp.mean(inner * unit, axis=-1, keepdims=True))
            dh[ro, :] = dhr
            ghf[pl.ds(al(s * seq + own + i * 16, 16), 16), :] = dhr.astype(BF)
            return carry + jnp.sum(grad * unit, axis=0, keepdims=True)

        return lax.fori_loop(0, rows // 16, body, jnp.zeros((1, width), F32))

    def grad_heads(s):
        at = pl.ds(s * seq, seq)
        for j in range(qp // 256):
            dob[at, pl.ds(j * 256, 256)] = nn(ghf[at, :], wo[:, pl.ds(j * 256, 256)]).astype(BF)

    def attend_back(s):
        at = pl.ds(s * seq, seq)
        cosine, sine = cosr[s], sinr[s]

        def body(g, carry):
            k = qkv[at, pl.ds(al(qp + g * LANES, LANES), LANES)]
            v = qkv[at, pl.ds(al(qp + kp + g * LANES, LANES), LANES)]
            dk = jnp.zeros((seq, LANES), F32)
            dv = jnp.zeros((seq, LANES), F32)
            for m in range(per_group):
                h = g * per_group + m
                hat = pl.ds(al(h * LANES, LANES), LANES)
                q = qkv[at, hat]
                do = dob[at, hat]
                p = pr[s * heads + h]
                dp = nt(do, v)
                ds = (p * (dp - jnp.sum(p * dp, axis=-1, keepdims=True))).astype(BF)
                dv = dv + tn(p.astype(BF), do)
                dk = dk + tn(ds, q)
                dq = nn(ds, k) * head_scale
                dq3[at, hat] = (dq * cosine - pltpu.roll(dq, LANES // 2, 1) * sine).astype(BF)
            dq3[at, pl.ds(al(qp + g * LANES, LANES), LANES)] = (
                dk * cosine - pltpu.roll(dk, LANES // 2, 1) * sine
            ).astype(BF)
            dq3[at, pl.ds(al(qp + kp + g * LANES, LANES), LANES)] = dv.astype(BF)
            return carry

        lax.fori_loop(0, groups, body, 0)

    def norm1_back(s):
        gain = gains[0:1, :]

        def body(i, carry):
            r = pl.ds(al(i * 16, 16), 16)
            ro = pl.ds(al(s * rows + i * 16, 16), 16)
            x = tbuf[s, r, :].astype(F32)
            scale = lax.rsqrt(jnp.mean(x * x, axis=-1, keepdims=True) + eps)
            unit = x * scale
            grad = acc[r, :]
            inner = grad * gain
            dh[ro, :] = dh[ro, :] + scale * (inner - unit * jnp.mean(inner * unit, axis=-1, keepdims=True))
            return carry + jnp.sum(grad * unit, axis=0, keepdims=True)

        total = lax.fori_loop(0, rows // 16, body, jnp.zeros((1, width), F32))
        pltpu.make_async_copy(
            dh.at[pl.ds(s * rows, rows)], gtok_h.at[s], osem.at[7 + s]
        ).start()
        return total

    X, COT, N2, GH = 0, 1, 2, 3
    BR, FFN, DN2, DN1 = 0, 1, 2, 3

    def attn_grad(s):
        grad_heads(s)
        attend_back(s)
        rs_sent(DN2, s)
        spread(s, pa, dq3, wi, 512)

    for s in (0, 1):
        pltpu.make_async_copy(tok.at[s], tbuf.at[s], lsem.at[5 + s]).start()
    w_start(0)
    ag(X, 0, 0)
    w_start(1)
    ag(X, 0, 1)
    w_relay(0)
    w_diag(0)
    ag(X, 0, 2)
    ag(X, 1, 0)
    w_relay(1)
    w_start(2)
    w_done(0)
    for j in range(4):
        at = pl.ds(j * pair, pair)
        gains[:, at] = (
            wgn[pl.ds(32 * j, 16), :].astype(F32) + wgn[pl.ds(32 * j + 16, 16), :].astype(F32)
        )
    ag(X, 0, 3)
    norm1(0)
    ag(X, 1, 1)
    w_diag(1)
    w_relay(2)
    w_start(3)
    w_done(1)
    project(0)
    w_diag(2)
    attend(0)
    ag(X, 1, 2)
    w_done(2)
    spread(0, pa, ob, wo, 512)
    rs(BR, 0, 0)
    w_start(4)
    ag(X, 1, 3)
    rs(BR, 0, 1)
    ag(COT, 0, 0)
    norm1(1)
    project(1)
    rs(BR, 0, 2)
    ag(COT, 0, 1)
    attend(1)
    for s in (0, 1):
        pltpu.make_async_copy(tok.at[s], tbuf.at[s], lsem.at[5 + s]).wait()
    rs(BR, 0, 3)
    norm2(0)
    ag(N2, 0, 0)
    ag(COT, 0, 2)
    spread(1, pa, ob, wo, 512)
    rs(BR, 1, 0)
    ag(N2, 0, 1)
    w_relay(3)
    ag(COT, 0, 3)
    zag_sent(COT, 0)
    mask_grad(0)
    rs(BR, 1, 1)
    ag(N2, 0, 2)
    w_relay(4)
    w_diag(3)
    rs(BR, 1, 2)
    ag(COT, 1, 0)
    w_diag(4)
    ag(N2, 0, 3)
    w_done(3)
    w_done(4)
    feed(0)
    rs(BR, 1, 3)
    norm2(1)
    ag(N2, 1, 0)
    ag(COT, 1, 1)
    zag_sent(X, 0)
    rs_sent(BR, 0)
    spread(0, pa, dgu, wu, 256)
    rs(DN2, 0, 0)
    ag(N2, 1, 1)
    rs(DN2, 0, 1)
    ag(COT, 1, 2)
    spread(0, pb, act, wd, 512)
    ag(N2, 1, 2)
    rs(DN2, 0, 2)
    ag(COT, 1, 3)
    zag_sent(COT, 1)
    mask_grad(1)
    ag(N2, 1, 3)
    rs(DN2, 0, 3)
    gain2 = norm2_back(0)
    ag(GH, 0, 0)
    rs(FFN, 0, 0)
    feed(1)
    zag_sent(X, 1)
    rs_sent(BR, 1)
    spread(1, pa, dgu, wu, 256)
    rs(DN2, 1, 0)
    ag(GH, 0, 1)
    rs(FFN, 0, 1)
    spread(1, pb, act, wd, 512)
    rs(DN2, 1, 1)
    ag(GH, 0, 2)
    rs(FFN, 0, 2)
    g_compute(0)
    rs(DN2, 1, 2)
    ag(GH, 0, 3)
    attn_grad(0)
    rs(DN1, 0, 0)
    rs(FFN, 0, 3)
    finish_out(0)
    rs(DN2, 1, 3)
    gain2 = gain2 + norm2_back(1)
    ag(GH, 1, 0)
    rs(DN1, 0, 1)
    g_first(0)
    g_compute(1)
    ag(GH, 1, 1)
    rs(DN1, 0, 2)
    g_second(0)
    g_first(1)
    ag(GH, 1, 2)
    g_finish(0)
    g_compute(2)
    rs(DN1, 0, 3)
    gain1 = norm1_back(0)
    rs(FFN, 1, 0)
    g_second(1)
    ag(GH, 1, 3)
    attn_grad(1)
    rs(DN1, 1, 0)
    rs(FFN, 1, 1)
    g_first(2)
    g_finish(1)
    g_compute(3)
    rs(DN1, 1, 1)
    rs(FFN, 1, 2)
    g_second(2)
    g_first(3)
    g_finish(2)
    g_compute(4)
    rs(DN1, 1, 2)
    g_second(3)
    g_first(4)
    rs(FFN, 1, 3)
    finish_out(1)
    g_finish(3)
    rs(DN1, 1, 3)
    gain1 = gain1 + norm1_back(1)
    for j in range(4):
        gsum[j : j + 1, :] = gain1[:, j * pair : (j + 1) * pair]
        gsum[4 + j : 5 + j, :] = gain2[:, j * pair : (j + 1) * pair]

    def e_copy(i, src):
        dev = {"tensor": (z + i + 1) % 4} if i < 3 else {"dp": (d + i - 2) % 8}
        return rcopy(src, gex.at[i], esend.at[i], erecv.at[i], dev)

    for i in range(3):
        e_copy(i, gsum).start()
    g_second(4)
    for i in range(3):
        e_copy(i, gsum).wait()
    gex[10] = gsum[...] + gex[0] + gex[1] + gex[2]
    for i in range(3, 10):
        e_copy(i, gex.at[10]).start()
    g_finish(4)
    for i in range(3, 10):
        e_copy(i, gex.at[10]).wait()
    total = gex[10]
    for i in range(3, 10):
        total = total + gex[i]
    gsum[...] = total
    last = pltpu.make_async_copy(gsum, ggain_h, osem.at[9])
    last.start()
    for u in range(5):
        w_sent(u)
    for u in (N2, GH):
        for s in (0, 1):
            zag_sent(u, s)
    for s in (0, 1):
        rs_sent(FFN, s)
        rs_sent(DN1, s)
    g_out(3).wait()
    g_out(4).wait()
    for s in (0, 1):
        pltpu.make_async_copy(ybuf.at[s], out_h.at[s], osem.at[5 + s]).wait()
        pltpu.make_async_copy(dh.at[pl.ds(s * rows, rows)], gtok_h.at[s], osem.at[7 + s]).wait()
    last.wait()


def pad_heads(weight):
    depth = weight.shape[0]
    halves = weight.reshape(depth, -1, 2, HEAD // 2)
    return jnp.pad(halves, ((0, 0), (0, 0), (0, 0), (0, 64 - HEAD // 2))).reshape(depth, -1)


def cut_heads(grad):
    depth = grad.shape[0]
    return grad.reshape(depth, -1, 2, 64)[..., : HEAD // 2].reshape(depth, -1)


def fused(
    tokens,
    cotangent,
    order,
    lengths,
    gain_attn,
    w_query,
    w_key,
    w_value,
    w_out,
    gain_ffn,
    w_gate,
    w_up,
    w_down,
):
    micro, rows, width = tokens.shape
    seq = rows * lax.axis_size("tensor")
    shard = w_query.shape[0]
    ff = w_gate.shape[1]
    groups = w_key.shape[1] // HEAD
    w_in = pad_heads(jnp.concatenate([w_query, w_key, w_value], axis=1))
    qp = w_query.shape[1] // HEAD * LANES
    kp = groups * LANES
    inw = qp + 2 * kp
    w_back = pad_heads(w_out.T)
    gate_up = jnp.concatenate([w_gate, w_up], axis=1)
    gain = jnp.stack([gain_attn, gain_ffn], axis=0)
    low = jnp.pad(gain, ((0, 14), (0, shard)))
    high = jnp.pad(gain, ((0, 14), (shard, 0)))
    gain = jnp.where(lax.axis_index("dp") % 2 == 0, low, high)

    starts = jnp.cumsum(lengths, axis=1, dtype=jnp.int32) - lengths
    docs = jnp.sum((order[:, :, None] >= starts[:, None, 1:]).astype(jnp.int32), axis=2)
    onehot = docs[:, :, None] == jnp.arange(lengths.shape[1], dtype=jnp.int32)
    first = jnp.sum(jnp.where(onehot, starts[:, None, :], 0), axis=2)
    real = (docs < lengths.shape[1] - 1).astype(F32)
    cols = jnp.stack([order.astype(F32), first.astype(F32), real], axis=2)
    freqs = rope_base ** (-2.0 * jnp.arange(HEAD // 2, dtype=F32) / HEAD)
    angles = (order - first).astype(F32)[:, :, None] * freqs
    gap = ((0, 0), (0, 0), (0, 64 - HEAD // 2))
    cosine, sine = jnp.pad(jnp.cos(angles), gap), jnp.pad(jnp.sin(angles), gap)
    cosine = jnp.concatenate([cosine, cosine], axis=2)
    sine = jnp.concatenate([-sine, sine], axis=2)

    total = micro * seq
    vm = pltpu.VMEM
    dma = pltpu.SemaphoreType.DMA
    scratch = [
        vm((8 * 16, 2 * shard), BF),
        vm((width, inw), BF),
        vm((width, qp), BF),
        vm((width, 2 * ff), BF),
        vm((width, ff), BF),
        vm((total, width), BF),
        vm((total, width), BF),
        vm((total, width), BF),
        vm((total, width), BF),
        vm((total, inw), BF),
        vm((total, qp), BF),
        vm((total, qp), BF),
        vm((total, ff), BF),
        vm((total, inw), BF),
        vm((total, 2 * ff), BF),
        vm((micro * qp // LANES, seq, seq), F32),
        vm((micro * rows, width), F32),
        vm((micro * rows, width), F32),
        vm((total, width), BF),
        vm((total, width), BF),
        vm((micro, 2, 3, rows, width), BF),
        vm((micro, 2, 3, rows, width), BF),
        vm((2, width, ff), BF),
        vm((2, width // 2, ff), BF),
        vm((2, shard, ff), BF),
        vm((2, 2, shard, ff), BF),
        vm((2, shard, ff), F32),
        vm((rows, width), F32),
        vm((16, width), F32),
        vm((8, width // 4), F32),
        vm((11, 8, width // 4), F32),
        vm((micro, rows, width), BF),
        vm((micro, rows, width), BF),
        dma((5, 7)),
        dma((5, 7)),
        dma((4, 2, 2, 3)),
        dma((4, 2, 2, 3)),
        dma((4, 2, 2, 3)),
        dma((4, 2, 2, 3)),
        dma((5, 7)),
        dma((5, 7)),
        dma((10,)),
        dma((10,)),
        dma((12,)),
        dma((10,)),
        pltpu.SemaphoreType.REGULAR((3,)),
    ]
    hbm = pl.BlockSpec(memory_space=pl.ANY)
    vmem = pl.BlockSpec(memory_space=pltpu.VMEM)
    shapes = [
        jax.ShapeDtypeStruct((micro, rows, width), BF),
        jax.ShapeDtypeStruct((micro, rows, width), F32),
        jax.ShapeDtypeStruct((shard, ff), F32),
        jax.ShapeDtypeStruct((shard, ff), F32),
        jax.ShapeDtypeStruct((shard, ff), F32),
        jax.ShapeDtypeStruct((shard, qp), F32),
        jax.ShapeDtypeStruct((shard, inw), F32),
        jax.ShapeDtypeStruct((8, width // 4), F32),
    ]
    dims = (rows, seq, width, shard, qp, kp, ff, groups)
    out, gtok, gdown, ggate, gup, gout, gin, ggain = pl.pallas_call(
        functools.partial(block_kernel, dims),
        out_shape=shapes,
        in_specs=[hbm] * 7 + [vmem] * 4,
        out_specs=[hbm] * 8,
        scratch_shapes=scratch,
        compiler_params=pltpu.CompilerParams(
            collective_id=0, has_side_effects=True, vmem_limit_bytes=67_043_328
        ),
        name="block",
    )(
        tokens,
        cotangent,
        gain,
        w_in,
        w_back,
        gate_up,
        w_down.T,
        order.astype(F32)[:, None, :],
        cols,
        cosine,
        sine,
    )
    gains = ggain.reshape(2, width)
    gain_own = lax.dynamic_slice_in_dim(gains, lax.axis_index("dp") * shard, shard, 1)
    grads_in = cut_heads(gin)
    q_cols, k_cols = w_query.shape[1], w_key.shape[1]
    return (
        out,
        gtok,
        gain_own[0],
        grads_in[:, :q_cols],
        grads_in[:, q_cols : q_cols + k_cols],
        grads_in[:, q_cols + k_cols :],
        cut_heads(gout).T,
        gain_own[1],
        ggate,
        gup,
        gdown.T,
    )


def local(tokens, *rest):
    fits = lax.axis_size("dp") == 8 and lax.axis_size("tensor") == 4 and tokens.shape[0] == 2
    return (fused if fits else spread_out)(tokens, *rest)


def solution(mesh):
    return jax.shard_map(
        local,
        mesh=mesh,
        in_specs=(
            P("dp", "tensor", None),
            P("dp", "tensor", None),
            P("dp", None),
            P("dp", None),
            P("dp"),
            P("dp", "tensor"),
            P("dp", "tensor"),
            P("dp", "tensor"),
            P("tensor", "dp"),
            P("dp"),
            P("dp", "tensor"),
            P("dp", "tensor"),
            P("tensor", "dp"),
        ),
        out_specs=(
            P("dp", "tensor", None),
            P("dp", "tensor", None),
            P("dp"),
            P("dp", "tensor"),
            P("dp", "tensor"),
            P("dp", "tensor"),
            P("tensor", "dp"),
            P("dp"),
            P("dp", "tensor"),
            P("dp", "tensor"),
            P("tensor", "dp"),
        ),
        check_vma=False,
    )
```

```python
import functools

import jax
import jax.numpy as jnp
from jax import lax
from jax.experimental import pallas as pl
from jax.experimental.pallas import tpu as pltpu
from jax.sharding import PartitionSpec as P

HEAD = 96


eps = 1e-05
rope_base = 100000.0


def rotate(field, cosine, sine):
    half = field.shape[-1] // 2
    first = field[..., :half]
    second = field[..., half:]
    return jnp.concatenate(
        [first * cosine - second * sine, second * cosine + first * sine], axis=-1
    )


def rotate_back(field, cosine, sine):
    half = field.shape[-1] // 2
    first = field[..., :half]
    second = field[..., half:]
    return jnp.concatenate(
        [first * cosine + second * sine, second * cosine - first * sine], axis=-1
    )


def layout(order, lengths):
    starts = jnp.cumsum(lengths, dtype=jnp.int32) - lengths
    docs = jnp.sum((order[:, None] >= starts[None, 1:]).astype(jnp.int32), axis=1, dtype=jnp.int32)
    onehot = docs[:, None] == jnp.arange(lengths.shape[0], dtype=jnp.int32)[None, :]
    first = jnp.sum(jnp.where(onehot, starts[None, :], 0), axis=1, dtype=jnp.int32)
    positions = (order - first).astype(jnp.float32)
    mask = (docs[:, None] == docs[None, :]) & (order[None, :] <= order[:, None])
    real = (docs < lengths.shape[0] - 1).astype(jnp.float32)
    return (positions, mask, real)


def norm_forward(rows, gain):
    scale = lax.rsqrt(jnp.mean(rows * rows, axis=-1, keepdims=True) + eps)
    unit = rows * scale
    return (unit, scale, (unit * gain).astype(jnp.bfloat16))


def norm_backward(grad, unit, scale, gain):
    inner = grad * gain
    return scale * (inner - unit * jnp.mean(inner * unit, axis=-1, keepdims=True))


def contract_rows(left, right):
    return lax.dot_general(
        left, right, (((0,), (0,)), ((), ())), preferred_element_type=jnp.float32
    )


def times_transpose(left, right):
    return lax.dot_general(
        left, right, (((1,), (1,)), ((), ())), preferred_element_type=jnp.float32
    )


def gather_weights(gain_attn, w_query, w_key, w_value, w_out, gain_ffn, w_gate, w_up, w_down):
    gains = lax.all_gather(jnp.stack([gain_attn, gain_ffn], axis=0), "dp", axis=1, tiled=True)
    attn = lax.all_gather(
        jnp.concatenate([w_query, w_key, w_value, w_out.T], axis=1), "dp", axis=0, tiled=True
    )
    gate_up = lax.all_gather(jnp.concatenate([w_gate, w_up], axis=1), "dp", axis=0, tiled=True)
    down = lax.all_gather(w_down.T, "dp", axis=0, tiled=True)
    return gains, attn, gate_up, down


def gather_rows(rows):
    return lax.all_gather(rows, "tensor", axis=1, tiled=True)


def scatter_rows(partial):
    low = partial.astype(jnp.bfloat16)
    return lax.psum_scatter(low, "tensor", scatter_dimension=1, tiled=True).astype(jnp.float32)


def reduce_weights(term):
    low = term.astype(jnp.bfloat16)
    return lax.psum_scatter(low, "dp", scatter_dimension=0, tiled=True).astype(jnp.float32)


def spread_out(
    tokens,
    cotangent,
    order,
    lengths,
    gain_attn,
    w_query,
    w_key,
    w_value,
    w_out,
    gain_ffn,
    w_gate,
    w_up,
    w_down,
):
    micro, rows, width = tokens.shape
    seq = rows * lax.axis_size("tensor")
    q_cols, k_cols, ff_cols = w_query.shape[1], w_key.shape[1], w_gate.shape[1]
    local_heads, local_kv = q_cols // HEAD, k_cols // HEAD
    group = local_heads // local_kv
    first_row = lax.axis_index("tensor") * rows
    freqs = rope_base ** (-2.0 * jnp.arange(HEAD // 2, dtype=jnp.float32) / HEAD)
    head_scale = HEAD ** (-0.5)

    gains, attn, gate_up, down = gather_weights(
        gain_attn, w_query, w_key, w_value, w_out, gain_ffn, w_gate, w_up, w_down
    )
    gain1, gain2 = gains[0].astype(jnp.float32), gains[1].astype(jnp.float32)
    in_cols = q_cols + 2 * k_cols
    w_in, w_out_t = attn[:, :in_cols], attn[:, in_cols:]

    positions, mask, real = jax.vmap(layout)(order, lengths)
    angles = positions[:, :, None] * freqs
    cosine, sine = jnp.cos(angles)[:, :, None, :], jnp.sin(angles)[:, :, None, :]
    mask = mask[:, None, None]
    real_rows = lax.dynamic_slice_in_dim(real, first_row, rows, 1)[:, :, None]

    stream = tokens.astype(jnp.float32)
    unit1, scale1, normed1 = norm_forward(stream, gain1)
    full1 = gather_rows(normed1)
    grad_out_rows = cotangent.astype(jnp.float32) * real_rows
    full_grad = gather_rows(grad_out_rows.astype(jnp.bfloat16))
    flat1 = full1.reshape(micro * seq, width)
    flat_grad = full_grad.reshape(micro * seq, width)

    mixed_in = jnp.dot(flat1, w_in, preferred_element_type=jnp.float32).reshape(micro, seq, in_cols)
    query = mixed_in[..., :q_cols].reshape(micro, seq, local_heads, HEAD)
    keys = mixed_in[..., q_cols : q_cols + k_cols].reshape(micro, seq, local_kv, HEAD)
    values = mixed_in[..., q_cols + k_cols :].reshape(micro, seq, local_kv, HEAD).astype(jnp.bfloat16)
    query = (rotate(query, cosine, sine) * head_scale).astype(jnp.bfloat16)
    query = query.reshape(micro, seq, local_kv, group, HEAD)
    keys = rotate(keys, cosine, sine).astype(jnp.bfloat16)
    scores = jnp.einsum("bqkgd,bskd->bkgqs", query, keys, preferred_element_type=jnp.float32)
    scores = jnp.where(mask, scores, -1e30)
    peak = jnp.max(scores, axis=-1, keepdims=True)
    expon = jnp.exp(scores - peak)
    total = jnp.sum(expon, axis=-1, keepdims=True)
    probs = expon / total
    probs_low = probs.astype(jnp.bfloat16)
    mixed = jnp.einsum("bkgqs,bskd->bqkgd", probs_low, values, preferred_element_type=jnp.float32)
    mixed = mixed.reshape(micro * seq, q_cols).astype(jnp.bfloat16)
    branch = scatter_rows(times_transpose(mixed, w_out_t).reshape(micro, seq, width))
    resid = stream + branch
    unit2, scale2, normed2 = norm_forward(resid, gain2)
    full2 = gather_rows(normed2).reshape(micro * seq, width)

    both = jnp.dot(full2, gate_up, preferred_element_type=jnp.float32)
    gate, upper = both[:, :ff_cols], both[:, ff_cols:]
    sigma = jax.nn.sigmoid(gate)
    hidden = (gate * sigma * upper).astype(jnp.bfloat16)
    ffn = scatter_rows(times_transpose(hidden, down).reshape(micro, seq, width))
    output = ((resid + ffn) * real_rows).astype(jnp.bfloat16)

    grad_hidden = jnp.dot(flat_grad, down, preferred_element_type=jnp.float32)
    grad_gate = (grad_hidden * upper * sigma * (1.0 + gate * (1.0 - sigma))).astype(jnp.bfloat16)
    grad_up = (grad_hidden * gate * sigma).astype(jnp.bfloat16)
    grad_both = jnp.concatenate([grad_gate, grad_up], axis=1)
    grad_norm2 = scatter_rows(times_transpose(grad_both, gate_up).reshape(micro, seq, width))
    final_down = reduce_weights(contract_rows(flat_grad, hidden))
    final_gate = reduce_weights(contract_rows(full2, grad_gate))
    final_up = reduce_weights(contract_rows(full2, grad_up))
    term_gain2 = jnp.sum(grad_norm2 * unit2, axis=(0, 1))
    grad_resid = grad_out_rows + norm_backward(grad_norm2, unit2, scale2, gain2)

    full_resid = gather_rows(grad_resid.astype(jnp.bfloat16)).reshape(micro * seq, width)
    grad_mixed = jnp.dot(full_resid, w_out_t, preferred_element_type=jnp.float32).astype(jnp.bfloat16)
    final_out = reduce_weights(contract_rows(full_resid, mixed))
    grad_heads = grad_mixed.reshape(micro, seq, local_kv, group, HEAD)
    grad_probs = jnp.einsum(
        "bqkgd,bskd->bkgqs", grad_heads, values, preferred_element_type=jnp.float32
    )
    grad_values = jnp.einsum(
        "bkgqs,bqkgd->bskd", probs_low, grad_heads, preferred_element_type=jnp.float32
    )
    grad_scores = (
        probs * (grad_probs - jnp.sum(probs * grad_probs, axis=-1, keepdims=True))
    ).astype(jnp.bfloat16)
    grad_query = jnp.einsum(
        "bkgqs,bskd->bqkgd", grad_scores, keys, preferred_element_type=jnp.float32
    ).reshape(micro, seq, local_heads, HEAD)
    grad_keys = jnp.einsum(
        "bkgqs,bqkgd->bskd", grad_scores, query, preferred_element_type=jnp.float32
    )
    grad_query = rotate_back(grad_query * head_scale, cosine, sine).reshape(micro * seq, q_cols)
    grad_keys = rotate_back(grad_keys, cosine, sine).reshape(micro * seq, k_cols)
    grad_values = grad_values.reshape(micro * seq, k_cols)
    grad_in = jnp.concatenate(
        [grad_query.astype(jnp.bfloat16), grad_keys.astype(jnp.bfloat16), grad_values.astype(jnp.bfloat16)],
        axis=1,
    )
    grad_norm1 = scatter_rows(times_transpose(grad_in, w_in).reshape(micro, seq, width))
    final_in = reduce_weights(contract_rows(flat1, grad_in))
    term_gain1 = jnp.sum(grad_norm1 * unit1, axis=(0, 1))
    grad_tokens = grad_resid + norm_backward(grad_norm1, unit1, scale1, gain1)

    gain_terms = lax.psum(jnp.stack([term_gain1, term_gain2], axis=0), ("dp", "tensor"))
    own = gain_attn.shape[0]
    gain_own = lax.dynamic_slice_in_dim(gain_terms, lax.axis_index("dp") * own, own, 1)
    return (
        output,
        grad_tokens,
        gain_own[0],
        final_in[:, :q_cols],
        final_in[:, q_cols : q_cols + k_cols],
        final_in[:, q_cols + k_cols :],
        final_out.T,
        gain_own[1],
        final_gate,
        final_up,
        final_down.T,
    )


BF = jnp.bfloat16
F32 = jnp.float32
MESH = pl.DeviceIdType.MESH
LANES = 128


def nn(left, right):
    return lax.dot_general(left, right, (((1,), (0,)), ((), ())), preferred_element_type=F32)


def nt(left, right):
    return lax.dot_general(left, right, (((1,), (1,)), ((), ())), preferred_element_type=F32)


def tn(left, right):
    return lax.dot_general(left, right, (((0,), (0,)), ((), ())), preferred_element_type=F32)


def al(value, unit):
    return pl.multiple_of(value, unit)


def block_kernel(dims, *refs):
    (rows, seq, width, shard, qp, kp, ff, groups) = dims
    (tok, cot, wg_h, wi_h, wo_h, wu_h, wd_h, ordr, cols, cosr, sinr) = refs[:11]
    (out_h, gtok_h, gdown_h, ggate_h, gup_h, gout_h, gin_h, ggain_h) = refs[11:19]
    (wgn, wi, wo, wu, wd, xf, n1, n2, gf, qkv, ob, dob, act, dq3, dgu, pr, hb, dh, pa, pb, ra, rb,
     gb, xb, hop, fin, stage, acc, gains, gpart, gsum, gex, ybuf, tbuf,
     wsend, wrecv, zsend, zrecv, rsend, rrecv, gsend, grecv, esend, erecv, lsem, osem, credit) = refs[19:]
    ghf = xf
    heads = qp // LANES
    per_group = heads // groups
    inw = qp + 2 * kp
    d = lax.axis_index("dp")
    z = lax.axis_index("tensor")
    c = d % 2
    flip = 1 - 2 * c
    near_x = d + 2 - 4 * ((d // 2) % 2)
    near_y = d + 4 - 8 * (d // 4)
    aa = near_x * (1 - c) + near_y * c
    bb = near_y * (1 - c) + near_x * c
    dd = aa + bb - d
    pp = d + flip
    chip_own, chip_a, chip_b, chip_d = d // 2, aa // 2, bb // 2, dd // 2
    chip_x, chip_y = near_x // 2, near_y // 2
    own = 1 * z * rows
    zdev = {"tensor": z + 1}, {"tensor": z - 1}

    def rcopy(src, dst, ssem, rsem, dev):
        return pltpu.make_async_remote_copy(
            src_ref=src, dst_ref=dst, send_sem=ssem, recv_sem=rsem, device_id=dev, device_id_type=MESH
        )

    barrier = pltpu.get_barrier_semaphore()
    for step in range(1, 8):
        pl.semaphore_signal(barrier, inc=1, device_id={"dp": (d + step) % 8}, device_id_type=MESH)
    for step in (1, 2, 3):
        pl.semaphore_signal(
            barrier, inc=1, device_id={"tensor": (z + step) % 4}, device_id_type=MESH
        )
    pl.semaphore_wait(barrier, 10)

    wunits = ((wg_h, wgn, 16), (wi_h, wi, shard), (wo_h, wo, shard), (wu_h, wu, shard), (wd_h, wd, shard))

    def wblk(u, i):
        n = wunits[u][2]
        return wunits[u][1].at[pl.ds(al(n * i, 16), n)]

    def w_start(u):
        src = wunits[u][0]
        pltpu.make_async_copy(src, wblk(u, d), lsem.at[u]).start()
        rcopy(src, wblk(u, d), wsend.at[u, 0], wrecv.at[u, 0], {"dp": aa}).start()
        rcopy(src, wblk(u, d), wsend.at[u, 1], wrecv.at[u, 1], {"dp": bb}).start()
        rcopy(src, wblk(u, d), wsend.at[u, 2], wrecv.at[u, 3], {"dp": pp}).start()

    def w_wait(u, slot, i):
        rcopy(wblk(u, i), wblk(u, i), wsend.at[u, 0], wrecv.at[u, slot], {"dp": aa}).wait_recv()

    def w_relayb(u):
        w_wait(u, 1, bb)
        rcopy(wblk(u, bb), wblk(u, bb), wsend.at[u, 3], wrecv.at[u, 2], {"dp": aa}).start()
        rcopy(wblk(u, bb), wblk(u, bb), wsend.at[u, 4], wrecv.at[u, 5], {"dp": pp}).start()

    def w_relaya(u):
        w_wait(u, 0, aa)
        rcopy(wblk(u, aa), wblk(u, aa), wsend.at[u, 5], wrecv.at[u, 4], {"dp": pp}).start()

    def w_diag(u):
        w_wait(u, 2, dd)
        rcopy(wblk(u, dd), wblk(u, dd), wsend.at[u, 6], wrecv.at[u, 6], {"dp": pp}).start()

    def w_done(u):
        w_wait(u, 3, pp)
        w_wait(u, 4, bb + flip)
        w_wait(u, 5, aa + flip)
        w_wait(u, 6, dd + flip)
        pltpu.make_async_copy(wunits[u][0], wblk(u, d), lsem.at[u]).wait()

    def w_sent(u):
        for slot in range(7):
            rcopy(wblk(u, d), wblk(u, d), wsend.at[u, slot], wrecv.at[u, 0], {"dp": aa}).wait_send()

    zfull = (xf, gf, n2, ghf)
    zhbm = (tok, cot, None, None)

    def zblk(u, s, i):
        return zfull[u].at[pl.ds(al(s * seq + i * rows, 16), rows)]

    def zag_send(u, s, k, way):
        i = z - k if way == 0 else z + k
        go = (z < 3) & (i >= 0) if way == 0 else (z > 0) & (i <= 3)

        @pl.when(go)
        def _():
            src = zhbm[u].at[s] if k == 0 and zhbm[u] is not None else zblk(u, s, i)
            rcopy(src, zblk(u, s, i), zsend.at[u, s, way, k], zrecv.at[u, s, way, k], zdev[way]).start()

    def zag_recv(u, s, k, way):
        i = z - 1 - k if way == 0 else z + 1 + k
        go = (i >= 0) if way == 0 else (i <= 3)

        @pl.when(go)
        def _():
            rcopy(
                zblk(u, s, i), zblk(u, s, i), zsend.at[u, s, way, k], zrecv.at[u, s, way, k], zdev[way]
            ).wait_recv()

    def zag_start(u, s):
        if zhbm[u] is not None:
            pltpu.make_async_copy(zhbm[u].at[s], zblk(u, s, z), lsem.at[8 + 2 * u + s]).start()
        for way in (0, 1):
            zag_send(u, s, 0, way)

    def ag(u, s, t, way=None):
        if t == 0:
            zag_start(u, s)
            return
        zag_recv(u, s, t - 1, way)
        if t < 3:
            zag_send(u, s, t, way)

    def own_here(u, s):
        pltpu.make_async_copy(zhbm[u].at[s], zblk(u, s, z), lsem.at[8 + 2 * u + s]).wait()

    def zag_sent(u, s):
        for k in range(3):
            for way in (0, 1):
                i = z - k if way == 0 else z + k
                go = (z < 3) & (i >= 0) if way == 0 else (z > 0) & (i <= 3)

                @pl.when(go)
                def _():
                    rcopy(
                        zblk(u, s, i), zblk(u, s, i), zsend.at[u, s, way, k], zrecv.at[u, s, way, k], zdev[way]
                    ).wait_send()

    zpart = (pa, pb, pa, pa)
    zgot = (ra, rb, ra, ra)

    def rs_copy(u, s, way, t, dest):
        return rcopy(
            zpart[u].at[pl.ds(al(s * seq + dest * rows, 16), rows)],
            zgot[u].at[s, way, t],
            rsend.at[u, s, way, t],
            rrecv.at[u, s, way, t],
            zdev[way],
        )

    def rs(u, s, t, ways=(0, 1)):
        for way in ways:
            from_end = z if way == 0 else 3 - z

            def wait_and(target, base):
                rs_copy(u, s, way, t - 1, z).wait_recv()

                def body(i, carry):
                    at = pl.ds(al(base + i * 16, 16), 16)
                    got = zgot[u][s, way, t - 1, pl.ds(al(i * 16, 16), 16), :].astype(F32)
                    target[at, :] = (target[at, :].astype(F32) + got).astype(target.dtype)
                    return carry

                lax.fori_loop(0, rows // 16, body, 0)

            if t == 3:
                if way == 0:
                    def first(i, carry):
                        at = pl.ds(al(i * 16, 16), 16)
                        acc[at, :] = zpart[u][pl.ds(al(s * seq + own + i * 16, 16), 16), :].astype(F32)
                        return carry

                    lax.fori_loop(0, rows // 16, first, 0)

                @pl.when(from_end > 0)
                def _():
                    wait_and(acc, 0)
            else:
                dest = 3 + z - t if way == 0 else t - from_end

                @pl.when(from_end <= t)
                def _():
                    if t > 0:
                        @pl.when(from_end > 0)
                        def _():
                            wait_and(zpart[u], s * seq + dest * rows)

                    rs_copy(u, s, way, t, dest).start()

    def rs_sent(u, s):
        for way in (0, 1):
            from_end = z if way == 0 else 3 - z
            for t in range(3):
                @pl.when(from_end <= t)
                def _():
                    rs_copy(u, s, way, t, z).wait_send()

    gunits = (
        (gf, act, 0, ff, gdown_h),
        (n2, dgu, 0, ff, ggate_h),
        (n2, dgu, ff, ff, gup_h),
        (ghf, ob, 0, qp, gout_h),
        (n1, dq3, 0, inw, gin_h),
    )
    pair = 2 * shard

    def xslot(u, chip):
        b, n = u % 2, gunits[u][3]
        return xb.at[b, pl.ds(al(chip * shard, 16), shard), pl.ds(0, n)]

    def gslot(u, chip, core):
        b, n = u % 2, gunits[u][3]
        return gb.at[b, pl.ds(al(chip * pair + core * shard, 16), shard), pl.ds(0, n)]

    def g_exchange(u, chip, i):
        return rcopy(gslot(u, chip, 1 - c), xslot(u, chip), gsend.at[u, i], grecv.at[u, i], {"dp": pp})

    chips = (chip_d, chip_x, chip_y, chip_own)

    def g_compute(u, i):
        left, right, at, n, _ = gunits[u]
        chip = chips[i]
        if u >= 2 and i == 0:
            pl.semaphore_wait(credit.at[0], 1)
        tile = 256

        def body(j, carry):
            lhs = left[:, pl.ds(al(chip * pair, LANES), pair)]
            got = tn(lhs, right[:, pl.ds(al(at + j * tile, tile), tile)])
            gb[u % 2, pl.ds(al(chip * pair, 16), pair), pl.ds(al(j * tile, tile), tile)] = got.astype(BF)
            return carry

        lax.fori_loop(0, n // tile, body, 0)
        g_exchange(u, chip, i).start()

    def g_add(u, chip, extra=None):
        b, n = u % 2, gunits[u][3]

        def body(i, carry):
            at = pl.ds(al(chip * shard + i * 16, 16), 16)
            mine = gb[b, pl.ds(al(chip * pair + c * shard + i * 16, 16), 16), pl.ds(0, n)].astype(F32)
            total = mine + xb[b, at, pl.ds(0, n)].astype(F32)
            if extra is not None:
                total = total + extra[b, pl.ds(al(i * 16, 16), 16), pl.ds(0, n)].astype(F32)
            xb[b, at, pl.ds(0, n)] = total.astype(BF)
            return carry

        lax.fori_loop(0, shard // 16, body, 0)

    def g_hop(u):
        b, n = u % 2, gunits[u][3]
        return rcopy(xslot(u, chip_d), hop.at[b, :, pl.ds(0, n)], gsend.at[u, 4], grecv.at[u, 4], {"dp": aa})

    def g_last(u, way):
        b, n = u % 2, gunits[u][3]
        chip, dev = (chip_a, aa) if way == 0 else (chip_b, bb)
        return rcopy(
            xslot(u, chip), fin.at[b, way, :, pl.ds(0, n)], gsend.at[u, 5 + way], grecv.at[u, 5 + way], {"dp": dev}
        )

    def g_first(u):
        g_exchange(u, chip_d, 0).wait_recv()
        g_add(u, chip_d)
        if u >= 2:
            pl.semaphore_wait(credit.at[1], 1)
        g_hop(u).start()

    def g_firstb(u):
        g_exchange(u, chip_x, 1).wait_recv()
        g_exchange(u, chip_y, 2).wait_recv()
        g_add(u, chip_a)
        g_last(u, 0).start()

    def g_second(u):
        g_hop(u).wait_recv()
        g_add(u, chip_b, hop)
        if u >= 2:
            pl.semaphore_wait(credit.at[2], 1)
        g_last(u, 1).start()

    def g_finish(u):
        b, n, out = u % 2, gunits[u][3], gunits[u][4]
        g_exchange(u, chip_own, 3).wait_recv()
        g_last(u, 0).wait_recv()
        g_last(u, 1).wait_recv()

        def body(i, carry):
            at = pl.ds(al(i * 16, 16), 16)
            total = gb[b, pl.ds(al(chip_own * pair + c * shard + i * 16, 16), 16), pl.ds(0, n)].astype(F32)
            total = total + xb[b, pl.ds(al(chip_own * shard + i * 16, 16), 16), pl.ds(0, n)].astype(F32)
            total = total + fin[b, 0, at, pl.ds(0, n)].astype(F32)
            stage[b, at, pl.ds(0, n)] = total + fin[b, 1, at, pl.ds(0, n)].astype(F32)
            return carry

        if u >= 2:
            g_out(u - 2).wait()
        lax.fori_loop(0, shard // 16, body, 0)
        g_out(u).start()
        for i in range(4):
            g_exchange(u, chips[i], i).wait_send()
        g_hop(u).wait_send()
        g_last(u, 0).wait_send()
        g_last(u, 1).wait_send()
        if u < 3:
            pl.semaphore_signal(credit.at[0], inc=1, device_id={"dp": pp}, device_id_type=MESH)
            pl.semaphore_signal(credit.at[1], inc=1, device_id={"dp": aa}, device_id_type=MESH)
            pl.semaphore_signal(credit.at[2], inc=1, device_id={"dp": bb}, device_id_type=MESH)

    def g_out(u):
        b, n, out = u % 2, gunits[u][3], gunits[u][4]
        return pltpu.make_async_copy(stage.at[b, :, pl.ds(0, n)], out, osem.at[u])

    def gain_rows():
        for j in range(4):
            at = pl.ds(j * pair, pair)
            gains[:, at] = (
                wgn[pl.ds(32 * j, 16), :].astype(F32) + wgn[pl.ds(32 * j + 16, 16), :].astype(F32)
            )

    def norm1(s, t):
        gain = gains[0:1, :]

        def shard_rows(i):
            def body(r, carry):
                at = pl.ds(al(s * seq + i * rows + r * 16, 16), 16)
                x = xf[at, :].astype(F32)
                scale = lax.rsqrt(jnp.mean(x * x, axis=-1, keepdims=True) + eps)
                n1[at, :] = (x * scale * gain).astype(BF)
                return carry

            lax.fori_loop(0, rows // 16, body, 0)

        if t == 0:
            own_here(0, s)
            shard_rows(z)
            return

        @pl.when(z - t >= 0)
        def _():
            shard_rows(z - t)

        @pl.when(z + t <= 3)
        def _():
            shard_rows(z + t)

    head_scale = HEAD ** (-0.5)

    def project(s):
        at = pl.ds(s * seq, seq)
        cosine, sine = cosr[s], sinr[s]
        for j in range(inw // 256):
            both = nn(n1[at, :], wi[:, pl.ds(j * 256, 256)])
            for half in range(2):
                col = j * 256 + half * LANES
                part = both[:, half * LANES : (half + 1) * LANES]
                if col < qp + kp:
                    part = part * cosine + pltpu.roll(part, LANES // 2, 1) * sine
                if col < qp:
                    part = part * head_scale
                qkv[at, pl.ds(col, LANES)] = part.astype(BF)

    def attend(s):
        at = pl.ds(s * seq, seq)
        oc = ordr[s]
        mask = (oc <= cols[s, :, 0:1]) & (oc >= cols[s, :, 1:2])

        def body(h, carry):
            g = h // per_group
            q = qkv[at, pl.ds(al(h * LANES, LANES), LANES)]
            k = qkv[at, pl.ds(al(qp + g * LANES, LANES), LANES)]
            v = qkv[at, pl.ds(al(qp + kp + g * LANES, LANES), LANES)]
            sc = jnp.where(mask, nt(q, k), -1e30)
            e = jnp.exp(sc - jnp.max(sc, axis=-1, keepdims=True))
            p = e * (1.0 / jnp.sum(e, axis=-1, keepdims=True))
            pr[s * heads + h] = p
            ob[at, pl.ds(al(h * LANES, LANES), LANES)] = nn(p.astype(BF), v).astype(BF)
            return carry

        lax.fori_loop(0, heads, body, 0)

    def spread(s, dst, left, weight, tile):
        at = pl.ds(s * seq, seq)

        def body(j, carry):
            col = al(j * tile, tile)
            dst[at, pl.ds(col, tile)] = nt(left[at, :], weight[pl.ds(col, tile), :]).astype(BF)
            return carry

        lax.fori_loop(0, width // tile, body, 0)

    def norm2(s):
        gain = gains[1:2, :]
        base = s * rows

        def body(i, carry):
            r = pl.ds(al(i * 16, 16), 16)
            h = tbuf[s, r, :].astype(F32) + acc[r, :]
            hb[pl.ds(al(base + i * 16, 16), 16), :] = h
            scale = lax.rsqrt(jnp.mean(h * h, axis=-1, keepdims=True) + eps)
            n2[pl.ds(al(s * seq + own + i * 16, 16), 16), :] = (h * scale * gain).astype(BF)
            return carry

        lax.fori_loop(0, rows // 16, body, 0)

    def feed(s):
        at = pl.ds(s * seq, seq)
        real = cols[s, :, 2:3]
        own_here(1, s)

        def body(t, carry):
            col = al(t * 256, 256)
            gate = nn(n2[at, :], wu[:, pl.ds(col, 256)])
            upper = nn(n2[at, :], wu[:, pl.ds(al(ff + t * 256, 256), 256)])
            back = nn(gf[at, :], wd[:, pl.ds(col, 256)]) * real
            sigma = 1.0 / (1.0 + jnp.exp(-gate))
            swish = gate * sigma
            act[at, pl.ds(col, 256)] = (swish * upper * real).astype(BF)
            dgu[at, pl.ds(col, 256)] = (back * upper * sigma * (1.0 + gate * (1.0 - sigma))).astype(BF)
            dgu[at, pl.ds(al(ff + t * 256, 256), 256)] = (back * swish).astype(BF)
            return carry

        lax.fori_loop(0, ff // 256, body, 0)

    def finish_out(s):
        def body(i, carry):
            r = pl.ds(al(i * 16, 16), 16)
            real = cols[s, pl.ds(al(own + i * 16, 16), 16), 2:3]
            y = (hb[pl.ds(al(s * rows + i * 16, 16), 16), :] + acc[r, :]) * real
            ybuf[s, r, :] = y.astype(BF)
            return carry

        lax.fori_loop(0, rows // 16, body, 0)
        pltpu.make_async_copy(ybuf.at[s], out_h.at[s], osem.at[5 + s]).start()

    def norm2_back(s):
        gain = gains[1:2, :]

        def body(i, carry):
            r = pl.ds(al(i * 16, 16), 16)
            ro = pl.ds(al(s * rows + i * 16, 16), 16)
            h = hb[ro, :]
            scale = lax.rsqrt(jnp.mean(h * h, axis=-1, keepdims=True) + eps)
            unit = h * scale
            grad = acc[r, :]
            inner = grad * gain
            dy = gf[pl.ds(al(s * seq + own + i * 16, 16), 16), :].astype(F32)
            dy = dy * cols[s, pl.ds(al(own + i * 16, 16), 16), 2:3]
            dhr = dy + scale * (inner - unit * jnp.mean(inner * unit, axis=-1, keepdims=True))
            dh[ro, :] = dhr
            ghf[pl.ds(al(s * seq + own + i * 16, 16), 16), :] = dhr.astype(BF)
            return carry + jnp.sum(grad * unit, axis=0, keepdims=True)

        gpart[1:2, :] += lax.fori_loop(0, rows // 16, body, jnp.zeros((1, width), F32))

    def grad_heads(s):
        at = pl.ds(s * seq, seq)
        for j in range(qp // 256):
            dob[at, pl.ds(j * 256, 256)] = nn(ghf[at, :], wo[:, pl.ds(j * 256, 256)]).astype(BF)

    def attend_back(s):
        at = pl.ds(s * seq, seq)
        cosine, sine = cosr[s], sinr[s]

        def body(g, carry):
            k = qkv[at, pl.ds(al(qp + g * LANES, LANES), LANES)]
            v = qkv[at, pl.ds(al(qp + kp + g * LANES, LANES), LANES)]
            dk = jnp.zeros((seq, LANES), F32)
            dv = jnp.zeros((seq, LANES), F32)
            for m in range(per_group):
                h = g * per_group + m
                hat = pl.ds(al(h * LANES, LANES), LANES)
                q = qkv[at, hat]
                do = dob[at, hat]
                p = pr[s * heads + h]
                dp = nt(do, v)
                ds = (p * (dp - jnp.sum(p * dp, axis=-1, keepdims=True))).astype(BF)
                dv = dv + tn(p.astype(BF), do)
                dk = dk + tn(ds, q)
                dq = nn(ds, k) * head_scale
                dq3[at, hat] = (dq * cosine - pltpu.roll(dq, LANES // 2, 1) * sine).astype(BF)
            dq3[at, pl.ds(al(qp + g * LANES, LANES), LANES)] = (
                dk * cosine - pltpu.roll(dk, LANES // 2, 1) * sine
            ).astype(BF)
            dq3[at, pl.ds(al(qp + kp + g * LANES, LANES), LANES)] = dv.astype(BF)
            return carry

        lax.fori_loop(0, groups, body, 0)

    def norm1_back(s):
        gain = gains[0:1, :]

        def body(i, carry):
            r = pl.ds(al(i * 16, 16), 16)
            ro = pl.ds(al(s * rows + i * 16, 16), 16)
            x = tbuf[s, r, :].astype(F32)
            scale = lax.rsqrt(jnp.mean(x * x, axis=-1, keepdims=True) + eps)
            unit = x * scale
            grad = acc[r, :]
            inner = grad * gain
            dh[ro, :] = dh[ro, :] + scale * (inner - unit * jnp.mean(inner * unit, axis=-1, keepdims=True))
            return carry + jnp.sum(grad * unit, axis=0, keepdims=True)

        gpart[0:1, :] += lax.fori_loop(0, rows // 16, body, jnp.zeros((1, width), F32))
        pltpu.make_async_copy(
            dh.at[pl.ds(s * rows, rows)], gtok_h.at[s], osem.at[7 + s]
        ).start()

    X, COT, N2, GH = 0, 1, 2, 3
    BR, FFN, DN2, DN1 = 0, 1, 2, 3

    def tok_copy(s):
        return pltpu.make_async_copy(tok.at[s], tbuf.at[s], lsem.at[5 + s])

    def fin_br(s):
        rs(BR, s, 3)
        tok_copy(s).wait()
        norm2(s)
        ag(N2, s, 0)

    def fin_dn2(s):
        rs(DN2, s, 3)
        norm2_back(s)
        ag(GH, s, 0)

    def fin_ffn(s):
        rs(FFN, s, 3)
        finish_out(s)

    def fin_dn1(s):
        rs(DN1, s, 3)
        norm1_back(s)

    def e_copy(i):
        dev = {"tensor": (z + i + 1) % 4} if i < 3 else {"dp": (d + i - 2) % 8}
        return rcopy(gsum if i < 3 else gex.at[10], gex.at[i], esend.at[i], erecv.at[i], dev)

    def e1s():
        for j in range(4):
            gsum[j : j + 1, :] = gpart[0:1, j * pair : (j + 1) * pair]
            gsum[4 + j : 5 + j, :] = gpart[1:2, j * pair : (j + 1) * pair]
        for i in range(3):
            e_copy(i).start()

    def e1w():
        for i in range(3):
            e_copy(i).wait()
        gex[10] = gsum[...] + gex[0] + gex[1] + gex[2]
        for i in range(3, 10):
            e_copy(i).start()

    def e2w():
        for i in range(3, 10):
            e_copy(i).wait()
        total = gex[10]
        for i in range(3, 10):
            total = total + gex[i]
        gsum[...] = total

    gpart[...] = jnp.zeros_like(gpart)
    for s in (0, 1):
        tok_copy(s).start()
    ag(X, 0, 0)
    w_start(0)
    w_start(1)
    ag(X, 1, 0)
    w_start(2)
    w_relayb(1)
    ag(X, 0, 1, 1)
    ag(X, 0, 1, 0)
    ag(X, 1, 1, 0)
    ag(X, 1, 1, 1)
    w_relaya(0)
    w_diag(1)
    w_relayb(0)
    ag(X, 0, 2, 0)
    w_diag(0)
    w_relaya(1)
    w_relayb(2)
    w_start(3)
    ag(X, 0, 2, 1)
    w_done(0)
    gain_rows()
    ag(COT, 0, 0)
    norm1(0, 1)
    ag(X, 1, 2, 0)
    norm1(0, 0)
    ag(COT, 1, 0)
    w_relaya(2)
    norm1(1, 0)
    ag(X, 1, 2, 1)
    w_done(1)
    ag(X, 0, 3, 0)
    w_diag(2)
    ag(X, 0, 3, 1)
    norm1(0, 2)
    norm1(0, 3)
    project(0)
    w_done(2)
    attend(0)
    spread(0, pa, ob, wo, 512)
    rs(BR, 0, 0, (1,))
    ag(COT, 0, 1, 1)
    rs(BR, 0, 0, (0,))
    ag(COT, 0, 1, 0)
    rs(BR, 0, 1, (0,))
    norm1(1, 1)
    w_relaya(3)
    rs(BR, 0, 1, (1,))
    w_relayb(3)
    rs(BR, 0, 2, (0,))
    ag(X, 1, 3, 0)
    ag(X, 1, 3, 1)
    norm1(1, 3)
    rs(BR, 0, 2, (1,))
    norm1(1, 2)
    project(1)
    ag(COT, 0, 2, 0)
    ag(COT, 0, 2, 1)
    w_start(4)
    attend(1)
    fin_br(0)
    rs_sent(BR, 0)
    spread(1, pa, ob, wo, 512)
    rs(BR, 1, 0, (0,))
    w_relayb(4)
    rs(BR, 1, 0, (1,))
    ag(N2, 0, 1, 1)
    ag(N2, 0, 1, 0)
    w_diag(3)
    rs(BR, 1, 1, (1,))
    w_relaya(4)
    rs(BR, 1, 1, (0,))
    zag_sent(X, 0)
    ag(COT, 0, 3, 1)
    ag(N2, 0, 2, 1)
    w_diag(4)
    ag(N2, 0, 2, 0)
    w_done(4)
    rs(BR, 1, 2, (1,))
    ag(N2, 0, 3, 0)
    rs(BR, 1, 2, (0,))
    ag(COT, 1, 1, 0)
    ag(N2, 0, 3, 1)
    ag(COT, 1, 1, 1)
    ag(COT, 0, 3, 0)
    w_done(3)
    feed(0)
    fin_br(1)
    spread(0, pa, dgu, wu, 256)
    rs(DN2, 0, 0, (0,))
    ag(COT, 1, 2, 0)
    ag(N2, 1, 1, 1)
    rs(DN2, 0, 0, (1,))
    ag(N2, 1, 1, 0)
    rs_sent(BR, 1)
    rs(DN2, 0, 1, (1,))
    ag(COT, 1, 2, 1)
    rs(DN2, 0, 1, (0,))
    spread(0, pb, act, wd, 512)
    rs(FFN, 0, 0, (1,))
    rs(FFN, 0, 0, (0,))
    ag(N2, 1, 2, 1)
    ag(N2, 1, 2, 0)
    zag_sent(X, 1)
    rs(DN2, 0, 2, (0,))
    ag(COT, 1, 3, 0)
    rs(DN2, 0, 2, (1,))
    ag(COT, 1, 3, 1)
    rs(FFN, 0, 1, (1,))
    rs(FFN, 0, 1, (0,))
    ag(N2, 1, 3, 0)
    ag(N2, 1, 3, 1)
    feed(1)
    fin_dn2(0)
    spread(1, pa, dgu, wu, 256)
    g_compute(0, 0)
    ag(GH, 0, 1, 1)
    rs(DN2, 1, 0, (1,))
    ag(GH, 0, 1, 0)
    rs(DN2, 1, 0, (0,))
    g_compute(0, 1)
    g_compute(0, 2)
    g_compute(0, 3)
    rs(DN2, 1, 1, (1,))
    g_first(0)
    rs(DN2, 1, 1, (0,))
    ag(GH, 0, 2, 0)
    g_compute(1, 0)
    ag(GH, 0, 2, 1)
    rs(DN2, 1, 2, (1,))
    rs(DN2, 1, 2, (0,))
    spread(1, pb, act, wd, 512)
    g_firstb(0)
    rs(FFN, 1, 0, (1,))
    rs_sent(DN2, 0)
    g_second(0)
    ag(GH, 0, 3, 0)
    g_compute(1, 1)
    g_compute(1, 2)
    g_compute(1, 3)
    rs(FFN, 1, 0, (0,))
    g_first(1)
    ag(GH, 0, 3, 1)
    fin_dn2(1)
    grad_heads(0)
    attend_back(0)
    spread(0, pa, dq3, wi, 512)
    rs(DN1, 0, 0, (0,))
    g_finish(0)
    rs(DN1, 0, 0, (1,))
    g_firstb(1)
    g_compute(2, 0)
    ag(GH, 1, 1, 0)
    ag(GH, 1, 1, 1)
    g_compute(2, 1)
    rs(DN1, 0, 1, (0,))
    rs(DN1, 0, 1, (1,))
    g_first(2)
    g_compute(2, 2)
    ag(GH, 1, 2, 0)
    rs(FFN, 1, 1, (0,))
    g_compute(2, 3)
    ag(GH, 1, 2, 1)
    rs_sent(DN2, 1)
    rs(FFN, 0, 2, (1,))
    rs(FFN, 1, 1, (1,))
    g_firstb(2)
    g_second(2)
    rs(FFN, 0, 2, (0,))
    ag(GH, 1, 3, 0)
    g_second(1)
    ag(GH, 1, 3, 1)
    grad_heads(1)
    attend_back(1)
    spread(1, pa, dq3, wi, 512)
    rs(DN1, 1, 0, (1,))
    rs(DN1, 1, 0, (0,))
    g_finish(1)
    g_compute(3, 0)
    g_compute(3, 1)
    rs(DN1, 1, 1, (0,))
    g_first(3)
    rs(DN1, 1, 1, (1,))
    g_finish(2)
    rs(DN1, 0, 2, (0,))
    g_compute(3, 2)
    fin_ffn(0)
    rs(DN1, 0, 2, (1,))
    g_compute(3, 3)
    g_firstb(3)
    g_compute(4, 0)
    g_second(3)
    rs(DN1, 1, 2, (0,))
    g_first(4)
    rs(DN1, 1, 2, (1,))
    g_compute(4, 1)
    g_compute(4, 2)
    g_firstb(4)
    g_compute(4, 3)
    rs(FFN, 1, 2, (1,))
    g_second(4)
    rs(FFN, 1, 2, (0,))
    fin_dn1(0)
    fin_dn1(1)
    e1s()
    g_finish(3)
    e1w()
    g_finish(4)
    fin_ffn(1)
    e2w()
    last = pltpu.make_async_copy(gsum, ggain_h, osem.at[9])
    last.start()
    for u in range(5):
        w_sent(u)
    for u in (COT, N2, GH):
        for s in (0, 1):
            zag_sent(u, s)
    for s in (0, 1):
        rs_sent(FFN, s)
        rs_sent(DN1, s)
    g_out(3).wait()
    g_out(4).wait()
    for s in (0, 1):
        pltpu.make_async_copy(ybuf.at[s], out_h.at[s], osem.at[5 + s]).wait()
        pltpu.make_async_copy(dh.at[pl.ds(s * rows, rows)], gtok_h.at[s], osem.at[7 + s]).wait()
    last.wait()


def pad_heads(weight):
    depth = weight.shape[0]
    halves = weight.reshape(depth, -1, 2, HEAD // 2)
    return jnp.pad(halves, ((0, 0), (0, 0), (0, 0), (0, 64 - HEAD // 2))).reshape(depth, -1)


def cut_heads(grad):
    depth = grad.shape[0]
    return grad.reshape(depth, -1, 2, 64)[..., : HEAD // 2].reshape(depth, -1)


def fused(
    tokens,
    cotangent,
    order,
    lengths,
    gain_attn,
    w_query,
    w_key,
    w_value,
    w_out,
    gain_ffn,
    w_gate,
    w_up,
    w_down,
):
    micro, rows, width = tokens.shape
    seq = rows * lax.axis_size("tensor")
    shard = w_query.shape[0]
    ff = w_gate.shape[1]
    groups = w_key.shape[1] // HEAD
    w_in = pad_heads(jnp.concatenate([w_query, w_key, w_value], axis=1))
    qp = w_query.shape[1] // HEAD * LANES
    kp = groups * LANES
    inw = qp + 2 * kp
    w_back = pad_heads(w_out.T)
    gate_up = jnp.concatenate([w_gate, w_up], axis=1)
    gain = jnp.stack([gain_attn, gain_ffn], axis=0)
    low = jnp.pad(gain, ((0, 14), (0, shard)))
    high = jnp.pad(gain, ((0, 14), (shard, 0)))
    gain = jnp.where(lax.axis_index("dp") % 2 == 0, low, high)

    starts = jnp.cumsum(lengths, axis=1, dtype=jnp.int32) - lengths
    docs = jnp.sum((order[:, :, None] >= starts[:, None, 1:]).astype(jnp.int32), axis=2)
    onehot = docs[:, :, None] == jnp.arange(lengths.shape[1], dtype=jnp.int32)
    first = jnp.sum(jnp.where(onehot, starts[:, None, :], 0), axis=2)
    real = (docs < lengths.shape[1] - 1).astype(F32)
    cols = jnp.stack([order.astype(F32), first.astype(F32), real], axis=2)
    freqs = rope_base ** (-2.0 * jnp.arange(HEAD // 2, dtype=F32) / HEAD)
    angles = (order - first).astype(F32)[:, :, None] * freqs
    gap = ((0, 0), (0, 0), (0, 64 - HEAD // 2))
    cosine, sine = jnp.pad(jnp.cos(angles), gap), jnp.pad(jnp.sin(angles), gap)
    cosine = jnp.concatenate([cosine, cosine], axis=2)
    sine = jnp.concatenate([-sine, sine], axis=2)

    total = micro * seq
    vm = pltpu.VMEM
    dma = pltpu.SemaphoreType.DMA
    scratch = [
        vm((8 * 16, 2 * shard), BF),
        vm((width, inw), BF),
        vm((width, qp), BF),
        vm((width, 2 * ff), BF),
        vm((width, ff), BF),
        vm((total, width), BF),
        vm((total, width), BF),
        vm((total, width), BF),
        vm((total, width), BF),
        vm((total, inw), BF),
        vm((total, qp), BF),
        vm((total, qp), BF),
        vm((total, ff), BF),
        vm((total, inw), BF),
        vm((total, 2 * ff), BF),
        vm((micro * qp // LANES, seq, seq), F32),
        vm((micro * rows, width), F32),
        vm((micro * rows, width), F32),
        vm((total, width), BF),
        vm((total, width), BF),
        vm((micro, 2, 3, rows, width), BF),
        vm((micro, 2, 3, rows, width), BF),
        vm((2, width, ff), BF),
        vm((2, width // 2, ff), BF),
        vm((2, shard, ff), BF),
        vm((2, 2, shard, ff), BF),
        vm((2, shard, ff), F32),
        vm((rows, width), F32),
        vm((16, width), F32),
        vm((8, width), F32),
        vm((8, width // 4), F32),
        vm((11, 8, width // 4), F32),
        vm((micro, rows, width), BF),
        vm((micro, rows, width), BF),
        dma((5, 7)),
        dma((5, 7)),
        dma((4, 2, 2, 3)),
        dma((4, 2, 2, 3)),
        dma((4, 2, 2, 3)),
        dma((4, 2, 2, 3)),
        dma((5, 7)),
        dma((5, 7)),
        dma((10,)),
        dma((10,)),
        dma((12,)),
        dma((10,)),
        pltpu.SemaphoreType.REGULAR((3,)),
    ]
    hbm = pl.BlockSpec(memory_space=pl.ANY)
    vmem = pl.BlockSpec(memory_space=pltpu.VMEM)
    shapes = [
        jax.ShapeDtypeStruct((micro, rows, width), BF),
        jax.ShapeDtypeStruct((micro, rows, width), F32),
        jax.ShapeDtypeStruct((shard, ff), F32),
        jax.ShapeDtypeStruct((shard, ff), F32),
        jax.ShapeDtypeStruct((shard, ff), F32),
        jax.ShapeDtypeStruct((shard, qp), F32),
        jax.ShapeDtypeStruct((shard, inw), F32),
        jax.ShapeDtypeStruct((8, width // 4), F32),
    ]
    dims = (rows, seq, width, shard, qp, kp, ff, groups)
    out, gtok, gdown, ggate, gup, gout, gin, ggain = pl.pallas_call(
        functools.partial(block_kernel, dims),
        out_shape=shapes,
        in_specs=[hbm] * 7 + [vmem] * 4,
        out_specs=[hbm] * 8,
        scratch_shapes=scratch,
        compiler_params=pltpu.CompilerParams(
            collective_id=0, has_side_effects=True, vmem_limit_bytes=67_043_328
        ),
        name="block",
    )(
        tokens,
        cotangent,
        gain,
        w_in,
        w_back,
        gate_up,
        w_down.T,
        order.astype(F32)[:, None, :],
        cols,
        cosine,
        sine,
    )
    gains = ggain.reshape(2, width)
    gain_own = lax.dynamic_slice_in_dim(gains, lax.axis_index("dp") * shard, shard, 1)
    grads_in = cut_heads(gin)
    q_cols, k_cols = w_query.shape[1], w_key.shape[1]
    return (
        out,
        gtok,
        gain_own[0],
        grads_in[:, :q_cols],
        grads_in[:, q_cols : q_cols + k_cols],
        grads_in[:, q_cols + k_cols :],
        cut_heads(gout).T,
        gain_own[1],
        ggate,
        gup,
        gdown.T,
    )


def local(tokens, *rest):
    fits = lax.axis_size("dp") == 8 and lax.axis_size("tensor") == 4 and tokens.shape[0] == 2
    return (fused if fits else spread_out)(tokens, *rest)


def solution(mesh):
    return jax.shard_map(
        local,
        mesh=mesh,
        in_specs=(
            P("dp", "tensor", None),
            P("dp", "tensor", None),
            P("dp", None),
            P("dp", None),
            P("dp"),
            P("dp", "tensor"),
            P("dp", "tensor"),
            P("dp", "tensor"),
            P("tensor", "dp"),
            P("dp"),
            P("dp", "tensor"),
            P("dp", "tensor"),
            P("tensor", "dp"),
        ),
        out_specs=(
            P("dp", "tensor", None),
            P("dp", "tensor", None),
            P("dp"),
            P("dp", "tensor"),
            P("dp", "tensor"),
            P("dp", "tensor"),
            P("tensor", "dp"),
            P("dp"),
            P("dp", "tensor"),
            P("dp", "tensor"),
            P("tensor", "dp"),
        ),
        check_vma=False,
    )
```

```python
import functools
import math

import jax
import jax.numpy as jnp
from jax import lax
from jax.experimental import pallas as pl
from jax.experimental.pallas import tpu as pltpu
from jax.sharding import PartitionSpec as P

HEAD = 96


eps = 1e-05
rope_base = 100000.0


def rotate(field, cosine, sine):
    half = field.shape[-1] // 2
    first = field[..., :half]
    second = field[..., half:]
    return jnp.concatenate(
        [first * cosine - second * sine, second * cosine + first * sine], axis=-1
    )


def rotate_back(field, cosine, sine):
    half = field.shape[-1] // 2
    first = field[..., :half]
    second = field[..., half:]
    return jnp.concatenate(
        [first * cosine + second * sine, second * cosine - first * sine], axis=-1
    )


def layout(order, lengths):
    starts = jnp.cumsum(lengths, dtype=jnp.int32) - lengths
    docs = jnp.sum((order[:, None] >= starts[None, 1:]).astype(jnp.int32), axis=1, dtype=jnp.int32)
    onehot = docs[:, None] == jnp.arange(lengths.shape[0], dtype=jnp.int32)[None, :]
    first = jnp.sum(jnp.where(onehot, starts[None, :], 0), axis=1, dtype=jnp.int32)
    positions = (order - first).astype(jnp.float32)
    mask = (docs[:, None] == docs[None, :]) & (order[None, :] <= order[:, None])
    real = (docs < lengths.shape[0] - 1).astype(jnp.float32)
    return (positions, mask, real)


def norm_forward(rows, gain):
    scale = lax.rsqrt(jnp.mean(rows * rows, axis=-1, keepdims=True) + eps)
    unit = rows * scale
    return (unit, scale, (unit * gain).astype(jnp.bfloat16))


def norm_backward(grad, unit, scale, gain):
    inner = grad * gain
    return scale * (inner - unit * jnp.mean(inner * unit, axis=-1, keepdims=True))


def contract_rows(left, right):
    return lax.dot_general(
        left, right, (((0,), (0,)), ((), ())), preferred_element_type=jnp.float32
    )


def times_transpose(left, right):
    return lax.dot_general(
        left, right, (((1,), (1,)), ((), ())), preferred_element_type=jnp.float32
    )


def gather_weights(gain_attn, w_query, w_key, w_value, w_out, gain_ffn, w_gate, w_up, w_down):
    gains = lax.all_gather(jnp.stack([gain_attn, gain_ffn], axis=0), "dp", axis=1, tiled=True)
    attn = lax.all_gather(
        jnp.concatenate([w_query, w_key, w_value, w_out.T], axis=1), "dp", axis=0, tiled=True
    )
    gate_up = lax.all_gather(jnp.concatenate([w_gate, w_up], axis=1), "dp", axis=0, tiled=True)
    down = lax.all_gather(w_down.T, "dp", axis=0, tiled=True)
    return gains, attn, gate_up, down


def gather_rows(rows):
    return lax.all_gather(rows, "tensor", axis=1, tiled=True)


def scatter_rows(partial):
    low = partial.astype(jnp.bfloat16)
    return lax.psum_scatter(low, "tensor", scatter_dimension=1, tiled=True).astype(jnp.float32)


def reduce_weights(term):
    low = term.astype(jnp.bfloat16)
    return lax.psum_scatter(low, "dp", scatter_dimension=0, tiled=True).astype(jnp.float32)


def spread_out(
    tokens,
    cotangent,
    order,
    lengths,
    gain_attn,
    w_query,
    w_key,
    w_value,
    w_out,
    gain_ffn,
    w_gate,
    w_up,
    w_down,
):
    micro, rows, width = tokens.shape
    seq = rows * lax.axis_size("tensor")
    q_cols, k_cols, ff_cols = w_query.shape[1], w_key.shape[1], w_gate.shape[1]
    local_heads, local_kv = q_cols // HEAD, k_cols // HEAD
    group = local_heads // local_kv
    first_row = lax.axis_index("tensor") * rows
    freqs = rope_base ** (-2.0 * jnp.arange(HEAD // 2, dtype=jnp.float32) / HEAD)
    head_scale = HEAD ** (-0.5)

    gains, attn, gate_up, down = gather_weights(
        gain_attn, w_query, w_key, w_value, w_out, gain_ffn, w_gate, w_up, w_down
    )
    gain1, gain2 = gains[0].astype(jnp.float32), gains[1].astype(jnp.float32)
    in_cols = q_cols + 2 * k_cols
    w_in, w_out_t = attn[:, :in_cols], attn[:, in_cols:]

    positions, mask, real = jax.vmap(layout)(order, lengths)
    angles = positions[:, :, None] * freqs
    cosine, sine = jnp.cos(angles)[:, :, None, :], jnp.sin(angles)[:, :, None, :]
    mask = mask[:, None, None]
    real_rows = lax.dynamic_slice_in_dim(real, first_row, rows, 1)[:, :, None]

    stream = tokens.astype(jnp.float32)
    unit1, scale1, normed1 = norm_forward(stream, gain1)
    full1 = gather_rows(normed1)
    grad_out_rows = cotangent.astype(jnp.float32) * real_rows
    full_grad = gather_rows(grad_out_rows.astype(jnp.bfloat16))
    flat1 = full1.reshape(micro * seq, width)
    flat_grad = full_grad.reshape(micro * seq, width)

    mixed_in = jnp.dot(flat1, w_in, preferred_element_type=jnp.float32).reshape(micro, seq, in_cols)
    query = mixed_in[..., :q_cols].reshape(micro, seq, local_heads, HEAD)
    keys = mixed_in[..., q_cols : q_cols + k_cols].reshape(micro, seq, local_kv, HEAD)
    values = mixed_in[..., q_cols + k_cols :].reshape(micro, seq, local_kv, HEAD).astype(jnp.bfloat16)
    query = (rotate(query, cosine, sine) * head_scale).astype(jnp.bfloat16)
    query = query.reshape(micro, seq, local_kv, group, HEAD)
    keys = rotate(keys, cosine, sine).astype(jnp.bfloat16)
    scores = jnp.einsum("bqkgd,bskd->bkgqs", query, keys, preferred_element_type=jnp.float32)
    scores = jnp.where(mask, scores, -1e30)
    peak = jnp.max(scores, axis=-1, keepdims=True)
    expon = jnp.exp(scores - peak)
    total = jnp.sum(expon, axis=-1, keepdims=True)
    probs = expon / total
    probs_low = probs.astype(jnp.bfloat16)
    mixed = jnp.einsum("bkgqs,bskd->bqkgd", probs_low, values, preferred_element_type=jnp.float32)
    mixed = mixed.reshape(micro * seq, q_cols).astype(jnp.bfloat16)
    branch = scatter_rows(times_transpose(mixed, w_out_t).reshape(micro, seq, width))
    resid = stream + branch
    unit2, scale2, normed2 = norm_forward(resid, gain2)
    full2 = gather_rows(normed2).reshape(micro * seq, width)

    both = jnp.dot(full2, gate_up, preferred_element_type=jnp.float32)
    gate, upper = both[:, :ff_cols], both[:, ff_cols:]
    sigma = jax.nn.sigmoid(gate)
    hidden = (gate * sigma * upper).astype(jnp.bfloat16)
    ffn = scatter_rows(times_transpose(hidden, down).reshape(micro, seq, width))
    output = ((resid + ffn) * real_rows).astype(jnp.bfloat16)

    grad_hidden = jnp.dot(flat_grad, down, preferred_element_type=jnp.float32)
    grad_gate = (grad_hidden * upper * sigma * (1.0 + gate * (1.0 - sigma))).astype(jnp.bfloat16)
    grad_up = (grad_hidden * gate * sigma).astype(jnp.bfloat16)
    grad_both = jnp.concatenate([grad_gate, grad_up], axis=1)
    grad_norm2 = scatter_rows(times_transpose(grad_both, gate_up).reshape(micro, seq, width))
    final_down = reduce_weights(contract_rows(flat_grad, hidden))
    final_gate = reduce_weights(contract_rows(full2, grad_gate))
    final_up = reduce_weights(contract_rows(full2, grad_up))
    term_gain2 = jnp.sum(grad_norm2 * unit2, axis=(0, 1))
    grad_resid = grad_out_rows + norm_backward(grad_norm2, unit2, scale2, gain2)

    full_resid = gather_rows(grad_resid.astype(jnp.bfloat16)).reshape(micro * seq, width)
    grad_mixed = jnp.dot(full_resid, w_out_t, preferred_element_type=jnp.float32).astype(jnp.bfloat16)
    final_out = reduce_weights(contract_rows(full_resid, mixed))
    grad_heads = grad_mixed.reshape(micro, seq, local_kv, group, HEAD)
    grad_probs = jnp.einsum(
        "bqkgd,bskd->bkgqs", grad_heads, values, preferred_element_type=jnp.float32
    )
    grad_values = jnp.einsum(
        "bkgqs,bqkgd->bskd", probs_low, grad_heads, preferred_element_type=jnp.float32
    )
    grad_scores = (
        probs * (grad_probs - jnp.sum(probs * grad_probs, axis=-1, keepdims=True))
    ).astype(jnp.bfloat16)
    grad_query = jnp.einsum(
        "bkgqs,bskd->bqkgd", grad_scores, keys, preferred_element_type=jnp.float32
    ).reshape(micro, seq, local_heads, HEAD)
    grad_keys = jnp.einsum(
        "bkgqs,bqkgd->bskd", grad_scores, query, preferred_element_type=jnp.float32
    )
    grad_query = rotate_back(grad_query * head_scale, cosine, sine).reshape(micro * seq, q_cols)
    grad_keys = rotate_back(grad_keys, cosine, sine).reshape(micro * seq, k_cols)
    grad_values = grad_values.reshape(micro * seq, k_cols)
    grad_in = jnp.concatenate(
        [grad_query.astype(jnp.bfloat16), grad_keys.astype(jnp.bfloat16), grad_values.astype(jnp.bfloat16)],
        axis=1,
    )
    grad_norm1 = scatter_rows(times_transpose(grad_in, w_in).reshape(micro, seq, width))
    final_in = reduce_weights(contract_rows(flat1, grad_in))
    term_gain1 = jnp.sum(grad_norm1 * unit1, axis=(0, 1))
    grad_tokens = grad_resid + norm_backward(grad_norm1, unit1, scale1, gain1)

    gain_terms = lax.psum(jnp.stack([term_gain1, term_gain2], axis=0), ("dp", "tensor"))
    own = gain_attn.shape[0]
    gain_own = lax.dynamic_slice_in_dim(gain_terms, lax.axis_index("dp") * own, own, 1)
    return (
        output,
        grad_tokens,
        gain_own[0],
        final_in[:, :q_cols],
        final_in[:, q_cols : q_cols + k_cols],
        final_in[:, q_cols + k_cols :],
        final_out.T,
        gain_own[1],
        final_gate,
        final_up,
        final_down.T,
    )


BF = jnp.bfloat16
F32 = jnp.float32
MESH = pl.DeviceIdType.MESH
LANES = 128


def nn(left, right):
    return lax.dot_general(left, right, (((1,), (0,)), ((), ())), preferred_element_type=F32)


def nt(left, right):
    return lax.dot_general(left, right, (((1,), (1,)), ((), ())), preferred_element_type=F32)


def tn(left, right):
    return lax.dot_general(left, right, (((0,), (0,)), ((), ())), preferred_element_type=F32)


def al(value, unit):
    return pl.multiple_of(value, unit)


def block_kernel(dims, *refs):
    (rows, seq, width, shard, qp, kp, ff, groups) = dims
    (tok, cot, wg_h, wq_h, wk_h, wv_h, wo_h, wa_h, wb_h, wd_h, ordr, lens) = refs[:12]
    (out_h, gtok_h, gdown_h, ggate_h, gup_h, gout_h, gin_h, ggain_h) = refs[12:20]
    (wgn, wi, wo, wu, wd, xf, n1, n2, gf, qkv, ob, dob, act, dq3, dgu, pr, hb, dh, pa, pb, ra, rb,
     gb, xb, hop, fin, stage, acc, gains, gpart, gsum, gex, ybuf, tbuf,
     wsend, wrecv, zsend, zrecv, rsend, rrecv, gsend, grecv, esend, erecv, lsem, osem, credit, psem, rq, rk, rv, ro, cols, cosr, sinr) = refs[20:]
    ghf = xf
    heads = qp // LANES
    per_group = heads // groups
    inw = qp + 2 * kp
    pair = 2 * shard
    d = lax.axis_index("dp")
    z = lax.axis_index("tensor")
    c = d % 2
    flip = 1 - 2 * c
    near_x = d + 2 - 4 * ((d // 2) % 2)
    near_y = d + 4 - 8 * (d // 4)
    aa = near_x * (1 - c) + near_y * c
    bb = near_y * (1 - c) + near_x * c
    dd = aa + bb - d
    pp = d + flip
    chip_own, chip_a, chip_b, chip_d = d // 2, aa // 2, bb // 2, dd // 2
    chip_x, chip_y = near_x // 2, near_y // 2
    own = 1 * z * rows
    zdev = {"tensor": z + 1}, {"tensor": z - 1}

    def rcopy(src, dst, ssem, rsem, dev):
        return pltpu.make_async_remote_copy(
            src_ref=src, dst_ref=dst, send_sem=ssem, recv_sem=rsem, device_id=dev, device_id_type=MESH
        )

    barrier = pltpu.get_barrier_semaphore()
    for step in range(1, 8):
        pl.semaphore_signal(barrier, inc=1, device_id={"dp": (d + step) % 8}, device_id_type=MESH)
    for step in (1, 2, 3):
        pl.semaphore_signal(
            barrier, inc=1, device_id={"tensor": (z + step) % 4}, device_id_type=MESH
        )

    def raw_copy(i):
        src, dst = (
            (wq_h, rq),
            (wk_h, rk),
            (wv_h, rv),
            (wo_h, ro),
            (wd_h, wd.at[pl.ds(al(shard * d, 16), shard), :]),
            (wa_h, wu.at[pl.ds(al(shard * d, 16), shard), pl.ds(0, ff)]),
            (wb_h, wu.at[pl.ds(al(shard * d, 16), shard), pl.ds(ff, ff)]),
        )[i]
        return pltpu.make_async_copy(src, dst, psem.at[i])

    def head_map(n):
        row = lax.broadcasted_iota(jnp.int32, (n // HEAD * HEAD, n // HEAD * LANES), 0)
        col = lax.broadcasted_iota(jnp.int32, (n // HEAD * HEAD, n // HEAD * LANES), 1)
        lane = col % 64
        want = (col // 64) * (HEAD // 2) + lane
        return jnp.where((lane < HEAD // 2) & (row == want), 1.0, 0.0).astype(BF)

    def prep_in():
        at = pl.ds(al(shard * d, 16), shard)
        for i in range(3):
            raw_copy(i).wait()
        wide = head_map(rq.shape[1])
        narrow = head_map(rk.shape[1])
        wi[at, pl.ds(0, qp)] = nn(rq[...], wide).astype(BF)
        wi[at, pl.ds(qp, kp)] = nn(rk[...], narrow).astype(BF)
        wi[at, pl.ds(qp + kp, kp)] = nn(rv[...], narrow).astype(BF)

    def prep_out():
        raw_copy(3).wait()
        wo[pl.ds(al(shard * d, 16), shard), :] = nn(ro[...], head_map(ro.shape[1])).astype(BF)

    def prep_rows(s):
        row = lax.broadcasted_iota(jnp.int32, (seq, seq), 0)
        col = lax.broadcasted_iota(jnp.int32, (seq, seq), 1)
        same = jnp.where(row == col, 1.0, 0.0).astype(BF)
        mid = seq // 2
        packed = (ordr[s : s + 1, :] - mid).astype(F32)
        place = nt(same, jnp.broadcast_to(packed, (LANES, seq)).astype(BF)) + mid
        start = lens[s, 0]
        first = jnp.zeros((seq, LANES), F32)
        for n in range(1, lens.shape[1]):
            begin = start.astype(F32)
            first = jnp.where(place >= begin, begin, first)
            real = jnp.where(place >= begin, 0.0, 1.0)
            start = start + lens[s, n]
        lane = lax.broadcasted_iota(jnp.int32, (seq, LANES), 1)
        cols[s] = jnp.where(lane == 0, place, jnp.where(lane == 1, first, real))
        one = lax.broadcasted_iota(jnp.int32, (8, LANES), 1)
        field = one % 64
        freqs = jnp.exp((-2.0 * math.log(rope_base) / HEAD) * field.astype(F32))
        freqs = jnp.where(field < HEAD // 2, freqs, 0.0)[0:1, :]
        angles = (place - first) * freqs
        cosr[s] = jnp.cos(angles)
        sine = jnp.sin(angles)
        sinr[s] = jnp.where(lane < 64, -sine, sine)

    wunits = (
        (wgn, 16, 0, pair),
        (wi, shard, 0, inw),
        (wo, shard, 0, qp),
        (wu, shard, 0, ff),
        (wu, shard, ff, ff),
        (wd, shard, 0, ff),
    )

    def wblk(u, i):
        ref, n, at, cut = wunits[u]
        return ref.at[pl.ds(al(n * i, 16), n), pl.ds(at, cut)]

    def w_start(u):
        src = wblk(u, d)
        if u == 0:
            src = wg_h
            pltpu.make_async_copy(src, wblk(u, d), lsem.at[u]).start()
        if u >= 3:
            raw_copy((5, 6, 4)[u - 3]).wait()
        rcopy(src, wblk(u, d), wsend.at[u, 0], wrecv.at[u, 0], {"dp": aa}).start()
        rcopy(src, wblk(u, d), wsend.at[u, 1], wrecv.at[u, 1], {"dp": bb}).start()
        rcopy(src, wblk(u, d), wsend.at[u, 2], wrecv.at[u, 3], {"dp": pp}).start()

    def w_wait(u, slot, i):
        rcopy(wblk(u, i), wblk(u, i), wsend.at[u, 0], wrecv.at[u, slot], {"dp": aa}).wait_recv()

    def w_relayb(u):
        w_wait(u, 1, bb)
        rcopy(wblk(u, bb), wblk(u, bb), wsend.at[u, 3], wrecv.at[u, 2], {"dp": aa}).start()
        rcopy(wblk(u, bb), wblk(u, bb), wsend.at[u, 4], wrecv.at[u, 5], {"dp": pp}).start()

    def w_relaya(u):
        w_wait(u, 0, aa)
        rcopy(wblk(u, aa), wblk(u, aa), wsend.at[u, 5], wrecv.at[u, 4], {"dp": pp}).start()

    def w_diag(u):
        w_wait(u, 2, dd)
        rcopy(wblk(u, dd), wblk(u, dd), wsend.at[u, 6], wrecv.at[u, 6], {"dp": pp}).start()

    def w_done(u):
        w_wait(u, 3, pp)
        w_wait(u, 4, bb + flip)
        w_wait(u, 5, aa + flip)
        w_wait(u, 6, dd + flip)
        if u == 0:
            pltpu.make_async_copy(wg_h, wblk(u, d), lsem.at[u]).wait()

    def w_sent(u):
        for slot in range(7):
            rcopy(wblk(u, d), wblk(u, d), wsend.at[u, slot], wrecv.at[u, 0], {"dp": aa}).wait_send()

    zfull = (xf, gf, n2, ghf)
    zhbm = (tok, cot, None, None)

    def zblk(u, s, i):
        return zfull[u].at[pl.ds(al(s * seq + i * rows, 16), rows)]

    def zag_send(u, s, k, way):
        i = z - k if way == 0 else z + k
        go = (z < 3) & (i >= 0) if way == 0 else (z > 0) & (i <= 3)

        @pl.when(go)
        def _():
            src = zhbm[u].at[s] if k == 0 and zhbm[u] is not None else zblk(u, s, i)
            rcopy(src, zblk(u, s, i), zsend.at[u, s, way, k], zrecv.at[u, s, way, k], zdev[way]).start()

    def zag_recv(u, s, k, way):
        i = z - 1 - k if way == 0 else z + 1 + k
        go = (i >= 0) if way == 0 else (i <= 3)

        @pl.when(go)
        def _():
            rcopy(
                zblk(u, s, i), zblk(u, s, i), zsend.at[u, s, way, k], zrecv.at[u, s, way, k], zdev[way]
            ).wait_recv()

    def zag_start(u, s):
        if zhbm[u] is not None:
            pltpu.make_async_copy(zhbm[u].at[s], zblk(u, s, z), lsem.at[8 + 2 * u + s]).start()
        for way in (0, 1):
            zag_send(u, s, 0, way)

    def ag(u, s, t, way=None):
        if t == 0:
            zag_start(u, s)
            return
        zag_recv(u, s, t - 1, way)
        if t < 3:
            zag_send(u, s, t, way)

    def own_here(u, s):
        pltpu.make_async_copy(zhbm[u].at[s], zblk(u, s, z), lsem.at[8 + 2 * u + s]).wait()

    def zag_sent(u, s):
        for k in range(3):
            for way in (0, 1):
                i = z - k if way == 0 else z + k
                go = (z < 3) & (i >= 0) if way == 0 else (z > 0) & (i <= 3)

                @pl.when(go)
                def _():
                    rcopy(
                        zblk(u, s, i), zblk(u, s, i), zsend.at[u, s, way, k], zrecv.at[u, s, way, k], zdev[way]
                    ).wait_send()

    zpart = (pa, pb, pa, pa)
    zgot = (ra, rb, ra, ra)

    def rs_copy(u, s, way, t, dest):
        return rcopy(
            zpart[u].at[pl.ds(al(s * seq + dest * rows, 16), rows)],
            zgot[u].at[s, way, t],
            rsend.at[u, s, way, t],
            rrecv.at[u, s, way, t],
            zdev[way],
        )

    def rs(u, s, t, ways=(0, 1)):
        for way in ways:
            from_end = z if way == 0 else 3 - z

            def wait_and(target, base):
                rs_copy(u, s, way, t - 1, z).wait_recv()

                def body(i, carry):
                    at = pl.ds(al(base + i * 16, 16), 16)
                    got = zgot[u][s, way, t - 1, pl.ds(al(i * 16, 16), 16), :].astype(F32)
                    target[at, :] = (target[at, :].astype(F32) + got).astype(target.dtype)
                    return carry

                lax.fori_loop(0, rows // 16, body, 0)

            if t == 3:
                if way == 0:
                    def first(i, carry):
                        at = pl.ds(al(i * 16, 16), 16)
                        acc[at, :] = zpart[u][pl.ds(al(s * seq + own + i * 16, 16), 16), :].astype(F32)
                        return carry

                    lax.fori_loop(0, rows // 16, first, 0)

                @pl.when(from_end > 0)
                def _():
                    wait_and(acc, 0)
            else:
                dest = 3 + z - t if way == 0 else t - from_end

                @pl.when(from_end <= t)
                def _():
                    if t > 0:
                        @pl.when(from_end > 0)
                        def _():
                            wait_and(zpart[u], s * seq + dest * rows)

                    rs_copy(u, s, way, t, dest).start()

    def rs_sent(u, s):
        for way in (0, 1):
            from_end = z if way == 0 else 3 - z
            for t in range(3):
                @pl.when(from_end <= t)
                def _():
                    rs_copy(u, s, way, t, z).wait_send()

    gunits = (
        (gf, act, 0, ff, gdown_h),
        (n2, dgu, 0, ff, ggate_h),
        (n2, dgu, ff, ff, gup_h),
        (ghf, ob, 0, qp, gout_h),
        (n1, dq3, 0, inw, gin_h),
    )
    def xslot(u, chip):
        b, n = u % 2, gunits[u][3]
        return xb.at[b, pl.ds(al(chip * shard, 16), shard), pl.ds(0, n)]

    def gslot(u, chip, core):
        b, n = u % 2, gunits[u][3]
        return gb.at[b, pl.ds(al(chip * pair + core * shard, 16), shard), pl.ds(0, n)]

    def g_exchange(u, chip, i):
        return rcopy(gslot(u, chip, 1 - c), xslot(u, chip), gsend.at[u, i], grecv.at[u, i], {"dp": pp})

    chips = (chip_d, chip_x, chip_y, chip_own)

    def g_compute(u, i):
        left, right, at, n, _ = gunits[u]
        chip = chips[i]
        if u >= 2 and i == 0:
            pl.semaphore_wait(credit.at[0], 1)
        tile = 256

        def body(j, carry):
            lhs = left[:, pl.ds(al(chip * pair, LANES), pair)]
            got = tn(lhs, right[:, pl.ds(al(at + j * tile, tile), tile)])
            gb[u % 2, pl.ds(al(chip * pair, 16), pair), pl.ds(al(j * tile, tile), tile)] = got.astype(BF)
            return carry

        lax.fori_loop(0, n // tile, body, 0)
        g_exchange(u, chip, i).start()

    def g_add(u, chip, extra=None):
        b, n = u % 2, gunits[u][3]

        def body(i, carry):
            at = pl.ds(al(chip * shard + i * 16, 16), 16)
            mine = gb[b, pl.ds(al(chip * pair + c * shard + i * 16, 16), 16), pl.ds(0, n)].astype(F32)
            total = mine + xb[b, at, pl.ds(0, n)].astype(F32)
            if extra is not None:
                total = total + extra[b, pl.ds(al(i * 16, 16), 16), pl.ds(0, n)].astype(F32)
            xb[b, at, pl.ds(0, n)] = total.astype(BF)
            return carry

        lax.fori_loop(0, shard // 16, body, 0)

    def g_hop(u):
        b, n = u % 2, gunits[u][3]
        return rcopy(xslot(u, chip_d), hop.at[b, :, pl.ds(0, n)], gsend.at[u, 4], grecv.at[u, 4], {"dp": aa})

    def g_last(u, way):
        b, n = u % 2, gunits[u][3]
        chip, dev = (chip_a, aa) if way == 0 else (chip_b, bb)
        return rcopy(
            xslot(u, chip), fin.at[b, way, :, pl.ds(0, n)], gsend.at[u, 5 + way], grecv.at[u, 5 + way], {"dp": dev}
        )

    def g_first(u):
        g_exchange(u, chip_d, 0).wait_recv()
        g_add(u, chip_d)
        if u >= 2:
            pl.semaphore_wait(credit.at[1], 1)
        g_hop(u).start()

    def g_firstb(u):
        g_exchange(u, chip_x, 1).wait_recv()
        g_exchange(u, chip_y, 2).wait_recv()
        g_add(u, chip_a)
        g_last(u, 0).start()

    def g_second(u):
        g_hop(u).wait_recv()
        g_add(u, chip_b, hop)
        if u >= 2:
            pl.semaphore_wait(credit.at[2], 1)
        g_last(u, 1).start()

    def g_finish(u):
        b, n, out = u % 2, gunits[u][3], gunits[u][4]
        g_exchange(u, chip_own, 3).wait_recv()
        g_last(u, 0).wait_recv()
        g_last(u, 1).wait_recv()

        def body(i, carry):
            at = pl.ds(al(i * 16, 16), 16)
            total = gb[b, pl.ds(al(chip_own * pair + c * shard + i * 16, 16), 16), pl.ds(0, n)].astype(F32)
            total = total + xb[b, pl.ds(al(chip_own * shard + i * 16, 16), 16), pl.ds(0, n)].astype(F32)
            total = total + fin[b, 0, at, pl.ds(0, n)].astype(F32)
            stage[b, at, pl.ds(0, n)] = total + fin[b, 1, at, pl.ds(0, n)].astype(F32)
            return carry

        if u >= 2:
            g_out(u - 2).wait()
        lax.fori_loop(0, shard // 16, body, 0)
        g_out(u).start()
        for i in range(4):
            g_exchange(u, chips[i], i).wait_send()
        g_hop(u).wait_send()
        g_last(u, 0).wait_send()
        g_last(u, 1).wait_send()
        if u < 3:
            pl.semaphore_signal(credit.at[0], inc=1, device_id={"dp": pp}, device_id_type=MESH)
            pl.semaphore_signal(credit.at[1], inc=1, device_id={"dp": aa}, device_id_type=MESH)
            pl.semaphore_signal(credit.at[2], inc=1, device_id={"dp": bb}, device_id_type=MESH)

    def g_out(u):
        b, n, out = u % 2, gunits[u][3], gunits[u][4]
        return pltpu.make_async_copy(stage.at[b, :, pl.ds(0, n)], out, osem.at[u])

    def gain_rows():
        for j in range(4):
            at = pl.ds(j * pair, pair)
            gains[:, at] = (
                wgn[pl.ds(32 * j, 16), :].astype(F32) + wgn[pl.ds(32 * j + 16, 16), :].astype(F32)
            )

    def norm1(s, t):
        gain = gains[0:1, :]

        def shard_rows(i):
            def body(r, carry):
                at = pl.ds(al(s * seq + i * rows + r * 16, 16), 16)
                x = xf[at, :].astype(F32)
                scale = lax.rsqrt(jnp.mean(x * x, axis=-1, keepdims=True) + eps)
                n1[at, :] = (x * scale * gain).astype(BF)
                return carry

            lax.fori_loop(0, rows // 16, body, 0)

        if t == 0:
            own_here(0, s)
            shard_rows(z)
            return

        @pl.when(z - t >= 0)
        def _():
            shard_rows(z - t)

        @pl.when(z + t <= 3)
        def _():
            shard_rows(z + t)

    head_scale = HEAD ** (-0.5)

    def project(s):
        at = pl.ds(s * seq, seq)
        cosine, sine = cosr[s], sinr[s]
        for j in range(inw // 256):
            both = nn(n1[at, :], wi[:, pl.ds(j * 256, 256)])
            for half in range(2):
                col = j * 256 + half * LANES
                part = both[:, half * LANES : (half + 1) * LANES]
                if col < qp + kp:
                    part = part * cosine + pltpu.roll(part, LANES // 2, 1) * sine
                if col < qp:
                    part = part * head_scale
                qkv[at, pl.ds(col, LANES)] = part.astype(BF)

    def attend(s, part):
        at = pl.ds(s * seq, seq)
        oc = ordr[s : s + 1, :].astype(F32)
        mask = (oc <= cols[s, :, 0:1]) & (oc >= cols[s, :, 1:2])

        def body(h, carry):
            g = h // per_group
            q = qkv[at, pl.ds(al(h * LANES, LANES), LANES)]
            k = qkv[at, pl.ds(al(qp + g * LANES, LANES), LANES)]
            v = qkv[at, pl.ds(al(qp + kp + g * LANES, LANES), LANES)]
            sc = jnp.where(mask, nt(q, k), -1e30)
            e = jnp.exp(sc - jnp.max(sc, axis=-1, keepdims=True))
            p = e * (1.0 / jnp.sum(e, axis=-1, keepdims=True))
            pr[s * heads + h] = p
            ob[at, pl.ds(al(h * LANES, LANES), LANES)] = nn(p.astype(BF), v).astype(BF)
            return carry

        half = heads // 2
        lax.fori_loop(part * half, (part + 1) * half, body, 0)

    def spread(s, dst, left, weight, tile, part=0, parts=1):
        at = pl.ds(s * seq, seq)

        def body(j, carry):
            col = al(j * tile, tile)
            dst[at, pl.ds(col, tile)] = nt(left[at, :], weight[pl.ds(col, tile), :]).astype(BF)
            return carry

        count = width // tile // parts
        lax.fori_loop(part * count, (part + 1) * count, body, 0)

    def spread_gain(s):
        at = pl.ds(s * seq, seq)
        tile = 512

        def body(j, carry):
            col = pl.ds(al(j * tile, tile), tile)
            got = nt(dq3[at, :], wi[col, :])
            pa[at, col] = got.astype(BF)
            gpart[0:1, col] += jnp.sum(got * n1[at, col].astype(F32), axis=0, keepdims=True)
            return carry

        lax.fori_loop(0, width // tile, body, 0)

    def norm2(s):
        gain = gains[1:2, :]
        base = s * rows

        def body(i, carry):
            r = pl.ds(al(i * 16, 16), 16)
            h = tbuf[s, r, :].astype(F32) + acc[r, :]
            hb[pl.ds(al(base + i * 16, 16), 16), :] = h
            scale = lax.rsqrt(jnp.mean(h * h, axis=-1, keepdims=True) + eps)
            n2[pl.ds(al(s * seq + own + i * 16, 16), 16), :] = (h * scale * gain).astype(BF)
            return carry

        lax.fori_loop(0, rows // 16, body, 0)

    def feed(s, part):
        at = pl.ds(s * seq, seq)
        real = cols[s, :, 2:3]
        if part == 0:
            own_here(1, s)

        def body(t, carry):
            col = al(t * 256, 256)
            gate = nn(n2[at, :], wu[:, pl.ds(col, 256)])
            upper = nn(n2[at, :], wu[:, pl.ds(al(ff + t * 256, 256), 256)])
            back = nn(gf[at, :], wd[:, pl.ds(col, 256)]) * real
            sigma = 1.0 / (1.0 + jnp.exp(-gate))
            swish = gate * sigma
            act[at, pl.ds(col, 256)] = (swish * upper * real).astype(BF)
            dgu[at, pl.ds(col, 256)] = (back * upper * sigma * (1.0 + gate * (1.0 - sigma))).astype(BF)
            dgu[at, pl.ds(al(ff + t * 256, 256), 256)] = (back * swish).astype(BF)
            return carry

        count = ff // 256 // 4
        lax.fori_loop(part * count, (part + 1) * count, body, 0)

    def finish_out(s):
        def body(i, carry):
            r = pl.ds(al(i * 16, 16), 16)
            real = cols[s, pl.ds(al(own + i * 16, 16), 16), 2:3]
            y = (hb[pl.ds(al(s * rows + i * 16, 16), 16), :] + acc[r, :]) * real
            ybuf[s, r, :] = y.astype(BF)
            return carry

        lax.fori_loop(0, rows // 16, body, 0)
        pltpu.make_async_copy(ybuf.at[s], out_h.at[s], osem.at[5 + s]).start()

    def norm2_back(s):
        gain = gains[1:2, :]

        def body(i, carry):
            r = pl.ds(al(i * 16, 16), 16)
            ro = pl.ds(al(s * rows + i * 16, 16), 16)
            h = hb[ro, :]
            scale = lax.rsqrt(jnp.mean(h * h, axis=-1, keepdims=True) + eps)
            unit = h * scale
            grad = acc[r, :]
            inner = grad * gain
            dy = gf[pl.ds(al(s * seq + own + i * 16, 16), 16), :].astype(F32)
            dy = dy * cols[s, pl.ds(al(own + i * 16, 16), 16), 2:3]
            dhr = dy + scale * (inner - unit * jnp.mean(inner * unit, axis=-1, keepdims=True))
            dh[ro, :] = dhr
            ghf[pl.ds(al(s * seq + own + i * 16, 16), 16), :] = dhr.astype(BF)
            return carry + jnp.sum(grad * unit, axis=0, keepdims=True)

        gpart[1:2, :] += lax.fori_loop(0, rows // 16, body, jnp.zeros((1, width), F32))

    def grad_heads(s):
        at = pl.ds(s * seq, seq)
        for j in range(qp // 256):
            dob[at, pl.ds(j * 256, 256)] = nn(ghf[at, :], wo[:, pl.ds(j * 256, 256)]).astype(BF)

    def attend_back(s):
        at = pl.ds(s * seq, seq)
        cosine, sine = cosr[s], sinr[s]

        def body(g, carry):
            k = qkv[at, pl.ds(al(qp + g * LANES, LANES), LANES)]
            v = qkv[at, pl.ds(al(qp + kp + g * LANES, LANES), LANES)]
            dk = jnp.zeros((seq, LANES), F32)
            dv = jnp.zeros((seq, LANES), F32)
            for m in range(per_group):
                h = g * per_group + m
                hat = pl.ds(al(h * LANES, LANES), LANES)
                q = qkv[at, hat]
                do = dob[at, hat]
                p = pr[s * heads + h]
                dp = nt(do, v)
                ds = (p * (dp - jnp.sum(p * dp, axis=-1, keepdims=True))).astype(BF)
                dv = dv + tn(p.astype(BF), do)
                dk = dk + tn(ds, q)
                dq = nn(ds, k) * head_scale
                dq3[at, hat] = (dq * cosine - pltpu.roll(dq, LANES // 2, 1) * sine).astype(BF)
            dq3[at, pl.ds(al(qp + g * LANES, LANES), LANES)] = (
                dk * cosine - pltpu.roll(dk, LANES // 2, 1) * sine
            ).astype(BF)
            dq3[at, pl.ds(al(qp + kp + g * LANES, LANES), LANES)] = dv.astype(BF)
            return carry

        lax.fori_loop(0, groups, body, 0)

    def norm1_back(s):
        gain = gains[0:1, :]

        def body(i, carry):
            r = pl.ds(al(i * 16, 16), 16)
            ro = pl.ds(al(s * rows + i * 16, 16), 16)
            x = tbuf[s, r, :].astype(F32)
            scale = lax.rsqrt(jnp.mean(x * x, axis=-1, keepdims=True) + eps)
            unit = x * scale
            grad = acc[r, :]
            inner = grad * gain
            dh[ro, :] = dh[ro, :] + scale * (inner - unit * jnp.mean(inner * unit, axis=-1, keepdims=True))
            return carry

        lax.fori_loop(0, rows // 16, body, 0)
        pltpu.make_async_copy(
            dh.at[pl.ds(s * rows, rows)], gtok_h.at[s], osem.at[7 + s]
        ).start()

    X, COT, N2, GH = 0, 1, 2, 3
    BR, FFN, DN2, DN1 = 0, 1, 2, 3

    def tok_copy(s):
        return pltpu.make_async_copy(tok.at[s], tbuf.at[s], lsem.at[5 + s])

    def fin_br(s):
        rs(BR, s, 3)
        tok_copy(s).wait()
        norm2(s)
        ag(N2, s, 0)

    def fin_dn2(s):
        rs(DN2, s, 3)
        norm2_back(s)
        ag(GH, s, 0)

    def fin_ffn(s):
        rs(FFN, s, 3)
        finish_out(s)

    def fin_dn1(s):
        rs(DN1, s, 3)
        norm1_back(s)

    def e_copy(i):
        dev = {"tensor": (z + i + 1) % 4} if i < 3 else {"dp": (d + i - 2) % 8}
        return rcopy(gsum if i < 3 else gex.at[10], gex.at[i], esend.at[i], erecv.at[i], dev)

    def e1s():
        for j in range(4):
            at = pl.ds(j * pair, pair)
            gsum[j : j + 1, :] = gpart[0:1, at] / gains[0:1, at]
            gsum[4 + j : 5 + j, :] = gpart[1:2, j * pair : (j + 1) * pair]
        for i in range(3):
            e_copy(i).start()

    def e1w():
        for i in range(3):
            e_copy(i).wait()
        gex[10] = gsum[...] + gex[0] + gex[1] + gex[2]
        for i in range(3, 10):
            e_copy(i).start()

    def e2w():
        for i in range(3, 10):
            e_copy(i).wait()
        total = gex[10]
        for i in range(3, 10):
            total = total + gex[i]
        gsum[...] = total

    for i in range(7):
        raw_copy(i).start()
    gpart[...] = jnp.zeros_like(gpart)
    for s in (0, 1):
        tok_copy(s).start()
    pl.semaphore_wait(barrier, 10)
    ag(X, 0, 0)
    ag(X, 1, 0)
    prep_out()
    prep_in()
    w_start(0)
    w_start(1)
    w_start(2)
    ag(X, 0, 1, 1)
    w_relayb(0)
    prep_rows(0)
    ag(X, 0, 1, 0)
    ag(COT, 0, 0)
    w_relaya(1)
    w_relayb(2)
    ag(X, 0, 2, 0)
    prep_rows(1)
    ag(X, 1, 1, 0)
    w_relaya(2)
    w_relayb(1)
    w_diag(0)
    w_diag(2)
    w_relaya(0)
    ag(X, 0, 2, 1)
    w_done(0)
    gain_rows()
    ag(X, 1, 1, 1)
    norm1(0, 0)
    w_start(3)
    ag(COT, 0, 1, 0)
    norm1(1, 0)
    norm1(0, 2)
    norm1(0, 1)
    ag(COT, 1, 0)
    w_diag(1)
    ag(X, 0, 3, 0)
    ag(X, 0, 3, 1)
    w_done(1)
    norm1(0, 3)
    project(0)
    attend(0, 0)
    attend(0, 1)
    w_start(4)
    ag(COT, 0, 1, 1)
    w_start(5)
    ag(X, 1, 2, 1)
    w_done(2)
    spread(0, pa, ob, wo, 512)
    rs(BR, 0, 0, (0,))
    rs(BR, 0, 1, (0,))
    ag(X, 1, 2, 0)
    rs(BR, 0, 0, (1,))
    rs(BR, 0, 1, (1,))
    rs(BR, 0, 2, (1,))
    norm1(1, 2)
    rs(BR, 0, 2, (0,))
    ag(COT, 0, 2, 0)
    ag(COT, 0, 2, 1)
    ag(X, 1, 3, 0)
    ag(X, 1, 3, 1)
    norm1(1, 3)
    w_relayb(3)
    norm1(1, 1)
    w_relayb(4)
    fin_br(0)
    project(1)
    w_relayb(5)
    w_relaya(4)
    rs_sent(BR, 0)
    attend(1, 0)
    attend(1, 1)
    w_relaya(3)
    spread(1, pa, ob, wo, 512)
    rs(BR, 1, 0, (1,))
    rs(BR, 1, 0, (0,))
    w_diag(3)
    zag_sent(X, 0)
    ag(COT, 0, 3, 0)
    w_relaya(5)
    ag(N2, 0, 1, 1)
    w_done(3)
    ag(N2, 0, 1, 0)
    w_diag(5)
    rs(BR, 1, 1, (1,))
    rs(BR, 1, 1, (0,))
    ag(N2, 0, 2, 1)
    ag(N2, 0, 2, 0)
    w_diag(4)
    w_done(4)
    ag(COT, 0, 3, 1)
    rs(BR, 1, 2, (1,))
    ag(N2, 0, 3, 1)
    w_done(5)
    rs(BR, 1, 2, (0,))
    ag(N2, 0, 3, 0)
    ag(COT, 1, 1, 0)
    feed(0, 0)
    feed(0, 1)
    feed(0, 2)
    ag(COT, 1, 1, 1)
    fin_br(1)
    feed(0, 3)
    spread(0, pa, dgu, wu, 256, 0, 2)
    spread(0, pa, dgu, wu, 256, 1, 2)
    rs(DN2, 0, 0, (1,))
    ag(COT, 1, 2, 0)
    rs(DN2, 0, 0, (0,))
    spread(0, pb, act, wd, 512)
    rs_sent(BR, 1)
    ag(N2, 1, 1, 1)
    ag(N2, 1, 1, 0)
    rs(DN2, 0, 1, (0,))
    ag(N2, 1, 2, 1)
    rs(DN2, 0, 1, (1,))
    rs(FFN, 0, 0, (1,))
    rs(FFN, 0, 0, (0,))
    ag(COT, 1, 2, 1)
    rs(DN2, 0, 2, (1,))
    zag_sent(X, 1)
    ag(N2, 1, 2, 0)
    rs(DN2, 0, 2, (0,))
    ag(COT, 1, 3, 0)
    rs(FFN, 0, 1, (1,))
    ag(COT, 1, 3, 1)
    ag(N2, 1, 3, 1)
    ag(N2, 1, 3, 0)
    feed(1, 0)
    rs(FFN, 0, 1, (0,))
    feed(1, 1)
    feed(1, 2)
    feed(1, 3)
    fin_dn2(0)
    spread(1, pa, dgu, wu, 256, 0, 2)
    spread(1, pa, dgu, wu, 256, 1, 2)
    rs(DN2, 1, 0, (1,))
    g_compute(0, 0)
    rs(DN2, 1, 0, (0,))
    g_compute(0, 1)
    g_compute(0, 2)
    ag(GH, 0, 1, 0)
    g_first(0)
    ag(GH, 0, 1, 1)
    g_compute(0, 3)
    rs(DN2, 1, 1, (0,))
    rs(DN2, 1, 1, (1,))
    g_firstb(0)
    ag(GH, 0, 2, 1)
    ag(GH, 0, 2, 0)
    g_compute(1, 0)
    rs(DN2, 1, 2, (0,))
    rs(DN2, 1, 2, (1,))
    g_compute(1, 1)
    spread(1, pb, act, wd, 512)
    rs(FFN, 1, 0, (0,))
    ag(GH, 0, 3, 0)
    g_second(0)
    rs(FFN, 1, 0, (1,))
    ag(GH, 0, 3, 1)
    g_compute(1, 2)
    g_first(1)
    fin_dn2(1)
    rs_sent(DN2, 0)
    g_firstb(1)
    grad_heads(0)
    attend_back(0)
    spread_gain(0)
    g_finish(0)
    rs(DN1, 0, 0, (1,))
    rs(DN1, 0, 0, (0,))
    ag(GH, 1, 1, 0)
    ag(GH, 1, 1, 1)
    rs(FFN, 1, 1, (0,))
    g_compute(1, 3)
    g_second(1)
    g_compute(2, 0)
    g_compute(2, 1)
    rs(FFN, 1, 1, (1,))
    ag(GH, 1, 2, 0)
    rs(DN1, 0, 1, (1,))
    ag(GH, 1, 2, 1)
    g_first(2)
    rs(DN1, 0, 1, (0,))
    rs_sent(DN2, 1)
    g_compute(2, 2)
    g_compute(2, 3)
    rs(FFN, 1, 2, (0,))
    g_finish(1)
    g_firstb(2)
    rs(FFN, 0, 2, (1,))
    ag(GH, 1, 3, 0)
    g_second(2)
    ag(GH, 1, 3, 1)
    g_compute(3, 0)
    grad_heads(1)
    attend_back(1)
    spread_gain(1)
    rs(DN1, 1, 0, (0,))
    g_compute(3, 1)
    g_first(3)
    rs(DN1, 1, 0, (1,))
    g_compute(3, 2)
    g_compute(3, 3)
    rs(FFN, 1, 2, (1,))
    e1s()
    g_firstb(3)
    rs(FFN, 0, 2, (0,))
    g_finish(2)
    g_compute(4, 0)
    g_second(3)
    rs(DN1, 1, 1, (1,))
    g_compute(4, 1)
    rs(DN1, 1, 1, (0,))
    rs(DN1, 0, 2, (0,))
    rs(DN1, 0, 2, (1,))
    g_first(4)
    g_compute(4, 2)
    g_compute(4, 3)
    fin_ffn(1)
    g_firstb(4)
    g_second(4)
    fin_ffn(0)
    rs(DN1, 1, 2, (1,))
    rs(DN1, 1, 2, (0,))
    g_finish(3)
    fin_dn1(0)
    e1w()
    g_finish(4)
    e2w()
    fin_dn1(1)
    last = pltpu.make_async_copy(gsum, ggain_h, osem.at[9])
    last.start()
    for u in range(6):
        w_sent(u)
    for u in (COT, N2, GH):
        for s in (0, 1):
            zag_sent(u, s)
    for s in (0, 1):
        rs_sent(FFN, s)
        rs_sent(DN1, s)
    g_out(3).wait()
    g_out(4).wait()
    for s in (0, 1):
        pltpu.make_async_copy(ybuf.at[s], out_h.at[s], osem.at[5 + s]).wait()
        pltpu.make_async_copy(dh.at[pl.ds(s * rows, rows)], gtok_h.at[s], osem.at[7 + s]).wait()
    last.wait()


def finish_kernel(dims, *refs):
    (qp, kp, shard) = dims
    ins, outs, bufs, (sem_in, sem_out) = refs[:8], refs[8:19], refs[19:33], refs[33:]
    given, made = bufs[:8], bufs[8:]
    d = lax.axis_index("dp")

    def load(i):
        return pltpu.make_async_copy(ins[i], given[i], sem_in.at[i])

    def save(i, src):
        return pltpu.make_async_copy(src, outs[i], sem_out.at[i])

    def head_map(n):
        row = lax.broadcasted_iota(jnp.int32, (n, n // HEAD * LANES), 0)
        col = lax.broadcasted_iota(jnp.int32, (n, n // HEAD * LANES), 1)
        lane = col % 64
        want = (col // 64) * (HEAD // 2) + lane
        return jnp.where((lane < HEAD // 2) & (row == want), 1.0, 0.0).astype(BF)

    def picked(value, which):
        high = value.astype(BF)
        rest = value - high.astype(F32)
        mid = rest.astype(BF)
        low = (rest - mid.astype(F32)).astype(BF)
        return nt(high, which) + (nt(mid, which) + nt(low, which))

    order = (1, 2, 0, 3, 4, 5, 6, 7)
    for i in order:
        load(i).start()
    ggain, gin, gout = given[:3]
    tone, ttwo, tq, tk, tv, tout = made
    wide, narrow = head_map(tq.shape[1]), head_map(tk.shape[1])
    load(1).wait()
    tq[...] = picked(gin[:, :qp], wide)
    save(2, tq).start()
    tk[...] = picked(gin[:, qp : qp + kp], narrow)
    save(3, tk).start()
    tv[...] = picked(gin[:, qp + kp :], narrow)
    save(4, tv).start()
    load(2).wait()
    tout[...] = picked(gout[...], wide)
    save(5, tout).start()
    load(0).wait()
    for i, ref in enumerate((tone, ttwo)):
        line = ggain[pl.ds(4 * i + d // 2, 1), :]
        ref[...] = jnp.where(d % 2 == 0, line[:, :shard], line[:, shard:])
        save(i, ref).start()
    for i in range(3, 8):
        load(i).wait()
        save(i + 3, given[i]).start()
    for i, ref in enumerate(made):
        save(i, ref).wait()
    for i in range(3, 8):
        save(i + 3, given[i]).wait()


def fused(
    tokens,
    cotangent,
    order,
    lengths,
    gain_attn,
    w_query,
    w_key,
    w_value,
    w_out,
    gain_ffn,
    w_gate,
    w_up,
    w_down,
):
    micro, rows, width = tokens.shape
    seq = rows * lax.axis_size("tensor")
    shard = w_query.shape[0]
    ff = w_gate.shape[1]
    groups = w_key.shape[1] // HEAD
    q_cols, k_cols = w_query.shape[1], w_key.shape[1]
    qp = q_cols // HEAD * LANES
    kp = groups * LANES
    inw = qp + 2 * kp
    even = lax.axis_index("dp") % 2 == 0

    def placed(gain):
        return jnp.where(even, jnp.pad(gain, (0, shard)), jnp.pad(gain, (shard, 0)))[None, :]

    line = lax.broadcasted_iota(jnp.int32, (16, 2 * shard), 0)
    gain = jnp.where(line == 0, placed(gain_attn), placed(gain_ffn))

    total = micro * seq
    vm = pltpu.VMEM
    dma = pltpu.SemaphoreType.DMA
    scratch = [
        vm((8 * 16, 2 * shard), BF),
        vm((width, inw), BF),
        vm((width, qp), BF),
        vm((width, 2 * ff), BF),
        vm((width, ff), BF),
        vm((total, width), BF),
        vm((total, width), BF),
        vm((total, width), BF),
        vm((total, width), BF),
        vm((total, inw), BF),
        vm((total, qp), BF),
        vm((total, qp), BF),
        vm((total, ff), BF),
        vm((total, inw), BF),
        vm((total, 2 * ff), BF),
        vm((micro * qp // LANES, seq, seq), F32),
        vm((micro * rows, width), F32),
        vm((micro * rows, width), F32),
        vm((total, width), BF),
        vm((total, width), BF),
        vm((micro, 2, 3, rows, width), BF),
        vm((micro, 2, 3, rows, width), BF),
        vm((2, width, ff), BF),
        vm((2, width // 2, ff), BF),
        vm((2, shard, ff), BF),
        vm((2, 2, shard, ff), BF),
        vm((2, shard, ff), F32),
        vm((rows, width), F32),
        vm((16, width), F32),
        vm((8, width), F32),
        vm((8, width // 4), F32),
        vm((11, 8, width // 4), F32),
        vm((micro, rows, width), BF),
        vm((micro, rows, width), BF),
        dma((6, 7)),
        dma((6, 7)),
        dma((4, 2, 2, 3)),
        dma((4, 2, 2, 3)),
        dma((4, 2, 2, 3)),
        dma((4, 2, 2, 3)),
        dma((5, 7)),
        dma((5, 7)),
        dma((10,)),
        dma((10,)),
        dma((12,)),
        dma((10,)),
        pltpu.SemaphoreType.REGULAR((3,)),
        dma((7,)),
        vm(w_query.shape, BF),
        vm(w_key.shape, BF),
        vm(w_value.shape, BF),
        vm(w_out.shape[::-1], BF),
        vm((micro, seq, LANES), F32),
        vm((micro, seq, LANES), F32),
        vm((micro, seq, LANES), F32),
    ]
    hbm = pl.BlockSpec(memory_space=pl.ANY)
    vmem = pl.BlockSpec(memory_space=pltpu.VMEM)
    smem = pl.BlockSpec(memory_space=pltpu.SMEM)
    shape = jax.ShapeDtypeStruct
    shapes = [
        shape((micro, rows, width), BF),
        shape((micro, rows, width), F32),
        shape((shard, ff), F32),
        shape((shard, ff), F32),
        shape((shard, ff), F32),
        shape((shard, qp), F32),
        shape((shard, inw), F32),
        shape((8, width // 4), F32),
    ]
    dims = (rows, seq, width, shard, qp, kp, ff, groups)
    out, gtok, gdown, ggate, gup, gout, gin, ggain = pl.pallas_call(
        functools.partial(block_kernel, dims),
        out_shape=shapes,
        in_specs=[hbm] * 10 + [vmem, smem],
        out_specs=[hbm] * 8,
        scratch_shapes=scratch,
        compiler_params=pltpu.CompilerParams(
            collective_id=0, has_side_effects=True, vmem_limit_bytes=67_043_328
        ),
        name="block",
    )(
        tokens,
        cotangent,
        gain,
        w_query,
        w_key,
        w_value,
        w_out.T,
        w_gate,
        w_up,
        w_down.T,
        order,
        lengths,
    )
    made = [
        shape((1, shard), F32),
        shape((1, shard), F32),
        shape((shard, q_cols), F32),
        shape((shard, k_cols), F32),
        shape((shard, k_cols), F32),
        shape((shard, q_cols), F32),
    ]
    given = [ggain, gin, gout, out, gtok, ggate, gup, gdown]
    one, two, gq, gk, gv, gout, out, gtok, ggate, gup, gdown = pl.pallas_call(
        functools.partial(finish_kernel, (qp, kp, shard)),
        out_shape=made + [shape(x.shape, x.dtype) for x in given[3:]],
        in_specs=[hbm] * 8,
        out_specs=[hbm] * 11,
        scratch_shapes=[vm(x.shape, x.dtype) for x in given + made] + [dma((8,)), dma((11,))],
        name="finish",
    )(*given)
    return out, gtok, one[0], gq, gk, gv, gout.T, two[0], ggate, gup, gdown.T


def local(tokens, *rest):
    fits = lax.axis_size("dp") == 8 and lax.axis_size("tensor") == 4 and tokens.shape[0] == 2
    return (fused if fits else spread_out)(tokens, *rest)


def solution(mesh):
    return jax.shard_map(
        local,
        mesh=mesh,
        in_specs=(
            P("dp", "tensor", None),
            P("dp", "tensor", None),
            P("dp", None),
            P("dp", None),
            P("dp"),
            P("dp", "tensor"),
            P("dp", "tensor"),
            P("dp", "tensor"),
            P("tensor", "dp"),
            P("dp"),
            P("dp", "tensor"),
            P("dp", "tensor"),
            P("tensor", "dp"),
        ),
        out_specs=(
            P("dp", "tensor", None),
            P("dp", "tensor", None),
            P("dp"),
            P("dp", "tensor"),
            P("dp", "tensor"),
            P("dp", "tensor"),
            P("tensor", "dp"),
            P("dp"),
            P("dp", "tensor"),
            P("dp", "tensor"),
            P("tensor", "dp"),
        ),
        check_vma=False,
    )
```

```python
import functools
import math

import jax
import jax.numpy as jnp
from jax import lax
from jax.experimental import pallas as pl
from jax.experimental.pallas import tpu as pltpu
from jax.sharding import PartitionSpec as P

HEAD = 96


eps = 1e-05
rope_base = 100000.0


def rotate(field, cosine, sine):
    half = field.shape[-1] // 2
    first = field[..., :half]
    second = field[..., half:]
    return jnp.concatenate(
        [first * cosine - second * sine, second * cosine + first * sine], axis=-1
    )


def rotate_back(field, cosine, sine):
    half = field.shape[-1] // 2
    first = field[..., :half]
    second = field[..., half:]
    return jnp.concatenate(
        [first * cosine + second * sine, second * cosine - first * sine], axis=-1
    )


def layout(order, lengths):
    starts = jnp.cumsum(lengths, dtype=jnp.int32) - lengths
    docs = jnp.sum((order[:, None] >= starts[None, 1:]).astype(jnp.int32), axis=1, dtype=jnp.int32)
    onehot = docs[:, None] == jnp.arange(lengths.shape[0], dtype=jnp.int32)[None, :]
    first = jnp.sum(jnp.where(onehot, starts[None, :], 0), axis=1, dtype=jnp.int32)
    positions = (order - first).astype(jnp.float32)
    mask = (docs[:, None] == docs[None, :]) & (order[None, :] <= order[:, None])
    real = (docs < lengths.shape[0] - 1).astype(jnp.float32)
    return (positions, mask, real)


def norm_forward(rows, gain):
    scale = lax.rsqrt(jnp.mean(rows * rows, axis=-1, keepdims=True) + eps)
    unit = rows * scale
    return (unit, scale, (unit * gain).astype(jnp.bfloat16))


def norm_backward(grad, unit, scale, gain):
    inner = grad * gain
    return scale * (inner - unit * jnp.mean(inner * unit, axis=-1, keepdims=True))


def contract_rows(left, right):
    return lax.dot_general(
        left, right, (((0,), (0,)), ((), ())), preferred_element_type=jnp.float32
    )


def times_transpose(left, right):
    return lax.dot_general(
        left, right, (((1,), (1,)), ((), ())), preferred_element_type=jnp.float32
    )


def gather_weights(gain_attn, w_query, w_key, w_value, w_out, gain_ffn, w_gate, w_up, w_down):
    gains = lax.all_gather(jnp.stack([gain_attn, gain_ffn], axis=0), "dp", axis=1, tiled=True)
    attn = lax.all_gather(
        jnp.concatenate([w_query, w_key, w_value, w_out.T], axis=1), "dp", axis=0, tiled=True
    )
    gate_up = lax.all_gather(jnp.concatenate([w_gate, w_up], axis=1), "dp", axis=0, tiled=True)
    down = lax.all_gather(w_down.T, "dp", axis=0, tiled=True)
    return gains, attn, gate_up, down


def gather_rows(rows):
    return lax.all_gather(rows, "tensor", axis=1, tiled=True)


def scatter_rows(partial):
    low = partial.astype(jnp.bfloat16)
    return lax.psum_scatter(low, "tensor", scatter_dimension=1, tiled=True).astype(jnp.float32)


def reduce_weights(term):
    low = term.astype(jnp.bfloat16)
    return lax.psum_scatter(low, "dp", scatter_dimension=0, tiled=True).astype(jnp.float32)


def spread_out(
    tokens,
    cotangent,
    order,
    lengths,
    gain_attn,
    w_query,
    w_key,
    w_value,
    w_out,
    gain_ffn,
    w_gate,
    w_up,
    w_down,
):
    micro, rows, width = tokens.shape
    seq = rows * lax.axis_size("tensor")
    q_cols, k_cols, ff_cols = w_query.shape[1], w_key.shape[1], w_gate.shape[1]
    local_heads, local_kv = q_cols // HEAD, k_cols // HEAD
    group = local_heads // local_kv
    first_row = lax.axis_index("tensor") * rows
    freqs = rope_base ** (-2.0 * jnp.arange(HEAD // 2, dtype=jnp.float32) / HEAD)
    head_scale = HEAD ** (-0.5)

    gains, attn, gate_up, down = gather_weights(
        gain_attn, w_query, w_key, w_value, w_out, gain_ffn, w_gate, w_up, w_down
    )
    gain1, gain2 = gains[0].astype(jnp.float32), gains[1].astype(jnp.float32)
    in_cols = q_cols + 2 * k_cols
    w_in, w_out_t = attn[:, :in_cols], attn[:, in_cols:]

    positions, mask, real = jax.vmap(layout)(order, lengths)
    angles = positions[:, :, None] * freqs
    cosine, sine = jnp.cos(angles)[:, :, None, :], jnp.sin(angles)[:, :, None, :]
    mask = mask[:, None, None]
    real_rows = lax.dynamic_slice_in_dim(real, first_row, rows, 1)[:, :, None]

    stream = tokens.astype(jnp.float32)
    unit1, scale1, normed1 = norm_forward(stream, gain1)
    full1 = gather_rows(normed1)
    grad_out_rows = cotangent.astype(jnp.float32) * real_rows
    full_grad = gather_rows(grad_out_rows.astype(jnp.bfloat16))
    flat1 = full1.reshape(micro * seq, width)
    flat_grad = full_grad.reshape(micro * seq, width)

    mixed_in = jnp.dot(flat1, w_in, preferred_element_type=jnp.float32).reshape(micro, seq, in_cols)
    query = mixed_in[..., :q_cols].reshape(micro, seq, local_heads, HEAD)
    keys = mixed_in[..., q_cols : q_cols + k_cols].reshape(micro, seq, local_kv, HEAD)
    values = mixed_in[..., q_cols + k_cols :].reshape(micro, seq, local_kv, HEAD).astype(jnp.bfloat16)
    query = (rotate(query, cosine, sine) * head_scale).astype(jnp.bfloat16)
    query = query.reshape(micro, seq, local_kv, group, HEAD)
    keys = rotate(keys, cosine, sine).astype(jnp.bfloat16)
    scores = jnp.einsum("bqkgd,bskd->bkgqs", query, keys, preferred_element_type=jnp.float32)
    scores = jnp.where(mask, scores, -1e30)
    peak = jnp.max(scores, axis=-1, keepdims=True)
    expon = jnp.exp(scores - peak)
    total = jnp.sum(expon, axis=-1, keepdims=True)
    probs = expon / total
    probs_low = probs.astype(jnp.bfloat16)
    mixed = jnp.einsum("bkgqs,bskd->bqkgd", probs_low, values, preferred_element_type=jnp.float32)
    mixed = mixed.reshape(micro * seq, q_cols).astype(jnp.bfloat16)
    branch = scatter_rows(times_transpose(mixed, w_out_t).reshape(micro, seq, width))
    resid = stream + branch
    unit2, scale2, normed2 = norm_forward(resid, gain2)
    full2 = gather_rows(normed2).reshape(micro * seq, width)

    both = jnp.dot(full2, gate_up, preferred_element_type=jnp.float32)
    gate, upper = both[:, :ff_cols], both[:, ff_cols:]
    sigma = jax.nn.sigmoid(gate)
    hidden = (gate * sigma * upper).astype(jnp.bfloat16)
    ffn = scatter_rows(times_transpose(hidden, down).reshape(micro, seq, width))
    output = ((resid + ffn) * real_rows).astype(jnp.bfloat16)

    grad_hidden = jnp.dot(flat_grad, down, preferred_element_type=jnp.float32)
    grad_gate = (grad_hidden * upper * sigma * (1.0 + gate * (1.0 - sigma))).astype(jnp.bfloat16)
    grad_up = (grad_hidden * gate * sigma).astype(jnp.bfloat16)
    grad_both = jnp.concatenate([grad_gate, grad_up], axis=1)
    grad_norm2 = scatter_rows(times_transpose(grad_both, gate_up).reshape(micro, seq, width))
    final_down = reduce_weights(contract_rows(flat_grad, hidden))
    final_gate = reduce_weights(contract_rows(full2, grad_gate))
    final_up = reduce_weights(contract_rows(full2, grad_up))
    term_gain2 = jnp.sum(grad_norm2 * unit2, axis=(0, 1))
    grad_resid = grad_out_rows + norm_backward(grad_norm2, unit2, scale2, gain2)

    full_resid = gather_rows(grad_resid.astype(jnp.bfloat16)).reshape(micro * seq, width)
    grad_mixed = jnp.dot(full_resid, w_out_t, preferred_element_type=jnp.float32).astype(jnp.bfloat16)
    final_out = reduce_weights(contract_rows(full_resid, mixed))
    grad_heads = grad_mixed.reshape(micro, seq, local_kv, group, HEAD)
    grad_probs = jnp.einsum(
        "bqkgd,bskd->bkgqs", grad_heads, values, preferred_element_type=jnp.float32
    )
    grad_values = jnp.einsum(
        "bkgqs,bqkgd->bskd", probs_low, grad_heads, preferred_element_type=jnp.float32
    )
    grad_scores = (
        probs * (grad_probs - jnp.sum(probs * grad_probs, axis=-1, keepdims=True))
    ).astype(jnp.bfloat16)
    grad_query = jnp.einsum(
        "bkgqs,bskd->bqkgd", grad_scores, keys, preferred_element_type=jnp.float32
    ).reshape(micro, seq, local_heads, HEAD)
    grad_keys = jnp.einsum(
        "bkgqs,bqkgd->bskd", grad_scores, query, preferred_element_type=jnp.float32
    )
    grad_query = rotate_back(grad_query * head_scale, cosine, sine).reshape(micro * seq, q_cols)
    grad_keys = rotate_back(grad_keys, cosine, sine).reshape(micro * seq, k_cols)
    grad_values = grad_values.reshape(micro * seq, k_cols)
    grad_in = jnp.concatenate(
        [grad_query.astype(jnp.bfloat16), grad_keys.astype(jnp.bfloat16), grad_values.astype(jnp.bfloat16)],
        axis=1,
    )
    grad_norm1 = scatter_rows(times_transpose(grad_in, w_in).reshape(micro, seq, width))
    final_in = reduce_weights(contract_rows(flat1, grad_in))
    term_gain1 = jnp.sum(grad_norm1 * unit1, axis=(0, 1))
    grad_tokens = grad_resid + norm_backward(grad_norm1, unit1, scale1, gain1)

    gain_terms = lax.psum(jnp.stack([term_gain1, term_gain2], axis=0), ("dp", "tensor"))
    own = gain_attn.shape[0]
    gain_own = lax.dynamic_slice_in_dim(gain_terms, lax.axis_index("dp") * own, own, 1)
    return (
        output,
        grad_tokens,
        gain_own[0],
        final_in[:, :q_cols],
        final_in[:, q_cols : q_cols + k_cols],
        final_in[:, q_cols + k_cols :],
        final_out.T,
        gain_own[1],
        final_gate,
        final_up,
        final_down.T,
    )


BF = jnp.bfloat16
F32 = jnp.float32
MESH = pl.DeviceIdType.MESH
LANES = 128


def nn(left, right):
    return lax.dot_general(left, right, (((1,), (0,)), ((), ())), preferred_element_type=F32)


def nt(left, right):
    return lax.dot_general(left, right, (((1,), (1,)), ((), ())), preferred_element_type=F32)


def tn(left, right):
    return lax.dot_general(left, right, (((0,), (0,)), ((), ())), preferred_element_type=F32)


def al(value, unit):
    return pl.multiple_of(value, unit)


def block_kernel(dims, *refs):
    (rows, seq, width, shard, qp, kp, ff, groups) = dims
    (tok, cot, ga_h, gf_h, wq_h, wk_h, wv_h, wo_h, wa_h, wb_h, wd_h, ordr, lens) = refs[:13]
    (out_v, gtok_v, gdown_v, ggate_v, gup_v, gout_v, gq_v, gk_v, gv_v, gone_v, gtwo_v) = refs[13:24]
    (wgn, wi, wo, wu, wd, xf, n1, n2, gf, qkv, ob, act, dq3, dgu, pr, hb, pa, pb, ra, rb,
     gb, xb, hop, fin, stage, acc, gains, gpart, gsum, gex, tbuf, rga, rgf, rq, rk, rv, ro, cols, cosr, sinr,
     wsend, wrecv, zsend, zrecv, rsend, rrecv, gsend, grecv, esend, erecv, lsem, psem, credit) = refs[24:]
    ghf = xf
    heads = qp // LANES
    per_group = heads // groups
    inw = qp + 2 * kp
    pair = 2 * shard
    d = lax.axis_index("dp")
    z = lax.axis_index("tensor")
    c = d % 2
    flip = 1 - 2 * c
    near_x = d + 2 - 4 * ((d // 2) % 2)
    near_y = d + 4 - 8 * (d // 4)
    aa = near_x * (1 - c) + near_y * c
    bb = near_y * (1 - c) + near_x * c
    dd = aa + bb - d
    pp = d + flip
    chip_own, chip_a, chip_b, chip_d = d // 2, aa // 2, bb // 2, dd // 2
    chip_x, chip_y = near_x // 2, near_y // 2
    own = z * rows
    half = width
    zdev = {"tensor": z + 1}, {"tensor": z - 1}

    def rcopy(src, dst, ssem, rsem, dev):
        return pltpu.make_async_remote_copy(
            src_ref=src, dst_ref=dst, send_sem=ssem, recv_sem=rsem, device_id=dev, device_id_type=MESH
        )

    barrier = pltpu.get_barrier_semaphore()
    for dev in (pp, aa, bb):
        pl.semaphore_signal(barrier, inc=1, device_id={"dp": dev}, device_id_type=MESH)
    for way in (0, 1):
        @pl.when((z < 3) if way == 0 else (z > 0))
        def _():
            pl.semaphore_signal(barrier, inc=1, device_id=zdev[way], device_id_type=MESH)

    def raw_copy(i):
        src, dst = (
            (wq_h, rq),
            (wk_h, rk),
            (wv_h, rv),
            (wo_h, ro),
            (wd_h, wd.at[pl.ds(al(shard * d, 16), shard), :]),
            (wa_h, wu.at[pl.ds(al(shard * d, 16), shard), pl.ds(0, ff)]),
            (wb_h, wu.at[pl.ds(al(shard * d, 16), shard), pl.ds(ff, ff)]),
            (ga_h, rga),
            (gf_h, rgf),
        )[i]
        return pltpu.make_async_copy(src, dst, psem.at[i])

    def head_map(n):
        row = lax.broadcasted_iota(jnp.int32, (n // HEAD * HEAD, n // HEAD * LANES), 0)
        col = lax.broadcasted_iota(jnp.int32, (n // HEAD * HEAD, n // HEAD * LANES), 1)
        lane = col % 64
        want = (col // 64) * (HEAD // 2) + lane
        return jnp.where((lane < HEAD // 2) & (row == want), 1.0, 0.0).astype(BF)

    head_pick = head_map

    def prep_gain():
        raw_copy(7).wait()
        raw_copy(8).wait()
        line = lax.broadcasted_iota(jnp.int32, (16, shard), 0)
        one = jnp.broadcast_to(rga[...].reshape(1, shard).astype(F32), (16, shard))
        two = jnp.broadcast_to(rgf[...].reshape(1, shard).astype(F32), (16, shard))
        row = lax.broadcasted_iota(jnp.int32, (shard, pair), 0)
        col = lax.broadcasted_iota(jnp.int32, (shard, pair), 1)
        place = jnp.where(col == row + shard * c, 1.0, 0.0).astype(BF)
        both = jnp.where(line == 0, one, two).astype(BF)
        wgn[pl.ds(al(16 * d, 16), 16), :] = nn(both, place).astype(BF)

    def prep_in():
        at = pl.ds(al(shard * d, 16), shard)
        for i in range(3):
            raw_copy(i).wait()
        wide = head_map(rq.shape[1])
        narrow = head_map(rk.shape[1])
        wi[at, pl.ds(0, qp)] = nn(rq[...], wide).astype(BF)
        wi[at, pl.ds(qp, kp)] = nn(rk[...], narrow).astype(BF)
        wi[at, pl.ds(qp + kp, kp)] = nn(rv[...], narrow).astype(BF)

    def prep_out():
        raw_copy(3).wait()
        wo[pl.ds(al(shard * d, 16), shard), :] = nn(ro[...], head_map(ro.shape[1])).astype(BF)

    def prep_rows(s):
        row = lax.broadcasted_iota(jnp.int32, (seq, seq), 0)
        col = lax.broadcasted_iota(jnp.int32, (seq, seq), 1)
        same = jnp.where(row == col, 1.0, 0.0).astype(BF)
        mid = seq // 2
        packed = (ordr[s : s + 1, :] - mid).astype(F32)
        place = nt(same, jnp.broadcast_to(packed, (LANES, seq)).astype(BF)) + mid
        start = lens[s, 0]
        first = jnp.zeros((seq, LANES), F32)
        for n in range(1, lens.shape[1]):
            begin = start.astype(F32)
            first = jnp.where(place >= begin, begin, first)
            real = jnp.where(place >= begin, 0.0, 1.0)
            start = start + lens[s, n]
        lane = lax.broadcasted_iota(jnp.int32, (seq, LANES), 1)
        cols[s] = jnp.where(lane == 0, place, jnp.where(lane == 1, first, real))
        one = lax.broadcasted_iota(jnp.int32, (8, LANES), 1)
        field = one % 64
        freqs = jnp.exp((-2.0 * math.log(rope_base) / HEAD) * field.astype(F32))
        freqs = jnp.where(field < HEAD // 2, freqs, 0.0)[0:1, :]
        angles = (place - first) * freqs
        cosr[s] = jnp.cos(angles)
        sine = jnp.sin(angles)
        sinr[s] = jnp.where(lane < 64, -sine, sine)

    wunits = (
        (wgn, 16, 0, pair),
        (wi, shard, 0, inw),
        (wo, shard, 0, qp),
        (wu, shard, 0, ff),
        (wu, shard, ff, ff),
        (wd, shard, 0, ff),
    )

    def wblk(u, i):
        ref, n, at, cut = wunits[u]
        return ref.at[pl.ds(al(n * i, 16), n), pl.ds(at, cut)]

    def w_start(u):
        src = wblk(u, d)
        if u >= 3:
            raw_copy((5, 6, 4)[u - 3]).wait()
        rcopy(src, src, wsend.at[u], wrecv.at[u, 0], {"dp": aa}).start()
        rcopy(src, src, wsend.at[u], wrecv.at[u, 1], {"dp": bb}).start()
        rcopy(src, src, wsend.at[u], wrecv.at[u, 3], {"dp": pp}).start()

    def w_many(u, count):
        ref, n, at, cut = wunits[u]
        part = ref.at[pl.ds(0, count * n), pl.ds(at, cut)]
        return rcopy(part, part, wsend.at[u], wrecv.at[u, 3], {"dp": pp})

    def w_wait(u, slot, i):
        rcopy(wblk(u, i), wblk(u, i), wsend.at[u], wrecv.at[u, slot], {"dp": aa}).wait_recv()

    def w_relayb(u):
        w_wait(u, 1, bb)
        rcopy(wblk(u, bb), wblk(u, bb), wsend.at[u], wrecv.at[u, 2], {"dp": aa}).start()
        rcopy(wblk(u, bb), wblk(u, bb), wsend.at[u], wrecv.at[u, 3], {"dp": pp}).start()

    def w_relaya(u):
        w_wait(u, 0, aa)
        rcopy(wblk(u, aa), wblk(u, aa), wsend.at[u], wrecv.at[u, 3], {"dp": pp}).start()

    def w_diag(u):
        w_wait(u, 2, dd)
        rcopy(wblk(u, dd), wblk(u, dd), wsend.at[u], wrecv.at[u, 3], {"dp": pp}).start()

    def w_done(u):
        w_many(u, 4).wait_recv()

    def w_sent(u):
        w_many(u, 7).wait_send()

    zfull = (xf, gf, n2, ghf)
    zhbm = (tok, cot, None, None)

    def zblk(u, s, i, h=None):
        at = pl.ds(al(s * seq + i * rows, 16), rows)
        return zfull[u].at[at] if h is None else zfull[u].at[at, pl.ds(h * half, half)]

    def zcopy(u, s, k, way, h, i, src=None):
        blk = zblk(u, s, i, h)
        return rcopy(
            blk if src is None else src, blk, zsend.at[u, s], zrecv.at[u % 3, s, way, k], zdev[way]
        )

    def zag_send(u, s, k, way, h):
        i = z - k if way == 0 else z + k
        go = (z < 3) & (i >= 0) if way == 0 else (z > 0) & (i <= 3)

        @pl.when(go)
        def _():
            src = zhbm[u].at[s, :, pl.ds(h * half, half)] if k == 0 and zhbm[u] is not None else None
            zcopy(u, s, k, way, h, i, src).start()

    def own_copy(u, s):
        return pltpu.make_async_copy(zhbm[u].at[s], zblk(u, s, z), lsem.at[2 + 2 * u + s])

    def ag(u, s, t, way=None, h=0):
        if t == 0:
            if zhbm[u] is not None:
                own_copy(u, s).start()
            for part in (0,):
                for side in (0, 1):
                    zag_send(u, s, 0, side, part)
            return
        i = z - t if way == 0 else z + t
        go = (i >= 0) if way == 0 else (i <= 3)

        @pl.when(go)
        def _():
            zcopy(u, s, t - 1, way, h, i).wait_recv()

        if t < 3:
            zag_send(u, s, t, way, h)

    def own_here(u, s):
        own_copy(u, s).wait()

    def zag_sent(u, s):
        def sent(count):
            part = zfull[u].at[pl.ds(0, count * rows)]
            rcopy(part, part, zsend.at[u, s], zrecv.at[u % 3, s, 0, 0], zdev[0]).wait_send()

        @pl.when((z == 0) | (z == 3))
        def _():
            sent(1)

        @pl.when((z > 0) & (z < 3))
        def _():
            sent(5)

    zpart = (pa, pb, pa, pa)
    zgot = (ra, rb, ra, ra)

    def rs_copy(u, s, way, t, dest, h):
        cut = pl.ds(h * half, half)
        return rcopy(
            zpart[u].at[pl.ds(al(s * seq + dest * rows, 16), rows), cut],
            zgot[u].at[s, way, t, :, cut],
            rsend.at[u, s],
            rrecv.at[1 if u == 1 else 0, s, way, t],
            zdev[way],
        )

    def rs_add(u, s, way, t, target, base, cut):
        def body(i, carry):
            at = pl.ds(al(base + i * 16, 16), 16)
            got = zgot[u][s, way, t, pl.ds(al(i * 16, 16), 16), cut].astype(F32)
            target[at, cut] = (target[at, cut].astype(F32) + got).astype(target.dtype)
            return carry

        lax.fori_loop(0, rows // 16, body, 0)

    def rs(u, s, t, way, h=0):
        from_end = z if way == 0 else 3 - z
        dest = 3 + z - t if way == 0 else t - from_end

        @pl.when(from_end <= t)
        def _():
            if t > 0:
                @pl.when(from_end > 0)
                def _():
                    rs_copy(u, s, way, t - 1, z, h).wait_recv()
                    rs_add(u, s, way, t - 1, zpart[u], s * seq + dest * rows, pl.ds(h * half, half))

            rs_copy(u, s, way, t, dest, h).start()

    def rs_final(u, s):
        def first(i, carry):
            at = pl.ds(al(i * 16, 16), 16)
            acc[at, :] = zpart[u][pl.ds(al(s * seq + own + i * 16, 16), 16), :].astype(F32)
            return carry

        lax.fori_loop(0, rows // 16, first, 0)
        for way in (0, 1):
            from_end = z if way == 0 else 3 - z

            @pl.when(from_end > 0)
            def _():
                for h in (0,):
                    rs_copy(u, s, way, 2, z, h).wait_recv()
                rs_add(u, s, way, 2, acc, 0, pl.ds(0, width))

    def rs_sent(u, s):
        part = zpart[u].at[pl.ds(0, 3 * rows)]
        rcopy(part, part, rsend.at[u, s], rrecv.at[0, s, 0, 0], zdev[0]).wait_send()

    gunits = (
        (gf, act, 0, ff),
        (n2, dgu, 0, ff),
        (n2, dgu, ff, ff),
        (ghf, ob, 0, qp),
        (n1, dq3, 0, inw),
    )

    def xslot(u, chip):
        b, n = u % 2, gunits[u][3]
        return xb.at[b, pl.ds(al(chip * shard, 16), shard), pl.ds(0, n)]

    def gslot(u, chip, core):
        b, n = u % 2, gunits[u][3]
        return gb.at[b, pl.ds(al(chip * pair + core * shard, 16), shard), pl.ds(0, n)]

    def g_exchange(u, chip, i):
        return rcopy(gslot(u, chip, 1 - c), xslot(u, chip), gsend.at[u % 2], grecv.at[u % 2, i], {"dp": pp})

    chips = (chip_d, chip_x, chip_y, chip_own)

    def g_compute(u, i):
        left, right, at, n = gunits[u]
        chip = chips[i]
        if u >= 2 and i == 0:
            pl.semaphore_wait(credit.at[0], 1)
        tile = 256

        def body(j, carry):
            lhs = left[:, pl.ds(al(chip * pair, LANES), pair)]
            got = tn(lhs, right[:, pl.ds(al(at + j * tile, tile), tile)])
            gb[u % 2, pl.ds(al(chip * pair, 16), pair), pl.ds(al(j * tile, tile), tile)] = got.astype(BF)
            return carry

        lax.fori_loop(0, n // tile, body, 0)
        g_exchange(u, chip, i).start()

    def g_add(u, chip, extra=None):
        b, n = u % 2, gunits[u][3]

        def body(i, carry):
            at = pl.ds(al(chip * shard + i * 16, 16), 16)
            mine = gb[b, pl.ds(al(chip * pair + c * shard + i * 16, 16), 16), pl.ds(0, n)].astype(F32)
            total = mine + xb[b, at, pl.ds(0, n)].astype(F32)
            if extra is not None:
                total = total + extra[b, pl.ds(al(i * 16, 16), 16), pl.ds(0, n)].astype(F32)
            xb[b, at, pl.ds(0, n)] = total.astype(BF)
            return carry

        lax.fori_loop(0, shard // 16, body, 0)

    def g_hop(u):
        b, n = u % 2, gunits[u][3]
        return rcopy(xslot(u, chip_d), hop.at[b, :, pl.ds(0, n)], gsend.at[b], grecv.at[b, 4], {"dp": aa})

    def g_last(u, way):
        b, n = u % 2, gunits[u][3]
        chip, dev = (chip_a, aa) if way == 0 else (chip_b, bb)
        return rcopy(
            xslot(u, chip), fin.at[b, way, :, pl.ds(0, n)], gsend.at[b], grecv.at[b, 5 + way], {"dp": dev}
        )

    def g_first(u):
        g_exchange(u, chip_d, 0).wait_recv()
        g_add(u, chip_d)
        if u >= 2:
            pl.semaphore_wait(credit.at[1], 1)
        g_hop(u).start()

    def g_firstb(u):
        g_exchange(u, chip_x, 1).wait_recv()
        g_exchange(u, chip_y, 2).wait_recv()
        g_add(u, chip_a)
        g_last(u, 0).start()

    def g_second(u):
        g_hop(u).wait_recv()
        g_add(u, chip_b, hop)
        if u >= 2:
            pl.semaphore_wait(credit.at[2], 1)
        g_last(u, 1).start()

    def picked(at, cut, which):
        value = stage[at, cut]
        high = value.astype(BF)
        rest = value - high.astype(F32)
        mid = rest.astype(BF)
        low = (rest - mid.astype(F32)).astype(BF)
        return nt(high, which) + (nt(mid, which) + nt(low, which))

    def g_finish(u):
        b, n = u % 2, gunits[u][3]
        g_exchange(u, chip_own, 3).wait_recv()
        g_last(u, 0).wait_recv()
        g_last(u, 1).wait_recv()
        out = (gdown_v, ggate_v, gup_v, stage, stage)[u]

        def body(i, carry):
            at = pl.ds(al(i * 16, 16), 16)
            total = gb[b, pl.ds(al(chip_own * pair + c * shard + i * 16, 16), 16), pl.ds(0, n)].astype(F32)
            total = total + xb[b, pl.ds(al(chip_own * shard + i * 16, 16), 16), pl.ds(0, n)].astype(F32)
            total = total + fin[b, 0, at, pl.ds(0, n)].astype(F32)
            out[at, pl.ds(0, n)] = total + fin[b, 1, at, pl.ds(0, n)].astype(F32)
            return carry

        lax.fori_loop(0, shard // 16, body, 0)
        rows_all = pl.ds(0, shard)
        if u == 3:
            gout_v[...] = picked(rows_all, pl.ds(0, qp), head_pick(gout_v.shape[1]))
        if u == 4:
            gq_v[...] = picked(rows_all, pl.ds(0, qp), head_pick(gq_v.shape[1]))
            gk_v[...] = picked(rows_all, pl.ds(qp, kp), head_pick(gk_v.shape[1]))
            gv_v[...] = picked(rows_all, pl.ds(qp + kp, kp), head_pick(gv_v.shape[1]))
        part = gb.at[b, pl.ds(0, 7 * shard), pl.ds(0, n)]
        rcopy(part, part, gsend.at[b], grecv.at[b, 0], {"dp": pp}).wait_send()
        if u < 3:
            pl.semaphore_signal(credit.at[0], inc=1, device_id={"dp": pp}, device_id_type=MESH)
            pl.semaphore_signal(credit.at[1], inc=1, device_id={"dp": aa}, device_id_type=MESH)
            pl.semaphore_signal(credit.at[2], inc=1, device_id={"dp": bb}, device_id_type=MESH)

    def gain_rows():
        for j in range(4):
            at = pl.ds(j * pair, pair)
            gains[:, at] = (
                wgn[pl.ds(32 * j, 16), :].astype(F32) + wgn[pl.ds(32 * j + 16, 16), :].astype(F32)
            )

    def norm1(s, t):
        gain = gains[0:1, :]

        def shard_rows(i):
            def body(r, carry):
                at = pl.ds(al(s * seq + i * rows + r * 16, 16), 16)
                x = xf[at, :].astype(F32)
                scale = lax.rsqrt(jnp.mean(x * x, axis=-1, keepdims=True) + eps)
                n1[at, :] = (x * scale * gain).astype(BF)
                return carry

            lax.fori_loop(0, rows // 16, body, 0)

        if t == 0:
            own_here(0, s)
            shard_rows(z)
            return

        @pl.when(z - t >= 0)
        def _():
            shard_rows(z - t)

        @pl.when(z + t <= 3)
        def _():
            shard_rows(z + t)

    head_scale = HEAD ** (-0.5)

    def project(s):
        at = pl.ds(s * seq, seq)
        cosine, sine = cosr[s], sinr[s]
        for j in range(inw // 256):
            both = nn(n1[at, :], wi[:, pl.ds(j * 256, 256)])
            for half in range(2):
                col = j * 256 + half * LANES
                part = both[:, half * LANES : (half + 1) * LANES]
                if col < qp + kp:
                    part = part * cosine + pltpu.roll(part, LANES // 2, 1) * sine
                if col < qp:
                    part = part * head_scale
                qkv[at, pl.ds(col, LANES)] = part.astype(BF)

    def attend(s, part):
        at = pl.ds(s * seq, seq)
        oc = ordr[s : s + 1, :].astype(F32)
        mask = (oc <= cols[s, :, 0:1]) & (oc >= cols[s, :, 1:2])

        def body(h, carry):
            g = h // per_group
            q = qkv[at, pl.ds(al(h * LANES, LANES), LANES)]
            k = qkv[at, pl.ds(al(qp + g * LANES, LANES), LANES)]
            v = qkv[at, pl.ds(al(qp + kp + g * LANES, LANES), LANES)]
            sc = jnp.where(mask, nt(q, k), -1e30)
            e = jnp.exp(sc - jnp.max(sc, axis=-1, keepdims=True))
            p = e * (1.0 / jnp.sum(e, axis=-1, keepdims=True))
            p = p.astype(BF)
            pr[s * heads + h] = p
            ob[at, pl.ds(al(h * LANES, LANES), LANES)] = nn(p, v).astype(BF)
            return carry

        half = heads // 2
        lax.fori_loop(part * half, (part + 1) * half, body, 0)

    def spread(s, dst, left, weight, tile, part=0, parts=1):
        at = pl.ds(s * seq, seq)

        def body(j, carry):
            col = al(j * tile, tile)
            dst[at, pl.ds(col, tile)] = nt(left[at, :], weight[pl.ds(col, tile), :]).astype(BF)
            return carry

        count = width // tile // parts
        lax.fori_loop(part * count, (part + 1) * count, body, 0)

    def spread_gain(s):
        at = pl.ds(s * seq, seq)
        tile = 512

        def body(j, carry):
            col = pl.ds(al(j * tile, tile), tile)
            got = nt(dq3[at, :], wi[col, :])
            pa[at, col] = got.astype(BF)
            gpart[0:1, col] += jnp.sum(got * n1[at, col].astype(F32), axis=0, keepdims=True)
            return carry

        lax.fori_loop(0, width // tile, body, 0)

    def norm2(s):
        gain = gains[1:2, :]
        base = s * rows

        def body(i, carry):
            r = pl.ds(al(i * 16, 16), 16)
            h = tbuf[s, r, :].astype(F32) + acc[r, :]
            hb[pl.ds(al(base + i * 16, 16), 16), :] = h
            scale = lax.rsqrt(jnp.mean(h * h, axis=-1, keepdims=True) + eps)
            real = cols[s, pl.ds(al(own + i * 16, 16), 16), 2:3]
            n2[pl.ds(al(s * seq + own + i * 16, 16), 16), :] = (h * (scale * real) * gain).astype(BF)
            return carry

        lax.fori_loop(0, rows // 16, body, 0)

    def feed(s, part):
        at = pl.ds(s * seq, seq)
        if part == 0:
            own_here(1, s)

        def body(t, carry):
            col = al(t * 256, 256)
            gate = nn(n2[at, :], wu[:, pl.ds(col, 256)])
            upper = nn(n2[at, :], wu[:, pl.ds(al(ff + t * 256, 256), 256)])
            back = nn(gf[at, :], wd[:, pl.ds(col, 256)])
            sigma = 1.0 / (1.0 + jnp.exp(-gate))
            swish = gate * sigma
            act[at, pl.ds(col, 256)] = (swish * upper).astype(BF)
            dgu[at, pl.ds(col, 256)] = (back * upper * sigma * (1.0 + gate * (1.0 - sigma))).astype(BF)
            dgu[at, pl.ds(al(ff + t * 256, 256), 256)] = (back * swish).astype(BF)
            return carry

        count = ff // 256 // 4
        lax.fori_loop(part * count, (part + 1) * count, body, 0)

    def finish_out(s):
        def body(i, carry):
            r = pl.ds(al(i * 16, 16), 16)
            real = cols[s, pl.ds(al(own + i * 16, 16), 16), 2:3]
            y = (hb[pl.ds(al(s * rows + i * 16, 16), 16), :] + acc[r, :]) * real
            out_v[s, r, :] = y.astype(BF)
            return carry

        lax.fori_loop(0, rows // 16, body, 0)

    def norm2_back(s):
        gain = gains[1:2, :]

        def body(i, carry):
            r = pl.ds(al(i * 16, 16), 16)
            ro = pl.ds(al(s * rows + i * 16, 16), 16)
            h = hb[ro, :]
            scale = lax.rsqrt(jnp.mean(h * h, axis=-1, keepdims=True) + eps)
            unit = h * scale
            grad = acc[r, :]
            inner = grad * gain
            dy = gf[pl.ds(al(s * seq + own + i * 16, 16), 16), :].astype(F32)
            dy = dy * cols[s, pl.ds(al(own + i * 16, 16), 16), 2:3]
            dhr = dy + scale * (inner - unit * jnp.mean(inner * unit, axis=-1, keepdims=True))
            gtok_v[s, r, :] = dhr
            ghf[pl.ds(al(s * seq + own + i * 16, 16), 16), :] = dhr.astype(BF)
            return carry + jnp.sum(grad * unit, axis=0, keepdims=True)

        gpart[1:2, :] += lax.fori_loop(0, rows // 16, body, jnp.zeros((1, width), F32))

    def grad_heads(s):
        at = pl.ds(s * seq, seq)
        for j in range(qp // 256):
            dq3[at, pl.ds(j * 256, 256)] = nn(ghf[at, :], wo[:, pl.ds(j * 256, 256)]).astype(BF)

    def attend_back(s):
        at = pl.ds(s * seq, seq)
        cosine, sine = cosr[s], sinr[s]

        def body(g, carry):
            k = qkv[at, pl.ds(al(qp + g * LANES, LANES), LANES)]
            v = qkv[at, pl.ds(al(qp + kp + g * LANES, LANES), LANES)]
            dk = jnp.zeros((seq, LANES), F32)
            dv = jnp.zeros((seq, LANES), F32)
            for m in range(per_group):
                h = g * per_group + m
                hat = pl.ds(al(h * LANES, LANES), LANES)
                q = qkv[at, hat]
                do = dq3[at, hat]
                low = pr[s * heads + h]
                p = low.astype(F32)
                dp = nt(do, v)
                ds = (p * (dp - jnp.sum(p * dp, axis=-1, keepdims=True))).astype(BF)
                dv = dv + tn(low, do)
                dk = dk + tn(ds, q)
                dq = nn(ds, k) * head_scale
                dq3[at, hat] = (dq * cosine - pltpu.roll(dq, LANES // 2, 1) * sine).astype(BF)
            dq3[at, pl.ds(al(qp + g * LANES, LANES), LANES)] = (
                dk * cosine - pltpu.roll(dk, LANES // 2, 1) * sine
            ).astype(BF)
            dq3[at, pl.ds(al(qp + kp + g * LANES, LANES), LANES)] = dv.astype(BF)
            return carry

        lax.fori_loop(0, groups, body, 0)

    def norm1_back(s):
        gain = gains[0:1, :]

        def body(i, carry):
            r = pl.ds(al(i * 16, 16), 16)
            x = tbuf[s, r, :].astype(F32)
            scale = lax.rsqrt(jnp.mean(x * x, axis=-1, keepdims=True) + eps)
            unit = x * scale
            grad = acc[r, :]
            inner = grad * gain
            gtok_v[s, r, :] += scale * (inner - unit * jnp.mean(inner * unit, axis=-1, keepdims=True))
            return carry

        lax.fori_loop(0, rows // 16, body, 0)

    X, COT, N2, GH = 0, 1, 2, 3
    BR, FFN, DN2, DN1 = 0, 1, 2, 3

    def tok_copy(s):
        return pltpu.make_async_copy(tok.at[s], tbuf.at[s], lsem.at[s])

    def fin_br(s):
        rs_final(BR, s)
        tok_copy(s).wait()
        norm2(s)
        ag(N2, s, 0)

    def fin_dn2(s):
        rs_final(DN2, s)
        norm2_back(s)
        ag(GH, s, 0)

    def fin_ffn(s):
        rs_final(FFN, s)
        finish_out(s)

    def fin_dn1(s):
        rs_final(DN1, s)
        norm1_back(s)

    def e_copy(i, src, dev):
        line = i < 6
        return rcopy(src, gex.at[i], esend.at[0 if line else 1], erecv.at[i if line else i // 2 + 3], dev)

    def e_line(t):
        if t == 0:
            for j in range(4):
                at = pl.ds(j * pair, pair)
                gsum[j : j + 1, :] = gpart[0:1, at] / gains[0:1, at]
                gsum[4 + j : 5 + j, :] = gpart[1:2, at]
        for way in (0, 1):
            here = (z - t >= 0) if way == 0 else (z + t <= 3)
            on = (z < 3) if way == 0 else (z > 0)
            slot = 3 * way + t

            @pl.when(here)
            def _():
                if t > 0:
                    e_copy(slot - 1, gsum, zdev[way]).wait_recv()
                if t < 3:
                    @pl.when(on)
                    def _():
                        e_copy(slot, gsum if t == 0 else gex.at[slot - 1], zdev[way]).start()

        if t == 3:
            gex[6] = gsum[...]
            for way in (0, 1):
                for k in (1, 2, 3):
                    @pl.when((z - k >= 0) if way == 0 else (z + k <= 3))
                    def _():
                        gex[6] += gex[3 * way + k - 1]

            e_copy(7, gex.at[6], {"dp": pp}).start()

    def e_plane(t):
        i = 7 + 2 * t
        dev = (pp, aa, bb)[t]
        e_copy(i, gex.at[i - 1], {"dp": dev}).wait()
        total = gex[i - 1] + gex[i]
        if t < 2:
            gex[i + 1] = total
            e_copy(i + 2, gex.at[i + 1], {"dp": (aa, bb)[t]}).start()
        else:
            gex[12] = total
            for at, out in ((0, gone_v), (4, gtwo_v)):
                line = gex[12, pl.ds(at + d // 2, 1), :]
                out[...] = jnp.where(c == 0, line[:, :shard], line[:, shard:])

    def e_sent():
        def sent(count):
            part = gex.at[pl.ds(0, count)]
            rcopy(part, part, esend.at[0], erecv.at[0], zdev[0]).wait_send()

        @pl.when((z == 0) | (z == 3))
        def _():
            sent(1)

        @pl.when((z > 0) & (z < 3))
        def _():
            sent(5)

    def clean(i):
        if i == 0:
            for u in range(6):
                w_sent(u)
        elif i < 4:
            for s in (0, 1):
                zag_sent((COT, N2, GH)[i - 1], s)
        else:
            rs_sent(FFN, i - 4)

    for i in (7, 8, 0, 1, 2, 3, 5, 6, 4):
        raw_copy(i).start()
    gpart[...] = jnp.zeros_like(gpart)
    for s in (0, 1):
        tok_copy(s).start()
    pl.semaphore_wait(barrier, 3 + (z + 3) // 4 + (6 - z) // 4)
    ag(X, 0, 0)
    prep_in()
    ag(X, 1, 0)
    prep_out()
    prep_rows(0)
    prep_gain()
    w_start(0)
    w_start(1)
    w_relayb(0)
    w_start(2)
    ag(X, 0, 1, 1)
    ag(X, 0, 1, 0)
    w_relaya(1)
    w_diag(0)
    ag(X, 1, 1, 0)
    ag(X, 0, 2, 0)
    w_relayb(1)
    ag(COT, 0, 0)
    w_relaya(0)
    w_done(0)
    gain_rows()
    norm1(0, 1)
    norm1(0, 0)
    w_relayb(2)
    ag(X, 0, 2, 1)
    ag(COT, 1, 0)
    ag(X, 1, 1, 1)
    norm1(1, 1)
    w_start(3)
    norm1(1, 0)
    prep_rows(1)
    w_start(4)
    norm1(0, 2)
    w_diag(1)
    ag(COT, 0, 1, 1)
    ag(X, 0, 3, 1)
    w_relaya(2)
    w_diag(2)
    ag(X, 0, 3, 0)
    norm1(0, 3)
    w_done(1)
    project(0)
    attend(0, 0)
    attend(0, 1)
    w_done(2)
    spread(0, pa, ob, wo, 512)
    rs(BR, 0, 0, 1)
    ag(COT, 0, 1, 0)
    rs(BR, 0, 1, 1)
    ag(X, 1, 2, 0)
    rs(BR, 0, 0, 0)
    rs(BR, 0, 1, 0)
    w_start(5)
    ag(X, 1, 2, 1)
    w_relaya(4)
    rs(BR, 0, 2, 1)
    rs(BR, 0, 2, 0)
    ag(COT, 0, 2, 0)
    norm1(1, 2)
    ag(X, 1, 3, 0)
    ag(X, 1, 3, 1)
    w_relayb(3)
    norm1(1, 3)
    project(1)
    attend(1, 0)
    w_relaya(3)
    fin_br(0)
    w_relayb(4)
    zag_sent(X, 0)
    ag(COT, 0, 2, 1)
    w_diag(3)
    attend(1, 1)
    spread(1, pa, ob, wo, 512)
    rs_sent(BR, 0)
    ag(N2, 0, 1, 1)
    rs(BR, 1, 0, 1)
    ag(N2, 0, 1, 0)
    w_relayb(5)
    rs(BR, 1, 0, 0)
    rs(BR, 1, 1, 1)
    w_done(3)
    ag(N2, 0, 2, 0)
    rs(BR, 1, 1, 0)
    ag(N2, 0, 2, 1)
    w_relaya(5)
    rs(BR, 1, 2, 0)
    w_diag(4)
    rs(BR, 1, 2, 1)
    w_diag(5)
    w_done(5)
    ag(COT, 0, 3, 0)
    ag(COT, 1, 1, 1)
    w_done(4)
    ag(COT, 1, 1, 0)
    ag(N2, 0, 3, 1)
    ag(N2, 0, 3, 0)
    ag(COT, 0, 3, 1)
    feed(0, 0)
    feed(0, 1)
    feed(0, 2)
    fin_br(1)
    feed(0, 3)
    spread(0, pa, dgu, wu, 256, 0, 2)
    spread(0, pa, dgu, wu, 256, 1, 2)
    ag(COT, 1, 2, 1)
    rs(DN2, 0, 0, 1)
    rs(DN2, 0, 0, 0)
    spread(0, pb, act, wd, 512)
    ag(N2, 1, 1, 0)
    rs(DN2, 0, 1, 0)
    ag(COT, 1, 3, 1)
    rs(FFN, 0, 0, 0)
    ag(N2, 1, 1, 1)
    ag(N2, 1, 2, 1)
    rs_sent(BR, 1)
    ag(COT, 1, 2, 0)
    rs(DN2, 0, 1, 1)
    ag(N2, 1, 2, 0)
    rs(FFN, 0, 0, 1)
    rs(DN2, 0, 2, 0)
    rs(DN2, 0, 2, 1)
    ag(N2, 1, 3, 0)
    zag_sent(X, 1)
    rs(FFN, 0, 1, 1)
    rs(FFN, 0, 1, 0)
    ag(N2, 1, 3, 1)
    ag(COT, 1, 3, 0)
    feed(1, 0)
    feed(1, 1)
    feed(1, 2)
    feed(1, 3)
    fin_dn2(0)
    spread(1, pa, dgu, wu, 256, 0, 2)
    spread(1, pa, dgu, wu, 256, 1, 2)
    rs(DN2, 1, 0, 0)
    g_compute(0, 0)
    rs(DN2, 1, 0, 1)
    g_compute(0, 1)
    ag(GH, 0, 1, 0)
    ag(GH, 0, 1, 1)
    g_first(0)
    g_compute(0, 2)
    g_compute(0, 3)
    rs(DN2, 1, 1, 1)
    rs(DN2, 1, 1, 0)
    ag(GH, 0, 2, 1)
    ag(GH, 0, 2, 0)
    g_compute(1, 0)
    g_firstb(0)
    rs(DN2, 1, 2, 0)
    rs(DN2, 1, 2, 1)
    spread(1, pb, act, wd, 512)
    rs(FFN, 1, 0, 1)
    rs(FFN, 1, 0, 0)
    rs_sent(DN2, 0)
    g_second(0)
    g_first(1)
    g_compute(1, 1)
    g_compute(1, 2)
    ag(GH, 0, 3, 1)
    ag(GH, 0, 3, 0)
    fin_dn2(1)
    g_firstb(1)
    grad_heads(0)
    attend_back(0)
    rs_sent(DN2, 1)
    spread_gain(0)
    rs(DN1, 0, 0, 0)
    ag(GH, 1, 1, 1)
    rs(DN1, 0, 0, 1)
    ag(GH, 1, 1, 0)
    g_second(1)
    rs(FFN, 1, 1, 0)
    g_finish(0)
    g_compute(1, 3)
    g_compute(2, 0)
    ag(GH, 1, 2, 1)
    rs(FFN, 1, 1, 1)
    g_first(2)
    rs(FFN, 0, 2, 1)
    ag(GH, 1, 2, 0)
    rs(FFN, 0, 2, 0)
    g_compute(2, 1)
    g_compute(2, 2)
    g_compute(2, 3)
    rs(DN1, 0, 1, 1)
    g_firstb(2)
    ag(GH, 1, 3, 0)
    rs(FFN, 1, 2, 0)
    ag(GH, 1, 3, 1)
    grad_heads(1)
    g_second(2)
    clean(3)
    attend_back(1)
    spread_gain(1)
    rs(DN1, 1, 0, 0)
    e_line(0)
    g_finish(1)
    g_compute(3, 0)
    rs(DN1, 1, 0, 1)
    rs(FFN, 1, 2, 1)
    rs(DN1, 0, 1, 0)
    g_compute(3, 1)
    g_compute(3, 2)
    g_compute(3, 3)
    g_first(3)
    clean(4)
    fin_ffn(0)
    g_firstb(3)
    clean(0)
    clean(1)
    clean(2)
    g_finish(2)
    g_compute(4, 0)
    g_compute(4, 1)
    e_line(1)
    g_second(3)
    g_compute(4, 2)
    rs(DN1, 1, 1, 1)
    rs(DN1, 1, 1, 0)
    e_line(2)
    g_first(4)
    e_line(3)
    rs(DN1, 0, 2, 1)
    g_finish(3)
    rs(DN1, 0, 2, 0)
    e_plane(0)
    g_firstb(4)
    g_compute(4, 3)
    rs(DN1, 1, 2, 1)
    g_second(4)
    rs(DN1, 1, 2, 0)
    fin_dn1(0)
    e_plane(1)
    clean(5)
    fin_ffn(1)
    e_plane(2)
    g_finish(4)
    fin_dn1(1)
    for s in (0, 1):
        rs_sent(DN1, s)
    e_sent()


def put_out(*refs):
    ins, outs, sem = refs[:11], refs[11:22], refs[22]
    copies = [pltpu.make_async_copy(src, dst, sem.at[i]) for i, (src, dst) in enumerate(zip(ins, outs))]
    for copy in copies:
        copy.start()
    for copy in copies:
        copy.wait()


def fused(
    tokens,
    cotangent,
    order,
    lengths,
    gain_attn,
    w_query,
    w_key,
    w_value,
    w_out,
    gain_ffn,
    w_gate,
    w_up,
    w_down,
):
    micro, rows, width = tokens.shape
    seq = rows * lax.axis_size("tensor")
    shard = w_query.shape[0]
    ff = w_gate.shape[1]
    groups = w_key.shape[1] // HEAD
    q_cols, k_cols = w_query.shape[1], w_key.shape[1]
    qp = q_cols // HEAD * LANES
    kp = groups * LANES
    inw = qp + 2 * kp
    total = micro * seq
    vm = pltpu.VMEM
    dma = pltpu.SemaphoreType.DMA
    scratch = [
        vm((8 * 16, 2 * shard), BF),
        vm((width, inw), BF),
        vm((width, qp), BF),
        vm((width, 2 * ff), BF),
        vm((width, ff), BF),
        vm((total, width), BF),
        vm((total, width), BF),
        vm((total, width), BF),
        vm((total, width), BF),
        vm((total, inw), BF),
        vm((total, qp), BF),
        vm((total, ff), BF),
        vm((total, inw), BF),
        vm((total, 2 * ff), BF),
        vm((micro * qp // LANES, seq, seq), BF),
        vm((micro * rows, width), F32),
        vm((total, width), BF),
        vm((total, width), BF),
        vm((micro, 2, 3, rows, width), BF),
        vm((micro, 2, 3, rows, width), BF),
        vm((2, width, ff), BF),
        vm((2, width // 2, ff), BF),
        vm((2, shard, ff), BF),
        vm((2, 2, shard, ff), BF),
        vm((shard, ff), F32),
        vm((rows, width), F32),
        vm((16, width), F32),
        vm((8, width), F32),
        vm((8, width // 4), F32),
        vm((13, 8, width // 4), F32),
        vm((micro, rows, width), BF),
        vm(gain_attn.shape, BF),
        vm(gain_ffn.shape, BF),
        vm(w_query.shape, BF),
        vm(w_key.shape, BF),
        vm(w_value.shape, BF),
        vm(w_out.shape[::-1], BF),
        vm((micro, seq, LANES), F32),
        vm((micro, seq, LANES), F32),
        vm((micro, seq, LANES), F32),
        dma((6,)),
        dma((6, 4)),
        dma((4, 2)),
        dma((3, 2, 2, 3)),
        dma((4, 2)),
        dma((2, 2, 2, 3)),
        dma((2,)),
        dma((2, 7)),
        dma((2,)),
        dma((9,)),
        dma((6,)),
        dma((9,)),
        pltpu.SemaphoreType.REGULAR((3,)),
    ]
    hbm = pl.BlockSpec(memory_space=pl.ANY)
    vmem = pl.BlockSpec(memory_space=pltpu.VMEM)
    smem = pl.BlockSpec(memory_space=pltpu.SMEM)
    shape = jax.ShapeDtypeStruct
    shapes = [
        vm((micro, rows, width), BF),
        vm((micro, rows, width), F32),
        vm((shard, ff), F32),
        vm((shard, ff), F32),
        vm((shard, ff), F32),
        vm((shard, q_cols), F32),
        vm((shard, q_cols), F32),
        vm((shard, k_cols), F32),
        vm((shard, k_cols), F32),
        vm((1, shard), F32),
        vm((1, shard), F32),
    ]
    dims = (rows, seq, width, shard, qp, kp, ff, groups)
    out, gtok, gdown, ggate, gup, gout, gq, gk, gv, one, two = pl.pallas_call(
        functools.partial(block_kernel, dims),
        out_shape=shapes,
        in_specs=[hbm] * 11 + [vmem, smem],
        out_specs=[vmem] * 11,
        scratch_shapes=scratch,
        compiler_params=pltpu.CompilerParams(
            collective_id=0, has_side_effects=True, vmem_limit_bytes=61_600_000
        ),
        name="block",
    )(
        tokens,
        cotangent,
        gain_attn,
        gain_ffn,
        w_query,
        w_key,
        w_value,
        w_out.T,
        w_gate,
        w_up,
        w_down.T,
        order,
        lengths,
    )
    results = [out, gtok, gdown, ggate, gup, gout, gq, gk, gv, one, two]
    out, gtok, gdown, ggate, gup, gout, gq, gk, gv, one, two = pl.pallas_call(
        put_out,
        out_shape=[shape(x.shape, x.dtype) for x in results],
        in_specs=[vmem] * 11,
        out_specs=[hbm] * 11,
        scratch_shapes=[dma((11,))],
        compiler_params=pltpu.CompilerParams(vmem_limit_bytes=2**18),
        name="put_out",
    )(*results)
    return out, gtok, one[0], gq, gk, gv, gout.T, two[0], ggate, gup, gdown.T


def local(tokens, *rest):
    fits = lax.axis_size("dp") == 8 and lax.axis_size("tensor") == 4 and tokens.shape[0] == 2
    return (fused if fits else spread_out)(tokens, *rest)


def solution(mesh):
    return jax.shard_map(
        local,
        mesh=mesh,
        in_specs=(
            P("dp", "tensor", None),
            P("dp", "tensor", None),
            P("dp", None),
            P("dp", None),
            P("dp"),
            P("dp", "tensor"),
            P("dp", "tensor"),
            P("dp", "tensor"),
            P("tensor", "dp"),
            P("dp"),
            P("dp", "tensor"),
            P("dp", "tensor"),
            P("tensor", "dp"),
        ),
        out_specs=(
            P("dp", "tensor", None),
            P("dp", "tensor", None),
            P("dp"),
            P("dp", "tensor"),
            P("dp", "tensor"),
            P("dp", "tensor"),
            P("tensor", "dp"),
            P("dp"),
            P("dp", "tensor"),
            P("dp", "tensor"),
            P("tensor", "dp"),
        ),
        check_vma=False,
    )
```

```python
import functools
import math

import jax
import jax.numpy as jnp
from jax import lax
from jax.experimental import pallas as pl
from jax.experimental.pallas import tpu as pltpu
from jax.sharding import PartitionSpec as P

HEAD = 96


eps = 1e-05
rope_base = 100000.0


def rotate(field, cosine, sine):
    half = field.shape[-1] // 2
    first = field[..., :half]
    second = field[..., half:]
    return jnp.concatenate(
        [first * cosine - second * sine, second * cosine + first * sine], axis=-1
    )


def rotate_back(field, cosine, sine):
    half = field.shape[-1] // 2
    first = field[..., :half]
    second = field[..., half:]
    return jnp.concatenate(
        [first * cosine + second * sine, second * cosine - first * sine], axis=-1
    )


def layout(order, lengths):
    starts = jnp.cumsum(lengths, dtype=jnp.int32) - lengths
    docs = jnp.sum((order[:, None] >= starts[None, 1:]).astype(jnp.int32), axis=1, dtype=jnp.int32)
    onehot = docs[:, None] == jnp.arange(lengths.shape[0], dtype=jnp.int32)[None, :]
    first = jnp.sum(jnp.where(onehot, starts[None, :], 0), axis=1, dtype=jnp.int32)
    positions = (order - first).astype(jnp.float32)
    mask = (docs[:, None] == docs[None, :]) & (order[None, :] <= order[:, None])
    real = (docs < lengths.shape[0] - 1).astype(jnp.float32)
    return (positions, mask, real)


def norm_forward(rows, gain):
    scale = lax.rsqrt(jnp.mean(rows * rows, axis=-1, keepdims=True) + eps)
    unit = rows * scale
    return (unit, scale, (unit * gain).astype(jnp.bfloat16))


def norm_backward(grad, unit, scale, gain):
    inner = grad * gain
    return scale * (inner - unit * jnp.mean(inner * unit, axis=-1, keepdims=True))


def contract_rows(left, right):
    return lax.dot_general(
        left, right, (((0,), (0,)), ((), ())), preferred_element_type=jnp.float32
    )


def times_transpose(left, right):
    return lax.dot_general(
        left, right, (((1,), (1,)), ((), ())), preferred_element_type=jnp.float32
    )


def gather_weights(gain_attn, w_query, w_key, w_value, w_out, gain_ffn, w_gate, w_up, w_down):
    gains = lax.all_gather(jnp.stack([gain_attn, gain_ffn], axis=0), "dp", axis=1, tiled=True)
    attn = lax.all_gather(
        jnp.concatenate([w_query, w_key, w_value, w_out.T], axis=1), "dp", axis=0, tiled=True
    )
    gate_up = lax.all_gather(jnp.concatenate([w_gate, w_up], axis=1), "dp", axis=0, tiled=True)
    down = lax.all_gather(w_down.T, "dp", axis=0, tiled=True)
    return gains, attn, gate_up, down


def gather_rows(rows):
    return lax.all_gather(rows, "tensor", axis=1, tiled=True)


def scatter_rows(partial):
    low = partial.astype(jnp.bfloat16)
    return lax.psum_scatter(low, "tensor", scatter_dimension=1, tiled=True).astype(jnp.float32)


def reduce_weights(term):
    low = term.astype(jnp.bfloat16)
    return lax.psum_scatter(low, "dp", scatter_dimension=0, tiled=True).astype(jnp.float32)


def spread_out(
    tokens,
    cotangent,
    order,
    lengths,
    gain_attn,
    w_query,
    w_key,
    w_value,
    w_out,
    gain_ffn,
    w_gate,
    w_up,
    w_down,
):
    micro, rows, width = tokens.shape
    seq = rows * lax.axis_size("tensor")
    q_cols, k_cols, ff_cols = w_query.shape[1], w_key.shape[1], w_gate.shape[1]
    local_heads, local_kv = q_cols // HEAD, k_cols // HEAD
    group = local_heads // local_kv
    first_row = lax.axis_index("tensor") * rows
    freqs = rope_base ** (-2.0 * jnp.arange(HEAD // 2, dtype=jnp.float32) / HEAD)
    head_scale = HEAD ** (-0.5)

    gains, attn, gate_up, down = gather_weights(
        gain_attn, w_query, w_key, w_value, w_out, gain_ffn, w_gate, w_up, w_down
    )
    gain1, gain2 = gains[0].astype(jnp.float32), gains[1].astype(jnp.float32)
    in_cols = q_cols + 2 * k_cols
    w_in, w_out_t = attn[:, :in_cols], attn[:, in_cols:]

    positions, mask, real = jax.vmap(layout)(order, lengths)
    angles = positions[:, :, None] * freqs
    cosine, sine = jnp.cos(angles)[:, :, None, :], jnp.sin(angles)[:, :, None, :]
    mask = mask[:, None, None]
    real_rows = lax.dynamic_slice_in_dim(real, first_row, rows, 1)[:, :, None]

    stream = tokens.astype(jnp.float32)
    unit1, scale1, normed1 = norm_forward(stream, gain1)
    full1 = gather_rows(normed1)
    grad_out_rows = cotangent.astype(jnp.float32) * real_rows
    full_grad = gather_rows(grad_out_rows.astype(jnp.bfloat16))
    flat1 = full1.reshape(micro * seq, width)
    flat_grad = full_grad.reshape(micro * seq, width)

    mixed_in = jnp.dot(flat1, w_in, preferred_element_type=jnp.float32).reshape(micro, seq, in_cols)
    query = mixed_in[..., :q_cols].reshape(micro, seq, local_heads, HEAD)
    keys = mixed_in[..., q_cols : q_cols + k_cols].reshape(micro, seq, local_kv, HEAD)
    values = mixed_in[..., q_cols + k_cols :].reshape(micro, seq, local_kv, HEAD).astype(jnp.bfloat16)
    query = (rotate(query, cosine, sine) * head_scale).astype(jnp.bfloat16)
    query = query.reshape(micro, seq, local_kv, group, HEAD)
    keys = rotate(keys, cosine, sine).astype(jnp.bfloat16)
    scores = jnp.einsum("bqkgd,bskd->bkgqs", query, keys, preferred_element_type=jnp.float32)
    scores = jnp.where(mask, scores, -1e30)
    peak = jnp.max(scores, axis=-1, keepdims=True)
    expon = jnp.exp(scores - peak)
    total = jnp.sum(expon, axis=-1, keepdims=True)
    probs = expon / total
    probs_low = probs.astype(jnp.bfloat16)
    mixed = jnp.einsum("bkgqs,bskd->bqkgd", probs_low, values, preferred_element_type=jnp.float32)
    mixed = mixed.reshape(micro * seq, q_cols).astype(jnp.bfloat16)
    branch = scatter_rows(times_transpose(mixed, w_out_t).reshape(micro, seq, width))
    resid = stream + branch
    unit2, scale2, normed2 = norm_forward(resid, gain2)
    full2 = gather_rows(normed2).reshape(micro * seq, width)

    both = jnp.dot(full2, gate_up, preferred_element_type=jnp.float32)
    gate, upper = both[:, :ff_cols], both[:, ff_cols:]
    sigma = jax.nn.sigmoid(gate)
    hidden = (gate * sigma * upper).astype(jnp.bfloat16)
    ffn = scatter_rows(times_transpose(hidden, down).reshape(micro, seq, width))
    output = ((resid + ffn) * real_rows).astype(jnp.bfloat16)

    grad_hidden = jnp.dot(flat_grad, down, preferred_element_type=jnp.float32)
    grad_gate = (grad_hidden * upper * sigma * (1.0 + gate * (1.0 - sigma))).astype(jnp.bfloat16)
    grad_up = (grad_hidden * gate * sigma).astype(jnp.bfloat16)
    grad_both = jnp.concatenate([grad_gate, grad_up], axis=1)
    grad_norm2 = scatter_rows(times_transpose(grad_both, gate_up).reshape(micro, seq, width))
    final_down = reduce_weights(contract_rows(flat_grad, hidden))
    final_gate = reduce_weights(contract_rows(full2, grad_gate))
    final_up = reduce_weights(contract_rows(full2, grad_up))
    term_gain2 = jnp.sum(grad_norm2 * unit2, axis=(0, 1))
    grad_resid = grad_out_rows + norm_backward(grad_norm2, unit2, scale2, gain2)

    full_resid = gather_rows(grad_resid.astype(jnp.bfloat16)).reshape(micro * seq, width)
    grad_mixed = jnp.dot(full_resid, w_out_t, preferred_element_type=jnp.float32).astype(jnp.bfloat16)
    final_out = reduce_weights(contract_rows(full_resid, mixed))
    grad_heads = grad_mixed.reshape(micro, seq, local_kv, group, HEAD)
    grad_probs = jnp.einsum(
        "bqkgd,bskd->bkgqs", grad_heads, values, preferred_element_type=jnp.float32
    )
    grad_values = jnp.einsum(
        "bkgqs,bqkgd->bskd", probs_low, grad_heads, preferred_element_type=jnp.float32
    )
    grad_scores = (
        probs * (grad_probs - jnp.sum(probs * grad_probs, axis=-1, keepdims=True))
    ).astype(jnp.bfloat16)
    grad_query = jnp.einsum(
        "bkgqs,bskd->bqkgd", grad_scores, keys, preferred_element_type=jnp.float32
    ).reshape(micro, seq, local_heads, HEAD)
    grad_keys = jnp.einsum(
        "bkgqs,bqkgd->bskd", grad_scores, query, preferred_element_type=jnp.float32
    )
    grad_query = rotate_back(grad_query * head_scale, cosine, sine).reshape(micro * seq, q_cols)
    grad_keys = rotate_back(grad_keys, cosine, sine).reshape(micro * seq, k_cols)
    grad_values = grad_values.reshape(micro * seq, k_cols)
    grad_in = jnp.concatenate(
        [grad_query.astype(jnp.bfloat16), grad_keys.astype(jnp.bfloat16), grad_values.astype(jnp.bfloat16)],
        axis=1,
    )
    grad_norm1 = scatter_rows(times_transpose(grad_in, w_in).reshape(micro, seq, width))
    final_in = reduce_weights(contract_rows(flat1, grad_in))
    term_gain1 = jnp.sum(grad_norm1 * unit1, axis=(0, 1))
    grad_tokens = grad_resid + norm_backward(grad_norm1, unit1, scale1, gain1)

    gain_terms = lax.psum(jnp.stack([term_gain1, term_gain2], axis=0), ("dp", "tensor"))
    own = gain_attn.shape[0]
    gain_own = lax.dynamic_slice_in_dim(gain_terms, lax.axis_index("dp") * own, own, 1)
    return (
        output,
        grad_tokens,
        gain_own[0],
        final_in[:, :q_cols],
        final_in[:, q_cols : q_cols + k_cols],
        final_in[:, q_cols + k_cols :],
        final_out.T,
        gain_own[1],
        final_gate,
        final_up,
        final_down.T,
    )


BF = jnp.bfloat16
F32 = jnp.float32
MESH = pl.DeviceIdType.MESH
LANES = 128


def nn(left, right):
    return lax.dot_general(left, right, (((1,), (0,)), ((), ())), preferred_element_type=F32)


def nt(left, right):
    return lax.dot_general(left, right, (((1,), (1,)), ((), ())), preferred_element_type=F32)


def tn(left, right):
    return lax.dot_general(left, right, (((0,), (0,)), ((), ())), preferred_element_type=F32)


def al(value, unit):
    return pl.multiple_of(value, unit)


def block_kernel(dims, *refs):
    (rows, seq, width, shard, qp, kp, ff, groups) = dims
    (tok, cot, ga_h, gf_h, wq_h, wk_h, wv_h, wo_h, wa_h, wb_h, wd_h, ordr, lens) = refs[:13]
    (out_v, gtok_v, gdown_v, ggate_v, gup_v, gout_v, gq_v, gk_v, gv_v, gone_v, gtwo_v) = refs[13:24]
    (wgn, wi, wo, wu, wd, xf, n1, n2, gf, qkv, ob, act, dq3, dgu, pr, hb, pa, pb, ra, rb,
     gb, xb, hop, fin, stage, acc, gains, gpart, gsum, gex, tbuf, rga, rgf, rq, rk, rv, ro, cols, cosr, sinr,
     wsend, wrecv, zsend, zrecv, rsend, rrecv, gsend, grecv, esend, erecv, lsem, psem, credit) = refs[24:]
    ghf = xf
    heads = qp // LANES
    per_group = heads // groups
    inw = qp + 2 * kp
    pair = 2 * shard
    d = lax.axis_index("dp")
    z = lax.axis_index("tensor")
    c = d % 2
    flip = 1 - 2 * c
    near_x = d + 2 - 4 * ((d // 2) % 2)
    near_y = d + 4 - 8 * (d // 4)
    aa = near_x * (1 - c) + near_y * c
    bb = near_y * (1 - c) + near_x * c
    dd = aa + bb - d
    pp = d + flip
    chip_own, chip_a, chip_b, chip_d = d // 2, aa // 2, bb // 2, dd // 2
    chip_x, chip_y = near_x // 2, near_y // 2
    own = z * rows
    half = width
    zdev = {"tensor": z + 1}, {"tensor": z - 1}

    def rcopy(src, dst, ssem, rsem, dev):
        return pltpu.make_async_remote_copy(
            src_ref=src, dst_ref=dst, send_sem=ssem, recv_sem=rsem, device_id=dev, device_id_type=MESH
        )

    barrier = pltpu.get_barrier_semaphore()
    for dev in (pp, aa, bb):
        pl.semaphore_signal(barrier, inc=1, device_id={"dp": dev}, device_id_type=MESH)
    for way in (0, 1):
        @pl.when((z < 3) if way == 0 else (z > 0))
        def _():
            pl.semaphore_signal(barrier, inc=1, device_id=zdev[way], device_id_type=MESH)

    def raw_copy(i):
        src, dst = (
            (wq_h, rq),
            (wk_h, rk),
            (wv_h, rv),
            (wo_h, ro),
            (wd_h, wd.at[pl.ds(al(shard * d, 16), shard), :]),
            (wa_h, wu.at[pl.ds(al(shard * d, 16), shard), pl.ds(0, ff)]),
            (wb_h, wu.at[pl.ds(al(shard * d, 16), shard), pl.ds(ff, ff)]),
            (ga_h, rga),
            (gf_h, rgf),
        )[i]
        return pltpu.make_async_copy(src, dst, psem.at[i])

    def head_map(n):
        row = lax.broadcasted_iota(jnp.int32, (n // HEAD * HEAD, n // HEAD * LANES), 0)
        col = lax.broadcasted_iota(jnp.int32, (n // HEAD * HEAD, n // HEAD * LANES), 1)
        lane = col % 64
        want = (col // 64) * (HEAD // 2) + lane
        return jnp.where((lane < HEAD // 2) & (row == want), 1.0, 0.0).astype(BF)

    head_pick = head_map

    def prep_gain():
        raw_copy(7).wait()
        raw_copy(8).wait()
        line = lax.broadcasted_iota(jnp.int32, (16, shard), 0)
        one = jnp.broadcast_to(rga[...].reshape(1, shard).astype(F32), (16, shard))
        two = jnp.broadcast_to(rgf[...].reshape(1, shard).astype(F32), (16, shard))
        row = lax.broadcasted_iota(jnp.int32, (shard, pair), 0)
        col = lax.broadcasted_iota(jnp.int32, (shard, pair), 1)
        place = jnp.where(col == row + shard * c, 1.0, 0.0).astype(BF)
        both = jnp.where(line == 0, one, two).astype(BF)
        wgn[pl.ds(al(16 * d, 16), 16), :] = nn(both, place).astype(BF)

    def prep_in():
        at = pl.ds(al(shard * d, 16), shard)
        for i in range(3):
            raw_copy(i).wait()
        wide = head_map(rq.shape[1])
        narrow = head_map(rk.shape[1])
        wi[at, pl.ds(0, qp)] = nn(rq[...], wide).astype(BF)
        wi[at, pl.ds(qp, kp)] = nn(rk[...], narrow).astype(BF)
        wi[at, pl.ds(qp + kp, kp)] = nn(rv[...], narrow).astype(BF)

    def prep_out():
        raw_copy(3).wait()
        wo[pl.ds(al(shard * d, 16), shard), :] = nn(ro[...], head_map(ro.shape[1])).astype(BF)

    def prep_rows(s):
        row = lax.broadcasted_iota(jnp.int32, (seq, seq), 0)
        col = lax.broadcasted_iota(jnp.int32, (seq, seq), 1)
        same = jnp.where(row == col, 1.0, 0.0).astype(BF)
        mid = seq // 2
        packed = (ordr[s : s + 1, :] - mid).astype(F32)
        place = nt(same, jnp.broadcast_to(packed, (LANES, seq)).astype(BF)) + mid
        start = lens[s, 0]
        first = jnp.zeros((seq, LANES), F32)
        for n in range(1, lens.shape[1]):
            begin = start.astype(F32)
            first = jnp.where(place >= begin, begin, first)
            real = jnp.where(place >= begin, 0.0, 1.0)
            start = start + lens[s, n]
        lane = lax.broadcasted_iota(jnp.int32, (seq, LANES), 1)
        cols[s] = jnp.where(lane == 0, place, jnp.where(lane == 1, first, real))
        one = lax.broadcasted_iota(jnp.int32, (8, LANES), 1)
        field = one % 64
        freqs = jnp.exp((-2.0 * math.log(rope_base) / HEAD) * field.astype(F32))
        freqs = jnp.where(field < HEAD // 2, freqs, 0.0)[0:1, :]
        angles = (place - first) * freqs
        cosr[s] = jnp.cos(angles)
        sine = jnp.sin(angles)
        sinr[s] = jnp.where(lane < 64, -sine, sine)

    wunits = (
        (wgn, 16, 0, pair),
        (wi, shard, 0, inw),
        (wo, shard, 0, qp),
        (wu, shard, 0, ff),
        (wu, shard, ff, ff),
        (wd, shard, 0, ff),
    )

    def wblk(u, i):
        ref, n, at, cut = wunits[u]
        return ref.at[pl.ds(al(n * i, 16), n), pl.ds(at, cut)]

    def w_start(u):
        src = wblk(u, d)
        if u >= 3:
            raw_copy((5, 6, 4)[u - 3]).wait()
        rcopy(src, src, wsend.at[u], wrecv.at[u, 0], {"dp": aa}).start()
        rcopy(src, src, wsend.at[u], wrecv.at[u, 1], {"dp": bb}).start()
        rcopy(src, src, wsend.at[u], wrecv.at[u, 3], {"dp": pp}).start()

    def w_many(u, count):
        ref, n, at, cut = wunits[u]
        part = ref.at[pl.ds(0, count * n), pl.ds(at, cut)]
        return rcopy(part, part, wsend.at[u], wrecv.at[u, 3], {"dp": pp})

    def w_wait(u, slot, i):
        rcopy(wblk(u, i), wblk(u, i), wsend.at[u], wrecv.at[u, slot], {"dp": aa}).wait_recv()

    def w_relayb(u):
        w_wait(u, 1, bb)
        rcopy(wblk(u, bb), wblk(u, bb), wsend.at[u], wrecv.at[u, 2], {"dp": aa}).start()
        rcopy(wblk(u, bb), wblk(u, bb), wsend.at[u], wrecv.at[u, 3], {"dp": pp}).start()

    def w_relaya(u):
        w_wait(u, 0, aa)
        rcopy(wblk(u, aa), wblk(u, aa), wsend.at[u], wrecv.at[u, 3], {"dp": pp}).start()

    def w_diag(u):
        w_wait(u, 2, dd)
        rcopy(wblk(u, dd), wblk(u, dd), wsend.at[u], wrecv.at[u, 3], {"dp": pp}).start()

    def w_done(u):
        w_many(u, 4).wait_recv()

    def w_sent(u):
        w_many(u, 7).wait_send()

    zfull = (xf, gf, n2, ghf)
    zhbm = (tok, cot, None, None)

    def zblk(u, s, i, h=None):
        at = pl.ds(al(s * seq + i * rows, 16), rows)
        return zfull[u].at[at] if h is None else zfull[u].at[at, pl.ds(h * half, half)]

    def zcopy(u, s, k, way, h, i, src=None):
        blk = zblk(u, s, i, h)
        return rcopy(
            blk if src is None else src, blk, zsend.at[u, s], zrecv.at[u % 3, s, way, k], zdev[way]
        )

    def zag_send(u, s, k, way, h):
        i = z - k if way == 0 else z + k
        go = (z < 3) & (i >= 0) if way == 0 else (z > 0) & (i <= 3)

        @pl.when(go)
        def _():
            src = zhbm[u].at[s, :, pl.ds(h * half, half)] if k == 0 and zhbm[u] is not None else None
            zcopy(u, s, k, way, h, i, src).start()

    def own_copy(u, s):
        return pltpu.make_async_copy(zhbm[u].at[s], zblk(u, s, z), lsem.at[2 + 2 * u + s])

    def ag(u, s, t, way=None, h=0):
        if t == 0:
            if zhbm[u] is not None:
                own_copy(u, s).start()
            for part in (0,):
                for side in (0, 1):
                    zag_send(u, s, 0, side, part)
            return
        i = z - t if way == 0 else z + t
        go = (i >= 0) if way == 0 else (i <= 3)

        @pl.when(go)
        def _():
            zcopy(u, s, t - 1, way, h, i).wait_recv()

        if t < 3:
            zag_send(u, s, t, way, h)

    def own_here(u, s):
        own_copy(u, s).wait()

    def zag_sent(u, s):
        def sent(count):
            part = zfull[u].at[pl.ds(0, count * rows)]
            rcopy(part, part, zsend.at[u, s], zrecv.at[u % 3, s, 0, 0], zdev[0]).wait_send()

        @pl.when((z == 0) | (z == 3))
        def _():
            sent(1)

        @pl.when((z > 0) & (z < 3))
        def _():
            sent(5)

    zpart = (pa, pb, pa, pa)
    zgot = (ra, rb, ra, ra)

    def rs_copy(u, s, way, t, dest, h):
        cut = pl.ds(h * half, half)
        return rcopy(
            zpart[u].at[pl.ds(al(s * seq + dest * rows, 16), rows), cut],
            zgot[u].at[s, way, t, :, cut],
            rsend.at[u, s],
            rrecv.at[1 if u == 1 else 0, s, way, t],
            zdev[way],
        )

    def rs_add(u, s, way, t, target, base, cut):
        def body(i, carry):
            at = pl.ds(al(base + i * 16, 16), 16)
            got = zgot[u][s, way, t, pl.ds(al(i * 16, 16), 16), cut].astype(F32)
            target[at, cut] = (target[at, cut].astype(F32) + got).astype(target.dtype)
            return carry

        lax.fori_loop(0, rows // 16, body, 0)

    def rs(u, s, t, way, h=0):
        from_end = z if way == 0 else 3 - z
        dest = 3 + z - t if way == 0 else t - from_end

        @pl.when(from_end <= t)
        def _():
            if t > 0:
                @pl.when(from_end > 0)
                def _():
                    rs_copy(u, s, way, t - 1, z, h).wait_recv()
                    rs_add(u, s, way, t - 1, zpart[u], s * seq + dest * rows, pl.ds(h * half, half))

            rs_copy(u, s, way, t, dest, h).start()

    def rs_final(u, s):
        def first(i, carry):
            at = pl.ds(al(i * 16, 16), 16)
            acc[at, :] = zpart[u][pl.ds(al(s * seq + own + i * 16, 16), 16), :].astype(F32)
            return carry

        lax.fori_loop(0, rows // 16, first, 0)
        for way in (0, 1):
            from_end = z if way == 0 else 3 - z

            @pl.when(from_end > 0)
            def _():
                for h in (0,):
                    rs_copy(u, s, way, 2, z, h).wait_recv()
                rs_add(u, s, way, 2, acc, 0, pl.ds(0, width))

    def rs_sent(u, s):
        part = zpart[u].at[pl.ds(0, 3 * rows)]
        rcopy(part, part, rsend.at[u, s], rrecv.at[0, s, 0, 0], zdev[0]).wait_send()

    gunits = (
        (gf, act, 0, ff),
        (n2, dgu, 0, ff),
        (n2, dgu, ff, ff),
        (ghf, ob, 0, qp),
        (n1, dq3, 0, inw),
    )

    def xslot(u, chip):
        b, n = u % 2, gunits[u][3]
        return xb.at[b, pl.ds(al(chip * shard, 16), shard), pl.ds(0, n)]

    def gslot(u, chip, core):
        b, n = u % 2, gunits[u][3]
        return gb.at[b, pl.ds(al(chip * pair + core * shard, 16), shard), pl.ds(0, n)]

    def g_exchange(u, chip, i):
        return rcopy(gslot(u, chip, 1 - c), xslot(u, chip), gsend.at[u % 2], grecv.at[u % 2, i], {"dp": pp})

    chips = (chip_d, chip_x, chip_y, chip_own)

    def g_compute(u, i):
        left, right, at, n = gunits[u]
        chip = chips[i]
        if u >= 2 and i == 0:
            pl.semaphore_wait(credit.at[0], 1)
        tile = 256

        def body(j, carry):
            lhs = left[:, pl.ds(al(chip * pair, LANES), pair)]
            got = tn(lhs, right[:, pl.ds(al(at + j * tile, tile), tile)])
            gb[u % 2, pl.ds(al(chip * pair, 16), pair), pl.ds(al(j * tile, tile), tile)] = got.astype(BF)
            return carry

        lax.fori_loop(0, n // tile, body, 0)
        g_exchange(u, chip, i).start()

    def g_add(u, chip, extra=None):
        b, n = u % 2, gunits[u][3]

        def body(i, carry):
            at = pl.ds(al(chip * shard + i * 16, 16), 16)
            mine = gb[b, pl.ds(al(chip * pair + c * shard + i * 16, 16), 16), pl.ds(0, n)].astype(F32)
            total = mine + xb[b, at, pl.ds(0, n)].astype(F32)
            if extra is not None:
                total = total + extra[b, pl.ds(al(i * 16, 16), 16), pl.ds(0, n)].astype(F32)
            xb[b, at, pl.ds(0, n)] = total.astype(BF)
            return carry

        lax.fori_loop(0, shard // 16, body, 0)

    def g_hop(u):
        b, n = u % 2, gunits[u][3]
        return rcopy(xslot(u, chip_d), hop.at[b, :, pl.ds(0, n)], gsend.at[b], grecv.at[b, 4], {"dp": aa})

    def g_last(u, way):
        b, n = u % 2, gunits[u][3]
        chip, dev = (chip_a, aa) if way == 0 else (chip_b, bb)
        return rcopy(
            xslot(u, chip), fin.at[b, way, :, pl.ds(0, n)], gsend.at[b], grecv.at[b, 5 + way], {"dp": dev}
        )

    def g_first(u):
        g_exchange(u, chip_d, 0).wait_recv()
        g_add(u, chip_d)
        if u >= 2:
            pl.semaphore_wait(credit.at[1], 1)
        g_hop(u).start()

    def g_firstb(u):
        g_exchange(u, chip_x, 1).wait_recv()
        g_exchange(u, chip_y, 2).wait_recv()
        g_add(u, chip_a)
        g_last(u, 0).start()

    def g_second(u):
        g_hop(u).wait_recv()
        g_add(u, chip_b, hop)
        if u >= 2:
            pl.semaphore_wait(credit.at[2], 1)
        g_last(u, 1).start()

    def picked(at, cut, which):
        value = stage[at, cut]
        high = value.astype(BF)
        rest = value - high.astype(F32)
        mid = rest.astype(BF)
        low = (rest - mid.astype(F32)).astype(BF)
        return nt(high, which) + (nt(mid, which) + nt(low, which))

    def g_finish(u):
        b, n = u % 2, gunits[u][3]
        g_exchange(u, chip_own, 3).wait_recv()
        g_last(u, 0).wait_recv()
        g_last(u, 1).wait_recv()
        out = (gdown_v, ggate_v, gup_v, stage, stage)[u]

        def body(i, carry):
            at = pl.ds(al(i * 16, 16), 16)
            total = gb[b, pl.ds(al(chip_own * pair + c * shard + i * 16, 16), 16), pl.ds(0, n)].astype(F32)
            total = total + xb[b, pl.ds(al(chip_own * shard + i * 16, 16), 16), pl.ds(0, n)].astype(F32)
            total = total + fin[b, 0, at, pl.ds(0, n)].astype(F32)
            out[at, pl.ds(0, n)] = total + fin[b, 1, at, pl.ds(0, n)].astype(F32)
            return carry

        lax.fori_loop(0, shard // 16, body, 0)
        rows_all = pl.ds(0, shard)
        if u == 3:
            gout_v[...] = picked(rows_all, pl.ds(0, qp), head_pick(gout_v.shape[1]))
        if u == 4:
            gq_v[...] = picked(rows_all, pl.ds(0, qp), head_pick(gq_v.shape[1]))
            gk_v[...] = picked(rows_all, pl.ds(qp, kp), head_pick(gk_v.shape[1]))
            gv_v[...] = picked(rows_all, pl.ds(qp + kp, kp), head_pick(gv_v.shape[1]))
        part = gb.at[b, pl.ds(0, 7 * shard), pl.ds(0, n)]
        rcopy(part, part, gsend.at[b], grecv.at[b, 0], {"dp": pp}).wait_send()
        if u < 3:
            pl.semaphore_signal(credit.at[0], inc=1, device_id={"dp": pp}, device_id_type=MESH)
            pl.semaphore_signal(credit.at[1], inc=1, device_id={"dp": aa}, device_id_type=MESH)
            pl.semaphore_signal(credit.at[2], inc=1, device_id={"dp": bb}, device_id_type=MESH)

    def gain_rows():
        for j in range(4):
            at = pl.ds(j * pair, pair)
            gains[:, at] = (
                wgn[pl.ds(32 * j, 16), :].astype(F32) + wgn[pl.ds(32 * j + 16, 16), :].astype(F32)
            )

    def norm1(s, t):
        gain = gains[0:1, :]

        def shard_rows(i):
            def body(r, carry):
                at = pl.ds(al(s * seq + i * rows + r * 16, 16), 16)
                x = xf[at, :].astype(F32)
                scale = lax.rsqrt(jnp.mean(x * x, axis=-1, keepdims=True) + eps)
                n1[at, :] = (x * scale * gain).astype(BF)
                return carry

            lax.fori_loop(0, rows // 16, body, 0)

        if t == 0:
            own_here(0, s)
            shard_rows(z)
            return

        @pl.when(z - t >= 0)
        def _():
            shard_rows(z - t)

        @pl.when(z + t <= 3)
        def _():
            shard_rows(z + t)

    head_scale = HEAD ** (-0.5)

    def project(s):
        at = pl.ds(s * seq, seq)
        cosine, sine = cosr[s], sinr[s]
        for j in range(inw // 256):
            both = nn(n1[at, :], wi[:, pl.ds(j * 256, 256)])
            for half in range(2):
                col = j * 256 + half * LANES
                part = both[:, half * LANES : (half + 1) * LANES]
                if col < qp + kp:
                    part = part * cosine + pltpu.roll(part, LANES // 2, 1) * sine
                if col < qp:
                    part = part * head_scale
                qkv[at, pl.ds(col, LANES)] = part.astype(BF)

    def attend(s, part):
        at = pl.ds(s * seq, seq)
        oc = ordr[s : s + 1, :].astype(F32)
        mask = (oc <= cols[s, :, 0:1]) & (oc >= cols[s, :, 1:2])

        def body(h, carry):
            g = h // per_group
            q = qkv[at, pl.ds(al(h * LANES, LANES), LANES)]
            k = qkv[at, pl.ds(al(qp + g * LANES, LANES), LANES)]
            v = qkv[at, pl.ds(al(qp + kp + g * LANES, LANES), LANES)]
            sc = jnp.where(mask, nt(q, k), -1e30)
            e = jnp.exp(sc - jnp.max(sc, axis=-1, keepdims=True))
            p = e * (1.0 / jnp.sum(e, axis=-1, keepdims=True))
            p = p.astype(BF)
            pr[s * heads + h] = p
            ob[at, pl.ds(al(h * LANES, LANES), LANES)] = nn(p, v).astype(BF)
            return carry

        half = heads // 2
        lax.fori_loop(part * half, (part + 1) * half, body, 0)

    def spread(s, dst, left, weight, tile, part=0, parts=1):
        at = pl.ds(s * seq, seq)

        def body(j, carry):
            col = al(j * tile, tile)
            dst[at, pl.ds(col, tile)] = nt(left[at, :], weight[pl.ds(col, tile), :]).astype(BF)
            return carry

        count = width // tile // parts
        lax.fori_loop(part * count, (part + 1) * count, body, 0)

    def spread_gain(s):
        at = pl.ds(s * seq, seq)
        tile = 512

        def body(j, carry):
            col = pl.ds(al(j * tile, tile), tile)
            got = nt(dq3[at, :], wi[col, :])
            pa[at, col] = got.astype(BF)
            gpart[0:1, col] += jnp.sum(got * n1[at, col].astype(F32), axis=0, keepdims=True)
            return carry

        lax.fori_loop(0, width // tile, body, 0)

    def norm2(s):
        gain = gains[1:2, :]
        base = s * rows

        def body(i, carry):
            r = pl.ds(al(i * 16, 16), 16)
            h = tbuf[s, r, :].astype(F32) + acc[r, :]
            hb[pl.ds(al(base + i * 16, 16), 16), :] = h
            scale = lax.rsqrt(jnp.mean(h * h, axis=-1, keepdims=True) + eps)
            real = cols[s, pl.ds(al(own + i * 16, 16), 16), 2:3]
            n2[pl.ds(al(s * seq + own + i * 16, 16), 16), :] = (h * (scale * real) * gain).astype(BF)
            return carry

        lax.fori_loop(0, rows // 16, body, 0)

    def feed_forward(s, part):
        at = pl.ds(s * seq, seq)
        one, two = pl.ds(part * 256, 256), pl.ds(ff + part * 256, 256)
        gate = nn(n2[at, :], wu[:, one])
        upper = nn(n2[at, :], wu[:, two])
        sigma = 1.0 / (1.0 + jnp.exp(-gate))
        swish = gate * sigma
        act[at, one] = (swish * upper).astype(BF)
        dgu[at, one] = (upper * sigma * (1.0 + gate * (1.0 - sigma))).astype(BF)
        dgu[at, two] = swish.astype(BF)

    def feed_back(s, part):
        if part == 0:
            own_here(1, s)
        at = pl.ds(s * seq, seq)
        one, two = pl.ds(part * 256, 256), pl.ds(ff + part * 256, 256)
        back = nn(gf[at, :], wd[:, one])
        dgu[at, one] = (back * dgu[at, one].astype(F32)).astype(BF)
        dgu[at, two] = (back * dgu[at, two].astype(F32)).astype(BF)

    def finish_out(s):
        def body(i, carry):
            r = pl.ds(al(i * 16, 16), 16)
            real = cols[s, pl.ds(al(own + i * 16, 16), 16), 2:3]
            y = (hb[pl.ds(al(s * rows + i * 16, 16), 16), :] + acc[r, :]) * real
            out_v[s, r, :] = y.astype(BF)
            return carry

        lax.fori_loop(0, rows // 16, body, 0)

    def norm2_back(s):
        gain = gains[1:2, :]

        def body(i, carry):
            r = pl.ds(al(i * 16, 16), 16)
            ro = pl.ds(al(s * rows + i * 16, 16), 16)
            h = hb[ro, :]
            scale = lax.rsqrt(jnp.mean(h * h, axis=-1, keepdims=True) + eps)
            unit = h * scale
            grad = acc[r, :]
            inner = grad * gain
            dy = gf[pl.ds(al(s * seq + own + i * 16, 16), 16), :].astype(F32)
            dy = dy * cols[s, pl.ds(al(own + i * 16, 16), 16), 2:3]
            dhr = dy + scale * (inner - unit * jnp.mean(inner * unit, axis=-1, keepdims=True))
            gtok_v[s, r, :] = dhr
            ghf[pl.ds(al(s * seq + own + i * 16, 16), 16), :] = dhr.astype(BF)
            return carry + jnp.sum(grad * unit, axis=0, keepdims=True)

        gpart[1:2, :] += lax.fori_loop(0, rows // 16, body, jnp.zeros((1, width), F32))

    def grad_heads(s):
        at = pl.ds(s * seq, seq)
        for j in range(qp // 256):
            dq3[at, pl.ds(j * 256, 256)] = nn(ghf[at, :], wo[:, pl.ds(j * 256, 256)]).astype(BF)

    def attend_back(s):
        at = pl.ds(s * seq, seq)
        cosine, sine = cosr[s], sinr[s]

        def body(g, carry):
            k = qkv[at, pl.ds(al(qp + g * LANES, LANES), LANES)]
            v = qkv[at, pl.ds(al(qp + kp + g * LANES, LANES), LANES)]
            dk = jnp.zeros((seq, LANES), F32)
            dv = jnp.zeros((seq, LANES), F32)
            for m in range(per_group):
                h = g * per_group + m
                hat = pl.ds(al(h * LANES, LANES), LANES)
                q = qkv[at, hat]
                do = dq3[at, hat]
                low = pr[s * heads + h]
                p = low.astype(F32)
                dp = nt(do, v)
                ds = (p * (dp - jnp.sum(p * dp, axis=-1, keepdims=True))).astype(BF)
                dv = dv + tn(low, do)
                dk = dk + tn(ds, q)
                dq = nn(ds, k) * head_scale
                dq3[at, hat] = (dq * cosine - pltpu.roll(dq, LANES // 2, 1) * sine).astype(BF)
            dq3[at, pl.ds(al(qp + g * LANES, LANES), LANES)] = (
                dk * cosine - pltpu.roll(dk, LANES // 2, 1) * sine
            ).astype(BF)
            dq3[at, pl.ds(al(qp + kp + g * LANES, LANES), LANES)] = dv.astype(BF)
            return carry

        lax.fori_loop(0, groups, body, 0)

    def norm1_back(s):
        gain = gains[0:1, :]

        def body(i, carry):
            r = pl.ds(al(i * 16, 16), 16)
            x = tbuf[s, r, :].astype(F32)
            scale = lax.rsqrt(jnp.mean(x * x, axis=-1, keepdims=True) + eps)
            unit = x * scale
            grad = acc[r, :]
            inner = grad * gain
            gtok_v[s, r, :] += scale * (inner - unit * jnp.mean(inner * unit, axis=-1, keepdims=True))
            return carry

        lax.fori_loop(0, rows // 16, body, 0)

    X, COT, N2, GH = 0, 1, 2, 3
    BR, FFN, DN2, DN1 = 0, 1, 2, 3

    def tok_copy(s):
        return pltpu.make_async_copy(tok.at[s], tbuf.at[s], lsem.at[s])

    def fin_br(s):
        rs_final(BR, s)
        tok_copy(s).wait()
        norm2(s)
        ag(N2, s, 0)

    def fin_dn2(s):
        rs_final(DN2, s)
        norm2_back(s)
        ag(GH, s, 0)

    def fin_ffn(s):
        rs_final(FFN, s)
        finish_out(s)

    def fin_dn1(s):
        rs_final(DN1, s)
        norm1_back(s)

    def e_copy(i, src, dev):
        line = i < 6
        return rcopy(src, gex.at[i], esend.at[0 if line else 1], erecv.at[i if line else i // 2 + 3], dev)

    def e_line(t):
        if t == 0:
            for j in range(4):
                at = pl.ds(j * pair, pair)
                gsum[j : j + 1, :] = gpart[0:1, at] / gains[0:1, at]
                gsum[4 + j : 5 + j, :] = gpart[1:2, at]
        for way in (0, 1):
            here = (z - t >= 0) if way == 0 else (z + t <= 3)
            on = (z < 3) if way == 0 else (z > 0)
            slot = 3 * way + t

            @pl.when(here)
            def _():
                if t > 0:
                    e_copy(slot - 1, gsum, zdev[way]).wait_recv()
                if t < 3:
                    @pl.when(on)
                    def _():
                        e_copy(slot, gsum if t == 0 else gex.at[slot - 1], zdev[way]).start()

        if t == 3:
            gex[6] = gsum[...]
            for way in (0, 1):
                for k in (1, 2, 3):
                    @pl.when((z - k >= 0) if way == 0 else (z + k <= 3))
                    def _():
                        gex[6] += gex[3 * way + k - 1]

            e_copy(7, gex.at[6], {"dp": pp}).start()

    def e_plane(t):
        i = 7 + 2 * t
        dev = (pp, aa, bb)[t]
        e_copy(i, gex.at[i - 1], {"dp": dev}).wait()
        total = gex[i - 1] + gex[i]
        if t < 2:
            gex[i + 1] = total
            e_copy(i + 2, gex.at[i + 1], {"dp": (aa, bb)[t]}).start()
        else:
            gex[12] = total
            for at, out in ((0, gone_v), (4, gtwo_v)):
                line = gex[12, pl.ds(at + d // 2, 1), :]
                out[...] = jnp.where(c == 0, line[:, :shard], line[:, shard:])

    def e_sent():
        def sent(count):
            part = gex.at[pl.ds(0, count)]
            rcopy(part, part, esend.at[0], erecv.at[0], zdev[0]).wait_send()

        @pl.when((z == 0) | (z == 3))
        def _():
            sent(1)

        @pl.when((z > 0) & (z < 3))
        def _():
            sent(5)

    def clean(i):
        if i == 0:
            for u in range(6):
                w_sent(u)
        elif i < 4:
            for s in (0, 1):
                zag_sent((COT, N2, GH)[i - 1], s)
        else:
            rs_sent(FFN, i - 4)

    for i in (7, 8, 0, 1, 2, 3, 5, 6, 4):
        raw_copy(i).start()
    gpart[...] = jnp.zeros_like(gpart)
    for s in (0, 1):
        tok_copy(s).start()
    pl.semaphore_wait(barrier, 3 + (z + 3) // 4 + (6 - z) // 4)
    ag(X, 0, 0)
    prep_gain()
    w_start(0)
    prep_in()
    w_start(1)
    prep_out()
    w_start(2)
    ag(X, 0, 1, 1)
    w_relayb(0)
    ag(X, 0, 1, 0)
    ag(X, 1, 0)
    prep_rows(0)
    w_relayb(1)
    w_relaya(1)
    ag(X, 0, 2, 0)
    w_diag(0)
    w_relaya(0)
    ag(X, 0, 2, 1)
    ag(COT, 0, 0)
    ag(X, 1, 1, 1)
    prep_rows(1)
    w_done(0)
    gain_rows()
    norm1(0, 1)
    w_relayb(2)
    norm1(0, 0)
    w_diag(1)
    norm1(0, 2)
    ag(X, 0, 3, 1)
    ag(X, 0, 3, 0)
    norm1(0, 3)
    w_relaya(2)
    ag(X, 1, 1, 0)
    w_done(1)
    project(0)
    w_diag(2)
    w_start(3)
    attend(0, 0)
    attend(0, 1)
    w_done(2)
    spread(0, pa, ob, wo, 512)
    rs(BR, 0, 0, 1)
    rs(BR, 0, 0, 0)
    ag(COT, 0, 1, 0)
    ag(X, 1, 2, 1)
    w_start(4)
    ag(COT, 0, 1, 1)
    rs(BR, 0, 1, 1)
    norm1(1, 0)
    ag(X, 1, 2, 0)
    ag(COT, 0, 2, 0)
    rs(BR, 0, 1, 0)
    norm1(1, 2)
    norm1(1, 1)
    rs(BR, 0, 2, 1)
    ag(X, 1, 3, 1)
    ag(X, 1, 3, 0)
    norm1(1, 3)
    rs(BR, 0, 2, 0)
    w_relayb(3)
    project(1)
    attend(1, 0)
    w_start(5)
    attend(1, 1)
    ag(COT, 0, 2, 1)
    spread(1, pa, ob, wo, 512)
    rs(BR, 1, 0, 0)
    rs(BR, 1, 0, 1)
    fin_br(0)
    rs_sent(BR, 0)
    rs(BR, 1, 1, 0)
    ag(N2, 0, 1, 0)
    w_relaya(3)
    w_relaya(4)
    rs(BR, 1, 1, 1)
    w_relayb(4)
    ag(N2, 0, 1, 1)
    ag(COT, 0, 3, 1)
    rs(BR, 1, 2, 0)
    rs(BR, 1, 2, 1)
    w_relayb(5)
    ag(N2, 0, 2, 1)
    w_diag(3)
    ag(N2, 0, 2, 0)
    ag(COT, 1, 0)
    w_diag(4)
    fin_br(1)
    ag(N2, 0, 3, 0)
    w_done(4)
    w_relaya(5)
    ag(N2, 0, 3, 1)
    w_done(3)
    feed_forward(0, 0)
    w_diag(5)
    rs_sent(BR, 1)
    feed_forward(0, 1)
    feed_forward(0, 2)
    feed_forward(0, 3)
    w_done(5)
    spread(0, pb, act, wd, 512)
    rs(FFN, 0, 0, 1)
    ag(COT, 1, 1, 1)
    ag(COT, 1, 1, 0)
    rs(FFN, 0, 0, 0)
    ag(COT, 0, 3, 0)
    feed_back(0, 0)
    feed_back(0, 1)
    feed_back(0, 2)
    feed_back(0, 3)
    spread(0, pa, dgu, wu, 256, 0, 2)
    spread(0, pa, dgu, wu, 256, 1, 2)
    rs(DN2, 0, 0, 0)
    zag_sent(X, 1)
    ag(N2, 1, 1, 1)
    ag(N2, 1, 1, 0)
    rs(DN2, 0, 0, 1)
    clean(0)
    rs(DN2, 0, 1, 1)
    rs(FFN, 0, 1, 1)
    rs(DN2, 0, 1, 0)
    ag(N2, 1, 2, 1)
    rs(FFN, 0, 1, 0)
    ag(N2, 1, 3, 1)
    ag(N2, 1, 2, 0)
    ag(N2, 1, 3, 0)
    ag(COT, 1, 2, 1)
    feed_forward(1, 0)
    feed_forward(1, 1)
    feed_forward(1, 2)
    ag(COT, 1, 2, 0)
    zag_sent(X, 0)
    rs(DN2, 0, 2, 0)
    feed_forward(1, 3)
    rs(DN2, 0, 2, 1)
    ag(COT, 1, 3, 0)
    ag(COT, 1, 3, 1)
    feed_back(1, 0)
    feed_back(1, 1)
    feed_back(1, 2)
    feed_back(1, 3)
    spread(1, pa, dgu, wu, 256, 0, 2)
    spread(1, pa, dgu, wu, 256, 1, 2)
    rs(DN2, 1, 0, 1)
    rs(DN2, 1, 0, 0)
    g_compute(0, 0)
    g_compute(0, 1)
    fin_dn2(0)
    g_first(0)
    g_compute(0, 2)
    g_compute(0, 3)
    g_firstb(0)
    rs(DN2, 1, 1, 0)
    rs(DN2, 1, 1, 1)
    g_compute(1, 0)
    g_compute(1, 1)
    g_second(0)
    ag(GH, 0, 1, 0)
    ag(GH, 0, 1, 1)
    g_compute(1, 2)
    rs(DN2, 1, 2, 0)
    rs(DN2, 1, 2, 1)
    spread(1, pb, act, wd, 512)
    rs(FFN, 1, 0, 1)
    ag(GH, 0, 2, 0)
    rs(FFN, 1, 0, 0)
    ag(GH, 0, 2, 1)
    g_first(1)
    g_firstb(1)
    fin_dn2(1)
    g_finish(0)
    rs_sent(DN2, 0)
    g_compute(1, 3)
    g_compute(2, 0)
    ag(GH, 0, 3, 0)
    g_second(1)
    ag(GH, 0, 3, 1)
    grad_heads(0)
    attend_back(0)
    ag(GH, 1, 1, 0)
    rs(FFN, 1, 1, 0)
    g_first(2)
    ag(GH, 1, 1, 1)
    rs(FFN, 1, 1, 1)
    g_compute(2, 1)
    spread_gain(0)
    rs(DN1, 0, 0, 0)
    g_compute(2, 2)
    ag(GH, 1, 2, 1)
    rs(DN1, 0, 0, 1)
    g_firstb(2)
    ag(GH, 1, 2, 0)
    rs(FFN, 0, 2, 0)
    g_finish(1)
    g_compute(2, 3)
    rs(FFN, 1, 2, 1)
    g_second(2)
    ag(GH, 1, 3, 0)
    ag(GH, 1, 3, 1)
    rs(FFN, 0, 2, 1)
    g_compute(3, 0)
    g_compute(3, 1)
    rs(FFN, 1, 2, 0)
    grad_heads(1)
    attend_back(1)
    g_first(3)
    rs_sent(DN2, 1)
    spread_gain(1)
    rs(DN1, 1, 0, 1)
    e_line(0)
    rs(DN1, 1, 0, 0)
    rs(DN1, 0, 1, 0)
    g_compute(3, 2)
    rs(DN1, 0, 1, 1)
    g_compute(3, 3)
    g_firstb(3)
    g_finish(2)
    g_compute(4, 0)
    g_second(3)
    g_first(4)
    rs(DN1, 1, 1, 1)
    g_compute(4, 1)
    e_line(1)
    g_compute(4, 2)
    rs(DN1, 1, 1, 0)
    clean(2)
    clean(5)
    g_firstb(4)
    fin_ffn(0)
    e_line(2)
    clean(3)
    rs(DN1, 0, 2, 0)
    g_finish(3)
    rs(DN1, 0, 2, 1)
    e_line(3)
    e_plane(0)
    rs(DN1, 1, 2, 0)
    g_second(4)
    g_compute(4, 3)
    fin_ffn(1)
    rs(DN1, 1, 2, 1)
    fin_dn1(0)
    clean(1)
    clean(4)
    e_plane(1)
    g_finish(4)
    e_plane(2)
    fin_dn1(1)
    for s in (0, 1):
        rs_sent(DN1, s)
    e_sent()


def put_out(*refs):
    ins, outs, sem = refs[:11], refs[11:22], refs[22]
    copies = [pltpu.make_async_copy(src, dst, sem.at[i]) for i, (src, dst) in enumerate(zip(ins, outs))]
    for copy in copies:
        copy.start()
    for copy in copies:
        copy.wait()


def fused(
    tokens,
    cotangent,
    order,
    lengths,
    gain_attn,
    w_query,
    w_key,
    w_value,
    w_out,
    gain_ffn,
    w_gate,
    w_up,
    w_down,
):
    micro, rows, width = tokens.shape
    seq = rows * lax.axis_size("tensor")
    shard = w_query.shape[0]
    ff = w_gate.shape[1]
    groups = w_key.shape[1] // HEAD
    q_cols, k_cols = w_query.shape[1], w_key.shape[1]
    qp = q_cols // HEAD * LANES
    kp = groups * LANES
    inw = qp + 2 * kp
    total = micro * seq
    vm = pltpu.VMEM
    dma = pltpu.SemaphoreType.DMA
    scratch = [
        vm((8 * 16, 2 * shard), BF),
        vm((width, inw), BF),
        vm((width, qp), BF),
        vm((width, 2 * ff), BF),
        vm((width, ff), BF),
        vm((total, width), BF),
        vm((total, width), BF),
        vm((total, width), BF),
        vm((total, width), BF),
        vm((total, inw), BF),
        vm((total, qp), BF),
        vm((total, ff), BF),
        vm((total, inw), BF),
        vm((total, 2 * ff), BF),
        vm((micro * qp // LANES, seq, seq), BF),
        vm((micro * rows, width), F32),
        vm((total, width), BF),
        vm((total, width), BF),
        vm((micro, 2, 3, rows, width), BF),
        vm((micro, 2, 3, rows, width), BF),
        vm((2, width, ff), BF),
        vm((2, width // 2, ff), BF),
        vm((2, shard, ff), BF),
        vm((2, 2, shard, ff), BF),
        vm((shard, ff), F32),
        vm((rows, width), F32),
        vm((16, width), F32),
        vm((8, width), F32),
        vm((8, width // 4), F32),
        vm((13, 8, width // 4), F32),
        vm((micro, rows, width), BF),
        vm(gain_attn.shape, BF),
        vm(gain_ffn.shape, BF),
        vm(w_query.shape, BF),
        vm(w_key.shape, BF),
        vm(w_value.shape, BF),
        vm(w_out.shape[::-1], BF),
        vm((micro, seq, LANES), F32),
        vm((micro, seq, LANES), F32),
        vm((micro, seq, LANES), F32),
        dma((6,)),
        dma((6, 4)),
        dma((4, 2)),
        dma((3, 2, 2, 3)),
        dma((4, 2)),
        dma((2, 2, 2, 3)),
        dma((2,)),
        dma((2, 7)),
        dma((2,)),
        dma((9,)),
        dma((6,)),
        dma((9,)),
        pltpu.SemaphoreType.REGULAR((3,)),
    ]
    hbm = pl.BlockSpec(memory_space=pl.ANY)
    vmem = pl.BlockSpec(memory_space=pltpu.VMEM)
    smem = pl.BlockSpec(memory_space=pltpu.SMEM)
    shape = jax.ShapeDtypeStruct
    shapes = [
        vm((micro, rows, width), BF),
        vm((micro, rows, width), F32),
        vm((shard, ff), F32),
        vm((shard, ff), F32),
        vm((shard, ff), F32),
        vm((shard, q_cols), F32),
        vm((shard, q_cols), F32),
        vm((shard, k_cols), F32),
        vm((shard, k_cols), F32),
        vm((1, shard), F32),
        vm((1, shard), F32),
    ]
    dims = (rows, seq, width, shard, qp, kp, ff, groups)
    out, gtok, gdown, ggate, gup, gout, gq, gk, gv, one, two = pl.pallas_call(
        functools.partial(block_kernel, dims),
        out_shape=shapes,
        in_specs=[hbm] * 11 + [vmem, smem],
        out_specs=[vmem] * 11,
        scratch_shapes=scratch,
        compiler_params=pltpu.CompilerParams(
            collective_id=0, has_side_effects=True, vmem_limit_bytes=61_600_000
        ),
        name="block",
    )(
        tokens,
        cotangent,
        gain_attn,
        gain_ffn,
        w_query,
        w_key,
        w_value,
        w_out.T,
        w_gate,
        w_up,
        w_down.T,
        order,
        lengths,
    )
    results = [out, gtok, gdown, ggate, gup, gout, gq, gk, gv, one, two]
    out, gtok, gdown, ggate, gup, gout, gq, gk, gv, one, two = pl.pallas_call(
        put_out,
        out_shape=[shape(x.shape, x.dtype) for x in results],
        in_specs=[vmem] * 11,
        out_specs=[hbm] * 11,
        scratch_shapes=[dma((11,))],
        compiler_params=pltpu.CompilerParams(vmem_limit_bytes=2**18),
        name="put_out",
    )(*results)
    return out, gtok, one[0], gq, gk, gv, gout.T, two[0], ggate, gup, gdown.T


def local(tokens, *rest):
    fits = lax.axis_size("dp") == 8 and lax.axis_size("tensor") == 4 and tokens.shape[0] == 2
    return (fused if fits else spread_out)(tokens, *rest)


def solution(mesh):
    return jax.shard_map(
        local,
        mesh=mesh,
        in_specs=(
            P("dp", "tensor", None),
            P("dp", "tensor", None),
            P("dp", None),
            P("dp", None),
            P("dp"),
            P("dp", "tensor"),
            P("dp", "tensor"),
            P("dp", "tensor"),
            P("tensor", "dp"),
            P("dp"),
            P("dp", "tensor"),
            P("dp", "tensor"),
            P("tensor", "dp"),
        ),
        out_specs=(
            P("dp", "tensor", None),
            P("dp", "tensor", None),
            P("dp"),
            P("dp", "tensor"),
            P("dp", "tensor"),
            P("dp", "tensor"),
            P("tensor", "dp"),
            P("dp"),
            P("dp", "tensor"),
            P("dp", "tensor"),
            P("tensor", "dp"),
        ),
        check_vma=False,
    )
```

```python
import functools
import math

import jax
import jax.numpy as jnp
from jax import lax
from jax.experimental import pallas as pl
from jax.experimental.pallas import tpu as pltpu
from jax.sharding import PartitionSpec as P

HEAD = 96


eps = 1e-05
rope_base = 100000.0


def rotate(field, cosine, sine):
    half = field.shape[-1] // 2
    first = field[..., :half]
    second = field[..., half:]
    return jnp.concatenate(
        [first * cosine - second * sine, second * cosine + first * sine], axis=-1
    )


def rotate_back(field, cosine, sine):
    half = field.shape[-1] // 2
    first = field[..., :half]
    second = field[..., half:]
    return jnp.concatenate(
        [first * cosine + second * sine, second * cosine - first * sine], axis=-1
    )


def layout(order, lengths):
    starts = jnp.cumsum(lengths, dtype=jnp.int32) - lengths
    docs = jnp.sum((order[:, None] >= starts[None, 1:]).astype(jnp.int32), axis=1, dtype=jnp.int32)
    onehot = docs[:, None] == jnp.arange(lengths.shape[0], dtype=jnp.int32)[None, :]
    first = jnp.sum(jnp.where(onehot, starts[None, :], 0), axis=1, dtype=jnp.int32)
    positions = (order - first).astype(jnp.float32)
    mask = (docs[:, None] == docs[None, :]) & (order[None, :] <= order[:, None])
    real = (docs < lengths.shape[0] - 1).astype(jnp.float32)
    return (positions, mask, real)


def norm_forward(rows, gain):
    scale = lax.rsqrt(jnp.mean(rows * rows, axis=-1, keepdims=True) + eps)
    unit = rows * scale
    return (unit, scale, (unit * gain).astype(jnp.bfloat16))


def norm_backward(grad, unit, scale, gain):
    inner = grad * gain
    return scale * (inner - unit * jnp.mean(inner * unit, axis=-1, keepdims=True))


def contract_rows(left, right):
    return lax.dot_general(
        left, right, (((0,), (0,)), ((), ())), preferred_element_type=jnp.float32
    )


def times_transpose(left, right):
    return lax.dot_general(
        left, right, (((1,), (1,)), ((), ())), preferred_element_type=jnp.float32
    )


def gather_weights(gain_attn, w_query, w_key, w_value, w_out, gain_ffn, w_gate, w_up, w_down):
    gains = lax.all_gather(jnp.stack([gain_attn, gain_ffn], axis=0), "dp", axis=1, tiled=True)
    attn = lax.all_gather(
        jnp.concatenate([w_query, w_key, w_value, w_out.T], axis=1), "dp", axis=0, tiled=True
    )
    gate_up = lax.all_gather(jnp.concatenate([w_gate, w_up], axis=1), "dp", axis=0, tiled=True)
    down = lax.all_gather(w_down.T, "dp", axis=0, tiled=True)
    return gains, attn, gate_up, down


def gather_rows(rows):
    return lax.all_gather(rows, "tensor", axis=1, tiled=True)


def scatter_rows(partial):
    low = partial.astype(jnp.bfloat16)
    return lax.psum_scatter(low, "tensor", scatter_dimension=1, tiled=True).astype(jnp.float32)


def reduce_weights(term):
    low = term.astype(jnp.bfloat16)
    return lax.psum_scatter(low, "dp", scatter_dimension=0, tiled=True).astype(jnp.float32)


def spread_out(
    tokens,
    cotangent,
    order,
    lengths,
    gain_attn,
    w_query,
    w_key,
    w_value,
    w_out,
    gain_ffn,
    w_gate,
    w_up,
    w_down,
):
    micro, rows, width = tokens.shape
    seq = rows * lax.axis_size("tensor")
    q_cols, k_cols, ff_cols = w_query.shape[1], w_key.shape[1], w_gate.shape[1]
    local_heads, local_kv = q_cols // HEAD, k_cols // HEAD
    group = local_heads // local_kv
    first_row = lax.axis_index("tensor") * rows
    freqs = rope_base ** (-2.0 * jnp.arange(HEAD // 2, dtype=jnp.float32) / HEAD)
    head_scale = HEAD ** (-0.5)

    gains, attn, gate_up, down = gather_weights(
        gain_attn, w_query, w_key, w_value, w_out, gain_ffn, w_gate, w_up, w_down
    )
    gain1, gain2 = gains[0].astype(jnp.float32), gains[1].astype(jnp.float32)
    in_cols = q_cols + 2 * k_cols
    w_in, w_out_t = attn[:, :in_cols], attn[:, in_cols:]

    positions, mask, real = jax.vmap(layout)(order, lengths)
    angles = positions[:, :, None] * freqs
    cosine, sine = jnp.cos(angles)[:, :, None, :], jnp.sin(angles)[:, :, None, :]
    mask = mask[:, None, None]
    real_rows = lax.dynamic_slice_in_dim(real, first_row, rows, 1)[:, :, None]

    stream = tokens.astype(jnp.float32)
    unit1, scale1, normed1 = norm_forward(stream, gain1)
    full1 = gather_rows(normed1)
    grad_out_rows = cotangent.astype(jnp.float32) * real_rows
    full_grad = gather_rows(grad_out_rows.astype(jnp.bfloat16))
    flat1 = full1.reshape(micro * seq, width)
    flat_grad = full_grad.reshape(micro * seq, width)

    mixed_in = jnp.dot(flat1, w_in, preferred_element_type=jnp.float32).reshape(micro, seq, in_cols)
    query = mixed_in[..., :q_cols].reshape(micro, seq, local_heads, HEAD)
    keys = mixed_in[..., q_cols : q_cols + k_cols].reshape(micro, seq, local_kv, HEAD)
    values = mixed_in[..., q_cols + k_cols :].reshape(micro, seq, local_kv, HEAD).astype(jnp.bfloat16)
    query = (rotate(query, cosine, sine) * head_scale).astype(jnp.bfloat16)
    query = query.reshape(micro, seq, local_kv, group, HEAD)
    keys = rotate(keys, cosine, sine).astype(jnp.bfloat16)
    scores = jnp.einsum("bqkgd,bskd->bkgqs", query, keys, preferred_element_type=jnp.float32)
    scores = jnp.where(mask, scores, -1e30)
    peak = jnp.max(scores, axis=-1, keepdims=True)
    expon = jnp.exp(scores - peak)
    total = jnp.sum(expon, axis=-1, keepdims=True)
    probs = expon / total
    probs_low = probs.astype(jnp.bfloat16)
    mixed = jnp.einsum("bkgqs,bskd->bqkgd", probs_low, values, preferred_element_type=jnp.float32)
    mixed = mixed.reshape(micro * seq, q_cols).astype(jnp.bfloat16)
    branch = scatter_rows(times_transpose(mixed, w_out_t).reshape(micro, seq, width))
    resid = stream + branch
    unit2, scale2, normed2 = norm_forward(resid, gain2)
    full2 = gather_rows(normed2).reshape(micro * seq, width)

    both = jnp.dot(full2, gate_up, preferred_element_type=jnp.float32)
    gate, upper = both[:, :ff_cols], both[:, ff_cols:]
    sigma = jax.nn.sigmoid(gate)
    hidden = (gate * sigma * upper).astype(jnp.bfloat16)
    ffn = scatter_rows(times_transpose(hidden, down).reshape(micro, seq, width))
    output = ((resid + ffn) * real_rows).astype(jnp.bfloat16)

    grad_hidden = jnp.dot(flat_grad, down, preferred_element_type=jnp.float32)
    grad_gate = (grad_hidden * upper * sigma * (1.0 + gate * (1.0 - sigma))).astype(jnp.bfloat16)
    grad_up = (grad_hidden * gate * sigma).astype(jnp.bfloat16)
    grad_both = jnp.concatenate([grad_gate, grad_up], axis=1)
    grad_norm2 = scatter_rows(times_transpose(grad_both, gate_up).reshape(micro, seq, width))
    final_down = reduce_weights(contract_rows(flat_grad, hidden))
    final_gate = reduce_weights(contract_rows(full2, grad_gate))
    final_up = reduce_weights(contract_rows(full2, grad_up))
    term_gain2 = jnp.sum(grad_norm2 * unit2, axis=(0, 1))
    grad_resid = grad_out_rows + norm_backward(grad_norm2, unit2, scale2, gain2)

    full_resid = gather_rows(grad_resid.astype(jnp.bfloat16)).reshape(micro * seq, width)
    grad_mixed = jnp.dot(full_resid, w_out_t, preferred_element_type=jnp.float32).astype(jnp.bfloat16)
    final_out = reduce_weights(contract_rows(full_resid, mixed))
    grad_heads = grad_mixed.reshape(micro, seq, local_kv, group, HEAD)
    grad_probs = jnp.einsum(
        "bqkgd,bskd->bkgqs", grad_heads, values, preferred_element_type=jnp.float32
    )
    grad_values = jnp.einsum(
        "bkgqs,bqkgd->bskd", probs_low, grad_heads, preferred_element_type=jnp.float32
    )
    grad_scores = (
        probs * (grad_probs - jnp.sum(probs * grad_probs, axis=-1, keepdims=True))
    ).astype(jnp.bfloat16)
    grad_query = jnp.einsum(
        "bkgqs,bskd->bqkgd", grad_scores, keys, preferred_element_type=jnp.float32
    ).reshape(micro, seq, local_heads, HEAD)
    grad_keys = jnp.einsum(
        "bkgqs,bqkgd->bskd", grad_scores, query, preferred_element_type=jnp.float32
    )
    grad_query = rotate_back(grad_query * head_scale, cosine, sine).reshape(micro * seq, q_cols)
    grad_keys = rotate_back(grad_keys, cosine, sine).reshape(micro * seq, k_cols)
    grad_values = grad_values.reshape(micro * seq, k_cols)
    grad_in = jnp.concatenate(
        [grad_query.astype(jnp.bfloat16), grad_keys.astype(jnp.bfloat16), grad_values.astype(jnp.bfloat16)],
        axis=1,
    )
    grad_norm1 = scatter_rows(times_transpose(grad_in, w_in).reshape(micro, seq, width))
    final_in = reduce_weights(contract_rows(flat1, grad_in))
    term_gain1 = jnp.sum(grad_norm1 * unit1, axis=(0, 1))
    grad_tokens = grad_resid + norm_backward(grad_norm1, unit1, scale1, gain1)

    gain_terms = lax.psum(jnp.stack([term_gain1, term_gain2], axis=0), ("dp", "tensor"))
    own = gain_attn.shape[0]
    gain_own = lax.dynamic_slice_in_dim(gain_terms, lax.axis_index("dp") * own, own, 1)
    return (
        output,
        grad_tokens,
        gain_own[0],
        final_in[:, :q_cols],
        final_in[:, q_cols : q_cols + k_cols],
        final_in[:, q_cols + k_cols :],
        final_out.T,
        gain_own[1],
        final_gate,
        final_up,
        final_down.T,
    )


BF = jnp.bfloat16
F32 = jnp.float32
MESH = pl.DeviceIdType.MESH
LANES = 128


def nn(left, right):
    return lax.dot_general(left, right, (((1,), (0,)), ((), ())), preferred_element_type=F32)


def nt(left, right):
    return lax.dot_general(left, right, (((1,), (1,)), ((), ())), preferred_element_type=F32)


def tn(left, right):
    return lax.dot_general(left, right, (((0,), (0,)), ((), ())), preferred_element_type=F32)


def al(value, unit):
    return pl.multiple_of(value, unit)


def block_kernel(dims, *refs):
    (rows, seq, width, shard, qp, kp, ff, groups) = dims
    (tok, cot, ga_h, gf_h, wq_h, wk_h, wv_h, wo_h, wa_h, wb_h, wd_h, ordr, lens) = refs[:13]
    (out_v, gtok_v, gdown_v, ggate_v, gup_v, gout_v, gq_v, gk_v, gv_v, gone_v, gtwo_v) = refs[13:24]
    (wgn, wi, wo, wu, wd, xf, n1, n2, gf, qkv, ob, act, dq3, dgu, pr, hb, pa, pb, ra, rb,
     gb, xb, hop, fin, stage, acc, gains, gpart, gsum, gex, tbuf, rga, rgf, rq, rk, rv, ro, cols, cosr, sinr,
     wsend, wrecv, zsend, zrecv, rsend, rrecv, gsend, grecv, esend, erecv, lsem, psem, credit) = refs[24:]
    ghf = xf
    heads = qp // LANES
    per_group = heads // groups
    inw = qp + 2 * kp
    pair = 2 * shard
    d = lax.axis_index("dp")
    z = lax.axis_index("tensor")
    c = d % 2
    flip = 1 - 2 * c
    near_x = d + 2 - 4 * ((d // 2) % 2)
    near_y = d + 4 - 8 * (d // 4)
    aa = near_x * (1 - c) + near_y * c
    bb = near_y * (1 - c) + near_x * c
    dd = aa + bb - d
    pp = d + flip
    chip_own, chip_a, chip_b, chip_d = d // 2, aa // 2, bb // 2, dd // 2
    chip_x, chip_y = near_x // 2, near_y // 2
    own = z * rows
    half = width // 2
    zdev = {"tensor": z + 1}, {"tensor": z - 1}

    def rcopy(src, dst, ssem, rsem, dev):
        return pltpu.make_async_remote_copy(
            src_ref=src, dst_ref=dst, send_sem=ssem, recv_sem=rsem, device_id=dev, device_id_type=MESH
        )

    barrier = pltpu.get_barrier_semaphore()
    for dev in (pp, aa, bb):
        pl.semaphore_signal(barrier, inc=1, device_id={"dp": dev}, device_id_type=MESH)
    for way in (0, 1):
        @pl.when((z < 3) if way == 0 else (z > 0))
        def _():
            pl.semaphore_signal(barrier, inc=1, device_id=zdev[way], device_id_type=MESH)

    def raw_copy(i):
        src, dst = (
            (wq_h, rq),
            (wk_h, rk),
            (wv_h, rv),
            (wo_h, ro),
            (wd_h, wd.at[pl.ds(al(shard * d, 16), shard), :]),
            (wa_h, wu.at[pl.ds(al(shard * d, 16), shard), pl.ds(0, ff)]),
            (wb_h, wu.at[pl.ds(al(shard * d, 16), shard), pl.ds(ff, ff)]),
            (ga_h, rga),
            (gf_h, rgf),
        )[i]
        return pltpu.make_async_copy(src, dst, psem.at[i])

    def head_map(n):
        row = lax.broadcasted_iota(jnp.int32, (n // HEAD * HEAD, n // HEAD * LANES), 0)
        col = lax.broadcasted_iota(jnp.int32, (n // HEAD * HEAD, n // HEAD * LANES), 1)
        lane = col % 64
        want = (col // 64) * (HEAD // 2) + lane
        return jnp.where((lane < HEAD // 2) & (row == want), 1.0, 0.0).astype(BF)

    head_pick = head_map

    def prep_gain():
        raw_copy(7).wait()
        raw_copy(8).wait()
        line = lax.broadcasted_iota(jnp.int32, (16, shard), 0)
        one = jnp.broadcast_to(rga[...].reshape(1, shard).astype(F32), (16, shard))
        two = jnp.broadcast_to(rgf[...].reshape(1, shard).astype(F32), (16, shard))
        row = lax.broadcasted_iota(jnp.int32, (shard, pair), 0)
        col = lax.broadcasted_iota(jnp.int32, (shard, pair), 1)
        place = jnp.where(col == row + shard * c, 1.0, 0.0).astype(BF)
        both = jnp.where(line == 0, one, two).astype(BF)
        wgn[pl.ds(al(16 * d, 16), 16), :] = nn(both, place).astype(BF)

    def prep_in():
        at = pl.ds(al(shard * d, 16), shard)
        for i in range(3):
            raw_copy(i).wait()
        wide = head_map(rq.shape[1])
        narrow = head_map(rk.shape[1])
        wi[at, pl.ds(0, qp)] = nn(rq[...], wide).astype(BF)
        wi[at, pl.ds(qp, kp)] = nn(rk[...], narrow).astype(BF)
        wi[at, pl.ds(qp + kp, kp)] = nn(rv[...], narrow).astype(BF)

    def prep_out():
        raw_copy(3).wait()
        wo[pl.ds(al(shard * d, 16), shard), :] = nn(ro[...], head_map(ro.shape[1])).astype(BF)

    def prep_rows(s):
        row = lax.broadcasted_iota(jnp.int32, (seq, seq), 0)
        col = lax.broadcasted_iota(jnp.int32, (seq, seq), 1)
        same = jnp.where(row == col, 1.0, 0.0).astype(BF)
        mid = seq // 2
        packed = (ordr[s : s + 1, :] - mid).astype(F32)
        place = nt(same, jnp.broadcast_to(packed, (LANES, seq)).astype(BF)) + mid
        start = lens[s, 0]
        first = jnp.zeros((seq, LANES), F32)
        for n in range(1, lens.shape[1]):
            begin = start.astype(F32)
            first = jnp.where(place >= begin, begin, first)
            real = jnp.where(place >= begin, 0.0, 1.0)
            start = start + lens[s, n]
        lane = lax.broadcasted_iota(jnp.int32, (seq, LANES), 1)
        cols[s] = jnp.where(lane == 0, place, jnp.where(lane == 1, first, real))
        one = lax.broadcasted_iota(jnp.int32, (8, LANES), 1)
        field = one % 64
        freqs = jnp.exp((-2.0 * math.log(rope_base) / HEAD) * field.astype(F32))
        freqs = jnp.where(field < HEAD // 2, freqs, 0.0)[0:1, :]
        angles = (place - first) * freqs
        cosr[s] = jnp.cos(angles)
        sine = jnp.sin(angles)
        sinr[s] = jnp.where(lane < 64, -sine, sine)

    wunits = (
        (wgn, 16, 0, pair),
        (wi, shard, 0, inw),
        (wo, shard, 0, qp),
        (wu, shard, 0, ff),
        (wu, shard, ff, ff),
        (wd, shard, 0, ff),
    )

    def wblk(u, i):
        ref, n, at, cut = wunits[u]
        return ref.at[pl.ds(al(n * i, 16), n), pl.ds(at, cut)]

    def w_start(u):
        src = wblk(u, d)
        if u >= 3:
            raw_copy((5, 6, 4)[u - 3]).wait()
        rcopy(src, src, wsend.at[u], wrecv.at[u, 0], {"dp": aa}).start()
        rcopy(src, src, wsend.at[u], wrecv.at[u, 1], {"dp": bb}).start()
        rcopy(src, src, wsend.at[u], wrecv.at[u, 3], {"dp": pp}).start()

    def w_many(u, count):
        ref, n, at, cut = wunits[u]
        part = ref.at[pl.ds(0, count * n), pl.ds(at, cut)]
        return rcopy(part, part, wsend.at[u], wrecv.at[u, 3], {"dp": pp})

    def w_wait(u, slot, i):
        rcopy(wblk(u, i), wblk(u, i), wsend.at[u], wrecv.at[u, slot], {"dp": aa}).wait_recv()

    def w_relayb(u):
        w_wait(u, 1, bb)
        rcopy(wblk(u, bb), wblk(u, bb), wsend.at[u], wrecv.at[u, 2], {"dp": aa}).start()
        rcopy(wblk(u, bb), wblk(u, bb), wsend.at[u], wrecv.at[u, 3], {"dp": pp}).start()

    def w_relaya(u):
        w_wait(u, 0, aa)
        rcopy(wblk(u, aa), wblk(u, aa), wsend.at[u], wrecv.at[u, 3], {"dp": pp}).start()

    def w_diag(u):
        w_wait(u, 2, dd)
        rcopy(wblk(u, dd), wblk(u, dd), wsend.at[u], wrecv.at[u, 3], {"dp": pp}).start()

    def w_done(u):
        w_many(u, 4).wait_recv()

    def w_sent(u):
        w_many(u, 7).wait_send()

    zfull = (xf, gf, n2, ghf)
    zhbm = (tok, cot, None, None)

    def zblk(u, s, i, h=None):
        at = pl.ds(al(s * seq + i * rows, 16), rows)
        return zfull[u].at[at] if h is None else zfull[u].at[at, pl.ds(h * half, half)]

    def zcopy(u, s, k, way, h, i, src=None):
        blk = zblk(u, s, i, h)
        return rcopy(
            blk if src is None else src, blk, zsend.at[u, s], zrecv.at[u % 3, s, way, k, h], zdev[way]
        )

    def zag_send(u, s, k, way, h):
        i = z - k if way == 0 else z + k
        go = (z < 3) & (i >= 0) if way == 0 else (z > 0) & (i <= 3)

        @pl.when(go)
        def _():
            src = zhbm[u].at[s, :, pl.ds(h * half, half)] if k == 0 and zhbm[u] is not None else None
            zcopy(u, s, k, way, h, i, src).start()

    def own_copy(u, s):
        return pltpu.make_async_copy(zhbm[u].at[s], zblk(u, s, z), lsem.at[2 + 2 * u + s])

    def ag(u, s, t, way=None):
        if t == 0:
            if zhbm[u] is not None:
                own_copy(u, s).start()
            for part in (0, 1):
                for side in (0, 1):
                    zag_send(u, s, 0, side, part)
            return
        i = z - t if way == 0 else z + t
        go = (i >= 0) if way == 0 else (i <= 3)

        for h in (0, 1):
            @pl.when(go)
            def _():
                zcopy(u, s, t - 1, way, h, i).wait_recv()

            if t < 3:
                zag_send(u, s, t, way, h)

    def own_here(u, s):
        own_copy(u, s).wait()

    def zag_sent(u, s):
        def sent(count):
            part = zfull[u].at[pl.ds(0, count * rows)]
            rcopy(part, part, zsend.at[u, s], zrecv.at[u % 3, s, 0, 0, 0], zdev[0]).wait_send()

        @pl.when((z == 0) | (z == 3))
        def _():
            sent(1)

        @pl.when((z > 0) & (z < 3))
        def _():
            sent(5)

    zpart = (pa, pb, pa, pa)
    zgot = (ra, rb, ra, ra)

    def rs_copy(u, s, way, t, dest, h):
        cut = pl.ds(h * half, half)
        return rcopy(
            zpart[u].at[pl.ds(al(s * seq + dest * rows, 16), rows), cut],
            zgot[u].at[s, way, t, :, cut],
            rsend.at[u, s],
            rrecv.at[1 if u == 1 else 0, s, way, t, h],
            zdev[way],
        )

    def rs_add(u, s, way, t, target, base, cut):
        def body(i, carry):
            at = pl.ds(al(base + i * 16, 16), 16)
            got = zgot[u][s, way, t, pl.ds(al(i * 16, 16), 16), cut].astype(F32)
            target[at, cut] = (target[at, cut].astype(F32) + got).astype(target.dtype)
            return carry

        lax.fori_loop(0, rows // 16, body, 0)

    def rs(u, s, t, way):
        from_end = z if way == 0 else 3 - z
        dest = 3 + z - t if way == 0 else t - from_end

        @pl.when(from_end <= t)
        def _():
            for h in (0, 1):
                if t > 0:
                    @pl.when(from_end > 0)
                    def _():
                        rs_copy(u, s, way, t - 1, z, h).wait_recv()
                        rs_add(u, s, way, t - 1, zpart[u], s * seq + dest * rows, pl.ds(h * half, half))

                rs_copy(u, s, way, t, dest, h).start()

    def rs_final(u, s):
        def first(i, carry):
            at = pl.ds(al(i * 16, 16), 16)
            acc[at, :] = zpart[u][pl.ds(al(s * seq + own + i * 16, 16), 16), :].astype(F32)
            return carry

        lax.fori_loop(0, rows // 16, first, 0)
        for way in (0, 1):
            from_end = z if way == 0 else 3 - z

            @pl.when(from_end > 0)
            def _():
                for h in (0, 1):
                    rs_copy(u, s, way, 2, z, h).wait_recv()
                rs_add(u, s, way, 2, acc, 0, pl.ds(0, width))

    def rs_sent(u, s):
        part = zpart[u].at[pl.ds(0, 3 * rows)]
        rcopy(part, part, rsend.at[u, s], rrecv.at[0, s, 0, 0, 0], zdev[0]).wait_send()

    gunits = (
        (gf, act, 0, ff),
        (n2, dgu, 0, ff),
        (n2, dgu, ff, ff),
        (ghf, ob, 0, qp),
        (n1, dq3, 0, inw),
    )

    def xslot(u, chip):
        b, n = u % 2, gunits[u][3]
        return xb.at[b, pl.ds(al(chip * shard, 16), shard), pl.ds(0, n)]

    def gslot(u, chip, core):
        b, n = u % 2, gunits[u][3]
        return gb.at[b, pl.ds(al(chip * pair + core * shard, 16), shard), pl.ds(0, n)]

    def g_exchange(u, chip, i):
        return rcopy(gslot(u, chip, 1 - c), xslot(u, chip), gsend.at[u % 2], grecv.at[u % 2, i], {"dp": pp})

    chips = (chip_d, chip_x, chip_y, chip_own)

    def g_compute(u, i):
        left, right, at, n = gunits[u]
        chip = chips[i]
        if u >= 2 and i == 0:
            pl.semaphore_wait(credit.at[0], 1)
        tile = 256

        def body(j, carry):
            lhs = left[:, pl.ds(al(chip * pair, LANES), pair)]
            got = tn(lhs, right[:, pl.ds(al(at + j * tile, tile), tile)])
            gb[u % 2, pl.ds(al(chip * pair, 16), pair), pl.ds(al(j * tile, tile), tile)] = got.astype(BF)
            return carry

        lax.fori_loop(0, n // tile, body, 0)
        g_exchange(u, chip, i).start()

    def g_add(u, chip, extra=None):
        b, n = u % 2, gunits[u][3]

        def body(i, carry):
            at = pl.ds(al(chip * shard + i * 16, 16), 16)
            mine = gb[b, pl.ds(al(chip * pair + c * shard + i * 16, 16), 16), pl.ds(0, n)].astype(F32)
            total = mine + xb[b, at, pl.ds(0, n)].astype(F32)
            if extra is not None:
                total = total + extra[b, pl.ds(al(i * 16, 16), 16), pl.ds(0, n)].astype(F32)
            xb[b, at, pl.ds(0, n)] = total.astype(BF)
            return carry

        lax.fori_loop(0, shard // 16, body, 0)

    def g_hop(u):
        b, n = u % 2, gunits[u][3]
        return rcopy(xslot(u, chip_d), hop.at[b, :, pl.ds(0, n)], gsend.at[b], grecv.at[b, 4], {"dp": aa})

    def g_last(u, way):
        b, n = u % 2, gunits[u][3]
        chip, dev = (chip_a, aa) if way == 0 else (chip_b, bb)
        return rcopy(
            xslot(u, chip), fin.at[b, way, :, pl.ds(0, n)], gsend.at[b], grecv.at[b, 5 + way], {"dp": dev}
        )

    def g_first(u):
        g_exchange(u, chip_d, 0).wait_recv()
        g_add(u, chip_d)
        if u >= 2:
            pl.semaphore_wait(credit.at[1], 1)
        g_hop(u).start()

    def g_firstb(u):
        g_exchange(u, chip_x, 1).wait_recv()
        g_exchange(u, chip_y, 2).wait_recv()
        g_add(u, chip_a)
        g_last(u, 0).start()

    def g_second(u):
        g_hop(u).wait_recv()
        g_add(u, chip_b, hop)
        if u >= 2:
            pl.semaphore_wait(credit.at[2], 1)
        g_last(u, 1).start()

    def picked(at, cut, which):
        value = stage[at, cut]
        high = value.astype(BF)
        rest = value - high.astype(F32)
        mid = rest.astype(BF)
        low = (rest - mid.astype(F32)).astype(BF)
        return nt(high, which) + (nt(mid, which) + nt(low, which))

    def g_finish(u):
        b, n = u % 2, gunits[u][3]
        g_exchange(u, chip_own, 3).wait_recv()
        g_last(u, 0).wait_recv()
        g_last(u, 1).wait_recv()
        out = (gdown_v, ggate_v, gup_v, stage, stage)[u]

        def body(i, carry):
            at = pl.ds(al(i * 16, 16), 16)
            total = gb[b, pl.ds(al(chip_own * pair + c * shard + i * 16, 16), 16), pl.ds(0, n)].astype(F32)
            total = total + xb[b, pl.ds(al(chip_own * shard + i * 16, 16), 16), pl.ds(0, n)].astype(F32)
            total = total + fin[b, 0, at, pl.ds(0, n)].astype(F32)
            out[at, pl.ds(0, n)] = total + fin[b, 1, at, pl.ds(0, n)].astype(F32)
            return carry

        lax.fori_loop(0, shard // 16, body, 0)
        rows_all = pl.ds(0, shard)
        if u == 3:
            gout_v[...] = picked(rows_all, pl.ds(0, qp), head_pick(gout_v.shape[1]))
        if u == 4:
            gq_v[...] = picked(rows_all, pl.ds(0, qp), head_pick(gq_v.shape[1]))
            gk_v[...] = picked(rows_all, pl.ds(qp, kp), head_pick(gk_v.shape[1]))
            gv_v[...] = picked(rows_all, pl.ds(qp + kp, kp), head_pick(gv_v.shape[1]))
        part = gb.at[b, pl.ds(0, 7 * shard), pl.ds(0, n)]
        rcopy(part, part, gsend.at[b], grecv.at[b, 0], {"dp": pp}).wait_send()
        if u < 3:
            pl.semaphore_signal(credit.at[0], inc=1, device_id={"dp": pp}, device_id_type=MESH)
            pl.semaphore_signal(credit.at[1], inc=1, device_id={"dp": aa}, device_id_type=MESH)
            pl.semaphore_signal(credit.at[2], inc=1, device_id={"dp": bb}, device_id_type=MESH)

    def gain_rows():
        for j in range(4):
            at = pl.ds(j * pair, pair)
            gains[:, at] = (
                wgn[pl.ds(32 * j, 16), :].astype(F32) + wgn[pl.ds(32 * j + 16, 16), :].astype(F32)
            )

    def norm1(s, t):
        gain = gains[0:1, :]

        def shard_rows(i):
            def body(r, carry):
                at = pl.ds(al(s * seq + i * rows + r * 16, 16), 16)
                x = xf[at, :].astype(F32)
                scale = lax.rsqrt(jnp.mean(x * x, axis=-1, keepdims=True) + eps)
                n1[at, :] = (x * scale * gain).astype(BF)
                return carry

            lax.fori_loop(0, rows // 16, body, 0)

        if t == 0:
            own_here(0, s)
            shard_rows(z)
            return

        @pl.when(z - t >= 0)
        def _():
            shard_rows(z - t)

        @pl.when(z + t <= 3)
        def _():
            shard_rows(z + t)

    head_scale = HEAD ** (-0.5)

    def project(s):
        at = pl.ds(s * seq, seq)
        cosine, sine = cosr[s], sinr[s]
        for j in range(inw // 256):
            both = nn(n1[at, :], wi[:, pl.ds(j * 256, 256)])
            for half in range(2):
                col = j * 256 + half * LANES
                part = both[:, half * LANES : (half + 1) * LANES]
                if col < qp + kp:
                    part = part * cosine + pltpu.roll(part, LANES // 2, 1) * sine
                if col < qp:
                    part = part * head_scale
                qkv[at, pl.ds(col, LANES)] = part.astype(BF)

    def attend(s, part):
        at = pl.ds(s * seq, seq)
        oc = ordr[s : s + 1, :].astype(F32)
        mask = (oc <= cols[s, :, 0:1]) & (oc >= cols[s, :, 1:2])

        def body(h, carry):
            g = h // per_group
            q = qkv[at, pl.ds(al(h * LANES, LANES), LANES)]
            k = qkv[at, pl.ds(al(qp + g * LANES, LANES), LANES)]
            v = qkv[at, pl.ds(al(qp + kp + g * LANES, LANES), LANES)]
            sc = jnp.where(mask, nt(q, k), -1e30)
            e = jnp.exp(sc - jnp.max(sc, axis=-1, keepdims=True))
            p = e * (1.0 / jnp.sum(e, axis=-1, keepdims=True))
            p = p.astype(BF)
            pr[s * heads + h] = p
            ob[at, pl.ds(al(h * LANES, LANES), LANES)] = nn(p, v).astype(BF)
            return carry

        half = heads // 2
        lax.fori_loop(part * half, (part + 1) * half, body, 0)

    def spread(s, dst, left, weight, tile, part=0, parts=1):
        at = pl.ds(s * seq, seq)

        def body(j, carry):
            col = al(j * tile, tile)
            dst[at, pl.ds(col, tile)] = nt(left[at, :], weight[pl.ds(col, tile), :]).astype(BF)
            return carry

        count = width // tile // parts
        lax.fori_loop(part * count, (part + 1) * count, body, 0)

    def spread_gain(s):
        at = pl.ds(s * seq, seq)
        tile = 512

        def body(j, carry):
            col = pl.ds(al(j * tile, tile), tile)
            got = nt(dq3[at, :], wi[col, :])
            pa[at, col] = got.astype(BF)
            gpart[0:1, col] += jnp.sum(got * n1[at, col].astype(F32), axis=0, keepdims=True)
            return carry

        lax.fori_loop(0, width // tile, body, 0)

    def norm2(s):
        gain = gains[1:2, :]
        base = s * rows

        def body(i, carry):
            r = pl.ds(al(i * 16, 16), 16)
            h = tbuf[s, r, :].astype(F32) + acc[r, :]
            hb[pl.ds(al(base + i * 16, 16), 16), :] = h
            scale = lax.rsqrt(jnp.mean(h * h, axis=-1, keepdims=True) + eps)
            real = cols[s, pl.ds(al(own + i * 16, 16), 16), 2:3]
            n2[pl.ds(al(s * seq + own + i * 16, 16), 16), :] = (h * (scale * real) * gain).astype(BF)
            return carry

        lax.fori_loop(0, rows // 16, body, 0)

    def feed_forward(s, part):
        at = pl.ds(s * seq, seq)
        one, two = pl.ds(part * 256, 256), pl.ds(ff + part * 256, 256)
        gate = nn(n2[at, :], wu[:, one])
        upper = nn(n2[at, :], wu[:, two])
        sigma = 1.0 / (1.0 + jnp.exp(-gate))
        swish = gate * sigma
        act[at, one] = (swish * upper).astype(BF)
        dgu[at, one] = (upper * sigma * (1.0 + gate * (1.0 - sigma))).astype(BF)
        dgu[at, two] = swish.astype(BF)

    def feed_back(s, part):
        if part == 0:
            own_here(1, s)
        at = pl.ds(s * seq, seq)
        one, two = pl.ds(part * 256, 256), pl.ds(ff + part * 256, 256)
        back = nn(gf[at, :], wd[:, one])
        dgu[at, one] = (back * dgu[at, one].astype(F32)).astype(BF)
        dgu[at, two] = (back * dgu[at, two].astype(F32)).astype(BF)

    def finish_out(s):
        def body(i, carry):
            r = pl.ds(al(i * 16, 16), 16)
            real = cols[s, pl.ds(al(own + i * 16, 16), 16), 2:3]
            y = (hb[pl.ds(al(s * rows + i * 16, 16), 16), :] + acc[r, :]) * real
            out_v[s, r, :] = y.astype(BF)
            return carry

        lax.fori_loop(0, rows // 16, body, 0)

    def norm2_back(s):
        gain = gains[1:2, :]

        def body(i, carry):
            r = pl.ds(al(i * 16, 16), 16)
            ro = pl.ds(al(s * rows + i * 16, 16), 16)
            h = hb[ro, :]
            scale = lax.rsqrt(jnp.mean(h * h, axis=-1, keepdims=True) + eps)
            unit = h * scale
            grad = acc[r, :]
            inner = grad * gain
            dy = gf[pl.ds(al(s * seq + own + i * 16, 16), 16), :].astype(F32)
            dy = dy * cols[s, pl.ds(al(own + i * 16, 16), 16), 2:3]
            dhr = dy + scale * (inner - unit * jnp.mean(inner * unit, axis=-1, keepdims=True))
            gtok_v[s, r, :] = dhr
            ghf[pl.ds(al(s * seq + own + i * 16, 16), 16), :] = dhr.astype(BF)
            return carry + jnp.sum(grad * unit, axis=0, keepdims=True)

        gpart[1:2, :] += lax.fori_loop(0, rows // 16, body, jnp.zeros((1, width), F32))

    def grad_heads(s):
        at = pl.ds(s * seq, seq)
        for j in range(qp // 256):
            dq3[at, pl.ds(j * 256, 256)] = nn(ghf[at, :], wo[:, pl.ds(j * 256, 256)]).astype(BF)

    def attend_back(s):
        at = pl.ds(s * seq, seq)
        cosine, sine = cosr[s], sinr[s]

        def body(g, carry):
            k = qkv[at, pl.ds(al(qp + g * LANES, LANES), LANES)]
            v = qkv[at, pl.ds(al(qp + kp + g * LANES, LANES), LANES)]
            dk = jnp.zeros((seq, LANES), F32)
            dv = jnp.zeros((seq, LANES), F32)
            for m in range(per_group):
                h = g * per_group + m
                hat = pl.ds(al(h * LANES, LANES), LANES)
                q = qkv[at, hat]
                do = dq3[at, hat]
                low = pr[s * heads + h]
                p = low.astype(F32)
                dp = nt(do, v)
                ds = (p * (dp - jnp.sum(p * dp, axis=-1, keepdims=True))).astype(BF)
                dv = dv + tn(low, do)
                dk = dk + tn(ds, q)
                dq = nn(ds, k) * head_scale
                dq3[at, hat] = (dq * cosine - pltpu.roll(dq, LANES // 2, 1) * sine).astype(BF)
            dq3[at, pl.ds(al(qp + g * LANES, LANES), LANES)] = (
                dk * cosine - pltpu.roll(dk, LANES // 2, 1) * sine
            ).astype(BF)
            dq3[at, pl.ds(al(qp + kp + g * LANES, LANES), LANES)] = dv.astype(BF)
            return carry

        lax.fori_loop(0, groups, body, 0)

    def norm1_back(s):
        gain = gains[0:1, :]

        def body(i, carry):
            r = pl.ds(al(i * 16, 16), 16)
            x = tbuf[s, r, :].astype(F32)
            scale = lax.rsqrt(jnp.mean(x * x, axis=-1, keepdims=True) + eps)
            unit = x * scale
            grad = acc[r, :]
            inner = grad * gain
            gtok_v[s, r, :] += scale * (inner - unit * jnp.mean(inner * unit, axis=-1, keepdims=True))
            return carry

        lax.fori_loop(0, rows // 16, body, 0)

    X, COT, N2, GH = 0, 1, 2, 3
    BR, FFN, DN2, DN1 = 0, 1, 2, 3

    def tok_copy(s):
        return pltpu.make_async_copy(tok.at[s], tbuf.at[s], lsem.at[s])

    def fin_br(s):
        rs_final(BR, s)
        tok_copy(s).wait()
        norm2(s)
        ag(N2, s, 0)

    def fin_dn2(s):
        rs_final(DN2, s)
        norm2_back(s)
        ag(GH, s, 0)

    def fin_ffn(s):
        rs_final(FFN, s)
        finish_out(s)

    def fin_dn1(s):
        rs_final(DN1, s)
        norm1_back(s)

    def e_copy(i, src, dev):
        line = i < 6
        return rcopy(src, gex.at[i], esend.at[0 if line else 1], erecv.at[i if line else i // 2 + 3], dev)

    def e_line(t):
        if t == 0:
            for j in range(4):
                at = pl.ds(j * pair, pair)
                gsum[j : j + 1, :] = gpart[0:1, at] / gains[0:1, at]
                gsum[4 + j : 5 + j, :] = gpart[1:2, at]
        for way in (0, 1):
            here = (z - t >= 0) if way == 0 else (z + t <= 3)
            on = (z < 3) if way == 0 else (z > 0)
            slot = 3 * way + t

            @pl.when(here)
            def _():
                if t > 0:
                    e_copy(slot - 1, gsum, zdev[way]).wait_recv()
                if t < 3:
                    @pl.when(on)
                    def _():
                        e_copy(slot, gsum if t == 0 else gex.at[slot - 1], zdev[way]).start()

        if t == 3:
            gex[6] = gsum[...]
            for way in (0, 1):
                for k in (1, 2, 3):
                    @pl.when((z - k >= 0) if way == 0 else (z + k <= 3))
                    def _():
                        gex[6] += gex[3 * way + k - 1]

            e_copy(7, gex.at[6], {"dp": pp}).start()

    def e_plane(t):
        i = 7 + 2 * t
        dev = (pp, aa, bb)[t]
        e_copy(i, gex.at[i - 1], {"dp": dev}).wait()
        total = gex[i - 1] + gex[i]
        if t < 2:
            gex[i + 1] = total
            e_copy(i + 2, gex.at[i + 1], {"dp": (aa, bb)[t]}).start()
        else:
            gex[12] = total
            for at, out in ((0, gone_v), (4, gtwo_v)):
                line = gex[12, pl.ds(at + d // 2, 1), :]
                out[...] = jnp.where(c == 0, line[:, :shard], line[:, shard:])

    def e_sent():
        def sent(count):
            part = gex.at[pl.ds(0, count)]
            rcopy(part, part, esend.at[0], erecv.at[0], zdev[0]).wait_send()

        @pl.when((z == 0) | (z == 3))
        def _():
            sent(1)

        @pl.when((z > 0) & (z < 3))
        def _():
            sent(5)

    def clean(i):
        if i == 0:
            for u in range(6):
                w_sent(u)
        elif i < 4:
            for s in (0, 1):
                zag_sent((COT, N2, GH)[i - 1], s)
        else:
            rs_sent(FFN, i - 4)

    for i in (7, 8, 0, 1, 2, 3, 5, 6, 4):
        raw_copy(i).start()
    gpart[...] = jnp.zeros_like(gpart)
    for s in (0, 1):
        tok_copy(s).start()
    pl.semaphore_wait(barrier, 3 + (z + 3) // 4 + (6 - z) // 4)
    ag(X, 0, 0)
    prep_gain()
    w_start(0)
    prep_in()
    w_start(1)
    prep_out()
    w_start(2)
    ag(X, 0, 1, 1)
    w_relayb(0)
    ag(X, 0, 1, 0)
    ag(X, 1, 0)
    prep_rows(0)
    w_relayb(1)
    w_relaya(1)
    ag(X, 0, 2, 0)
    w_diag(0)
    w_relaya(0)
    ag(X, 0, 2, 1)
    ag(COT, 0, 0)
    ag(X, 1, 1, 1)
    prep_rows(1)
    w_done(0)
    gain_rows()
    norm1(0, 1)
    w_relayb(2)
    norm1(0, 0)
    w_diag(1)
    norm1(0, 2)
    ag(X, 0, 3, 1)
    ag(X, 0, 3, 0)
    norm1(0, 3)
    w_relaya(2)
    ag(X, 1, 1, 0)
    w_done(1)
    project(0)
    w_diag(2)
    w_start(3)
    attend(0, 0)
    attend(0, 1)
    w_done(2)
    spread(0, pa, ob, wo, 512)
    rs(BR, 0, 0, 1)
    rs(BR, 0, 0, 0)
    ag(COT, 0, 1, 0)
    ag(X, 1, 2, 1)
    w_start(4)
    ag(COT, 0, 1, 1)
    rs(BR, 0, 1, 1)
    norm1(1, 0)
    ag(X, 1, 2, 0)
    ag(COT, 0, 2, 0)
    rs(BR, 0, 1, 0)
    norm1(1, 2)
    norm1(1, 1)
    rs(BR, 0, 2, 1)
    ag(X, 1, 3, 1)
    ag(X, 1, 3, 0)
    norm1(1, 3)
    rs(BR, 0, 2, 0)
    w_relayb(3)
    project(1)
    attend(1, 0)
    w_start(5)
    attend(1, 1)
    ag(COT, 0, 2, 1)
    spread(1, pa, ob, wo, 512)
    rs(BR, 1, 0, 0)
    rs(BR, 1, 0, 1)
    fin_br(0)
    rs_sent(BR, 0)
    rs(BR, 1, 1, 0)
    ag(N2, 0, 1, 0)
    w_relaya(3)
    w_relaya(4)
    rs(BR, 1, 1, 1)
    w_relayb(4)
    ag(N2, 0, 1, 1)
    ag(COT, 0, 3, 1)
    rs(BR, 1, 2, 0)
    rs(BR, 1, 2, 1)
    w_relayb(5)
    ag(N2, 0, 2, 1)
    w_diag(3)
    ag(N2, 0, 2, 0)
    ag(COT, 1, 0)
    w_diag(4)
    fin_br(1)
    ag(N2, 0, 3, 0)
    w_done(4)
    w_relaya(5)
    ag(N2, 0, 3, 1)
    w_done(3)
    feed_forward(0, 0)
    w_diag(5)
    rs_sent(BR, 1)
    feed_forward(0, 1)
    feed_forward(0, 2)
    feed_forward(0, 3)
    w_done(5)
    spread(0, pb, act, wd, 512)
    rs(FFN, 0, 0, 1)
    ag(COT, 1, 1, 1)
    ag(COT, 1, 1, 0)
    rs(FFN, 0, 0, 0)
    ag(COT, 0, 3, 0)
    feed_back(0, 0)
    feed_back(0, 1)
    feed_back(0, 2)
    feed_back(0, 3)
    spread(0, pa, dgu, wu, 256, 0, 2)
    spread(0, pa, dgu, wu, 256, 1, 2)
    rs(DN2, 0, 0, 0)
    zag_sent(X, 1)
    ag(N2, 1, 1, 1)
    ag(N2, 1, 1, 0)
    rs(DN2, 0, 0, 1)
    clean(0)
    rs(DN2, 0, 1, 1)
    rs(FFN, 0, 1, 1)
    rs(DN2, 0, 1, 0)
    ag(N2, 1, 2, 1)
    rs(FFN, 0, 1, 0)
    ag(N2, 1, 3, 1)
    ag(N2, 1, 2, 0)
    ag(N2, 1, 3, 0)
    ag(COT, 1, 2, 1)
    feed_forward(1, 0)
    feed_forward(1, 1)
    feed_forward(1, 2)
    ag(COT, 1, 2, 0)
    zag_sent(X, 0)
    rs(DN2, 0, 2, 0)
    feed_forward(1, 3)
    rs(DN2, 0, 2, 1)
    ag(COT, 1, 3, 0)
    ag(COT, 1, 3, 1)
    feed_back(1, 0)
    feed_back(1, 1)
    feed_back(1, 2)
    feed_back(1, 3)
    spread(1, pa, dgu, wu, 256, 0, 2)
    spread(1, pa, dgu, wu, 256, 1, 2)
    rs(DN2, 1, 0, 1)
    rs(DN2, 1, 0, 0)
    g_compute(0, 0)
    g_compute(0, 1)
    fin_dn2(0)
    g_first(0)
    g_compute(0, 2)
    g_compute(0, 3)
    g_firstb(0)
    rs(DN2, 1, 1, 0)
    rs(DN2, 1, 1, 1)
    g_compute(1, 0)
    g_compute(1, 1)
    g_second(0)
    ag(GH, 0, 1, 0)
    ag(GH, 0, 1, 1)
    g_compute(1, 2)
    rs(DN2, 1, 2, 0)
    rs(DN2, 1, 2, 1)
    spread(1, pb, act, wd, 512)
    rs(FFN, 1, 0, 1)
    ag(GH, 0, 2, 0)
    rs(FFN, 1, 0, 0)
    ag(GH, 0, 2, 1)
    g_first(1)
    g_firstb(1)
    fin_dn2(1)
    g_finish(0)
    rs_sent(DN2, 0)
    g_compute(1, 3)
    g_compute(2, 0)
    ag(GH, 0, 3, 0)
    g_second(1)
    ag(GH, 0, 3, 1)
    grad_heads(0)
    attend_back(0)
    ag(GH, 1, 1, 0)
    rs(FFN, 1, 1, 0)
    g_first(2)
    ag(GH, 1, 1, 1)
    rs(FFN, 1, 1, 1)
    g_compute(2, 1)
    spread_gain(0)
    rs(DN1, 0, 0, 0)
    g_compute(2, 2)
    ag(GH, 1, 2, 1)
    rs(DN1, 0, 0, 1)
    g_firstb(2)
    ag(GH, 1, 2, 0)
    rs(FFN, 0, 2, 0)
    g_finish(1)
    g_compute(2, 3)
    rs(FFN, 1, 2, 1)
    g_second(2)
    ag(GH, 1, 3, 0)
    ag(GH, 1, 3, 1)
    rs(FFN, 0, 2, 1)
    g_compute(3, 0)
    g_compute(3, 1)
    rs(FFN, 1, 2, 0)
    grad_heads(1)
    attend_back(1)
    g_first(3)
    rs_sent(DN2, 1)
    spread_gain(1)
    rs(DN1, 1, 0, 1)
    e_line(0)
    rs(DN1, 1, 0, 0)
    rs(DN1, 0, 1, 0)
    g_compute(3, 2)
    rs(DN1, 0, 1, 1)
    g_compute(3, 3)
    g_firstb(3)
    g_finish(2)
    g_compute(4, 0)
    g_second(3)
    g_first(4)
    rs(DN1, 1, 1, 1)
    g_compute(4, 1)
    e_line(1)
    g_compute(4, 2)
    rs(DN1, 1, 1, 0)
    clean(2)
    clean(5)
    g_firstb(4)
    fin_ffn(0)
    e_line(2)
    clean(3)
    rs(DN1, 0, 2, 0)
    g_finish(3)
    rs(DN1, 0, 2, 1)
    e_line(3)
    e_plane(0)
    rs(DN1, 1, 2, 0)
    g_second(4)
    g_compute(4, 3)
    fin_ffn(1)
    rs(DN1, 1, 2, 1)
    fin_dn1(0)
    clean(1)
    clean(4)
    e_plane(1)
    g_finish(4)
    e_plane(2)
    fin_dn1(1)
    for s in (0, 1):
        rs_sent(DN1, s)
    e_sent()


def put_out(*refs):
    ins, outs, sem = refs[:11], refs[11:22], refs[22]
    copies = [pltpu.make_async_copy(src, dst, sem.at[i]) for i, (src, dst) in enumerate(zip(ins, outs))]
    for copy in copies:
        copy.start()
    for copy in copies:
        copy.wait()


def fused(
    tokens,
    cotangent,
    order,
    lengths,
    gain_attn,
    w_query,
    w_key,
    w_value,
    w_out,
    gain_ffn,
    w_gate,
    w_up,
    w_down,
):
    micro, rows, width = tokens.shape
    seq = rows * lax.axis_size("tensor")
    shard = w_query.shape[0]
    ff = w_gate.shape[1]
    groups = w_key.shape[1] // HEAD
    q_cols, k_cols = w_query.shape[1], w_key.shape[1]
    qp = q_cols // HEAD * LANES
    kp = groups * LANES
    inw = qp + 2 * kp
    total = micro * seq
    vm = pltpu.VMEM
    dma = pltpu.SemaphoreType.DMA
    scratch = [
        vm((8 * 16, 2 * shard), BF),
        vm((width, inw), BF),
        vm((width, qp), BF),
        vm((width, 2 * ff), BF),
        vm((width, ff), BF),
        vm((total, width), BF),
        vm((total, width), BF),
        vm((total, width), BF),
        vm((total, width), BF),
        vm((total, inw), BF),
        vm((total, qp), BF),
        vm((total, ff), BF),
        vm((total, inw), BF),
        vm((total, 2 * ff), BF),
        vm((micro * qp // LANES, seq, seq), BF),
        vm((micro * rows, width), F32),
        vm((total, width), BF),
        vm((total, width), BF),
        vm((micro, 2, 3, rows, width), BF),
        vm((micro, 2, 3, rows, width), BF),
        vm((2, width, ff), BF),
        vm((2, width // 2, ff), BF),
        vm((2, shard, ff), BF),
        vm((2, 2, shard, ff), BF),
        vm((shard, ff), F32),
        vm((rows, width), F32),
        vm((16, width), F32),
        vm((8, width), F32),
        vm((8, width // 4), F32),
        vm((13, 8, width // 4), F32),
        vm((micro, rows, width), BF),
        vm(gain_attn.shape, BF),
        vm(gain_ffn.shape, BF),
        vm(w_query.shape, BF),
        vm(w_key.shape, BF),
        vm(w_value.shape, BF),
        vm(w_out.shape[::-1], BF),
        vm((micro, seq, LANES), F32),
        vm((micro, seq, LANES), F32),
        vm((micro, seq, LANES), F32),
        dma((6,)),
        dma((6, 4)),
        dma((4, 2)),
        dma((3, 2, 2, 3, 2)),
        dma((4, 2)),
        dma((2, 2, 2, 3, 2)),
        dma((2,)),
        dma((2, 7)),
        dma((2,)),
        dma((9,)),
        dma((6,)),
        dma((9,)),
        pltpu.SemaphoreType.REGULAR((3,)),
    ]
    hbm = pl.BlockSpec(memory_space=pl.ANY)
    vmem = pl.BlockSpec(memory_space=pltpu.VMEM)
    smem = pl.BlockSpec(memory_space=pltpu.SMEM)
    shape = jax.ShapeDtypeStruct
    shapes = [
        vm((micro, rows, width), BF),
        vm((micro, rows, width), F32),
        vm((shard, ff), F32),
        vm((shard, ff), F32),
        vm((shard, ff), F32),
        vm((shard, q_cols), F32),
        vm((shard, q_cols), F32),
        vm((shard, k_cols), F32),
        vm((shard, k_cols), F32),
        vm((1, shard), F32),
        vm((1, shard), F32),
    ]
    dims = (rows, seq, width, shard, qp, kp, ff, groups)
    out, gtok, gdown, ggate, gup, gout, gq, gk, gv, one, two = pl.pallas_call(
        functools.partial(block_kernel, dims),
        out_shape=shapes,
        in_specs=[hbm] * 11 + [vmem, smem],
        out_specs=[vmem] * 11,
        scratch_shapes=scratch,
        compiler_params=pltpu.CompilerParams(
            collective_id=0, has_side_effects=True, vmem_limit_bytes=61_600_000
        ),
        name="block",
    )(
        tokens,
        cotangent,
        gain_attn,
        gain_ffn,
        w_query,
        w_key,
        w_value,
        w_out.T,
        w_gate,
        w_up,
        w_down.T,
        order,
        lengths,
    )
    results = [out, gtok, gdown, ggate, gup, gout, gq, gk, gv, one, two]
    out, gtok, gdown, ggate, gup, gout, gq, gk, gv, one, two = pl.pallas_call(
        put_out,
        out_shape=[shape(x.shape, x.dtype) for x in results],
        in_specs=[vmem] * 11,
        out_specs=[hbm] * 11,
        scratch_shapes=[dma((11,))],
        compiler_params=pltpu.CompilerParams(vmem_limit_bytes=2**18),
        name="put_out",
    )(*results)
    return out, gtok, one[0], gq, gk, gv, gout.T, two[0], ggate, gup, gdown.T


def local(tokens, *rest):
    fits = lax.axis_size("dp") == 8 and lax.axis_size("tensor") == 4 and tokens.shape[0] == 2
    return (fused if fits else spread_out)(tokens, *rest)


def solution(mesh):
    return jax.shard_map(
        local,
        mesh=mesh,
        in_specs=(
            P("dp", "tensor", None),
            P("dp", "tensor", None),
            P("dp", None),
            P("dp", None),
            P("dp"),
            P("dp", "tensor"),
            P("dp", "tensor"),
            P("dp", "tensor"),
            P("tensor", "dp"),
            P("dp"),
            P("dp", "tensor"),
            P("dp", "tensor"),
            P("tensor", "dp"),
        ),
        out_specs=(
            P("dp", "tensor", None),
            P("dp", "tensor", None),
            P("dp"),
            P("dp", "tensor"),
            P("dp", "tensor"),
            P("dp", "tensor"),
            P("tensor", "dp"),
            P("dp"),
            P("dp", "tensor"),
            P("dp", "tensor"),
            P("tensor", "dp"),
        ),
        check_vma=False,
    )
```

```python
import functools
import math

import jax
import jax.numpy as jnp
from jax import lax
from jax.experimental import pallas as pl
from jax.experimental.pallas import tpu as pltpu
from jax.sharding import PartitionSpec as P

HEAD = 96


eps = 1e-05
rope_base = 100000.0


def rotate(field, cosine, sine):
    half = field.shape[-1] // 2
    first = field[..., :half]
    second = field[..., half:]
    return jnp.concatenate(
        [first * cosine - second * sine, second * cosine + first * sine], axis=-1
    )


def rotate_back(field, cosine, sine):
    half = field.shape[-1] // 2
    first = field[..., :half]
    second = field[..., half:]
    return jnp.concatenate(
        [first * cosine + second * sine, second * cosine - first * sine], axis=-1
    )


def layout(order, lengths):
    starts = jnp.cumsum(lengths, dtype=jnp.int32) - lengths
    docs = jnp.sum((order[:, None] >= starts[None, 1:]).astype(jnp.int32), axis=1, dtype=jnp.int32)
    onehot = docs[:, None] == jnp.arange(lengths.shape[0], dtype=jnp.int32)[None, :]
    first = jnp.sum(jnp.where(onehot, starts[None, :], 0), axis=1, dtype=jnp.int32)
    positions = (order - first).astype(jnp.float32)
    mask = (docs[:, None] == docs[None, :]) & (order[None, :] <= order[:, None])
    real = (docs < lengths.shape[0] - 1).astype(jnp.float32)
    return (positions, mask, real)


def norm_forward(rows, gain):
    scale = lax.rsqrt(jnp.mean(rows * rows, axis=-1, keepdims=True) + eps)
    unit = rows * scale
    return (unit, scale, (unit * gain).astype(jnp.bfloat16))


def norm_backward(grad, unit, scale, gain):
    inner = grad * gain
    return scale * (inner - unit * jnp.mean(inner * unit, axis=-1, keepdims=True))


def contract_rows(left, right):
    return lax.dot_general(
        left, right, (((0,), (0,)), ((), ())), preferred_element_type=jnp.float32
    )


def times_transpose(left, right):
    return lax.dot_general(
        left, right, (((1,), (1,)), ((), ())), preferred_element_type=jnp.float32
    )


def gather_weights(gain_attn, w_query, w_key, w_value, w_out, gain_ffn, w_gate, w_up, w_down):
    gains = lax.all_gather(jnp.stack([gain_attn, gain_ffn], axis=0), "dp", axis=1, tiled=True)
    attn = lax.all_gather(
        jnp.concatenate([w_query, w_key, w_value, w_out.T], axis=1), "dp", axis=0, tiled=True
    )
    gate_up = lax.all_gather(jnp.concatenate([w_gate, w_up], axis=1), "dp", axis=0, tiled=True)
    down = lax.all_gather(w_down.T, "dp", axis=0, tiled=True)
    return gains, attn, gate_up, down


def gather_rows(rows):
    return lax.all_gather(rows, "tensor", axis=1, tiled=True)


def scatter_rows(partial):
    low = partial.astype(jnp.bfloat16)
    return lax.psum_scatter(low, "tensor", scatter_dimension=1, tiled=True).astype(jnp.float32)


def reduce_weights(term):
    low = term.astype(jnp.bfloat16)
    return lax.psum_scatter(low, "dp", scatter_dimension=0, tiled=True).astype(jnp.float32)


def spread_out(
    tokens,
    cotangent,
    order,
    lengths,
    gain_attn,
    w_query,
    w_key,
    w_value,
    w_out,
    gain_ffn,
    w_gate,
    w_up,
    w_down,
):
    micro, rows, width = tokens.shape
    seq = rows * lax.axis_size("tensor")
    q_cols, k_cols, ff_cols = w_query.shape[1], w_key.shape[1], w_gate.shape[1]
    local_heads, local_kv = q_cols // HEAD, k_cols // HEAD
    group = local_heads // local_kv
    first_row = lax.axis_index("tensor") * rows
    freqs = rope_base ** (-2.0 * jnp.arange(HEAD // 2, dtype=jnp.float32) / HEAD)
    head_scale = HEAD ** (-0.5)

    gains, attn, gate_up, down = gather_weights(
        gain_attn, w_query, w_key, w_value, w_out, gain_ffn, w_gate, w_up, w_down
    )
    gain1, gain2 = gains[0].astype(jnp.float32), gains[1].astype(jnp.float32)
    in_cols = q_cols + 2 * k_cols
    w_in, w_out_t = attn[:, :in_cols], attn[:, in_cols:]

    positions, mask, real = jax.vmap(layout)(order, lengths)
    angles = positions[:, :, None] * freqs
    cosine, sine = jnp.cos(angles)[:, :, None, :], jnp.sin(angles)[:, :, None, :]
    mask = mask[:, None, None]
    real_rows = lax.dynamic_slice_in_dim(real, first_row, rows, 1)[:, :, None]

    stream = tokens.astype(jnp.float32)
    unit1, scale1, normed1 = norm_forward(stream, gain1)
    full1 = gather_rows(normed1)
    grad_out_rows = cotangent.astype(jnp.float32) * real_rows
    full_grad = gather_rows(grad_out_rows.astype(jnp.bfloat16))
    flat1 = full1.reshape(micro * seq, width)
    flat_grad = full_grad.reshape(micro * seq, width)

    mixed_in = jnp.dot(flat1, w_in, preferred_element_type=jnp.float32).reshape(micro, seq, in_cols)
    query = mixed_in[..., :q_cols].reshape(micro, seq, local_heads, HEAD)
    keys = mixed_in[..., q_cols : q_cols + k_cols].reshape(micro, seq, local_kv, HEAD)
    values = mixed_in[..., q_cols + k_cols :].reshape(micro, seq, local_kv, HEAD).astype(jnp.bfloat16)
    query = (rotate(query, cosine, sine) * head_scale).astype(jnp.bfloat16)
    query = query.reshape(micro, seq, local_kv, group, HEAD)
    keys = rotate(keys, cosine, sine).astype(jnp.bfloat16)
    scores = jnp.einsum("bqkgd,bskd->bkgqs", query, keys, preferred_element_type=jnp.float32)
    scores = jnp.where(mask, scores, -1e30)
    peak = jnp.max(scores, axis=-1, keepdims=True)
    expon = jnp.exp(scores - peak)
    total = jnp.sum(expon, axis=-1, keepdims=True)
    probs = expon / total
    probs_low = probs.astype(jnp.bfloat16)
    mixed = jnp.einsum("bkgqs,bskd->bqkgd", probs_low, values, preferred_element_type=jnp.float32)
    mixed = mixed.reshape(micro * seq, q_cols).astype(jnp.bfloat16)
    branch = scatter_rows(times_transpose(mixed, w_out_t).reshape(micro, seq, width))
    resid = stream + branch
    unit2, scale2, normed2 = norm_forward(resid, gain2)
    full2 = gather_rows(normed2).reshape(micro * seq, width)

    both = jnp.dot(full2, gate_up, preferred_element_type=jnp.float32)
    gate, upper = both[:, :ff_cols], both[:, ff_cols:]
    sigma = jax.nn.sigmoid(gate)
    hidden = (gate * sigma * upper).astype(jnp.bfloat16)
    ffn = scatter_rows(times_transpose(hidden, down).reshape(micro, seq, width))
    output = ((resid + ffn) * real_rows).astype(jnp.bfloat16)

    grad_hidden = jnp.dot(flat_grad, down, preferred_element_type=jnp.float32)
    grad_gate = (grad_hidden * upper * sigma * (1.0 + gate * (1.0 - sigma))).astype(jnp.bfloat16)
    grad_up = (grad_hidden * gate * sigma).astype(jnp.bfloat16)
    grad_both = jnp.concatenate([grad_gate, grad_up], axis=1)
    grad_norm2 = scatter_rows(times_transpose(grad_both, gate_up).reshape(micro, seq, width))
    final_down = reduce_weights(contract_rows(flat_grad, hidden))
    final_gate = reduce_weights(contract_rows(full2, grad_gate))
    final_up = reduce_weights(contract_rows(full2, grad_up))
    term_gain2 = jnp.sum(grad_norm2 * unit2, axis=(0, 1))
    grad_resid = grad_out_rows + norm_backward(grad_norm2, unit2, scale2, gain2)

    full_resid = gather_rows(grad_resid.astype(jnp.bfloat16)).reshape(micro * seq, width)
    grad_mixed = jnp.dot(full_resid, w_out_t, preferred_element_type=jnp.float32).astype(jnp.bfloat16)
    final_out = reduce_weights(contract_rows(full_resid, mixed))
    grad_heads = grad_mixed.reshape(micro, seq, local_kv, group, HEAD)
    grad_probs = jnp.einsum(
        "bqkgd,bskd->bkgqs", grad_heads, values, preferred_element_type=jnp.float32
    )
    grad_values = jnp.einsum(
        "bkgqs,bqkgd->bskd", probs_low, grad_heads, preferred_element_type=jnp.float32
    )
    grad_scores = (
        probs * (grad_probs - jnp.sum(probs * grad_probs, axis=-1, keepdims=True))
    ).astype(jnp.bfloat16)
    grad_query = jnp.einsum(
        "bkgqs,bskd->bqkgd", grad_scores, keys, preferred_element_type=jnp.float32
    ).reshape(micro, seq, local_heads, HEAD)
    grad_keys = jnp.einsum(
        "bkgqs,bqkgd->bskd", grad_scores, query, preferred_element_type=jnp.float32
    )
    grad_query = rotate_back(grad_query * head_scale, cosine, sine).reshape(micro * seq, q_cols)
    grad_keys = rotate_back(grad_keys, cosine, sine).reshape(micro * seq, k_cols)
    grad_values = grad_values.reshape(micro * seq, k_cols)
    grad_in = jnp.concatenate(
        [grad_query.astype(jnp.bfloat16), grad_keys.astype(jnp.bfloat16), grad_values.astype(jnp.bfloat16)],
        axis=1,
    )
    grad_norm1 = scatter_rows(times_transpose(grad_in, w_in).reshape(micro, seq, width))
    final_in = reduce_weights(contract_rows(flat1, grad_in))
    term_gain1 = jnp.sum(grad_norm1 * unit1, axis=(0, 1))
    grad_tokens = grad_resid + norm_backward(grad_norm1, unit1, scale1, gain1)

    gain_terms = lax.psum(jnp.stack([term_gain1, term_gain2], axis=0), ("dp", "tensor"))
    own = gain_attn.shape[0]
    gain_own = lax.dynamic_slice_in_dim(gain_terms, lax.axis_index("dp") * own, own, 1)
    return (
        output,
        grad_tokens,
        gain_own[0],
        final_in[:, :q_cols],
        final_in[:, q_cols : q_cols + k_cols],
        final_in[:, q_cols + k_cols :],
        final_out.T,
        gain_own[1],
        final_gate,
        final_up,
        final_down.T,
    )


BF = jnp.bfloat16
F32 = jnp.float32
MESH = pl.DeviceIdType.MESH
LANES = 128


def nn(left, right):
    return lax.dot_general(left, right, (((1,), (0,)), ((), ())), preferred_element_type=F32)


def nt(left, right):
    return lax.dot_general(left, right, (((1,), (1,)), ((), ())), preferred_element_type=F32)


def tn(left, right):
    return lax.dot_general(left, right, (((0,), (0,)), ((), ())), preferred_element_type=F32)


def al(value, unit):
    return pl.multiple_of(value, unit)


def block_kernel(dims, *refs):
    (rows, seq, width, shard, qp, kp, ff, groups) = dims
    (tok, cot, ga_h, gf_h, wq_h, wk_h, wv_h, wo_h, wa_h, wb_h, wd_h, ordr, lens) = refs[:13]
    (out_v, gtok_v, gdown_v, ggate_v, gup_v, gout_v, gq_v, gk_v, gv_v, gone_v, gtwo_v) = refs[13:24]
    (wgn, wi, wo, wu, wd, xf, n1, n2, gf, qkv, ob, act, dq3, dgu, pr, hb, pa, pb, ra, rb,
     gb, xb, hop, fin, stage, acc, gains, gpart, gsum, gex, tbuf, rga, rgf, rq, rk, rv, ro, cols, cosr, sinr,
     wsend, wrecv, zsend, zrecv, rsend, rrecv, gsend, grecv, esend, erecv, lsem, psem, credit) = refs[24:]
    ghf = xf
    heads = qp // LANES
    per_group = heads // groups
    inw = qp + 2 * kp
    pair = 2 * shard
    d = lax.axis_index("dp")
    z = lax.axis_index("tensor")
    c = d % 2
    flip = 1 - 2 * c
    near_x = d + 2 - 4 * ((d // 2) % 2)
    near_y = d + 4 - 8 * (d // 4)
    aa = near_x * (1 - c) + near_y * c
    bb = near_y * (1 - c) + near_x * c
    dd = aa + bb - d
    pp = d + flip
    chip_own, chip_a, chip_b, chip_d = d // 2, aa // 2, bb // 2, dd // 2
    chip_x, chip_y = near_x // 2, near_y // 2
    own = z * rows
    half = width // 2
    zdev = {"tensor": z + 1}, {"tensor": z - 1}

    def rcopy(src, dst, ssem, rsem, dev):
        return pltpu.make_async_remote_copy(
            src_ref=src, dst_ref=dst, send_sem=ssem, recv_sem=rsem, device_id=dev, device_id_type=MESH
        )

    barrier = pltpu.get_barrier_semaphore()
    for dev in (pp, aa, bb):
        pl.semaphore_signal(barrier, inc=1, device_id={"dp": dev}, device_id_type=MESH)
    for way in (0, 1):
        @pl.when((z < 3) if way == 0 else (z > 0))
        def _():
            pl.semaphore_signal(barrier, inc=1, device_id=zdev[way], device_id_type=MESH)

    def raw_copy(i):
        src, dst = (
            (wq_h, rq),
            (wk_h, rk),
            (wv_h, rv),
            (wo_h, ro),
            (wd_h, wd.at[pl.ds(al(shard * d, 16), shard), :]),
            (wa_h, wu.at[pl.ds(al(shard * d, 16), shard), pl.ds(0, ff)]),
            (wb_h, wu.at[pl.ds(al(shard * d, 16), shard), pl.ds(ff, ff)]),
            (ga_h, rga),
            (gf_h, rgf),
        )[i]
        return pltpu.make_async_copy(src, dst, psem.at[i])

    def head_map(n):
        row = lax.broadcasted_iota(jnp.int32, (n // HEAD * HEAD, n // HEAD * LANES), 0)
        col = lax.broadcasted_iota(jnp.int32, (n // HEAD * HEAD, n // HEAD * LANES), 1)
        lane = col % 64
        want = (col // 64) * (HEAD // 2) + lane
        return jnp.where((lane < HEAD // 2) & (row == want), 1.0, 0.0).astype(BF)

    head_pick = head_map

    def prep_gain():
        raw_copy(7).wait()
        raw_copy(8).wait()
        line = lax.broadcasted_iota(jnp.int32, (16, shard), 0)
        one = jnp.broadcast_to(rga[...].reshape(1, shard).astype(F32), (16, shard))
        two = jnp.broadcast_to(rgf[...].reshape(1, shard).astype(F32), (16, shard))
        row = lax.broadcasted_iota(jnp.int32, (shard, pair), 0)
        col = lax.broadcasted_iota(jnp.int32, (shard, pair), 1)
        place = jnp.where(col == row + shard * c, 1.0, 0.0).astype(BF)
        both = jnp.where(line == 0, one, two).astype(BF)
        wgn[pl.ds(al(16 * d, 16), 16), :] = nn(both, place).astype(BF)

    def prep_in():
        at = pl.ds(al(shard * d, 16), shard)
        for i in range(3):
            raw_copy(i).wait()
        wide = head_map(rq.shape[1])
        narrow = head_map(rk.shape[1])
        wi[at, pl.ds(0, qp)] = nn(rq[...], wide).astype(BF)
        wi[at, pl.ds(qp, kp)] = nn(rk[...], narrow).astype(BF)
        wi[at, pl.ds(qp + kp, kp)] = nn(rv[...], narrow).astype(BF)

    def prep_out():
        raw_copy(3).wait()
        wo[pl.ds(al(shard * d, 16), shard), :] = nn(ro[...], head_map(ro.shape[1])).astype(BF)

    def prep_rows(s):
        row = lax.broadcasted_iota(jnp.int32, (seq, seq), 0)
        col = lax.broadcasted_iota(jnp.int32, (seq, seq), 1)
        same = jnp.where(row == col, 1.0, 0.0).astype(BF)
        mid = seq // 2
        packed = (ordr[s : s + 1, :] - mid).astype(F32)
        place = nt(same, jnp.broadcast_to(packed, (LANES, seq)).astype(BF)) + mid
        start = lens[s, 0]
        first = jnp.zeros((seq, LANES), F32)
        for n in range(1, lens.shape[1]):
            begin = start.astype(F32)
            first = jnp.where(place >= begin, begin, first)
            real = jnp.where(place >= begin, 0.0, 1.0)
            start = start + lens[s, n]
        lane = lax.broadcasted_iota(jnp.int32, (seq, LANES), 1)
        cols[s] = jnp.where(lane == 0, place, jnp.where(lane == 1, first, real))
        one = lax.broadcasted_iota(jnp.int32, (8, LANES), 1)
        field = one % 64
        freqs = jnp.exp((-2.0 * math.log(rope_base) / HEAD) * field.astype(F32))
        freqs = jnp.where(field < HEAD // 2, freqs, 0.0)[0:1, :]
        angles = (place - first) * freqs
        cosr[s] = jnp.cos(angles)
        sine = jnp.sin(angles)
        sinr[s] = jnp.where(lane < 64, -sine, sine)

    wunits = (
        (wgn, 16, 0, pair),
        (wi, shard, 0, inw),
        (wo, shard, 0, qp),
        (wu, shard, 0, ff),
        (wu, shard, ff, ff),
        (wd, shard, 0, ff),
    )

    def wblk(u, i):
        ref, n, at, cut = wunits[u]
        return ref.at[pl.ds(al(n * i, 16), n), pl.ds(at, cut)]

    def w_start(u):
        src = wblk(u, d)
        if u >= 3:
            raw_copy((5, 6, 4)[u - 3]).wait()
        rcopy(src, src, wsend.at[u], wrecv.at[u, 0], {"dp": aa}).start()
        rcopy(src, src, wsend.at[u], wrecv.at[u, 1], {"dp": bb}).start()
        rcopy(src, src, wsend.at[u], wrecv.at[u, 3], {"dp": pp}).start()

    def w_many(u, count):
        ref, n, at, cut = wunits[u]
        part = ref.at[pl.ds(0, count * n), pl.ds(at, cut)]
        return rcopy(part, part, wsend.at[u], wrecv.at[u, 3], {"dp": pp})

    def w_wait(u, slot, i):
        rcopy(wblk(u, i), wblk(u, i), wsend.at[u], wrecv.at[u, slot], {"dp": aa}).wait_recv()

    def w_relayb(u):
        w_wait(u, 1, bb)
        rcopy(wblk(u, bb), wblk(u, bb), wsend.at[u], wrecv.at[u, 2], {"dp": aa}).start()
        rcopy(wblk(u, bb), wblk(u, bb), wsend.at[u], wrecv.at[u, 3], {"dp": pp}).start()

    def w_relaya(u):
        w_wait(u, 0, aa)
        rcopy(wblk(u, aa), wblk(u, aa), wsend.at[u], wrecv.at[u, 3], {"dp": pp}).start()

    def w_diag(u):
        w_wait(u, 2, dd)
        rcopy(wblk(u, dd), wblk(u, dd), wsend.at[u], wrecv.at[u, 3], {"dp": pp}).start()

    def w_done(u):
        w_many(u, 4).wait_recv()

    def w_sent(u):
        w_many(u, 7).wait_send()

    zfull = (xf, gf, n2, ghf)
    zhbm = (tok, cot, None, None)

    def zblk(u, s, i, h=None):
        at = pl.ds(al(s * seq + i * rows, 16), rows)
        return zfull[u].at[at] if h is None else zfull[u].at[at, pl.ds(h * half, half)]

    def zcopy(u, s, k, way, h, i, src=None):
        blk = zblk(u, s, i, h)
        return rcopy(
            blk if src is None else src, blk, zsend.at[u, s], zrecv.at[1 if u == 1 else 0, s, way, k, h], zdev[way]
        )

    def zag_send(u, s, k, way, h):
        i = z - k if way == 0 else z + k
        go = (z < 3) & (i >= 0) if way == 0 else (z > 0) & (i <= 3)

        @pl.when(go)
        def _():
            src = zhbm[u].at[s, :, pl.ds(h * half, half)] if k == 0 and zhbm[u] is not None else None
            zcopy(u, s, k, way, h, i, src).start()

    def own_copy(u, s):
        return pltpu.make_async_copy(zhbm[u].at[s], zblk(u, s, z), lsem.at[2 + 2 * u + s])

    def ag(u, s, t, way=None):
        if t == 0:
            if zhbm[u] is not None:
                own_copy(u, s).start()
            for part in (0, 1):
                for side in (0, 1):
                    zag_send(u, s, 0, side, part)
            return
        i = z - t if way == 0 else z + t
        go = (i >= 0) if way == 0 else (i <= 3)

        for h in (0, 1):
            @pl.when(go)
            def _():
                zcopy(u, s, t - 1, way, h, i).wait_recv()

            if t < 3:
                zag_send(u, s, t, way, h)

    def own_here(u, s):
        own_copy(u, s).wait()

    def zag_sent(u, s):
        def sent(count):
            part = zfull[u].at[pl.ds(0, count * rows)]
            rcopy(part, part, zsend.at[u, s], zrecv.at[1 if u == 1 else 0, s, 0, 0, 0], zdev[0]).wait_send()

        @pl.when((z == 0) | (z == 3))
        def _():
            sent(1)

        @pl.when((z > 0) & (z < 3))
        def _():
            sent(5)

    zpart = (pa, pb, pa, pa)
    zgot = (ra, rb, ra, ra)

    def rs_copy(u, s, way, t, dest, h):
        cut = pl.ds(h * half, half)
        return rcopy(
            zpart[u].at[pl.ds(al(s * seq + dest * rows, 16), rows), cut],
            zgot[u].at[s, way, t, :, cut],
            rsend.at[u, s],
            rrecv.at[1 if u == 1 else 0, s, way, t, h],
            zdev[way],
        )

    def rs_add(u, s, way, t, target, base, cut):
        def body(i, carry):
            at = pl.ds(al(base + i * 16, 16), 16)
            got = zgot[u][s, way, t, pl.ds(al(i * 16, 16), 16), cut].astype(F32)
            target[at, cut] = (target[at, cut].astype(F32) + got).astype(target.dtype)
            return carry

        lax.fori_loop(0, rows // 16, body, 0)

    def rs(u, s, t, way):
        from_end = z if way == 0 else 3 - z
        dest = 3 + z - t if way == 0 else t - from_end

        @pl.when(from_end <= t)
        def _():
            for h in (0, 1):
                if t > 0:
                    @pl.when(from_end > 0)
                    def _():
                        rs_copy(u, s, way, t - 1, z, h).wait_recv()
                        rs_add(u, s, way, t - 1, zpart[u], s * seq + dest * rows, pl.ds(h * half, half))

                rs_copy(u, s, way, t, dest, h).start()

    def rs_final(u, s):
        def first(i, carry):
            at = pl.ds(al(i * 16, 16), 16)
            acc[at, :] = zpart[u][pl.ds(al(s * seq + own + i * 16, 16), 16), :].astype(F32)
            return carry

        lax.fori_loop(0, rows // 16, first, 0)
        for way in (0, 1):
            from_end = z if way == 0 else 3 - z

            @pl.when(from_end > 0)
            def _():
                for h in (0, 1):
                    rs_copy(u, s, way, 2, z, h).wait_recv()
                rs_add(u, s, way, 2, acc, 0, pl.ds(0, width))

    def rs_sent(u, s):
        part = zpart[u].at[pl.ds(0, 3 * rows)]
        rcopy(part, part, rsend.at[u, s], rrecv.at[0, s, 0, 0, 0], zdev[0]).wait_send()

    gunits = (
        (gf, act, 0, ff),
        (n2, dgu, 0, ff),
        (n2, dgu, ff, ff),
        (ghf, ob, 0, qp),
        (n1, dq3, 0, inw),
    )

    def xslot(u, chip):
        b, n = u % 2, gunits[u][3]
        return xb.at[b, pl.ds(al(chip * shard, 16), shard), pl.ds(0, n)]

    def gslot(u, chip, core):
        b, n = u % 2, gunits[u][3]
        return gb.at[b, pl.ds(al(chip * pair + core * shard, 16), shard), pl.ds(0, n)]

    def g_exchange(u, chip, i):
        return rcopy(gslot(u, chip, 1 - c), xslot(u, chip), gsend.at[u % 2], grecv.at[u % 2, i], {"dp": pp})

    chips = (chip_d, chip_x, chip_y, chip_own)

    def g_compute(u, i):
        left, right, at, n = gunits[u]
        chip = chips[i]
        if u >= 2 and i == 0:
            pl.semaphore_wait(credit.at[0], 1)
        tile = 256

        def body(j, carry):
            lhs = left[:, pl.ds(al(chip * pair, LANES), pair)]
            got = tn(lhs, right[:, pl.ds(al(at + j * tile, tile), tile)])
            gb[u % 2, pl.ds(al(chip * pair, 16), pair), pl.ds(al(j * tile, tile), tile)] = got.astype(BF)
            return carry

        lax.fori_loop(0, n // tile, body, 0)
        g_exchange(u, chip, i).start()

    def g_add(u, chip, extra=None):
        b, n = u % 2, gunits[u][3]

        def body(i, carry):
            at = pl.ds(al(chip * shard + i * 16, 16), 16)
            mine = gb[b, pl.ds(al(chip * pair + c * shard + i * 16, 16), 16), pl.ds(0, n)].astype(F32)
            total = mine + xb[b, at, pl.ds(0, n)].astype(F32)
            if extra is not None:
                total = total + extra[b, pl.ds(al(i * 16, 16), 16), pl.ds(0, n)].astype(F32)
            xb[b, at, pl.ds(0, n)] = total.astype(BF)
            return carry

        lax.fori_loop(0, shard // 16, body, 0)

    def g_hop(u):
        b, n = u % 2, gunits[u][3]
        return rcopy(xslot(u, chip_d), hop.at[b, :, pl.ds(0, n)], gsend.at[b], grecv.at[b, 4], {"dp": aa})

    def g_last(u, way):
        b, n = u % 2, gunits[u][3]
        chip, dev = (chip_a, aa) if way == 0 else (chip_b, bb)
        return rcopy(
            xslot(u, chip), fin.at[b, way, :, pl.ds(0, n)], gsend.at[b], grecv.at[b, 5 + way], {"dp": dev}
        )

    def g_first(u):
        g_exchange(u, chip_d, 0).wait_recv()
        g_add(u, chip_d)
        if u >= 2:
            pl.semaphore_wait(credit.at[1], 1)
        g_hop(u).start()

    def g_firstb(u):
        g_exchange(u, chip_x, 1).wait_recv()
        g_exchange(u, chip_y, 2).wait_recv()
        g_add(u, chip_a)
        g_last(u, 0).start()

    def g_second(u):
        g_hop(u).wait_recv()
        g_add(u, chip_b, hop)
        if u >= 2:
            pl.semaphore_wait(credit.at[2], 1)
        g_last(u, 1).start()

    def picked(at, cut, which):
        value = stage[at, cut]
        high = value.astype(BF)
        rest = value - high.astype(F32)
        mid = rest.astype(BF)
        low = (rest - mid.astype(F32)).astype(BF)
        return nt(high, which) + (nt(mid, which) + nt(low, which))

    def g_finish(u):
        b, n = u % 2, gunits[u][3]
        g_exchange(u, chip_own, 3).wait_recv()
        g_last(u, 0).wait_recv()
        g_last(u, 1).wait_recv()
        out = (gdown_v, ggate_v, gup_v, stage, stage)[u]

        def body(i, carry):
            at = pl.ds(al(i * 16, 16), 16)
            total = gb[b, pl.ds(al(chip_own * pair + c * shard + i * 16, 16), 16), pl.ds(0, n)].astype(F32)
            total = total + xb[b, pl.ds(al(chip_own * shard + i * 16, 16), 16), pl.ds(0, n)].astype(F32)
            total = total + fin[b, 0, at, pl.ds(0, n)].astype(F32)
            out[at, pl.ds(0, n)] = total + fin[b, 1, at, pl.ds(0, n)].astype(F32)
            return carry

        lax.fori_loop(0, shard // 16, body, 0)
        rows_all = pl.ds(0, shard)
        if u == 3:
            gout_v[...] = picked(rows_all, pl.ds(0, qp), head_pick(gout_v.shape[1]))
        if u == 4:
            gq_v[...] = picked(rows_all, pl.ds(0, qp), head_pick(gq_v.shape[1]))
            gk_v[...] = picked(rows_all, pl.ds(qp, kp), head_pick(gk_v.shape[1]))
            gv_v[...] = picked(rows_all, pl.ds(qp + kp, kp), head_pick(gv_v.shape[1]))
        part = gb.at[b, pl.ds(0, 7 * shard), pl.ds(0, n)]
        rcopy(part, part, gsend.at[b], grecv.at[b, 0], {"dp": pp}).wait_send()
        if u < 3:
            pl.semaphore_signal(credit.at[0], inc=1, device_id={"dp": pp}, device_id_type=MESH)
            pl.semaphore_signal(credit.at[1], inc=1, device_id={"dp": aa}, device_id_type=MESH)
            pl.semaphore_signal(credit.at[2], inc=1, device_id={"dp": bb}, device_id_type=MESH)

    def gain_rows():
        for j in range(4):
            at = pl.ds(j * pair, pair)
            gains[:, at] = (
                wgn[pl.ds(32 * j, 16), :].astype(F32) + wgn[pl.ds(32 * j + 16, 16), :].astype(F32)
            )

    def norm1(s, t):
        gain = gains[0:1, :]

        def shard_rows(i):
            def body(r, carry):
                at = pl.ds(al(s * seq + i * rows + r * 16, 16), 16)
                x = xf[at, :].astype(F32)
                scale = lax.rsqrt(jnp.mean(x * x, axis=-1, keepdims=True) + eps)
                n1[at, :] = (x * scale * gain).astype(BF)
                return carry

            lax.fori_loop(0, rows // 16, body, 0)

        if t == 0:
            own_here(0, s)
            shard_rows(z)
            return

        @pl.when(z - t >= 0)
        def _():
            shard_rows(z - t)

        @pl.when(z + t <= 3)
        def _():
            shard_rows(z + t)

    head_scale = HEAD ** (-0.5)

    def project(s):
        at = pl.ds(s * seq, seq)
        cosine, sine = cosr[s], sinr[s]
        for j in range(inw // 256):
            both = nn(n1[at, :], wi[:, pl.ds(j * 256, 256)])
            for half in range(2):
                col = j * 256 + half * LANES
                part = both[:, half * LANES : (half + 1) * LANES]
                if col < qp + kp:
                    part = part * cosine + pltpu.roll(part, LANES // 2, 1) * sine
                if col < qp:
                    part = part * head_scale
                qkv[at, pl.ds(col, LANES)] = part.astype(BF)

    def attend(s, part):
        at = pl.ds(s * seq, seq)
        oc = ordr[s : s + 1, :].astype(F32)
        mask = (oc <= cols[s, :, 0:1]) & (oc >= cols[s, :, 1:2])

        def body(h, carry):
            g = h // per_group
            q = qkv[at, pl.ds(al(h * LANES, LANES), LANES)]
            k = qkv[at, pl.ds(al(qp + g * LANES, LANES), LANES)]
            v = qkv[at, pl.ds(al(qp + kp + g * LANES, LANES), LANES)]
            sc = jnp.where(mask, nt(q, k), -1e30)
            e = jnp.exp(sc - jnp.max(sc, axis=-1, keepdims=True))
            p = e * (1.0 / jnp.sum(e, axis=-1, keepdims=True))
            p = p.astype(BF)
            pr[s * heads + h] = p
            ob[at, pl.ds(al(h * LANES, LANES), LANES)] = nn(p, v).astype(BF)
            return carry

        half = heads // 2
        lax.fori_loop(part * half, (part + 1) * half, body, 0)

    def spread(s, dst, left, weight, tile, part=0, parts=1):
        at = pl.ds(s * seq, seq)

        def body(j, carry):
            col = al(j * tile, tile)
            dst[at, pl.ds(col, tile)] = nt(left[at, :], weight[pl.ds(col, tile), :]).astype(BF)
            return carry

        count = width // tile // parts
        lax.fori_loop(part * count, (part + 1) * count, body, 0)

    def spread_gain(s):
        at = pl.ds(s * seq, seq)
        tile = 512

        def body(j, carry):
            col = pl.ds(al(j * tile, tile), tile)
            got = nt(dq3[at, :], wi[col, :])
            pa[at, col] = got.astype(BF)
            gpart[0:1, col] += jnp.sum(got * n1[at, col].astype(F32), axis=0, keepdims=True)
            return carry

        lax.fori_loop(0, width // tile, body, 0)

    def norm2(s):
        gain = gains[1:2, :]
        base = s * rows

        def body(i, carry):
            r = pl.ds(al(i * 16, 16), 16)
            h = tbuf[s, r, :].astype(F32) + acc[r, :]
            hb[pl.ds(al(base + i * 16, 16), 16), :] = h
            scale = lax.rsqrt(jnp.mean(h * h, axis=-1, keepdims=True) + eps)
            real = cols[s, pl.ds(al(own + i * 16, 16), 16), 2:3]
            n2[pl.ds(al(s * seq + own + i * 16, 16), 16), :] = (h * (scale * real) * gain).astype(BF)
            return carry

        lax.fori_loop(0, rows // 16, body, 0)

    def feed_forward(s, part):
        at = pl.ds(s * seq, seq)
        one, two = pl.ds(part * 256, 256), pl.ds(ff + part * 256, 256)
        gate = nn(n2[at, :], wu[:, one])
        upper = nn(n2[at, :], wu[:, two])
        sigma = 1.0 / (1.0 + jnp.exp(-gate))
        swish = gate * sigma
        act[at, one] = (swish * upper).astype(BF)
        dgu[at, one] = (upper * sigma * (1.0 + gate * (1.0 - sigma))).astype(BF)
        dgu[at, two] = swish.astype(BF)

    def feed_back(s, part):
        if part == 0:
            own_here(1, s)
        at = pl.ds(s * seq, seq)
        one, two = pl.ds(part * 256, 256), pl.ds(ff + part * 256, 256)
        back = nn(gf[at, :], wd[:, one])
        dgu[at, one] = (back * dgu[at, one].astype(F32)).astype(BF)
        dgu[at, two] = (back * dgu[at, two].astype(F32)).astype(BF)

    def finish_out(s):
        def body(i, carry):
            r = pl.ds(al(i * 16, 16), 16)
            real = cols[s, pl.ds(al(own + i * 16, 16), 16), 2:3]
            y = (hb[pl.ds(al(s * rows + i * 16, 16), 16), :] + acc[r, :]) * real
            out_v[s, r, :] = y.astype(BF)
            return carry

        lax.fori_loop(0, rows // 16, body, 0)

    def norm2_back(s):
        gain = gains[1:2, :]

        def body(i, carry):
            r = pl.ds(al(i * 16, 16), 16)
            ro = pl.ds(al(s * rows + i * 16, 16), 16)
            h = hb[ro, :]
            scale = lax.rsqrt(jnp.mean(h * h, axis=-1, keepdims=True) + eps)
            unit = h * scale
            grad = acc[r, :]
            inner = grad * gain
            dy = gf[pl.ds(al(s * seq + own + i * 16, 16), 16), :].astype(F32)
            dy = dy * cols[s, pl.ds(al(own + i * 16, 16), 16), 2:3]
            dhr = dy + scale * (inner - unit * jnp.mean(inner * unit, axis=-1, keepdims=True))
            gtok_v[s, r, :] = dhr
            ghf[pl.ds(al(s * seq + own + i * 16, 16), 16), :] = dhr.astype(BF)
            return carry + jnp.sum(grad * unit, axis=0, keepdims=True)

        gpart[1:2, :] += lax.fori_loop(0, rows // 16, body, jnp.zeros((1, width), F32))

    def grad_heads(s):
        at = pl.ds(s * seq, seq)
        for j in range(qp // 256):
            dq3[at, pl.ds(j * 256, 256)] = nn(ghf[at, :], wo[:, pl.ds(j * 256, 256)]).astype(BF)

    def attend_back(s):
        at = pl.ds(s * seq, seq)
        cosine, sine = cosr[s], sinr[s]

        def body(g, carry):
            k = qkv[at, pl.ds(al(qp + g * LANES, LANES), LANES)]
            v = qkv[at, pl.ds(al(qp + kp + g * LANES, LANES), LANES)]
            dk = jnp.zeros((seq, LANES), F32)
            dv = jnp.zeros((seq, LANES), F32)
            for m in range(per_group):
                h = g * per_group + m
                hat = pl.ds(al(h * LANES, LANES), LANES)
                q = qkv[at, hat]
                do = dq3[at, hat]
                low = pr[s * heads + h]
                p = low.astype(F32)
                dp = nt(do, v)
                ds = (p * (dp - jnp.sum(p * dp, axis=-1, keepdims=True))).astype(BF)
                dv = dv + tn(low, do)
                dk = dk + tn(ds, q)
                dq = nn(ds, k) * head_scale
                dq3[at, hat] = (dq * cosine - pltpu.roll(dq, LANES // 2, 1) * sine).astype(BF)
            dq3[at, pl.ds(al(qp + g * LANES, LANES), LANES)] = (
                dk * cosine - pltpu.roll(dk, LANES // 2, 1) * sine
            ).astype(BF)
            dq3[at, pl.ds(al(qp + kp + g * LANES, LANES), LANES)] = dv.astype(BF)
            return carry

        lax.fori_loop(0, groups, body, 0)

    def norm1_back(s):
        gain = gains[0:1, :]

        def body(i, carry):
            r = pl.ds(al(i * 16, 16), 16)
            x = tbuf[s, r, :].astype(F32)
            scale = lax.rsqrt(jnp.mean(x * x, axis=-1, keepdims=True) + eps)
            unit = x * scale
            grad = acc[r, :]
            inner = grad * gain
            gtok_v[s, r, :] += scale * (inner - unit * jnp.mean(inner * unit, axis=-1, keepdims=True))
            return carry

        lax.fori_loop(0, rows // 16, body, 0)

    X, COT, N2, GH = 0, 1, 2, 3
    BR, FFN, DN2, DN1 = 0, 1, 2, 3

    def tok_copy(s):
        return pltpu.make_async_copy(tok.at[s], tbuf.at[s], lsem.at[s])

    def fin_br(s):
        rs_final(BR, s)
        tok_copy(s).wait()
        norm2(s)
        ag(N2, s, 0)

    def fin_dn2(s):
        rs_final(DN2, s)
        norm2_back(s)
        ag(GH, s, 0)

    def fin_ffn(s):
        rs_final(FFN, s)
        finish_out(s)

    def fin_dn1(s):
        rs_final(DN1, s)
        norm1_back(s)

    def e_copy(i, src, dev):
        line = i < 6
        return rcopy(src, gex.at[i], esend.at[0 if line else 1], erecv.at[i if line else i // 2 + 3], dev)

    def e_line(t):
        if t == 0:
            for j in range(4):
                at = pl.ds(j * pair, pair)
                gsum[j : j + 1, :] = gpart[0:1, at] / gains[0:1, at]
                gsum[4 + j : 5 + j, :] = gpart[1:2, at]
        for way in (0, 1):
            here = (z - t >= 0) if way == 0 else (z + t <= 3)
            on = (z < 3) if way == 0 else (z > 0)
            slot = 3 * way + t

            @pl.when(here)
            def _():
                if t > 0:
                    e_copy(slot - 1, gsum, zdev[way]).wait_recv()
                if t < 3:
                    @pl.when(on)
                    def _():
                        e_copy(slot, gsum if t == 0 else gex.at[slot - 1], zdev[way]).start()

        if t == 3:
            gex[6] = gsum[...]
            for way in (0, 1):
                for k in (1, 2, 3):
                    @pl.when((z - k >= 0) if way == 0 else (z + k <= 3))
                    def _():
                        gex[6] += gex[3 * way + k - 1]

            e_copy(7, gex.at[6], {"dp": pp}).start()

    def e_plane(t):
        i = 7 + 2 * t
        dev = (pp, aa, bb)[t]
        e_copy(i, gex.at[i - 1], {"dp": dev}).wait()
        total = gex[i - 1] + gex[i]
        if t < 2:
            gex[i + 1] = total
            e_copy(i + 2, gex.at[i + 1], {"dp": (aa, bb)[t]}).start()
        else:
            gex[12] = total
            for at, out in ((0, gone_v), (4, gtwo_v)):
                line = gex[12, pl.ds(at + d // 2, 1), :]
                out[...] = jnp.where(c == 0, line[:, :shard], line[:, shard:])

    def e_sent():
        def sent(count):
            part = gex.at[pl.ds(0, count)]
            rcopy(part, part, esend.at[0], erecv.at[0], zdev[0]).wait_send()

        @pl.when((z == 0) | (z == 3))
        def _():
            sent(1)

        @pl.when((z > 0) & (z < 3))
        def _():
            sent(5)

    def clean(i):
        if i == 0:
            for u in range(6):
                w_sent(u)
        elif i < 4:
            for s in (0, 1):
                zag_sent((COT, N2, GH)[i - 1], s)
        else:
            rs_sent(FFN, i - 4)

    for i in (7, 8, 0, 1, 2, 3, 5, 6, 4):
        raw_copy(i).start()
    gpart[...] = jnp.zeros_like(gpart)
    for s in (0, 1):
        tok_copy(s).start()
    pl.semaphore_wait(barrier, 3 + (z + 3) // 4 + (6 - z) // 4)
    ag(X, 0, 0)
    prep_gain()
    w_start(0)
    prep_in()
    w_start(1)
    prep_out()
    w_start(2)
    ag(X, 0, 1, 1)
    w_relayb(0)
    ag(X, 0, 1, 0)
    ag(X, 1, 0)
    prep_rows(0)
    w_relayb(1)
    w_relaya(1)
    ag(X, 0, 2, 0)
    w_diag(0)
    w_relaya(0)
    ag(X, 0, 2, 1)
    ag(COT, 0, 0)
    ag(X, 1, 1, 1)
    prep_rows(1)
    w_done(0)
    gain_rows()
    norm1(0, 1)
    w_relayb(2)
    norm1(0, 0)
    w_diag(1)
    norm1(0, 2)
    ag(X, 0, 3, 1)
    ag(X, 0, 3, 0)
    norm1(0, 3)
    w_relaya(2)
    ag(X, 1, 1, 0)
    w_done(1)
    project(0)
    w_diag(2)
    w_start(3)
    attend(0, 0)
    attend(0, 1)
    w_done(2)
    spread(0, pa, ob, wo, 512)
    rs(BR, 0, 0, 1)
    rs(BR, 0, 0, 0)
    ag(COT, 0, 1, 0)
    ag(X, 1, 2, 1)
    w_start(4)
    ag(COT, 0, 1, 1)
    rs(BR, 0, 1, 1)
    norm1(1, 0)
    ag(X, 1, 2, 0)
    ag(COT, 0, 2, 0)
    rs(BR, 0, 1, 0)
    norm1(1, 2)
    norm1(1, 1)
    rs(BR, 0, 2, 1)
    ag(X, 1, 3, 1)
    ag(X, 1, 3, 0)
    norm1(1, 3)
    rs(BR, 0, 2, 0)
    w_relayb(3)
    project(1)
    attend(1, 0)
    w_start(5)
    attend(1, 1)
    ag(COT, 0, 2, 1)
    spread(1, pa, ob, wo, 512)
    rs(BR, 1, 0, 0)
    rs(BR, 1, 0, 1)
    fin_br(0)
    rs_sent(BR, 0)
    rs(BR, 1, 1, 0)
    ag(N2, 0, 1, 0)
    w_relaya(3)
    w_relaya(4)
    rs(BR, 1, 1, 1)
    w_relayb(4)
    ag(N2, 0, 1, 1)
    ag(COT, 0, 3, 1)
    rs(BR, 1, 2, 0)
    rs(BR, 1, 2, 1)
    w_relayb(5)
    ag(N2, 0, 2, 1)
    w_diag(3)
    ag(N2, 0, 2, 0)
    ag(COT, 1, 0)
    w_diag(4)
    fin_br(1)
    ag(N2, 0, 3, 0)
    w_done(4)
    w_relaya(5)
    ag(N2, 0, 3, 1)
    w_done(3)
    feed_forward(0, 0)
    w_diag(5)
    rs_sent(BR, 1)
    feed_forward(0, 1)
    feed_forward(0, 2)
    feed_forward(0, 3)
    w_done(5)
    spread(0, pb, act, wd, 512)
    rs(FFN, 0, 0, 1)
    ag(COT, 1, 1, 1)
    ag(COT, 1, 1, 0)
    rs(FFN, 0, 0, 0)
    ag(COT, 0, 3, 0)
    feed_back(0, 0)
    feed_back(0, 1)
    feed_back(0, 2)
    feed_back(0, 3)
    spread(0, pa, dgu, wu, 256, 0, 2)
    spread(0, pa, dgu, wu, 256, 1, 2)
    rs(DN2, 0, 0, 0)
    zag_sent(X, 1)
    ag(N2, 1, 1, 1)
    ag(N2, 1, 1, 0)
    rs(DN2, 0, 0, 1)
    clean(0)
    rs(DN2, 0, 1, 1)
    rs(FFN, 0, 1, 1)
    rs(DN2, 0, 1, 0)
    ag(N2, 1, 2, 1)
    rs(FFN, 0, 1, 0)
    ag(N2, 1, 3, 1)
    ag(N2, 1, 2, 0)
    ag(N2, 1, 3, 0)
    ag(COT, 1, 2, 1)
    feed_forward(1, 0)
    feed_forward(1, 1)
    feed_forward(1, 2)
    ag(COT, 1, 2, 0)
    zag_sent(X, 0)
    rs(DN2, 0, 2, 0)
    feed_forward(1, 3)
    rs(DN2, 0, 2, 1)
    ag(COT, 1, 3, 0)
    ag(COT, 1, 3, 1)
    feed_back(1, 0)
    feed_back(1, 1)
    feed_back(1, 2)
    feed_back(1, 3)
    spread(1, pa, dgu, wu, 256, 0, 2)
    spread(1, pa, dgu, wu, 256, 1, 2)
    rs(DN2, 1, 0, 1)
    rs(DN2, 1, 0, 0)
    g_compute(0, 0)
    g_compute(0, 1)
    fin_dn2(0)
    g_first(0)
    g_compute(0, 2)
    g_compute(0, 3)
    g_firstb(0)
    rs(DN2, 1, 1, 0)
    rs(DN2, 1, 1, 1)
    g_compute(1, 0)
    g_compute(1, 1)
    g_second(0)
    ag(GH, 0, 1, 0)
    ag(GH, 0, 1, 1)
    g_compute(1, 2)
    rs(DN2, 1, 2, 0)
    rs(DN2, 1, 2, 1)
    spread(1, pb, act, wd, 512)
    rs(FFN, 1, 0, 1)
    ag(GH, 0, 2, 0)
    rs(FFN, 1, 0, 0)
    ag(GH, 0, 2, 1)
    g_first(1)
    g_firstb(1)
    fin_dn2(1)
    g_finish(0)
    rs_sent(DN2, 0)
    g_compute(1, 3)
    g_compute(2, 0)
    ag(GH, 0, 3, 0)
    g_second(1)
    ag(GH, 0, 3, 1)
    grad_heads(0)
    attend_back(0)
    ag(GH, 1, 1, 0)
    rs(FFN, 1, 1, 0)
    g_first(2)
    ag(GH, 1, 1, 1)
    rs(FFN, 1, 1, 1)
    g_compute(2, 1)
    spread_gain(0)
    rs(DN1, 0, 0, 0)
    g_compute(2, 2)
    ag(GH, 1, 2, 1)
    rs(DN1, 0, 0, 1)
    g_firstb(2)
    ag(GH, 1, 2, 0)
    rs(FFN, 0, 2, 0)
    g_finish(1)
    g_compute(2, 3)
    rs(FFN, 1, 2, 1)
    g_second(2)
    ag(GH, 1, 3, 0)
    ag(GH, 1, 3, 1)
    rs(FFN, 0, 2, 1)
    g_compute(3, 0)
    g_compute(3, 1)
    rs(FFN, 1, 2, 0)
    grad_heads(1)
    attend_back(1)
    g_first(3)
    rs_sent(DN2, 1)
    spread_gain(1)
    rs(DN1, 1, 0, 1)
    e_line(0)
    rs(DN1, 1, 0, 0)
    rs(DN1, 0, 1, 0)
    g_compute(3, 2)
    rs(DN1, 0, 1, 1)
    g_compute(3, 3)
    g_firstb(3)
    g_finish(2)
    g_compute(4, 0)
    g_second(3)
    g_first(4)
    rs(DN1, 1, 1, 1)
    g_compute(4, 1)
    e_line(1)
    g_compute(4, 2)
    rs(DN1, 1, 1, 0)
    clean(2)
    clean(5)
    g_firstb(4)
    fin_ffn(0)
    e_line(2)
    clean(3)
    rs(DN1, 0, 2, 0)
    g_finish(3)
    rs(DN1, 0, 2, 1)
    e_line(3)
    e_plane(0)
    rs(DN1, 1, 2, 0)
    g_second(4)
    g_compute(4, 3)
    fin_ffn(1)
    rs(DN1, 1, 2, 1)
    fin_dn1(0)
    clean(1)
    clean(4)
    e_plane(1)
    g_finish(4)
    e_plane(2)
    fin_dn1(1)
    for s in (0, 1):
        rs_sent(DN1, s)
    e_sent()


def put_out(*refs):
    ins, outs, sem = refs[:11], refs[11:22], refs[22]
    copies = [pltpu.make_async_copy(src, dst, sem.at[i]) for i, (src, dst) in enumerate(zip(ins, outs))]
    for copy in copies:
        copy.start()
    for copy in copies:
        copy.wait()


def fused(
    tokens,
    cotangent,
    order,
    lengths,
    gain_attn,
    w_query,
    w_key,
    w_value,
    w_out,
    gain_ffn,
    w_gate,
    w_up,
    w_down,
):
    micro, rows, width = tokens.shape
    seq = rows * lax.axis_size("tensor")
    shard = w_query.shape[0]
    ff = w_gate.shape[1]
    groups = w_key.shape[1] // HEAD
    q_cols, k_cols = w_query.shape[1], w_key.shape[1]
    qp = q_cols // HEAD * LANES
    kp = groups * LANES
    inw = qp + 2 * kp
    total = micro * seq
    vm = pltpu.VMEM
    dma = pltpu.SemaphoreType.DMA
    scratch = [
        vm((8 * 16, 2 * shard), BF),
        vm((width, inw), BF),
        vm((width, qp), BF),
        vm((width, 2 * ff), BF),
        vm((width, ff), BF),
        vm((total, width), BF),
        vm((total, width), BF),
        vm((total, width), BF),
        vm((total, width), BF),
        vm((total, inw), BF),
        vm((total, qp), BF),
        vm((total, ff), BF),
        vm((total, inw), BF),
        vm((total, 2 * ff), BF),
        vm((micro * qp // LANES, seq, seq), BF),
        vm((micro * rows, width), F32),
        vm((total, width), BF),
        vm((total, width), BF),
        vm((micro, 2, 3, rows, width), BF),
        vm((micro, 2, 3, rows, width), BF),
        vm((2, width, ff), BF),
        vm((2, width // 2, ff), BF),
        vm((2, shard, ff), BF),
        vm((2, 2, shard, ff), BF),
        vm((shard, ff), F32),
        vm((rows, width), F32),
        vm((16, width), F32),
        vm((8, width), F32),
        vm((8, width // 4), F32),
        vm((13, 8, width // 4), F32),
        vm((micro, rows, width), BF),
        vm(gain_attn.shape, BF),
        vm(gain_ffn.shape, BF),
        vm(w_query.shape, BF),
        vm(w_key.shape, BF),
        vm(w_value.shape, BF),
        vm(w_out.shape[::-1], BF),
        vm((micro, seq, LANES), F32),
        vm((micro, seq, LANES), F32),
        vm((micro, seq, LANES), F32),
        dma((6,)),
        dma((6, 4)),
        dma((4, 2)),
        dma((2, 2, 2, 3, 2)),
        dma((4, 2)),
        dma((2, 2, 2, 3, 2)),
        dma((2,)),
        dma((2, 7)),
        dma((2,)),
        dma((9,)),
        dma((6,)),
        dma((9,)),
        pltpu.SemaphoreType.REGULAR((3,)),
    ]
    hbm = pl.BlockSpec(memory_space=pl.ANY)
    vmem = pl.BlockSpec(memory_space=pltpu.VMEM)
    smem = pl.BlockSpec(memory_space=pltpu.SMEM)
    shape = jax.ShapeDtypeStruct
    shapes = [
        vm((micro, rows, width), BF),
        vm((micro, rows, width), F32),
        vm((shard, ff), F32),
        vm((shard, ff), F32),
        vm((shard, ff), F32),
        vm((shard, q_cols), F32),
        vm((shard, q_cols), F32),
        vm((shard, k_cols), F32),
        vm((shard, k_cols), F32),
        vm((1, shard), F32),
        vm((1, shard), F32),
    ]
    dims = (rows, seq, width, shard, qp, kp, ff, groups)
    out, gtok, gdown, ggate, gup, gout, gq, gk, gv, one, two = pl.pallas_call(
        functools.partial(block_kernel, dims),
        out_shape=shapes,
        in_specs=[hbm] * 11 + [vmem, smem],
        out_specs=[vmem] * 11,
        scratch_shapes=scratch,
        compiler_params=pltpu.CompilerParams(
            collective_id=0, has_side_effects=True, vmem_limit_bytes=61_600_000
        ),
        name="block",
    )(
        tokens,
        cotangent,
        gain_attn,
        gain_ffn,
        w_query,
        w_key,
        w_value,
        w_out.T,
        w_gate,
        w_up,
        w_down.T,
        order,
        lengths,
    )
    results = [out, gtok, gdown, ggate, gup, gout, gq, gk, gv, one, two]
    out, gtok, gdown, ggate, gup, gout, gq, gk, gv, one, two = pl.pallas_call(
        put_out,
        out_shape=[shape(x.shape, x.dtype) for x in results],
        in_specs=[vmem] * 11,
        out_specs=[hbm] * 11,
        scratch_shapes=[dma((11,))],
        compiler_params=pltpu.CompilerParams(vmem_limit_bytes=2**18),
        name="put_out",
    )(*results)
    return out, gtok, one[0], gq, gk, gv, gout.T, two[0], ggate, gup, gdown.T


def local(tokens, *rest):
    fits = lax.axis_size("dp") == 8 and lax.axis_size("tensor") == 4 and tokens.shape[0] == 2
    return (fused if fits else spread_out)(tokens, *rest)


def solution(mesh):
    return jax.shard_map(
        local,
        mesh=mesh,
        in_specs=(
            P("dp", "tensor", None),
            P("dp", "tensor", None),
            P("dp", None),
            P("dp", None),
            P("dp"),
            P("dp", "tensor"),
            P("dp", "tensor"),
            P("dp", "tensor"),
            P("tensor", "dp"),
            P("dp"),
            P("dp", "tensor"),
            P("dp", "tensor"),
            P("tensor", "dp"),
        ),
        out_specs=(
            P("dp", "tensor", None),
            P("dp", "tensor", None),
            P("dp"),
            P("dp", "tensor"),
            P("dp", "tensor"),
            P("dp", "tensor"),
            P("tensor", "dp"),
            P("dp"),
            P("dp", "tensor"),
            P("dp", "tensor"),
            P("tensor", "dp"),
        ),
        check_vma=False,
    )
```
